32 devices in a mesh: dp: 2 (over x), tp: 4 (over z), sp: 4 (over y, core).
Axes of the slice: x: 2, y: 2, z: 4, core: 2. Of those that a mesh axis runs over, the one named last changes fastest.
Arguments:
- x_in: bfloat16 [256, 3840], P('dp'), parts along dimension 0
- cur_pos: int32 [256], P('dp'), parts along dimension 0
- w_pre: float32 [3840], replicated
- w_q: bfloat16 [3840, 4096], P(None, 'tp')
- w_k: bfloat16 [3840, 2048], P(None, 'tp')
- w_v: bfloat16 [3840, 2048], P(None, 'tp')
- w_o: bfloat16 [4096, 3840], P('tp')
- w_post: float32 [3840], replicated
- k_cache: bfloat16 [256, 256, 8, 256], P('dp', 'sp', 'tp'), parts along dimension 0
- v_cache: bfloat16 [256, 256, 8, 256], P('dp', 'sp', 'tp'), parts along dimension 0
Outputs:
- output 1: bfloat16 [256, 3840], P('dp'), parts along dimension 0
- output 2: bfloat16 [256, 256, 8, 256], P('dp', 'sp', 'tp'), parts along dimension 0
- output 3: bfloat16 [256, 256, 8, 256], P('dp', 'sp', 'tp'), parts along dimension 0
There are 2 independent parts. The reference program is written for one: setup_inputs(seed, part) draws one part's arguments, and reference() takes and returns one part's arrays. A program takes and returns all parts, laid end to end along the dimension named above; an argument that names none is the same for every part.
All inputs are finite; a program needn't handle non-finite values.
Results may differ from the reference program's by a relative error of at most 0.00644205.
Values sent between devices are 32-bit elements.
A program may use at most 1 GiB of HBM per device.

```python
import jax
import jax.numpy as jnp
from jax import lax

BATCH_SIZE = 128
SEQ_LEN = 256
D_MODEL = 3840
NUM_HEADS = 16
KV_HEADS = 8
HEAD_DIM = 256
HOT_KEYS = 48

SOFT_CAP = 50.0
ROPE_BASE = 10000.0
NORM_EPS = 1e-6


def rms_scale(tensor, gain_w):
    mean_sq = jnp.mean(tensor * tensor, axis=-1, keepdims=True)
    return tensor * lax.rsqrt(mean_sq + NORM_EPS) * (1.0 + gain_w)


def rotary(tensor, positions):
    half_dim = tensor.shape[-1] // 2
    inv_freq = ROPE_BASE ** (-2.0 * jnp.arange(half_dim, dtype=jnp.float32) / (2 * half_dim))
    angles = positions.astype(jnp.float32)[:, None] * inv_freq[None, :]
    angles = angles.reshape((angles.shape[0],) + (1,) * (tensor.ndim - 2) + (half_dim,))
    cos_tab = jnp.cos(angles)
    sin_tab = jnp.sin(angles)
    lo_half = tensor[..., :half_dim]
    hi_half = tensor[..., half_dim:]
    return jnp.concatenate([lo_half * cos_tab - hi_half * sin_tab, hi_half * cos_tab + lo_half * sin_tab], axis=-1)


def setup_inputs(seed: int = 0, part: int = 0) -> dict:
    part_keys = jax.random.split(jax.random.fold_in(jax.random.key(seed), part), 6)
    shared_keys = jax.random.split(jax.random.key(seed + 1), 7)
    q_cols = NUM_HEADS * HEAD_DIM
    kv_cols = KV_HEADS * HEAD_DIM
    cache_shape = (BATCH_SIZE, SEQ_LEN, KV_HEADS, HEAD_DIM)
    x_in = jax.random.normal(part_keys[0], (BATCH_SIZE, D_MODEL), jnp.float32).astype(jnp.bfloat16)
    drawn_pos = jax.random.randint(part_keys[1], (BATCH_SIZE,), 0, SEQ_LEN)
    long_row = jax.random.randint(part_keys[2], (), 0, BATCH_SIZE)
    cur_pos = jnp.where(jnp.arange(BATCH_SIZE) == long_row, SEQ_LEN - 1, drawn_pos).astype(jnp.int32)
    hot_mark = jax.random.randint(part_keys[3], (BATCH_SIZE, SEQ_LEN, KV_HEADS, 1), 0, SEQ_LEN) < HOT_KEYS
    key_scale = jnp.where(hot_mark, 2.5, 0.03)
    k_cache = (jax.random.normal(part_keys[4], cache_shape, jnp.float32) * key_scale).astype(jnp.bfloat16)
    v_cache = jax.random.normal(part_keys[5], cache_shape, jnp.float32).astype(jnp.bfloat16)
    w_pre = 0.5 * jax.random.normal(shared_keys[0], (D_MODEL,), jnp.float32)
    w_q = (jax.random.normal(shared_keys[1], (D_MODEL, q_cols), jnp.float32) * (36.0 * D_MODEL ** -0.5)).astype(jnp.bfloat16)
    w_k = (jax.random.normal(shared_keys[2], (D_MODEL, kv_cols), jnp.float32) * (2.2 * D_MODEL ** -0.5)).astype(jnp.bfloat16)
    w_v = (jax.random.normal(shared_keys[3], (D_MODEL, kv_cols), jnp.float32) * D_MODEL ** -0.5).astype(jnp.bfloat16)
    w_o = (jax.random.normal(shared_keys[4], (q_cols, D_MODEL), jnp.float32) * q_cols ** -0.5).astype(jnp.bfloat16)
    w_post = 0.5 * jax.random.normal(shared_keys[5], (D_MODEL,), jnp.float32)
    return {'x_in': x_in, 'cur_pos': cur_pos, 'w_pre': w_pre, 'w_q': w_q, 'w_k': w_k, 'w_v': w_v, 'w_o': w_o, 'w_post': w_post, 'k_cache': k_cache, 'v_cache': v_cache}


def reference(x_in, cur_pos, w_pre, w_q, w_k, w_v, w_o, w_post, k_cache, v_cache):
    group_size = NUM_HEADS // KV_HEADS
    seq_ids = jnp.arange(SEQ_LEN)
    normed = rms_scale(x_in.astype(jnp.float32), w_pre).astype(jnp.bfloat16)
    q_proj = jnp.dot(normed, w_q, preferred_element_type=jnp.float32).reshape(BATCH_SIZE, NUM_HEADS, HEAD_DIM)
    k_proj = jnp.dot(normed, w_k, preferred_element_type=jnp.float32).reshape(BATCH_SIZE, KV_HEADS, HEAD_DIM)
    q_rot = rotary(q_proj, cur_pos).astype(jnp.bfloat16)
    k_new = rotary(k_proj, cur_pos).astype(jnp.bfloat16)
    v_new = jnp.dot(normed, w_v, preferred_element_type=jnp.float32).reshape(BATCH_SIZE, KV_HEADS, HEAD_DIM).astype(jnp.bfloat16)
    slot_hit = (seq_ids[None, :] == cur_pos[:, None])[:, :, None, None]
    k_out = jnp.where(slot_hit, k_new[:, None], k_cache)
    v_out = jnp.where(slot_hit, v_new[:, None], v_cache)

    def one_row(row_data):
        q_row, k_row, v_row, pos_row = row_data
        q_grp = q_row.astype(jnp.float32).reshape(KV_HEADS, group_size, HEAD_DIM)
        raw_score = jnp.einsum('grd,tgd->grt', q_grp, k_row.astype(jnp.float32)) * HEAD_DIM ** -0.5
        capped = SOFT_CAP * jnp.tanh(raw_score / SOFT_CAP)
        capped = jnp.where(seq_ids <= pos_row, capped, -jnp.inf)
        prob_w = jax.nn.softmax(capped, axis=-1)
        attn_row = jnp.einsum('grt,tgd->grd', prob_w, v_row.astype(jnp.float32))
        return attn_row.reshape(NUM_HEADS * HEAD_DIM)

    attn_out = lax.map(one_row, (q_rot, k_out, v_out, cur_pos))
    proj_sum = jnp.dot(attn_out.astype(jnp.bfloat16), w_o, preferred_element_type=jnp.float32)
    x_out = (x_in.astype(jnp.float32) + rms_scale(proj_sum, w_post)).astype(jnp.bfloat16)
    return (x_out, k_out, v_out)
```

```python
import functools

import jax
import jax.numpy as jnp
from jax import lax
from jax.experimental import pallas as pl
from jax.experimental.pallas import tpu as pltpu
from jax.sharding import PartitionSpec as P

SOFT_CAP = 50.0
ROPE_BASE = 10000.0
NORM_EPS = 1e-6

ROWS = 128
DM = 3840
HD = 256
TB = 64
RP = 136
LANES = 128
BCH = 16
NCH = ROWS // BCH
SHIFT = 20.0
CW = 256
NC = DM // CW
OWN = 32
MESH = pl.DeviceIdType.MESH


def rope_tables(positions):
    half = HD // 2
    inv_freq = ROPE_BASE ** (-2.0 * jnp.arange(half, dtype=jnp.float32) / (2 * half))
    ang = positions.astype(jnp.float32)[:, None] * inv_freq[None, :]
    return jnp.cos(ang), jnp.sin(ang)


def attn_kernel(pos_ref, x_h, cos_ref, sin_ref, wpre_ref, wq_h, wk_h, wv_h, kc_h, vc_h,
                o_ref, ko_h, vo_h,
                x_buf, a_buf, w_buf, kbuf, vbuf, qs, ks, vs,
                x_sem, w_sem, ki_sem, vi_sem, kw_sem, vw_sem):
    sp = lax.axis_index('sp')
    tbase = sp * TB

    def w_copy(i):
        if i < 2:
            src = wk_h.at[:, pl.ds(i * HD, HD)]
        elif i < 4:
            src = wv_h.at[:, pl.ds((i - 2) * HD, HD)]
        else:
            src = wq_h.at[:, pl.ds((i - 4) * HD, HD)]
        return pltpu.make_async_copy(src, w_buf.at[i], w_sem.at[i])

    def k_in(i):
        return pltpu.make_async_copy(kc_h.at[pl.ds(i * BCH, BCH)], kbuf.at[pl.ds(i * BCH, BCH)], ki_sem.at[i])

    def v_in(i):
        return pltpu.make_async_copy(vc_h.at[pl.ds(i * BCH, BCH)], vbuf.at[pl.ds(i * BCH, BCH)], vi_sem.at[i])

    def k_out(i):
        return pltpu.make_async_copy(kbuf.at[pl.ds(i * BCH, BCH)], ko_h.at[pl.ds(i * BCH, BCH)], kw_sem.at[i])

    def v_out(i):
        return pltpu.make_async_copy(vbuf.at[pl.ds(i * BCH, BCH)], vo_h.at[pl.ds(i * BCH, BCH)], vw_sem.at[i])

    x_copy = pltpu.make_async_copy(x_h, x_buf, x_sem)
    x_copy.start()
    ahead = 5
    for i in range(ahead):
        w_copy(i).start()
    x_copy.wait()

    gain = 1.0 + wpre_ref[...]

    def norm_rows(i, carry):
        r = pl.multiple_of(i * 16, 16)
        xb = x_buf[pl.ds(r, 16), :].astype(jnp.float32)
        ms = jnp.mean(xb * xb, axis=-1, keepdims=True)
        a_buf[pl.ds(r, 16), :] = (xb * lax.rsqrt(ms + NORM_EPS) * gain).astype(jnp.bfloat16)
        return carry

    lax.fori_loop(0, ROWS // 16, norm_rows, 0)

    for i in range(8):
        w_copy(i).wait()
        if i + ahead < 8:
            w_copy(i + ahead).start()
        else:
            c = i + ahead - 8
            k_in(c).start()
            v_in(c).start()
        y = jnp.dot(a_buf[...], w_buf[i], preferred_element_type=jnp.float32)
        lo, hi = y[:, :LANES], y[:, LANES:]
        if 2 <= i < 4:
            h = i - 2
            for rep in range(2):
                vs[pl.ds((rep * 4 + h) * RP, ROWS), :] = lo
                vs[pl.ds((rep * 4 + 2 + h) * RP, ROWS), :] = hi
        else:
            cos_t, sin_t = cos_ref[...], sin_ref[...]
            rlo = lo * cos_t - hi * sin_t
            rhi = hi * cos_t + lo * sin_t
            if i < 2:
                for rep in range(2):
                    ks[pl.ds((rep * 4 + i) * RP, ROWS), :] = rlo
                    ks[pl.ds((rep * 4 + 2 + i) * RP, ROWS), :] = rhi
            else:
                qs[pl.ds((i - 4) * RP, ROWS), :] = rlo
                qs[pl.ds((4 + i - 4) * RP, ROWS), :] = rhi
    for c in range(ahead, NCH):
        k_in(c).start()
        v_in(c).start()

    lane = lax.broadcasted_iota(jnp.int32, (8, LANES), 1)
    row = lax.broadcasted_iota(jnp.int32, (8, LANES), 0)
    row_c = row // 4
    row_h = (row // 2) % 2
    match = (((lane // 2) % 2) == row_c) & ((lane % 2) == row_h)
    match_f = jnp.where(match, 1.0, 0.0).astype(jnp.float32)
    first = row_c == 0
    t_half = [jnp.where(match, lane // 4 + 32 * hf, 1 << 20) for hf in range(2)]
    quad = lax.broadcasted_iota(jnp.int32, (16, LANES), 0) // 4
    zero = jnp.zeros((8, LANES), jnp.float32)

    def chunk(i, l_acc):
        k_in(i).wait()
        v_in(i).wait()
        tls = []
        for u in range(BCH):
            b = i * BCH + u
            tl = pos_ref[b] - tbase
            tls.append(tl)
            hit = jnp.logical_and(tl >= 0, tl < TB)
            tc = jnp.clip(tl, 0, TB - 1)
            tile = tc // 4
            tgt = jnp.where(hit, tc - tile * 4, -1)
            sel = quad == tgt
            off = pl.multiple_of(tile * 16, 16)
            kn = ks[pl.ds(b, 8, stride=RP), :]
            vn = vs[pl.ds(b, 8, stride=RP), :]
            kt = kbuf[b, pl.ds(off, 16), :].astype(jnp.float32)
            vt = vbuf[b, pl.ds(off, 16), :].astype(jnp.float32)
            kbuf[b, pl.ds(off, 16), :] = jnp.where(sel, jnp.concatenate([kn, kn], 0), kt).astype(jnp.bfloat16)
            vbuf[b, pl.ds(off, 16), :] = jnp.where(sel, jnp.concatenate([vn, vn], 0), vt).astype(jnp.bfloat16)
        scores = []
        for u in range(0, BCH, 2):
            b = i * BCH + u
            q0 = qs[pl.ds(b, 8, stride=RP), :]
            q1 = qs[pl.ds(b + 1, 8, stride=RP), :]
            lhs = jnp.concatenate([jnp.concatenate([q0, zero], 1), jnp.concatenate([zero, q1], 1)], 0).astype(jnp.bfloat16)
            kk = jnp.concatenate([kbuf[b], kbuf[b + 1]], 1)
            scores.append(lax.dot_general(lhs, kk, (((1,), (1,)), ((), ())), preferred_element_type=jnp.float32))
        weights = []
        for u in range(0, BCH, 2):
            pair = []
            for w in range(2):
                part = scores[u // 2][8 * w:8 * w + 8]
                es = []
                for hf in range(2):
                    a = part[:, hf * LANES:(hf + 1) * LANES] * match_f
                    e = pltpu.roll(a, 4, 0)
                    f = jnp.where(first, pltpu.roll(e, LANES - 2, 1), pltpu.roll(e, 2, 1))
                    s = SOFT_CAP * jnp.tanh((a + f) * (HD ** -0.5 / SOFT_CAP))
                    es.append(jnp.where(t_half[hf] <= tls[u + w], jnp.exp(s - SHIFT), 0.0))
                tot = jnp.sum(es[0] + es[1], axis=1, keepdims=True)
                inv = jnp.where(tot > 0.0, 1.0 / tot, 0.0)
                pair.append(jnp.concatenate([es[0] * inv, es[1] * inv], 1))
                l_acc = jnp.where(lane == i * BCH + u + w, tot, l_acc)
            weights.append(jnp.concatenate(pair, 0).astype(jnp.bfloat16))
        for u in range(0, BCH, 2):
            b = i * BCH + u
            vv = jnp.concatenate([vbuf[b], vbuf[b + 1]], 1)
            o = jnp.dot(weights[u // 2], vv, preferred_element_type=jnp.float32)
            o_ref[pl.ds(b, 8, stride=RP), :] = o[0:8, 0:LANES]
            o_ref[pl.ds(b + 1, 8, stride=RP), :] = o[8:16, LANES:]
        k_out(i).start()
        v_out(i).start()
        return l_acc

    l_acc = lax.fori_loop(0, NCH, chunk, zero)
    l_full = jnp.concatenate([l_acc, jnp.zeros((ROWS - 8, LANES), jnp.float32)], 0)
    o_ref[pl.ds(8 * RP, ROWS), :] = l_full.T
    for i in range(NCH):
        k_out(i).wait()
        v_out(i).wait()


def comm_kernel(x_ref, wpost_ref, o_ref, wo_h, out_ref,
                wo_buf, r1, m1, r2, lhs, p_buf, rr, rl, sr, sl, s_all,
                w_sem, r1_send, r1_recv, r2_send, r2_recv,
                right_send, right_recv, left_send, left_recv,
                part_send, part_recv, y_send, y_recv, f_send, f_recv):
    z = lax.axis_index('tp')
    sp = lax.axis_index('sp')
    core = sp % 2
    yy = sp // 2
    partner = sp + 1 - 2 * core
    ypeer = (sp + 2) % 4
    diag = 3 - sp

    def wo_copy(k):
        return pltpu.make_async_copy(wo_h.at[:, pl.ds(pl.multiple_of(k * CW, CW), CW)], wo_buf.at[k], w_sem.at[k])

    for k in range(NC):
        wo_copy(k).start()

    @pl.when(z == 0)
    def _():
        rr[...] = jnp.zeros_like(rr)

    @pl.when(z == 3)
    def _():
        rl[...] = jnp.zeros_like(rl)

    bar = pltpu.get_barrier_semaphore()
    pl.semaphore_signal(bar, inc=1, device_id={'sp': partner}, device_id_type=MESH)
    pl.semaphore_signal(bar, inc=1, device_id={'sp': ypeer}, device_id_type=MESH)

    @pl.when(z > 0)
    def _():
        pl.semaphore_signal(bar, inc=1, device_id={'tp': z - 1}, device_id_type=MESH)

    @pl.when(z < 3)
    def _():
        pl.semaphore_signal(bar, inc=1, device_id={'tp': z + 1}, device_id_type=MESH)

    pl.semaphore_wait(bar, 3 + (z * (3 - z)) // 2)

    def to_partner(slot):
        ychip = (1 - yy) if slot == 0 else yy
        r0 = pl.multiple_of(ychip * 64 + (1 - core) * OWN, OWN)
        return pltpu.make_async_remote_copy(
            src_ref=o_ref.at[:, pl.ds(r0, OWN), :], dst_ref=r1.at[slot],
            send_sem=r1_send.at[slot], recv_sem=r1_recv.at[slot], device_id={'sp': partner}, device_id_type=MESH)

    to_partner(0).start()
    to_partner(1).start()

    def merge(load_a, load_b, write):
        la, lb = load_a(8), load_b(8)
        tot = la + lb
        inv = jnp.where(tot > 0.0, 1.0 / tot, 0.0)
        fa, fb = la * inv, lb * inv
        for j in range(8):
            write(j, load_a(j) * fa[:, j:j + 1] + load_b(j) * fb[:, j:j + 1])
        write(8, tot)

    def own_rows(ychip):
        r0 = pl.multiple_of(ychip * 64 + core * OWN, OWN)
        return lambda j: o_ref[j, pl.ds(r0, OWN), :]

    def put_m1(j, val):
        m1[j] = val

    to_partner(0).wait()
    merge(own_rows(1 - yy), lambda j: r1[0, j], put_m1)
    y_merge = pltpu.make_async_remote_copy(
        src_ref=m1, dst_ref=r2, send_sem=r2_send, recv_sem=r2_recv, device_id={'sp': ypeer}, device_id_type=MESH)
    y_merge.start()
    to_partner(1).wait()

    def put_r1(j, val):
        r1[1, j] = val

    merge(own_rows(yy), lambda j: r1[1, j], put_r1)
    y_merge.wait()

    def put_lhs(j, val):
        if j < 8:
            c, hq = j // 4, j % 4
            lhs[:, (hq * 2 + c) * LANES:(hq * 2 + c + 1) * LANES] = val.astype(jnp.bfloat16)

    merge(lambda j: r1[1, j], lambda j: r2[j], put_lhs)

    def right_copy(k):
        return pltpu.make_async_remote_copy(
            src_ref=sr.at[k], dst_ref=rr.at[k], send_sem=right_send.at[k], recv_sem=right_recv.at[k],
            device_id={'tp': z + 1}, device_id_type=MESH)

    def left_copy(k):
        return pltpu.make_async_remote_copy(
            src_ref=sl.at[k], dst_ref=rl.at[k], send_sem=left_send.at[k], recv_sem=left_recv.at[k],
            device_id={'tp': z - 1}, device_id_type=MESH)

    def part_copy(k):
        return pltpu.make_async_remote_copy(
            src_ref=s_all.at[sp, k], dst_ref=s_all.at[sp, k], send_sem=part_send.at[k], recv_sem=part_recv.at[k],
            device_id={'sp': partner}, device_id_type=MESH)

    def y_copy(k):
        return pltpu.make_async_remote_copy(
            src_ref=s_all.at[sp, k], dst_ref=s_all.at[sp, k], send_sem=y_send.at[k], recv_sem=y_recv.at[k],
            device_id={'sp': ypeer}, device_id_type=MESH)

    def fwd_copy(k):
        return pltpu.make_async_remote_copy(
            src_ref=s_all.at[ypeer, k], dst_ref=s_all.at[ypeer, k], send_sem=f_send.at[k], recv_sem=f_recv.at[k],
            device_id={'sp': partner}, device_id_type=MESH)

    hop = 3
    lag_r = hop * z
    lag_l = hop * (3 - z)
    lag_s = hop * (3 - (z * (3 - z)) // 2)

    def tick(i, carry):
        @pl.when(i < NC)
        def _():
            wo_copy(i).wait()
            p_buf[i] = jnp.dot(lhs[...], wo_buf[i], preferred_element_type=jnp.float32)

        kr = i - lag_r

        @pl.when(jnp.logical_and(kr >= 0, kr < NC))
        def _():
            @pl.when(z > 0)
            def _():
                right_copy(kr).wait_recv()

            @pl.when(z < 3)
            def _():
                sr[kr] = p_buf[kr] + rr[kr]
                right_copy(kr).start()

        kl = i - lag_l

        @pl.when(jnp.logical_and(kl >= 0, kl < NC))
        def _():
            @pl.when(z < 3)
            def _():
                left_copy(kl).wait_recv()

            @pl.when(z > 0)
            def _():
                sl[kl] = p_buf[kl] + rl[kl]
                left_copy(kl).start()

        k_s = i - lag_s

        @pl.when(jnp.logical_and(k_s >= 0, k_s < NC))
        def _():
            s_all[sp, k_s] = p_buf[k_s] + rr[k_s] + rl[k_s]
            y_copy(k_s).start()
            part_copy(k_s).start()

        k_y = i - lag_s - hop

        @pl.when(jnp.logical_and(k_y >= 0, k_y < NC))
        def _():
            y_copy(k_y).wait_recv()
            fwd_copy(k_y).start()

        return carry

    lax.fori_loop(0, NC + 4 * hop, tick, 0)

    def drain(k, carry):
        part_copy(k).wait()
        y_copy(k).wait_send()
        fwd_copy(k).wait()

        @pl.when(z < 3)
        def _():
            right_copy(k).wait_send()

        @pl.when(z > 0)
        def _():
            left_copy(k).wait_send()

        return carry

    lax.fori_loop(0, NC, drain, 0)

    def finish(i, carry):
        g = i // 2
        r = pl.multiple_of((i % 2) * 16, 16)
        parts = [s_all[g, k, pl.ds(r, 16), :] for k in range(NC)]
        sq = parts[0] * parts[0]
        for k in range(1, NC):
            sq = sq + parts[k] * parts[k]
        ms = jnp.sum(sq, axis=-1, keepdims=True) * (1.0 / DM)
        rs = lax.rsqrt(ms + NORM_EPS)
        r16 = pl.multiple_of(i * 16, 16)
        for k in range(NC):
            cs = slice(k * CW, (k + 1) * CW)
            val = s_all[g, k, pl.ds(r, 16), :] * rs * (1.0 + wpost_ref[:, cs])
            out_ref[pl.ds(r16, 16), cs] = (x_ref[pl.ds(r16, 16), cs].astype(jnp.float32) + val).astype(jnp.bfloat16)
        return carry

    lax.fori_loop(0, ROWS // 16, finish, 0)


def solution(mesh):
    cache_spec = P('dp', 'sp', 'tp', None)
    hbm = pl.BlockSpec(memory_space=pltpu.HBM)
    vmem = pl.BlockSpec(memory_space=pltpu.VMEM)
    smem = pl.BlockSpec(memory_space=pltpu.SMEM)

    def in_hbm(arr):
        return pltpu.with_memory_space_constraint(arr, pltpu.HBM)

    def to_rows(c):
        b, t, h, d = c.shape
        return c.reshape(b, t, h, 2, LANES).transpose(0, 1, 3, 2, 4).reshape(b, t * 2 * h, LANES)

    def from_rows(r):
        return r.reshape(ROWS, TB, 2, 2, LANES).transpose(0, 1, 3, 2, 4).reshape(ROWS, TB, 2, HD)

    def local_step(x_in, cur_pos, w_pre, w_q, w_k, w_v, w_o, w_post, k_cache, v_cache):
        cos_t, sin_t = rope_tables(cur_pos)
        kr, vr = to_rows(k_cache), to_rows(v_cache)
        f32, bf16 = jnp.float32, jnp.bfloat16
        o_part, k_new, v_new = pl.pallas_call(
            attn_kernel,
            out_shape=(jax.ShapeDtypeStruct((9 * RP, LANES), f32),
                       jax.ShapeDtypeStruct(kr.shape, bf16), jax.ShapeDtypeStruct(vr.shape, bf16)),
            in_specs=[smem, hbm, vmem, vmem, vmem, hbm, hbm, hbm, hbm, hbm],
            out_specs=(vmem, hbm, hbm),
            scratch_shapes=[
                pltpu.VMEM((ROWS, DM), bf16), pltpu.VMEM((ROWS, DM), bf16), pltpu.VMEM((8, DM, HD), bf16),
                pltpu.VMEM(kr.shape, bf16), pltpu.VMEM(vr.shape, bf16),
                pltpu.VMEM((8 * RP, LANES), f32), pltpu.VMEM((8 * RP, LANES), f32), pltpu.VMEM((8 * RP, LANES), f32),
                pltpu.SemaphoreType.DMA, pltpu.SemaphoreType.DMA((8,)),
                pltpu.SemaphoreType.DMA((NCH,)), pltpu.SemaphoreType.DMA((NCH,)),
                pltpu.SemaphoreType.DMA((NCH,)), pltpu.SemaphoreType.DMA((NCH,)),
            ],
            compiler_params=pltpu.CompilerParams(vmem_limit_bytes=56 << 20),
            name='attend',
        )(cur_pos, in_hbm(x_in), cos_t, sin_t, w_pre.reshape(1, DM), in_hbm(w_q), in_hbm(w_k), in_hbm(w_v),
          in_hbm(kr), in_hbm(vr))
        dma = pltpu.SemaphoreType.DMA
        big = pltpu.VMEM((NC, OWN, CW), f32)
        x_out = pl.pallas_call(
            comm_kernel,
            out_shape=jax.ShapeDtypeStruct((ROWS, DM), bf16),
            in_specs=[vmem, vmem, vmem, hbm],
            out_specs=vmem,
            scratch_shapes=[
                pltpu.VMEM((NC, 1024, CW), bf16), pltpu.VMEM((2, 9, OWN, LANES), f32), pltpu.VMEM((9, OWN, LANES), f32),
                pltpu.VMEM((9, OWN, LANES), f32), pltpu.VMEM((OWN, 1024), bf16),
                big, big, big, big, big, pltpu.VMEM((4, NC, OWN, CW), f32),
                dma((NC,)), dma((2,)), dma((2,)), dma, dma,
                dma((NC,)), dma((NC,)), dma((NC,)), dma((NC,)),
                dma((NC,)), dma((NC,)), dma((NC,)), dma((NC,)), dma((NC,)), dma((NC,)),
            ],
            compiler_params=pltpu.CompilerParams(vmem_limit_bytes=40 << 20, collective_id=0, has_side_effects=True),
            name='combine',
        )(x_in, w_post.reshape(1, DM), o_part.reshape(9, RP, LANES), in_hbm(w_o))
        return x_out, from_rows(k_new), from_rows(v_new)

    return jax.shard_map(local_step, mesh=mesh,
                         in_specs=(P('dp', None), P('dp'), P(None), P(None, 'tp'), P(None, 'tp'), P(None, 'tp'), P('tp', None), P(None), cache_spec, cache_spec),
                         out_specs=(P('dp', None), cache_spec, cache_spec), check_vma=False)
```

```python
import functools

import jax
import jax.numpy as jnp
from jax import lax
from jax.experimental import pallas as pl
from jax.experimental.pallas import tpu as pltpu
from jax.sharding import PartitionSpec as P

SOFT_CAP = 50.0
ROPE_BASE = 10000.0
NORM_EPS = 1e-6

ROWS = 128
DM = 3840
HD = 256
TB = 64
RP = 136
LANES = 128
BCH = 16
NCH = ROWS // BCH
SHIFT = 20.0
CW = 256
NC = DM // CW
OWN = 32
MESH = pl.DeviceIdType.MESH


def attn_kernel(pos_h, posv_h, freq_h, x_h, wpre_h, wq_h, wk_h, wv_h, kc_h, vc_h,
                o_ref, ko_h, vo_h,
                pos_ref, posv, freq, wpre_ref, cos_ref, sin_ref,
                x_buf, a_buf, w_buf, kbuf, vbuf, qs, ks, vs,
                x_sem, s_sem, w_sem, ki_sem, vi_sem, kw_sem, vw_sem):
    sp = lax.axis_index('sp')
    tbase = sp * TB

    def w_copy(i):
        if i < 2:
            src = wk_h.at[:, pl.ds(i * HD, HD)]
        elif i < 4:
            src = wv_h.at[:, pl.ds((i - 2) * HD, HD)]
        else:
            src = wq_h.at[:, pl.ds((i - 4) * HD, HD)]
        return pltpu.make_async_copy(src, w_buf.at[i], w_sem.at[i])

    def k_in(i):
        return pltpu.make_async_copy(kc_h.at[pl.ds(i * BCH, BCH)], kbuf.at[pl.ds(i * BCH, BCH)], ki_sem.at[i])

    def v_in(i):
        return pltpu.make_async_copy(vc_h.at[pl.ds(i * BCH, BCH)], vbuf.at[pl.ds(i * BCH, BCH)], vi_sem.at[i])

    def k_out(i):
        return pltpu.make_async_copy(kbuf.at[pl.ds(i * BCH, BCH)], ko_h.at[pl.ds(i * BCH, BCH)], kw_sem.at[i])

    def v_out(i):
        return pltpu.make_async_copy(vbuf.at[pl.ds(i * BCH, BCH)], vo_h.at[pl.ds(i * BCH, BCH)], vw_sem.at[i])

    x_copy = pltpu.make_async_copy(x_h, x_buf, x_sem)
    x_copy.start()
    small = [pltpu.make_async_copy(a, b, s_sem.at[i]) for i, (a, b) in enumerate(
        ((wpre_h, wpre_ref), (posv_h, posv), (freq_h, freq), (pos_h, pos_ref)))]
    for c in small:
        c.start()
    ahead = 5
    for i in range(ahead):
        w_copy(i).start()
    for c in small[1:]:
        c.wait()
    pos_col = jnp.broadcast_to(posv[...].astype(jnp.float32), (ROWS, LANES)).T
    ang = pos_col * freq[...]
    cos_ref[...] = jnp.cos(ang)
    sin_ref[...] = jnp.sin(ang)
    small[0].wait()
    x_copy.wait()

    gain = 1.0 + jnp.concatenate([wpre_ref[k:k + 1, :] for k in range(DM // LANES)], 1)

    def norm_rows(i, carry):
        r = pl.multiple_of(i * 16, 16)
        xb = x_buf[pl.ds(r, 16), :].astype(jnp.float32)
        ms = jnp.mean(xb * xb, axis=-1, keepdims=True)
        a_buf[pl.ds(r, 16), :] = (xb * lax.rsqrt(ms + NORM_EPS) * gain).astype(jnp.bfloat16)
        return carry

    lax.fori_loop(0, ROWS // 16, norm_rows, 0)

    for i in range(8):
        w_copy(i).wait()
        if i + ahead < 8:
            w_copy(i + ahead).start()
        else:
            c = i + ahead - 8
            k_in(c).start()
            v_in(c).start()
        y = jnp.dot(a_buf[...], w_buf[i], preferred_element_type=jnp.float32)
        lo, hi = y[:, :LANES], y[:, LANES:]
        if 2 <= i < 4:
            h = i - 2
            for rep in range(2):
                vs[pl.ds((rep * 4 + h) * RP, ROWS), :] = lo
                vs[pl.ds((rep * 4 + 2 + h) * RP, ROWS), :] = hi
        else:
            cos_t, sin_t = cos_ref[...], sin_ref[...]
            rlo = lo * cos_t - hi * sin_t
            rhi = hi * cos_t + lo * sin_t
            if i < 2:
                for rep in range(2):
                    ks[pl.ds((rep * 4 + i) * RP, ROWS), :] = rlo
                    ks[pl.ds((rep * 4 + 2 + i) * RP, ROWS), :] = rhi
            else:
                qs[pl.ds((i - 4) * RP, ROWS), :] = rlo
                qs[pl.ds((4 + i - 4) * RP, ROWS), :] = rhi
    for c in range(ahead, NCH):
        k_in(c).start()
        v_in(c).start()

    lane = lax.broadcasted_iota(jnp.int32, (8, LANES), 1)
    row = lax.broadcasted_iota(jnp.int32, (8, LANES), 0)
    row_c = row // 4
    row_h = (row // 2) % 2
    match = (((lane // 2) % 2) == row_c) & ((lane % 2) == row_h)
    match_f = jnp.where(match, 1.0, 0.0).astype(jnp.float32)
    first = row_c == 0
    t_half = [jnp.where(match, lane // 4 + 32 * hf, 1 << 20) for hf in range(2)]
    quad = lax.broadcasted_iota(jnp.int32, (16, LANES), 0) // 4
    zero = jnp.zeros((8, LANES), jnp.float32)

    def chunk(i, l_acc):
        k_in(i).wait()
        v_in(i).wait()
        tls = []
        for u in range(BCH):
            b = i * BCH + u
            tl = pos_ref[b] - tbase
            tls.append(tl)
            hit = jnp.logical_and(tl >= 0, tl < TB)
            tc = jnp.clip(tl, 0, TB - 1)
            tile = tc // 4
            tgt = jnp.where(hit, tc - tile * 4, -1)
            sel = quad == tgt
            off = pl.multiple_of(tile * 16, 16)
            kn = ks[pl.ds(b, 8, stride=RP), :]
            vn = vs[pl.ds(b, 8, stride=RP), :]
            kt = kbuf[b, pl.ds(off, 16), :].astype(jnp.float32)
            vt = vbuf[b, pl.ds(off, 16), :].astype(jnp.float32)
            kbuf[b, pl.ds(off, 16), :] = jnp.where(sel, jnp.concatenate([kn, kn], 0), kt).astype(jnp.bfloat16)
            vbuf[b, pl.ds(off, 16), :] = jnp.where(sel, jnp.concatenate([vn, vn], 0), vt).astype(jnp.bfloat16)
        scores = []
        for u in range(0, BCH, 2):
            b = i * BCH + u
            q0 = qs[pl.ds(b, 8, stride=RP), :]
            q1 = qs[pl.ds(b + 1, 8, stride=RP), :]
            lhs = jnp.concatenate([jnp.concatenate([q0, zero], 1), jnp.concatenate([zero, q1], 1)], 0).astype(jnp.bfloat16)
            kk = jnp.concatenate([kbuf[b], kbuf[b + 1]], 1)
            scores.append(lax.dot_general(lhs, kk, (((1,), (1,)), ((), ())), preferred_element_type=jnp.float32))
        weights = []
        for u in range(0, BCH, 2):
            pair = []
            for w in range(2):
                part = scores[u // 2][8 * w:8 * w + 8]
                es = []
                for hf in range(2):
                    a = part[:, hf * LANES:(hf + 1) * LANES] * match_f
                    e = pltpu.roll(a, 4, 0)
                    f = jnp.where(first, pltpu.roll(e, LANES - 2, 1), pltpu.roll(e, 2, 1))
                    s = SOFT_CAP * jnp.tanh((a + f) * (HD ** -0.5 / SOFT_CAP))
                    es.append(jnp.where(t_half[hf] <= tls[u + w], jnp.exp(s - SHIFT), 0.0))
                tot = jnp.sum(es[0] + es[1], axis=1, keepdims=True)
                inv = jnp.where(tot > 0.0, 1.0 / tot, 0.0)
                pair.append(jnp.concatenate([es[0] * inv, es[1] * inv], 1))
                l_acc = jnp.where(lane == i * BCH + u + w, tot, l_acc)
            weights.append(jnp.concatenate(pair, 0).astype(jnp.bfloat16))
        for u in range(0, BCH, 2):
            b = i * BCH + u
            vv = jnp.concatenate([vbuf[b], vbuf[b + 1]], 1)
            o = jnp.dot(weights[u // 2], vv, preferred_element_type=jnp.float32)
            o_ref[pl.ds(b, 8, stride=RP), :] = o[0:8, 0:LANES]
            o_ref[pl.ds(b + 1, 8, stride=RP), :] = o[8:16, LANES:]
        k_out(i).start()
        v_out(i).start()
        return l_acc

    l_acc = lax.fori_loop(0, NCH, chunk, zero)
    l_full = jnp.concatenate([l_acc, jnp.zeros((ROWS - 8, LANES), jnp.float32)], 0)
    o_ref[pl.ds(8 * RP, ROWS), :] = l_full.T
    for i in range(NCH):
        k_out(i).wait()
        v_out(i).wait()


def comm_kernel(o_ref, wo_h, s_all,
                wo_buf, r1, m1, r2, lhs, p_buf, rr, rl, sr, sl,
                w_sem, r1_send, r1_recv, r2_send, r2_recv,
                right_send, right_recv, left_send, left_recv,
                part_send, part_recv, y_send, y_recv, f_send, f_recv):
    z = lax.axis_index('tp')
    sp = lax.axis_index('sp')
    core = sp % 2
    yy = sp // 2
    partner = sp + 1 - 2 * core
    ypeer = (sp + 2) % 4
    diag = 3 - sp

    def wo_copy(k):
        return pltpu.make_async_copy(wo_h.at[:, pl.ds(pl.multiple_of(k * CW, CW), CW)], wo_buf.at[k], w_sem.at[k])

    for k in range(NC):
        wo_copy(k).start()

    @pl.when(z == 0)
    def _():
        rr[...] = jnp.zeros_like(rr)

    @pl.when(z == 3)
    def _():
        rl[...] = jnp.zeros_like(rl)

    bar = pltpu.get_barrier_semaphore()
    pl.semaphore_signal(bar, inc=1, device_id={'sp': partner}, device_id_type=MESH)
    pl.semaphore_signal(bar, inc=1, device_id={'sp': ypeer}, device_id_type=MESH)

    @pl.when(z > 0)
    def _():
        pl.semaphore_signal(bar, inc=1, device_id={'tp': z - 1}, device_id_type=MESH)

    @pl.when(z < 3)
    def _():
        pl.semaphore_signal(bar, inc=1, device_id={'tp': z + 1}, device_id_type=MESH)

    pl.semaphore_wait(bar, 3 + (z * (3 - z)) // 2)

    def to_partner(slot):
        ychip = (1 - yy) if slot == 0 else yy
        r0 = pl.multiple_of(ychip * 64 + (1 - core) * OWN, OWN)
        return pltpu.make_async_remote_copy(
            src_ref=o_ref.at[:, pl.ds(r0, OWN), :], dst_ref=r1.at[slot],
            send_sem=r1_send.at[slot], recv_sem=r1_recv.at[slot], device_id={'sp': partner}, device_id_type=MESH)

    to_partner(0).start()
    to_partner(1).start()

    def merge(load_a, load_b, write):
        la, lb = load_a(8), load_b(8)
        tot = la + lb
        inv = jnp.where(tot > 0.0, 1.0 / tot, 0.0)
        fa, fb = la * inv, lb * inv
        for j in range(8):
            write(j, load_a(j) * fa[:, j:j + 1] + load_b(j) * fb[:, j:j + 1])
        write(8, tot)

    def own_rows(ychip):
        r0 = pl.multiple_of(ychip * 64 + core * OWN, OWN)
        return lambda j: o_ref[j, pl.ds(r0, OWN), :]

    def put_m1(j, val):
        m1[j] = val

    to_partner(0).wait()
    merge(own_rows(1 - yy), lambda j: r1[0, j], put_m1)
    y_merge = pltpu.make_async_remote_copy(
        src_ref=m1, dst_ref=r2, send_sem=r2_send, recv_sem=r2_recv, device_id={'sp': ypeer}, device_id_type=MESH)
    y_merge.start()
    to_partner(1).wait()

    def put_r1(j, val):
        r1[1, j] = val

    merge(own_rows(yy), lambda j: r1[1, j], put_r1)
    y_merge.wait()

    def put_lhs(j, val):
        if j < 8:
            c, hq = j // 4, j % 4
            lhs[:, (hq * 2 + c) * LANES:(hq * 2 + c + 1) * LANES] = val.astype(jnp.bfloat16)

    merge(lambda j: r1[1, j], lambda j: r2[j], put_lhs)

    def right_copy(k):
        return pltpu.make_async_remote_copy(
            src_ref=sr.at[k], dst_ref=rr.at[k], send_sem=right_send.at[k], recv_sem=right_recv.at[k],
            device_id={'tp': z + 1}, device_id_type=MESH)

    def left_copy(k):
        return pltpu.make_async_remote_copy(
            src_ref=sl.at[k], dst_ref=rl.at[k], send_sem=left_send.at[k], recv_sem=left_recv.at[k],
            device_id={'tp': z - 1}, device_id_type=MESH)

    def part_copy(k):
        return pltpu.make_async_remote_copy(
            src_ref=s_all.at[sp, k], dst_ref=s_all.at[sp, k], send_sem=part_send.at[k], recv_sem=part_recv.at[k],
            device_id={'sp': partner}, device_id_type=MESH)

    def y_copy(k):
        return pltpu.make_async_remote_copy(
            src_ref=s_all.at[sp, k], dst_ref=s_all.at[sp, k], send_sem=y_send.at[k], recv_sem=y_recv.at[k],
            device_id={'sp': ypeer}, device_id_type=MESH)

    def fwd_copy(k):
        return pltpu.make_async_remote_copy(
            src_ref=s_all.at[ypeer, k], dst_ref=s_all.at[ypeer, k], send_sem=f_send.at[k], recv_sem=f_recv.at[k],
            device_id={'sp': partner}, device_id_type=MESH)

    hop = 3
    lag_r = hop * z
    lag_l = hop * (3 - z)
    lag_s = hop * (3 - (z * (3 - z)) // 2)

    def tick(i, carry):
        @pl.when(i < NC)
        def _():
            wo_copy(i).wait()
            p_buf[i] = jnp.dot(lhs[...], wo_buf[i], preferred_element_type=jnp.float32)

        kr = i - lag_r

        @pl.when(jnp.logical_and(kr >= 0, kr < NC))
        def _():
            @pl.when(z > 0)
            def _():
                right_copy(kr).wait_recv()

            @pl.when(z < 3)
            def _():
                sr[kr] = p_buf[kr] + rr[kr]
                right_copy(kr).start()

        kl = i - lag_l

        @pl.when(jnp.logical_and(kl >= 0, kl < NC))
        def _():
            @pl.when(z < 3)
            def _():
                left_copy(kl).wait_recv()

            @pl.when(z > 0)
            def _():
                sl[kl] = p_buf[kl] + rl[kl]
                left_copy(kl).start()

        k_s = i - lag_s

        @pl.when(jnp.logical_and(k_s >= 0, k_s < NC))
        def _():
            s_all[sp, k_s] = p_buf[k_s] + rr[k_s] + rl[k_s]
            y_copy(k_s).start()
            part_copy(k_s).start()

        k_y = i - lag_s - hop

        @pl.when(jnp.logical_and(k_y >= 0, k_y < NC))
        def _():
            y_copy(k_y).wait_recv()
            fwd_copy(k_y).start()

        return carry

    lax.fori_loop(0, NC + 4 * hop, tick, 0)

    def drain(k, carry):
        part_copy(k).wait()
        y_copy(k).wait_send()
        fwd_copy(k).wait()

        @pl.when(z < 3)
        def _():
            right_copy(k).wait_send()

        @pl.when(z > 0)
        def _():
            left_copy(k).wait_send()

        return carry

    lax.fori_loop(0, NC, drain, 0)


def finish_kernel(s_all, x_ref, wpost_ref, out_h, out_buf, sem):
    blk = 16

    def out_copy(i):
        rows = pl.ds(i * blk, blk)
        return pltpu.make_async_copy(out_buf.at[rows], out_h.at[rows], sem.at[i])

    for i in range(ROWS // blk):
        g, r = (i * blk) // OWN, (i * blk) % OWN
        parts = [s_all[g, k, r:r + blk, :] for k in range(NC)]
        sq = parts[0] * parts[0]
        for k in range(1, NC):
            sq = sq + parts[k] * parts[k]
        rs = lax.rsqrt(jnp.sum(sq, axis=-1, keepdims=True) * (1.0 / DM) + NORM_EPS)
        for k in range(NC):
            for hf in range(CW // LANES):
                col = k * CW + hf * LANES
                gain = 1.0 + wpost_ref[col // LANES:col // LANES + 1, :]
                val = s_all[g, k, r:r + blk, hf * LANES:(hf + 1) * LANES] * rs * gain
                cs = slice(col, col + LANES)
                out_buf[i * blk:(i + 1) * blk, cs] = (x_ref[i * blk:(i + 1) * blk, cs].astype(jnp.float32) + val).astype(jnp.bfloat16)
        out_copy(i).start()
    for i in range(ROWS // blk):
        out_copy(i).wait()


def solution(mesh):
    cache_spec = P('dp', 'sp', 'tp', None)
    hbm = pl.BlockSpec(memory_space=pltpu.HBM)
    vmem = pl.BlockSpec(memory_space=pltpu.VMEM)

    def in_hbm(arr):
        return pltpu.with_memory_space_constraint(arr, pltpu.HBM)

    def to_rows(c):
        b, t, h, d = c.shape
        return c.reshape(b, t, h, 2, LANES).transpose(0, 1, 3, 2, 4).reshape(b, t * 2 * h, LANES)

    def from_rows(r):
        return r.reshape(ROWS, TB, 2, 2, LANES).transpose(0, 1, 3, 2, 4).reshape(ROWS, TB, 2, HD)

    def local_step(x_in, cur_pos, w_pre, w_q, w_k, w_v, w_o, w_post, k_cache, v_cache):
        half = HD // 2
        inv_freq = ROPE_BASE ** (-2.0 * jnp.arange(half, dtype=jnp.float32) / (2 * half))
        kr, vr = to_rows(k_cache), to_rows(v_cache)
        f32, bf16 = jnp.float32, jnp.bfloat16
        o_part, k_new, v_new = pl.pallas_call(
            attn_kernel,
            out_shape=(pltpu.VMEM((9 * RP, LANES), f32),
                       jax.ShapeDtypeStruct(kr.shape, bf16), jax.ShapeDtypeStruct(vr.shape, bf16)),
            in_specs=[hbm] * 10,
            out_specs=(vmem, hbm, hbm),
            scratch_shapes=[
                pltpu.SMEM((ROWS,), jnp.int32), pltpu.VMEM((1, ROWS), jnp.int32), pltpu.VMEM((1, LANES), f32),
                pltpu.VMEM((DM // LANES, LANES), f32), pltpu.VMEM((ROWS, LANES), f32), pltpu.VMEM((ROWS, LANES), f32),
                pltpu.VMEM((ROWS, DM), bf16), pltpu.VMEM((ROWS, DM), bf16), pltpu.VMEM((8, DM, HD), bf16),
                pltpu.VMEM(kr.shape, bf16), pltpu.VMEM(vr.shape, bf16),
                pltpu.VMEM((8 * RP, LANES), f32), pltpu.VMEM((8 * RP, LANES), f32), pltpu.VMEM((8 * RP, LANES), f32),
                pltpu.SemaphoreType.DMA, pltpu.SemaphoreType.DMA((4,)), pltpu.SemaphoreType.DMA((8,)),
                pltpu.SemaphoreType.DMA((NCH,)), pltpu.SemaphoreType.DMA((NCH,)),
                pltpu.SemaphoreType.DMA((NCH,)), pltpu.SemaphoreType.DMA((NCH,)),
            ],
            compiler_params=pltpu.CompilerParams(vmem_limit_bytes=56 << 20),
            name='attend',
        )(in_hbm(cur_pos), in_hbm(cur_pos.reshape(1, ROWS)), in_hbm(inv_freq.reshape(1, LANES)), in_hbm(x_in),
          in_hbm(w_pre.reshape(DM // LANES, LANES)), in_hbm(w_q), in_hbm(w_k), in_hbm(w_v), in_hbm(kr), in_hbm(vr))
        dma = pltpu.SemaphoreType.DMA
        big = pltpu.VMEM((NC, OWN, CW), f32)
        sums = pl.pallas_call(
            comm_kernel,
            out_shape=pltpu.VMEM((4, NC, OWN, CW), f32),
            in_specs=[vmem, hbm],
            out_specs=vmem,
            scratch_shapes=[
                pltpu.VMEM((NC, 1024, CW), bf16), pltpu.VMEM((2, 9, OWN, LANES), f32), pltpu.VMEM((9, OWN, LANES), f32),
                pltpu.VMEM((9, OWN, LANES), f32), pltpu.VMEM((OWN, 1024), bf16),
                big, big, big, big, big,
                dma((NC,)), dma((2,)), dma((2,)), dma, dma,
                dma((NC,)), dma((NC,)), dma((NC,)), dma((NC,)),
                dma((NC,)), dma((NC,)), dma((NC,)), dma((NC,)), dma((NC,)), dma((NC,)),
            ],
            compiler_params=pltpu.CompilerParams(vmem_limit_bytes=40 << 20, collective_id=0, has_side_effects=True),
            name='combine',
        )(pltpu.with_memory_space_constraint(o_part.reshape(9, RP, LANES), pltpu.VMEM), in_hbm(w_o))
        x_out = pl.pallas_call(
            finish_kernel,
            out_shape=jax.ShapeDtypeStruct((ROWS, DM), bf16),
            in_specs=[vmem, vmem, vmem],
            out_specs=hbm,
            scratch_shapes=[pltpu.VMEM((ROWS, DM), bf16), dma((ROWS // 16,))],
            compiler_params=pltpu.CompilerParams(vmem_limit_bytes=16 << 20),
            name='finish',
        )(pltpu.with_memory_space_constraint(sums, pltpu.VMEM), x_in, w_post.reshape(DM // LANES, LANES))
        return x_out, from_rows(k_new), from_rows(v_new)

    return jax.shard_map(local_step, mesh=mesh,
                         in_specs=(P('dp', None), P('dp'), P(None), P(None, 'tp'), P(None, 'tp'), P(None, 'tp'), P('tp', None), P(None), cache_spec, cache_spec),
                         out_specs=(P('dp', None), cache_spec, cache_spec), check_vma=False)
```

```python
import functools

import jax
import jax.numpy as jnp
from jax import lax
from jax.experimental import pallas as pl
from jax.experimental.pallas import tpu as pltpu
from jax.sharding import PartitionSpec as P

SOFT_CAP = 50.0
ROPE_BASE = 10000.0
NORM_EPS = 1e-6

ROWS = 128
DM = 3840
HD = 256
TB = 64
RP = 136
LANES = 128
BCH = 16
NCH = ROWS // BCH
SHIFT = 20.0
CW = 256
NC = DM // CW
OWN = 32
MESH = pl.DeviceIdType.MESH


def attn_kernel(pos_h, posv_h, freq_h, x_h, wpre_h, wq_h, wk_h, wv_h, kc_h, vc_h,
                o_ref, ko_h, vo_h,
                pos_ref, posv, freq, wpre_ref, cos_ref, sin_ref,
                x_buf, a_buf, w_buf, kbuf, vbuf, qs, ks, vs,
                x_sem, s_sem, w_sem, ki_sem, vi_sem, kw_sem, vw_sem):
    sp = lax.axis_index('sp')
    tbase = sp * TB

    def w_copy(i):
        if i < 2:
            src = wk_h.at[:, pl.ds(i * HD, HD)]
        elif i < 4:
            src = wv_h.at[:, pl.ds((i - 2) * HD, HD)]
        else:
            src = wq_h.at[:, pl.ds((i - 4) * HD, HD)]
        return pltpu.make_async_copy(src, w_buf.at[i], w_sem.at[i])

    def k_in(i):
        return pltpu.make_async_copy(kc_h.at[pl.ds(i * BCH, BCH)], kbuf.at[pl.ds(i * BCH, BCH)], ki_sem.at[i])

    def v_in(i):
        return pltpu.make_async_copy(vc_h.at[pl.ds(i * BCH, BCH)], vbuf.at[pl.ds(i * BCH, BCH)], vi_sem.at[i])

    def k_out(i):
        return pltpu.make_async_copy(kbuf.at[pl.ds(i * BCH, BCH)], ko_h.at[pl.ds(i * BCH, BCH)], kw_sem.at[i])

    def v_out(i):
        return pltpu.make_async_copy(vbuf.at[pl.ds(i * BCH, BCH)], vo_h.at[pl.ds(i * BCH, BCH)], vw_sem.at[i])

    x_copy = pltpu.make_async_copy(x_h, x_buf, x_sem)
    x_copy.start()
    small = [pltpu.make_async_copy(a, b, s_sem.at[i]) for i, (a, b) in enumerate(
        ((wpre_h, wpre_ref), (posv_h, posv), (freq_h, freq), (pos_h, pos_ref)))]
    for c in small:
        c.start()
    ahead = 5
    for i in range(ahead):
        w_copy(i).start()
    for c in small[1:]:
        c.wait()
    pos_col = jnp.broadcast_to(posv[...].astype(jnp.float32), (ROWS, LANES)).T
    ang = pos_col * freq[...]
    cos_ref[...] = jnp.cos(ang)
    sin_ref[...] = jnp.sin(ang)
    small[0].wait()
    x_copy.wait()

    gain = 1.0 + jnp.concatenate([wpre_ref[k:k + 1, :] for k in range(DM // LANES)], 1)

    def norm_rows(i, carry):
        r = pl.multiple_of(i * 16, 16)
        xb = x_buf[pl.ds(r, 16), :].astype(jnp.float32)
        ms = jnp.mean(xb * xb, axis=-1, keepdims=True)
        a_buf[pl.ds(r, 16), :] = (xb * lax.rsqrt(ms + NORM_EPS) * gain).astype(jnp.bfloat16)
        return carry

    lax.fori_loop(0, ROWS // 16, norm_rows, 0)

    for i in range(8):
        w_copy(i).wait()
        if i + ahead < 8:
            w_copy(i + ahead).start()
        else:
            c = i + ahead - 8
            k_in(c).start()
            v_in(c).start()
        y = jnp.dot(a_buf[...], w_buf[i], preferred_element_type=jnp.float32)
        lo, hi = y[:, :LANES], y[:, LANES:]
        if 2 <= i < 4:
            h = i - 2
            for rep in range(2):
                vs[pl.ds((rep * 4 + h) * RP, ROWS), :] = lo
                vs[pl.ds((rep * 4 + 2 + h) * RP, ROWS), :] = hi
        else:
            cos_t, sin_t = cos_ref[...], sin_ref[...]
            rlo = lo * cos_t - hi * sin_t
            rhi = hi * cos_t + lo * sin_t
            if i < 2:
                for rep in range(2):
                    ks[pl.ds((rep * 4 + i) * RP, ROWS), :] = rlo
                    ks[pl.ds((rep * 4 + 2 + i) * RP, ROWS), :] = rhi
            else:
                qs[pl.ds((i - 4) * RP, ROWS), :] = rlo
                qs[pl.ds((4 + i - 4) * RP, ROWS), :] = rhi
    for c in range(ahead, NCH):
        k_in(c).start()
        v_in(c).start()

    lane = lax.broadcasted_iota(jnp.int32, (8, LANES), 1)
    row = lax.broadcasted_iota(jnp.int32, (8, LANES), 0)
    row_c = row // 4
    row_h = (row // 2) % 2
    match = (((lane // 2) % 2) == row_c) & ((lane % 2) == row_h)
    match_f = jnp.where(match, 1.0, 0.0).astype(jnp.float32)
    first = row_c == 0
    t_half = [jnp.where(match, lane // 4 + 32 * hf, 1 << 20) for hf in range(2)]
    quad = lax.broadcasted_iota(jnp.int32, (16, LANES), 0) // 4
    zero = jnp.zeros((8, LANES), jnp.float32)

    def chunk(i, l_acc):
        k_in(i).wait()
        v_in(i).wait()
        tls = []
        for u in range(BCH):
            b = i * BCH + u
            tl = pos_ref[b] - tbase
            tls.append(tl)
            hit = jnp.logical_and(tl >= 0, tl < TB)
            tc = jnp.clip(tl, 0, TB - 1)
            tile = tc // 4
            tgt = jnp.where(hit, tc - tile * 4, -1)
            sel = quad == tgt
            off = pl.multiple_of(tile * 16, 16)
            kn = ks[pl.ds(b, 8, stride=RP), :]
            vn = vs[pl.ds(b, 8, stride=RP), :]
            kt = kbuf[b, pl.ds(off, 16), :].astype(jnp.float32)
            vt = vbuf[b, pl.ds(off, 16), :].astype(jnp.float32)
            kbuf[b, pl.ds(off, 16), :] = jnp.where(sel, jnp.concatenate([kn, kn], 0), kt).astype(jnp.bfloat16)
            vbuf[b, pl.ds(off, 16), :] = jnp.where(sel, jnp.concatenate([vn, vn], 0), vt).astype(jnp.bfloat16)
        scores = []
        for u in range(0, BCH, 2):
            b = i * BCH + u
            q0 = qs[pl.ds(b, 8, stride=RP), :]
            q1 = qs[pl.ds(b + 1, 8, stride=RP), :]
            lhs = jnp.concatenate([jnp.concatenate([q0, zero], 1), jnp.concatenate([zero, q1], 1)], 0).astype(jnp.bfloat16)
            kk = jnp.concatenate([kbuf[b], kbuf[b + 1]], 1)
            scores.append(lax.dot_general(lhs, kk, (((1,), (1,)), ((), ())), preferred_element_type=jnp.float32))
        weights = []
        for u in range(0, BCH, 2):
            pair = []
            for w in range(2):
                part = scores[u // 2][8 * w:8 * w + 8]
                es = []
                for hf in range(2):
                    a = part[:, hf * LANES:(hf + 1) * LANES] * match_f
                    e = pltpu.roll(a, 4, 0)
                    f = jnp.where(first, pltpu.roll(e, LANES - 2, 1), pltpu.roll(e, 2, 1))
                    s = SOFT_CAP * jnp.tanh((a + f) * (HD ** -0.5 / SOFT_CAP))
                    es.append(jnp.where(t_half[hf] <= tls[u + w], jnp.exp(s - SHIFT), 0.0))
                tot = jnp.sum(es[0] + es[1], axis=1, keepdims=True)
                inv = jnp.where(tot > 0.0, 1.0 / tot, 0.0)
                pair.append(jnp.concatenate([es[0] * inv, es[1] * inv], 1))
                l_acc = jnp.where(lane == i * BCH + u + w, tot, l_acc)
            weights.append(jnp.concatenate(pair, 0).astype(jnp.bfloat16))
        for u in range(0, BCH, 2):
            b = i * BCH + u
            vv = jnp.concatenate([vbuf[b], vbuf[b + 1]], 1)
            o = jnp.dot(weights[u // 2], vv, preferred_element_type=jnp.float32)
            o_ref[pl.ds(b, 8, stride=RP), :] = o[0:8, 0:LANES]
            o_ref[pl.ds(b + 1, 8, stride=RP), :] = o[8:16, LANES:]
        k_out(i).start()
        v_out(i).start()
        return l_acc

    l_acc = lax.fori_loop(0, NCH, chunk, zero)
    l_full = jnp.concatenate([l_acc, jnp.zeros((ROWS - 8, LANES), jnp.float32)], 0)
    o_ref[pl.ds(8 * RP, ROWS), :] = l_full.T
    for i in range(NCH):
        k_out(i).wait()
        v_out(i).wait()


def comm_kernel(o_ref, wo_h, s_all,
                wo_buf, r1, m1, r2, lhs, p_buf, rr, rl, sr, sl,
                w_sem, r1_send, r1_recv, r2_send, r2_recv,
                right_send, right_recv, left_send, left_recv,
                part_send, part_recv, y_send, y_recv, f_send, f_recv):
    z = lax.axis_index('tp')
    sp = lax.axis_index('sp')
    core = sp % 2
    yy = sp // 2
    partner = sp + 1 - 2 * core
    ypeer = (sp + 2) % 4
    diag = 3 - sp

    def wo_copy(k):
        return pltpu.make_async_copy(wo_h.at[:, pl.ds(pl.multiple_of(k * CW, CW), CW)], wo_buf.at[k], w_sem.at[k])

    for k in range(NC):
        wo_copy(k).start()

    @pl.when(z == 0)
    def _():
        rr[...] = jnp.zeros_like(rr)

    @pl.when(z == 3)
    def _():
        rl[...] = jnp.zeros_like(rl)

    bar = pltpu.get_barrier_semaphore()
    pl.semaphore_signal(bar, inc=1, device_id={'sp': partner}, device_id_type=MESH)
    pl.semaphore_signal(bar, inc=1, device_id={'sp': ypeer}, device_id_type=MESH)

    @pl.when(z > 0)
    def _():
        pl.semaphore_signal(bar, inc=1, device_id={'tp': z - 1}, device_id_type=MESH)

    @pl.when(z < 3)
    def _():
        pl.semaphore_signal(bar, inc=1, device_id={'tp': z + 1}, device_id_type=MESH)

    pl.semaphore_wait(bar, 3 + (z * (3 - z)) // 2)

    def to_partner(slot):
        ychip = (1 - yy) if slot == 0 else yy
        r0 = pl.multiple_of(ychip * 64 + (1 - core) * OWN, OWN)
        return pltpu.make_async_remote_copy(
            src_ref=o_ref.at[:, pl.ds(r0, OWN), :], dst_ref=r1.at[slot],
            send_sem=r1_send.at[slot], recv_sem=r1_recv.at[slot], device_id={'sp': partner}, device_id_type=MESH)

    to_partner(0).start()
    to_partner(1).start()

    def merge(load_a, load_b, write):
        la, lb = load_a(8), load_b(8)
        tot = la + lb
        inv = jnp.where(tot > 0.0, 1.0 / tot, 0.0)
        fa, fb = la * inv, lb * inv
        for j in range(8):
            write(j, load_a(j) * fa[:, j:j + 1] + load_b(j) * fb[:, j:j + 1])
        write(8, tot)

    def own_rows(ychip):
        r0 = pl.multiple_of(ychip * 64 + core * OWN, OWN)
        return lambda j: o_ref[j, pl.ds(r0, OWN), :]

    def put_m1(j, val):
        m1[j] = val

    to_partner(0).wait()
    merge(own_rows(1 - yy), lambda j: r1[0, j], put_m1)
    y_merge = pltpu.make_async_remote_copy(
        src_ref=m1, dst_ref=r2, send_sem=r2_send, recv_sem=r2_recv, device_id={'sp': ypeer}, device_id_type=MESH)
    y_merge.start()
    to_partner(1).wait()

    def put_r1(j, val):
        r1[1, j] = val

    merge(own_rows(yy), lambda j: r1[1, j], put_r1)
    y_merge.wait()

    def put_lhs(j, val):
        if j < 8:
            c, hq = j // 4, j % 4
            lhs[:, (hq * 2 + c) * LANES:(hq * 2 + c + 1) * LANES] = val.astype(jnp.bfloat16)

    merge(lambda j: r1[1, j], lambda j: r2[j], put_lhs)

    def right_copy(k):
        return pltpu.make_async_remote_copy(
            src_ref=sr.at[k], dst_ref=rr.at[k], send_sem=right_send.at[k], recv_sem=right_recv.at[k],
            device_id={'tp': z + 1}, device_id_type=MESH)

    def left_copy(k):
        return pltpu.make_async_remote_copy(
            src_ref=sl.at[k], dst_ref=rl.at[k], send_sem=left_send.at[k], recv_sem=left_recv.at[k],
            device_id={'tp': z - 1}, device_id_type=MESH)

    def part_copy(k):
        return pltpu.make_async_remote_copy(
            src_ref=s_all.at[sp, k], dst_ref=s_all.at[sp, k], send_sem=part_send.at[k], recv_sem=part_recv.at[k],
            device_id={'sp': partner}, device_id_type=MESH)

    def y_copy(k):
        return pltpu.make_async_remote_copy(
            src_ref=s_all.at[sp, k], dst_ref=s_all.at[sp, k], send_sem=y_send.at[k], recv_sem=y_recv.at[k],
            device_id={'sp': ypeer}, device_id_type=MESH)

    def fwd_copy(k):
        return pltpu.make_async_remote_copy(
            src_ref=s_all.at[ypeer, k], dst_ref=s_all.at[ypeer, k], send_sem=f_send.at[k], recv_sem=f_recv.at[k],
            device_id={'sp': partner}, device_id_type=MESH)

    hop = 6
    lag_r = hop * z
    lag_l = hop * (3 - z)
    lag_s = hop * (3 - (z * (3 - z)) // 2)

    def tick(i, carry):
        @pl.when(i < NC)
        def _():
            wo_copy(i).wait()
            p_buf[i] = jnp.dot(lhs[...], wo_buf[i], preferred_element_type=jnp.float32)

        kr = i - lag_r

        @pl.when(jnp.logical_and(kr >= 0, kr < NC))
        def _():
            @pl.when(z > 0)
            def _():
                right_copy(kr).wait_recv()

            @pl.when(z < 3)
            def _():
                sr[kr] = p_buf[kr] + rr[kr]
                right_copy(kr).start()

        kl = i - lag_l

        @pl.when(jnp.logical_and(kl >= 0, kl < NC))
        def _():
            @pl.when(z < 3)
            def _():
                left_copy(kl).wait_recv()

            @pl.when(z > 0)
            def _():
                sl[kl] = p_buf[kl] + rl[kl]
                left_copy(kl).start()

        k_s = i - lag_s

        @pl.when(jnp.logical_and(k_s >= 0, k_s < NC))
        def _():
            s_all[sp, k_s] = p_buf[k_s] + rr[k_s] + rl[k_s]
            y_copy(k_s).start()
            part_copy(k_s).start()

        k_y = i - lag_s - hop

        @pl.when(jnp.logical_and(k_y >= 0, k_y < NC))
        def _():
            y_copy(k_y).wait_recv()
            fwd_copy(k_y).start()

        return carry

    lax.fori_loop(0, NC + 4 * hop, tick, 0)

    def drain(k, carry):
        part_copy(k).wait()
        y_copy(k).wait_send()
        fwd_copy(k).wait()

        @pl.when(z < 3)
        def _():
            right_copy(k).wait_send()

        @pl.when(z > 0)
        def _():
            left_copy(k).wait_send()

        return carry

    lax.fori_loop(0, NC, drain, 0)


def finish_kernel(s_all, x_ref, wpost_ref, out_h, out_buf, sem):
    blk = 16

    def out_copy(i):
        rows = pl.ds(i * blk, blk)
        return pltpu.make_async_copy(out_buf.at[rows], out_h.at[rows], sem.at[i])

    for i in range(ROWS // blk):
        g, r = (i * blk) // OWN, (i * blk) % OWN
        parts = [s_all[g, k, r:r + blk, :] for k in range(NC)]
        sq = parts[0] * parts[0]
        for k in range(1, NC):
            sq = sq + parts[k] * parts[k]
        rs = lax.rsqrt(jnp.sum(sq, axis=-1, keepdims=True) * (1.0 / DM) + NORM_EPS)
        for k in range(NC):
            for hf in range(CW // LANES):
                col = k * CW + hf * LANES
                gain = 1.0 + wpost_ref[col // LANES:col // LANES + 1, :]
                val = s_all[g, k, r:r + blk, hf * LANES:(hf + 1) * LANES] * rs * gain
                cs = slice(col, col + LANES)
                out_buf[i * blk:(i + 1) * blk, cs] = (x_ref[i * blk:(i + 1) * blk, cs].astype(jnp.float32) + val).astype(jnp.bfloat16)
        out_copy(i).start()
    for i in range(ROWS // blk):
        out_copy(i).wait()


def solution(mesh):
    cache_spec = P('dp', 'sp', 'tp', None)
    hbm = pl.BlockSpec(memory_space=pltpu.HBM)
    vmem = pl.BlockSpec(memory_space=pltpu.VMEM)

    def in_hbm(arr):
        return pltpu.with_memory_space_constraint(arr, pltpu.HBM)

    def to_rows(c):
        b, t, h, d = c.shape
        return c.reshape(b, t, h, 2, LANES).transpose(0, 1, 3, 2, 4).reshape(b, t * 2 * h, LANES)

    def from_rows(r):
        return r.reshape(ROWS, TB, 2, 2, LANES).transpose(0, 1, 3, 2, 4).reshape(ROWS, TB, 2, HD)

    def local_step(x_in, cur_pos, w_pre, w_q, w_k, w_v, w_o, w_post, k_cache, v_cache):
        half = HD // 2
        inv_freq = ROPE_BASE ** (-2.0 * jnp.arange(half, dtype=jnp.float32) / (2 * half))
        kr, vr = to_rows(k_cache), to_rows(v_cache)
        f32, bf16 = jnp.float32, jnp.bfloat16
        o_part, k_new, v_new = pl.pallas_call(
            attn_kernel,
            out_shape=(pltpu.VMEM((9 * RP, LANES), f32),
                       jax.ShapeDtypeStruct(kr.shape, bf16), jax.ShapeDtypeStruct(vr.shape, bf16)),
            in_specs=[hbm] * 10,
            out_specs=(vmem, hbm, hbm),
            scratch_shapes=[
                pltpu.SMEM((ROWS,), jnp.int32), pltpu.VMEM((1, ROWS), jnp.int32), pltpu.VMEM((1, LANES), f32),
                pltpu.VMEM((DM // LANES, LANES), f32), pltpu.VMEM((ROWS, LANES), f32), pltpu.VMEM((ROWS, LANES), f32),
                pltpu.VMEM((ROWS, DM), bf16), pltpu.VMEM((ROWS, DM), bf16), pltpu.VMEM((8, DM, HD), bf16),
                pltpu.VMEM(kr.shape, bf16), pltpu.VMEM(vr.shape, bf16),
                pltpu.VMEM((8 * RP, LANES), f32), pltpu.VMEM((8 * RP, LANES), f32), pltpu.VMEM((8 * RP, LANES), f32),
                pltpu.SemaphoreType.DMA, pltpu.SemaphoreType.DMA((4,)), pltpu.SemaphoreType.DMA((8,)),
                pltpu.SemaphoreType.DMA((NCH,)), pltpu.SemaphoreType.DMA((NCH,)),
                pltpu.SemaphoreType.DMA((NCH,)), pltpu.SemaphoreType.DMA((NCH,)),
            ],
            compiler_params=pltpu.CompilerParams(vmem_limit_bytes=56 << 20),
            name='attend',
        )(in_hbm(cur_pos), in_hbm(cur_pos.reshape(1, ROWS)), in_hbm(inv_freq.reshape(1, LANES)), in_hbm(x_in),
          in_hbm(w_pre.reshape(DM // LANES, LANES)), in_hbm(w_q), in_hbm(w_k), in_hbm(w_v), in_hbm(kr), in_hbm(vr))
        dma = pltpu.SemaphoreType.DMA
        big = pltpu.VMEM((NC, OWN, CW), f32)
        sums = pl.pallas_call(
            comm_kernel,
            out_shape=pltpu.VMEM((4, NC, OWN, CW), f32),
            in_specs=[vmem, hbm],
            out_specs=vmem,
            scratch_shapes=[
                pltpu.VMEM((NC, 1024, CW), bf16), pltpu.VMEM((2, 9, OWN, LANES), f32), pltpu.VMEM((9, OWN, LANES), f32),
                pltpu.VMEM((9, OWN, LANES), f32), pltpu.VMEM((OWN, 1024), bf16),
                big, big, big, big, big,
                dma((NC,)), dma((2,)), dma((2,)), dma, dma,
                dma((NC,)), dma((NC,)), dma((NC,)), dma((NC,)),
                dma((NC,)), dma((NC,)), dma((NC,)), dma((NC,)), dma((NC,)), dma((NC,)),
            ],
            compiler_params=pltpu.CompilerParams(vmem_limit_bytes=40 << 20, collective_id=0, has_side_effects=True),
            name='combine',
        )(pltpu.with_memory_space_constraint(o_part.reshape(9, RP, LANES), pltpu.VMEM), in_hbm(w_o))
        x_out = pl.pallas_call(
            finish_kernel,
            out_shape=jax.ShapeDtypeStruct((ROWS, DM), bf16),
            in_specs=[vmem, vmem, vmem],
            out_specs=hbm,
            scratch_shapes=[pltpu.VMEM((ROWS, DM), bf16), dma((ROWS // 16,))],
            compiler_params=pltpu.CompilerParams(vmem_limit_bytes=16 << 20),
            name='finish',
        )(pltpu.with_memory_space_constraint(sums, pltpu.VMEM), x_in, w_post.reshape(DM // LANES, LANES))
        return x_out, from_rows(k_new), from_rows(v_new)

    return jax.shard_map(local_step, mesh=mesh,
                         in_specs=(P('dp', None), P('dp'), P(None), P(None, 'tp'), P(None, 'tp'), P(None, 'tp'), P('tp', None), P(None), cache_spec, cache_spec),
                         out_specs=(P('dp', None), cache_spec, cache_spec), check_vma=False)
```

```python
import functools

import jax
import jax.numpy as jnp
from jax import lax
from jax.experimental import pallas as pl
from jax.experimental.pallas import tpu as pltpu
from jax.sharding import PartitionSpec as P

SOFT_CAP = 50.0
ROPE_BASE = 10000.0
NORM_EPS = 1e-6

ROWS = 128
DM = 3840
HD = 256
TB = 64
RP = 136
LANES = 128
BCH = 16
HALF = ROWS // 2
HP = 72
NCH = HALF // BCH
SHIFT = 20.0
CW = 256
NC = DM // CW
OWN = 32
MP = 40
MESH = pl.DeviceIdType.MESH


def attend_rows(row0, nchunk, pos_ref, kbuf, vbuf, qs, ks, vs, o_ref, before, after):
    tbase = lax.axis_index('sp') * TB
    lane = lax.broadcasted_iota(jnp.int32, (8, LANES), 1)
    row = lax.broadcasted_iota(jnp.int32, (8, LANES), 0)
    row_c = row // 4
    row_h = (row // 2) % 2
    match = (((lane // 2) % 2) == row_c) & ((lane % 2) == row_h)
    match_f = jnp.where(match, 1.0, 0.0).astype(jnp.float32)
    first = row_c == 0
    t_half = [jnp.where(match, lane // 4 + 32 * hf, 1 << 20) for hf in range(2)]
    quad = lax.broadcasted_iota(jnp.int32, (16, LANES), 0) // 4
    zero = jnp.zeros((8, LANES), jnp.float32)

    def chunk(i, l_acc):
        before(i)
        tls = []
        for u in range(BCH):
            lb = i * BCH + u
            b = row0 + lb
            tl = pos_ref[b] - tbase
            tls.append(tl)
            hit = jnp.logical_and(tl >= 0, tl < TB)
            tc = jnp.clip(tl, 0, TB - 1)
            tile = tc // 4
            tgt = jnp.where(hit, tc - tile * 4, -1)
            sel = quad == tgt
            off = pl.multiple_of(tile * 16, 16)
            kn = ks[pl.ds(b, 8, stride=RP), :]
            vn = vs[pl.ds(b, 8, stride=RP), :]
            kt = kbuf[lb, pl.ds(off, 16), :].astype(jnp.float32)
            vt = vbuf[lb, pl.ds(off, 16), :].astype(jnp.float32)
            kbuf[lb, pl.ds(off, 16), :] = jnp.where(sel, jnp.concatenate([kn, kn], 0), kt).astype(jnp.bfloat16)
            vbuf[lb, pl.ds(off, 16), :] = jnp.where(sel, jnp.concatenate([vn, vn], 0), vt).astype(jnp.bfloat16)
        scores = []
        for u in range(0, BCH, 2):
            lb = i * BCH + u
            q0 = qs[pl.ds(row0 + lb, 8, stride=RP), :]
            q1 = qs[pl.ds(row0 + lb + 1, 8, stride=RP), :]
            lhs = jnp.concatenate([jnp.concatenate([q0, zero], 1), jnp.concatenate([zero, q1], 1)], 0).astype(jnp.bfloat16)
            kk = jnp.concatenate([kbuf[lb], kbuf[lb + 1]], 1)
            scores.append(lax.dot_general(lhs, kk, (((1,), (1,)), ((), ())), preferred_element_type=jnp.float32))
        weights = []
        for u in range(0, BCH, 2):
            pair = []
            for w in range(2):
                part = scores[u // 2][8 * w:8 * w + 8]
                es = []
                for hf in range(2):
                    a = part[:, hf * LANES:(hf + 1) * LANES] * match_f
                    e = pltpu.roll(a, 4, 0)
                    f = jnp.where(first, pltpu.roll(e, LANES - 2, 1), pltpu.roll(e, 2, 1))
                    s = SOFT_CAP * jnp.tanh((a + f) * (HD ** -0.5 / SOFT_CAP))
                    es.append(jnp.where(t_half[hf] <= tls[u + w], jnp.exp(s - SHIFT), 0.0))
                tot = jnp.sum(es[0] + es[1], axis=1, keepdims=True)
                inv = jnp.where(tot > 0.0, 1.0 / tot, 0.0)
                pair.append(jnp.concatenate([es[0] * inv, es[1] * inv], 1))
                l_acc = jnp.where(lane == i * BCH + u + w, tot, l_acc)
            weights.append(jnp.concatenate(pair, 0).astype(jnp.bfloat16))
        for u in range(0, BCH, 2):
            lb = i * BCH + u
            vv = jnp.concatenate([vbuf[lb], vbuf[lb + 1]], 1)
            o = jnp.dot(weights[u // 2], vv, preferred_element_type=jnp.float32)
            o_ref[pl.ds(lb, 8, stride=HP), :] = o[0:8, 0:LANES]
            o_ref[pl.ds(lb + 1, 8, stride=HP), :] = o[8:16, LANES:]
        after(i)
        return l_acc

    l_acc = lax.fori_loop(0, nchunk, chunk, zero)
    o_ref[pl.ds(HALF, 8, stride=HP), :] = l_acc


def far_kernel(pos_h, posv_h, freq_h, x_h, wpre_h, wq_h, wk_h, wv_h, kc_h, vc_h,
               o_ref, kbuf, vbuf, qs, ks, vs,
               pos_ref, posv, freq, wpre_ref, cos_ref, sin_ref, x_buf, a_buf, w_buf,
               x_sem, s_sem, w_sem, ki_sem, vi_sem):
    row0 = (1 - lax.axis_index('sp') // 2) * HALF

    def w_copy(i):
        if i < 2:
            src = wk_h.at[:, pl.ds(i * HD, HD)]
        elif i < 4:
            src = wv_h.at[:, pl.ds((i - 2) * HD, HD)]
        else:
            src = wq_h.at[:, pl.ds((i - 4) * HD, HD)]
        return pltpu.make_async_copy(src, w_buf.at[i], w_sem.at[i])

    def k_in(i):
        return pltpu.make_async_copy(kc_h.at[pl.ds(row0 + i * BCH, BCH)], kbuf.at[pl.ds(i * BCH, BCH)], ki_sem.at[i])

    def v_in(i):
        return pltpu.make_async_copy(vc_h.at[pl.ds(row0 + i * BCH, BCH)], vbuf.at[pl.ds(i * BCH, BCH)], vi_sem.at[i])

    x_copy = pltpu.make_async_copy(x_h, x_buf, x_sem)
    x_copy.start()
    small = [pltpu.make_async_copy(a, b, s_sem.at[i]) for i, (a, b) in enumerate(
        ((wpre_h, wpre_ref), (posv_h, posv), (freq_h, freq), (pos_h, pos_ref)))]
    for c in small:
        c.start()
    ahead = 5
    for i in range(ahead):
        w_copy(i).start()
    for c in small[1:]:
        c.wait()
    pos_col = jnp.broadcast_to(posv[...].astype(jnp.float32), (ROWS, LANES)).T
    ang = pos_col * freq[...]
    cos_ref[...] = jnp.cos(ang)
    sin_ref[...] = jnp.sin(ang)
    small[0].wait()
    x_copy.wait()

    gain = 1.0 + jnp.concatenate([wpre_ref[k:k + 1, :] for k in range(DM // LANES)], 1)

    def norm_rows(i, carry):
        r = pl.multiple_of(i * 16, 16)
        xb = x_buf[pl.ds(r, 16), :].astype(jnp.float32)
        ms = jnp.mean(xb * xb, axis=-1, keepdims=True)
        a_buf[pl.ds(r, 16), :] = (xb * lax.rsqrt(ms + NORM_EPS) * gain).astype(jnp.bfloat16)
        return carry

    lax.fori_loop(0, ROWS // 16, norm_rows, 0)

    issued = 0
    for i in range(8):
        w_copy(i).wait()
        if i + ahead < 8:
            w_copy(i + ahead).start()
        elif issued < NCH:
            k_in(issued).start()
            v_in(issued).start()
            issued += 1
        y = jnp.dot(a_buf[...], w_buf[i], preferred_element_type=jnp.float32)
        lo, hi = y[:, :LANES], y[:, LANES:]
        if 2 <= i < 4:
            h = i - 2
            for rep in range(2):
                vs[pl.ds((rep * 4 + h) * RP, ROWS), :] = lo
                vs[pl.ds((rep * 4 + 2 + h) * RP, ROWS), :] = hi
        else:
            cos_t, sin_t = cos_ref[...], sin_ref[...]
            rlo = lo * cos_t - hi * sin_t
            rhi = hi * cos_t + lo * sin_t
            if i < 2:
                for rep in range(2):
                    ks[pl.ds((rep * 4 + i) * RP, ROWS), :] = rlo
                    ks[pl.ds((rep * 4 + 2 + i) * RP, ROWS), :] = rhi
            else:
                qs[pl.ds((i - 4) * RP, ROWS), :] = rlo
                qs[pl.ds((4 + i - 4) * RP, ROWS), :] = rhi
    for c in range(issued, NCH):
        k_in(c).start()
        v_in(c).start()

    def before(i):
        k_in(i).wait()
        v_in(i).wait()

    attend_rows(row0, NCH, pos_ref, kbuf, vbuf, qs, ks, vs, o_ref, before, lambda i: None)


def near_kernel(pos_h, qs, ks, vs, kfar, vfar, kc_h, vc_h,
                o_ref, ko_h, vo_h,
                pos_ref, kbuf, vbuf, p_sem, ki_sem, vi_sem, kw_sem, vw_sem, kf_sem, vf_sem):
    yy = lax.axis_index('sp') // 2
    row0 = yy * HALF
    far0 = (1 - yy) * HALF

    def k_in(i):
        return pltpu.make_async_copy(kc_h.at[pl.ds(row0 + i * BCH, BCH)], kbuf.at[pl.ds(i * BCH, BCH)], ki_sem.at[i])

    def v_in(i):
        return pltpu.make_async_copy(vc_h.at[pl.ds(row0 + i * BCH, BCH)], vbuf.at[pl.ds(i * BCH, BCH)], vi_sem.at[i])

    def k_out(i):
        return pltpu.make_async_copy(kbuf.at[pl.ds(i * BCH, BCH)], ko_h.at[pl.ds(row0 + i * BCH, BCH)], kw_sem.at[i])

    def v_out(i):
        return pltpu.make_async_copy(vbuf.at[pl.ds(i * BCH, BCH)], vo_h.at[pl.ds(row0 + i * BCH, BCH)], vw_sem.at[i])

    def kf_out(i):
        return pltpu.make_async_copy(kfar.at[pl.ds(i * BCH, BCH)], ko_h.at[pl.ds(far0 + i * BCH, BCH)], kf_sem.at[i])

    def vf_out(i):
        return pltpu.make_async_copy(vfar.at[pl.ds(i * BCH, BCH)], vo_h.at[pl.ds(far0 + i * BCH, BCH)], vf_sem.at[i])

    p_copy = pltpu.make_async_copy(pos_h, pos_ref, p_sem)
    p_copy.start()
    for i in range(NCH):
        k_in(i).start()
        v_in(i).start()
    for i in range(NCH):
        kf_out(i).start()
        vf_out(i).start()
    p_copy.wait()

    def before(i):
        k_in(i).wait()
        v_in(i).wait()

    def after(i):
        k_out(i).start()
        v_out(i).start()

    attend_rows(row0, NCH, pos_ref, kbuf, vbuf, qs, ks, vs, o_ref, before, after)
    for i in range(NCH):
        kf_out(i).wait()
        vf_out(i).wait()
        k_out(i).wait()
        v_out(i).wait()


def comm_kernel(o_own, o_got, wo_h, s_all,
                wo_buf, fac, m1, m2, r1, lhs, p_buf, rr, rl, sr, sl,
                w_sem, r1_send, r1_recv,
                right_send, right_recv, left_send, left_recv,
                part_send, part_recv, y_send, y_recv, f_send, f_recv):
    z = lax.axis_index('tp')
    sp = lax.axis_index('sp')
    core = sp % 2
    partner = sp + 1 - 2 * core
    ypeer = (sp + 2) % 4

    def wo_copy(k):
        return pltpu.make_async_copy(wo_h.at[:, pl.ds(pl.multiple_of(k * CW, CW), CW)], wo_buf.at[k], w_sem.at[k])

    for k in range(NC):
        wo_copy(k).start()

    @pl.when(z == 0)
    def _():
        rr[...] = jnp.zeros_like(rr)

    @pl.when(z == 3)
    def _():
        rl[...] = jnp.zeros_like(rl)

    bar = pltpu.get_barrier_semaphore()
    pl.semaphore_signal(bar, inc=1, device_id={'sp': partner}, device_id_type=MESH)
    pl.semaphore_signal(bar, inc=1, device_id={'sp': ypeer}, device_id_type=MESH)

    @pl.when(z > 0)
    def _():
        pl.semaphore_signal(bar, inc=1, device_id={'tp': z - 1}, device_id_type=MESH)

    @pl.when(z < 3)
    def _():
        pl.semaphore_signal(bar, inc=1, device_id={'tp': z + 1}, device_id_type=MESH)

    pl.semaphore_wait(bar, 3 + (z * (3 - z)) // 2)

    def shares(l_a, l_b, slot):
        tot = l_a + l_b
        inv = jnp.where(tot > 0.0, 1.0 / tot, 0.0)
        for w, l in enumerate((l_a, l_b)):
            fac[slot + w] = jnp.concatenate([l * inv, jnp.zeros((LANES - 8, LANES), jnp.float32)], 0).T
        return tot

    mine = pl.multiple_of(core * OWN, OWN)
    theirs = pl.multiple_of((1 - core) * OWN, OWN)
    tot = shares(o_own[pl.ds(HALF, 8, stride=HP), :], o_got[pl.ds(HALF, 8, stride=HP), :], 0)

    def merge_half(r0, dst, stride):
        fa, fb = fac[0, pl.ds(r0, OWN), :], fac[1, pl.ds(r0, OWN), :]
        for j in range(8):
            rows = pl.ds(pl.multiple_of(j * HP + r0, 8), OWN)
            dst[pl.ds(j * stride, OWN), :] = o_own[rows, :] * fa[:, j:j + 1] + o_got[rows, :] * fb[:, j:j + 1]

    merge_half(theirs, m1, MP)
    m1[pl.ds(OWN, 8, stride=MP), :] = tot
    pair = pltpu.make_async_remote_copy(
        src_ref=m1, dst_ref=r1, send_sem=r1_send, recv_sem=r1_recv, device_id={'sp': partner}, device_id_type=MESH)
    pair.start()
    merge_half(mine, m2, OWN)
    pair.wait()
    shares(tot, r1[pl.ds(OWN, 8, stride=MP), :], 2)
    fa, fb = fac[2, pl.ds(mine, OWN), :], fac[3, pl.ds(mine, OWN), :]
    for j in range(8):
        c, hq = j // 4, j % 4
        val = m2[j * OWN:(j + 1) * OWN, :] * fa[:, j:j + 1] + r1[j * MP:j * MP + OWN, :] * fb[:, j:j + 1]
        lhs[:, (hq * 2 + c) * LANES:(hq * 2 + c + 1) * LANES] = val.astype(jnp.bfloat16)

    def right_copy(k):
        return pltpu.make_async_remote_copy(
            src_ref=sr.at[k], dst_ref=rr.at[k], send_sem=right_send.at[k], recv_sem=right_recv.at[k],
            device_id={'tp': z + 1}, device_id_type=MESH)

    def left_copy(k):
        return pltpu.make_async_remote_copy(
            src_ref=sl.at[k], dst_ref=rl.at[k], send_sem=left_send.at[k], recv_sem=left_recv.at[k],
            device_id={'tp': z - 1}, device_id_type=MESH)

    def part_copy(k):
        return pltpu.make_async_remote_copy(
            src_ref=s_all.at[sp, k], dst_ref=s_all.at[sp, k], send_sem=part_send.at[k], recv_sem=part_recv.at[k],
            device_id={'sp': partner}, device_id_type=MESH)

    def y_copy(k):
        return pltpu.make_async_remote_copy(
            src_ref=s_all.at[sp, k], dst_ref=s_all.at[sp, k], send_sem=y_send.at[k], recv_sem=y_recv.at[k],
            device_id={'sp': ypeer}, device_id_type=MESH)

    def fwd_copy(k):
        return pltpu.make_async_remote_copy(
            src_ref=s_all.at[ypeer, k], dst_ref=s_all.at[ypeer, k], send_sem=f_send.at[k], recv_sem=f_recv.at[k],
            device_id={'sp': partner}, device_id_type=MESH)

    hop = 6
    lag_r = hop * z
    lag_l = hop * (3 - z)
    lag_s = hop * (3 - (z * (3 - z)) // 2)

    def tick(i, carry):
        @pl.when(i < NC)
        def _():
            wo_copy(i).wait()
            p_buf[i] = jnp.dot(lhs[...], wo_buf[i], preferred_element_type=jnp.float32)

        kr = i - lag_r

        @pl.when(jnp.logical_and(kr >= 0, kr < NC))
        def _():
            @pl.when(z > 0)
            def _():
                right_copy(kr).wait_recv()

            @pl.when(z < 3)
            def _():
                sr[kr] = p_buf[kr] + rr[kr]
                right_copy(kr).start()

        kl = i - lag_l

        @pl.when(jnp.logical_and(kl >= 0, kl < NC))
        def _():
            @pl.when(z < 3)
            def _():
                left_copy(kl).wait_recv()

            @pl.when(z > 0)
            def _():
                sl[kl] = p_buf[kl] + rl[kl]
                left_copy(kl).start()

        k_s = i - lag_s

        @pl.when(jnp.logical_and(k_s >= 0, k_s < NC))
        def _():
            s_all[sp, k_s] = p_buf[k_s] + rr[k_s] + rl[k_s]
            y_copy(k_s).start()
            part_copy(k_s).start()

        k_y = i - lag_s - hop

        @pl.when(jnp.logical_and(k_y >= 0, k_y < NC))
        def _():
            y_copy(k_y).wait_recv()
            fwd_copy(k_y).start()

        return carry

    lax.fori_loop(0, NC + 4 * hop, tick, 0)

    def drain(k, carry):
        part_copy(k).wait()
        y_copy(k).wait_send()
        fwd_copy(k).wait()

        @pl.when(z < 3)
        def _():
            right_copy(k).wait_send()

        @pl.when(z > 0)
        def _():
            left_copy(k).wait_send()

        return carry

    lax.fori_loop(0, NC, drain, 0)


def finish_kernel(s_all, x_ref, wpost_ref, out_h, out_buf, sem):
    blk = 16

    def out_copy(i):
        rows = pl.ds(i * blk, blk)
        return pltpu.make_async_copy(out_buf.at[rows], out_h.at[rows], sem.at[i])

    for i in range(ROWS // blk):
        g, r = (i * blk) // OWN, (i * blk) % OWN
        parts = [s_all[g, k, r:r + blk, :] for k in range(NC)]
        sq = parts[0] * parts[0]
        for k in range(1, NC):
            sq = sq + parts[k] * parts[k]
        rs = lax.rsqrt(jnp.sum(sq, axis=-1, keepdims=True) * (1.0 / DM) + NORM_EPS)
        for k in range(NC):
            for hf in range(CW // LANES):
                col = k * CW + hf * LANES
                gain = 1.0 + wpost_ref[col // LANES:col // LANES + 1, :]
                val = s_all[g, k, r:r + blk, hf * LANES:(hf + 1) * LANES] * rs * gain
                cs = slice(col, col + LANES)
                out_buf[i * blk:(i + 1) * blk, cs] = (x_ref[i * blk:(i + 1) * blk, cs].astype(jnp.float32) + val).astype(jnp.bfloat16)
        out_copy(i).start()
    for i in range(ROWS // blk):
        out_copy(i).wait()


def solution(mesh):
    cache_spec = P('dp', 'sp', 'tp', None)
    hbm = pl.BlockSpec(memory_space=pltpu.HBM)
    vmem = pl.BlockSpec(memory_space=pltpu.VMEM)

    def in_hbm(arr):
        return pltpu.with_memory_space_constraint(arr, pltpu.HBM)

    def in_vmem(arr):
        return pltpu.with_memory_space_constraint(arr, pltpu.VMEM)

    def to_rows(c):
        b, t, h, d = c.shape
        return c.reshape(b, t, h, 2, LANES).transpose(0, 1, 3, 2, 4).reshape(b, t * 2 * h, LANES)

    def from_rows(r):
        return r.reshape(ROWS, TB, 2, 2, LANES).transpose(0, 1, 3, 2, 4).reshape(ROWS, TB, 2, HD)

    def local_step(x_in, cur_pos, w_pre, w_q, w_k, w_v, w_o, w_post, k_cache, v_cache):
        half = HD // 2
        inv_freq = ROPE_BASE ** (-2.0 * jnp.arange(half, dtype=jnp.float32) / (2 * half))
        kr, vr = to_rows(k_cache), to_rows(v_cache)
        f32, bf16 = jnp.float32, jnp.bfloat16
        dma = pltpu.SemaphoreType.DMA
        half_shape = (HALF,) + kr.shape[1:]
        o_far, k_far, v_far, qs, ks, vs = pl.pallas_call(
            far_kernel,
            out_shape=(jax.ShapeDtypeStruct((8 * HP, LANES), f32),
                       pltpu.VMEM(half_shape, bf16), pltpu.VMEM(half_shape, bf16),
                       pltpu.VMEM((8 * RP, LANES), f32), pltpu.VMEM((8 * RP, LANES), f32), pltpu.VMEM((8 * RP, LANES), f32)),
            in_specs=[hbm] * 10,
            out_specs=(vmem,) * 6,
            scratch_shapes=[
                pltpu.SMEM((ROWS,), jnp.int32), pltpu.VMEM((1, ROWS), jnp.int32), pltpu.VMEM((1, LANES), f32),
                pltpu.VMEM((DM // LANES, LANES), f32), pltpu.VMEM((ROWS, LANES), f32), pltpu.VMEM((ROWS, LANES), f32),
                pltpu.VMEM((ROWS, DM), bf16), pltpu.VMEM((ROWS, DM), bf16), pltpu.VMEM((8, DM, HD), bf16),
                dma, dma((4,)), dma((8,)), dma((NCH,)), dma((NCH,)),
            ],
            compiler_params=pltpu.CompilerParams(vmem_limit_bytes=40 << 20),
            cost_estimate=pl.CostEstimate(flops=2 * 10 ** 9, bytes_accessed=25 * 10 ** 6, transcendentals=0),
            name='attend_far',
        )(in_hbm(cur_pos), in_hbm(cur_pos.reshape(1, ROWS)), in_hbm(inv_freq.reshape(1, LANES)), in_hbm(x_in),
          in_hbm(w_pre.reshape(DM // LANES, LANES)), in_hbm(w_q), in_hbm(w_k), in_hbm(w_v), in_hbm(kr), in_hbm(vr))
        o_got = lax.ppermute(o_far, 'sp', [(0, 2), (1, 3), (2, 0), (3, 1)])
        o_own, k_new, v_new = pl.pallas_call(
            near_kernel,
            out_shape=(pltpu.VMEM((8 * HP, LANES), f32),
                       jax.ShapeDtypeStruct(kr.shape, bf16), jax.ShapeDtypeStruct(vr.shape, bf16)),
            in_specs=[hbm, vmem, vmem, vmem, vmem, vmem, hbm, hbm],
            out_specs=(vmem, hbm, hbm),
            scratch_shapes=[
                pltpu.SMEM((ROWS,), jnp.int32), pltpu.VMEM(half_shape, bf16), pltpu.VMEM(half_shape, bf16),
                dma, dma((NCH,)), dma((NCH,)), dma((NCH,)), dma((NCH,)), dma((NCH,)), dma((NCH,)),
            ],
            compiler_params=pltpu.CompilerParams(vmem_limit_bytes=28 << 20),
            cost_estimate=pl.CostEstimate(flops=10 ** 10, bytes_accessed=25 * 10 ** 6, transcendentals=0),
            name='attend_near',
        )(in_hbm(cur_pos), in_vmem(qs), in_vmem(ks), in_vmem(vs), in_vmem(k_far), in_vmem(v_far), in_hbm(kr), in_hbm(vr))
        big = pltpu.VMEM((NC, OWN, CW), f32)
        sums = pl.pallas_call(
            comm_kernel,
            out_shape=pltpu.VMEM((4, NC, OWN, CW), f32),
            in_specs=[vmem, vmem, hbm],
            out_specs=vmem,
            scratch_shapes=[
                pltpu.VMEM((NC, 1024, CW), bf16), pltpu.VMEM((4, LANES, LANES), f32), pltpu.VMEM((8 * MP, LANES), f32),
                pltpu.VMEM((8 * OWN, LANES), f32), pltpu.VMEM((8 * MP, LANES), f32), pltpu.VMEM((OWN, 1024), bf16),
                big, big, big, big, big,
                dma((NC,)), dma, dma,
                dma((NC,)), dma((NC,)), dma((NC,)), dma((NC,)),
                dma((NC,)), dma((NC,)), dma((NC,)), dma((NC,)), dma((NC,)), dma((NC,)),
            ],
            compiler_params=pltpu.CompilerParams(vmem_limit_bytes=40 << 20, collective_id=0, has_side_effects=True),
            name='combine',
        )(in_vmem(o_own), o_got, in_hbm(w_o))
        x_out = pl.pallas_call(
            finish_kernel,
            out_shape=jax.ShapeDtypeStruct((ROWS, DM), bf16),
            in_specs=[vmem, vmem, vmem],
            out_specs=hbm,
            scratch_shapes=[pltpu.VMEM((ROWS, DM), bf16), dma((ROWS // 16,))],
            compiler_params=pltpu.CompilerParams(vmem_limit_bytes=16 << 20),
            name='finish',
        )(in_vmem(sums), x_in, w_post.reshape(DM // LANES, LANES))
        return x_out, from_rows(k_new), from_rows(v_new)

    return jax.shard_map(local_step, mesh=mesh,
                         in_specs=(P('dp', None), P('dp'), P(None), P(None, 'tp'), P(None, 'tp'), P(None, 'tp'), P('tp', None), P(None), cache_spec, cache_spec),
                         out_specs=(P('dp', None), cache_spec, cache_spec), check_vma=False)
```

```python
import functools

import jax
import jax.numpy as jnp
import numpy as np
from jax import lax
from jax.experimental import pallas as pl
from jax.experimental.pallas import tpu as pltpu
from jax.sharding import PartitionSpec as P

SOFT_CAP = 50.0
ROPE_BASE = 10000.0
NORM_EPS = 1e-6

ROWS = 128
DM = 3840
HD = 256
TB = 64
RP = 136
LANES = 128
BCH = 16
HALF = ROWS // 2
HP = 72
NCH = HALF // BCH
KC = 768
NKC = DM // KC
SHIFT = 20.0
CW = 256
NC = DM // CW
OWN = 32
MP = 40
MESH = pl.DeviceIdType.MESH


def attend_rows(row0, nchunk, pos_ref, kbuf, vbuf, qs, ks, vs, o_ref, before, after):
    tbase = lax.axis_index('sp') * TB
    lane = lax.broadcasted_iota(jnp.int32, (8, LANES), 1)
    row = lax.broadcasted_iota(jnp.int32, (8, LANES), 0)
    row_c = row // 4
    row_h = (row // 2) % 2
    match = (((lane // 2) % 2) == row_c) & ((lane % 2) == row_h)
    match_f = jnp.where(match, 1.0, 0.0).astype(jnp.float32)
    first = row_c == 0
    t_half = [jnp.where(match, lane // 4 + 32 * hf, 1 << 20) for hf in range(2)]
    quad = lax.broadcasted_iota(jnp.int32, (16, LANES), 0) // 4
    zero = jnp.zeros((8, LANES), jnp.float32)

    def chunk(i, l_acc):
        before(i)
        tls = []
        for u in range(BCH):
            lb = i * BCH + u
            b = row0 + lb
            tl = pos_ref[b] - tbase
            tls.append(tl)
            hit = jnp.logical_and(tl >= 0, tl < TB)
            tc = jnp.clip(tl, 0, TB - 1)
            tile = tc // 4
            tgt = jnp.where(hit, tc - tile * 4, -1)
            sel = quad == tgt
            off = pl.multiple_of(tile * 16, 16)
            kn = ks[pl.ds(b, 8, stride=RP), :]
            vn = vs[pl.ds(b, 8, stride=RP), :]
            kt = kbuf[lb, pl.ds(off, 16), :].astype(jnp.float32)
            vt = vbuf[lb, pl.ds(off, 16), :].astype(jnp.float32)
            kbuf[lb, pl.ds(off, 16), :] = jnp.where(sel, jnp.concatenate([kn, kn], 0), kt).astype(jnp.bfloat16)
            vbuf[lb, pl.ds(off, 16), :] = jnp.where(sel, jnp.concatenate([vn, vn], 0), vt).astype(jnp.bfloat16)
        scores = []
        for u in range(0, BCH, 2):
            lb = i * BCH + u
            q0 = qs[pl.ds(row0 + lb, 8, stride=RP), :]
            q1 = qs[pl.ds(row0 + lb + 1, 8, stride=RP), :]
            lhs = jnp.concatenate([jnp.concatenate([q0, zero], 1), jnp.concatenate([zero, q1], 1)], 0).astype(jnp.bfloat16)
            kk = jnp.concatenate([kbuf[lb], kbuf[lb + 1]], 1)
            scores.append(lax.dot_general(lhs, kk, (((1,), (1,)), ((), ())), preferred_element_type=jnp.float32))
        weights = []
        for u in range(0, BCH, 2):
            pair = []
            for w in range(2):
                part = scores[u // 2][8 * w:8 * w + 8]
                es = []
                for hf in range(2):
                    a = part[:, hf * LANES:(hf + 1) * LANES] * match_f
                    e = pltpu.roll(a, 4, 0)
                    f = jnp.where(first, pltpu.roll(e, LANES - 2, 1), pltpu.roll(e, 2, 1))
                    s = SOFT_CAP * jnp.tanh((a + f) * (HD ** -0.5 / SOFT_CAP))
                    es.append(jnp.where(t_half[hf] <= tls[u + w], jnp.exp(s - SHIFT), 0.0))
                tot = jnp.sum(es[0] + es[1], axis=1, keepdims=True)
                inv = jnp.where(tot > 0.0, 1.0 / tot, 0.0)
                pair.append(jnp.concatenate([es[0] * inv, es[1] * inv], 1))
                l_acc = jnp.where(lane == i * BCH + u + w, tot, l_acc)
            weights.append(jnp.concatenate(pair, 0).astype(jnp.bfloat16))
        for u in range(0, BCH, 2):
            lb = i * BCH + u
            vv = jnp.concatenate([vbuf[lb], vbuf[lb + 1]], 1)
            o = jnp.dot(weights[u // 2], vv, preferred_element_type=jnp.float32)
            o_ref[pl.ds(lb, 8, stride=HP), :] = o[0:8, 0:LANES]
            o_ref[pl.ds(lb + 1, 8, stride=HP), :] = o[8:16, LANES:]
        after(i)
        return l_acc

    l_acc = lax.fori_loop(0, nchunk, chunk, zero)
    o_ref[pl.ds(HALF, 8, stride=HP), :] = l_acc


def far_kernel(pos_h, posv_h, freq_h, x_h, wpre_h, wq_h, wk_h, wv_h, kc_h, vc_h,
               o_ref, kbuf, vbuf, qs, ks, vs,
               pos_ref, posv, freq, wpre_ref, cos_ref, sin_ref, x_buf, a_buf, wq_buf, wk_buf, wv_buf, acc,
               x_sem, s_sem, w_sem, ki_sem, vi_sem):
    row0 = (1 - lax.axis_index('sp') // 2) * HALF

    def w_start(c):
        rows = pl.ds(c * KC, KC)
        for n, (src, dst) in enumerate(((wk_h, wk_buf), (wv_h, wv_buf), (wq_h, wq_buf))):
            pltpu.make_async_copy(src.at[rows, :], dst.at[rows, :], w_sem.at[3 * c + n]).start()

    def w_wait(c):
        rows = pl.ds(c * KC, KC)
        for n, (src, dst) in enumerate(((wk_h, wk_buf), (wv_h, wv_buf), (wq_h, wq_buf))):
            pltpu.make_async_copy(src.at[rows, :], dst.at[rows, :], w_sem.at[3 * c + n]).wait()

    def k_in(i):
        return pltpu.make_async_copy(kc_h.at[pl.ds(row0 + i * BCH, BCH)], kbuf.at[pl.ds(i * BCH, BCH)], ki_sem.at[i])

    def v_in(i):
        return pltpu.make_async_copy(vc_h.at[pl.ds(row0 + i * BCH, BCH)], vbuf.at[pl.ds(i * BCH, BCH)], vi_sem.at[i])

    small = [pltpu.make_async_copy(a, b, s_sem.at[i]) for i, (a, b) in enumerate(
        ((wpre_h, wpre_ref), (posv_h, posv), (freq_h, freq), (pos_h, pos_ref)))]
    for c in small:
        c.start()
    x_copy = pltpu.make_async_copy(x_h, x_buf, x_sem)
    x_copy.start()
    w_start(0)
    for c in small:
        c.wait()
    w_start(1)
    pos_col = jnp.broadcast_to(posv[...].astype(jnp.float32), (ROWS, LANES)).T
    ang = pos_col * freq[...]
    cos_ref[...] = jnp.cos(ang)
    sin_ref[...] = jnp.sin(ang)
    x_copy.wait()
    w_start(2)

    gain = 1.0 + jnp.concatenate([wpre_ref[k:k + 1, :] for k in range(DM // LANES)], 1)

    def norm_rows(i, carry):
        r = pl.multiple_of(i * 16, 16)
        xb = x_buf[pl.ds(r, 16), :].astype(jnp.float32)
        ms = jnp.mean(xb * xb, axis=-1, keepdims=True)
        a_buf[pl.ds(r, 16), :] = (xb * lax.rsqrt(ms + NORM_EPS) * gain).astype(jnp.bfloat16)
        return carry

    lax.fori_loop(0, ROWS // 16, norm_rows, 0)

    for c in range(NKC):
        w_wait(c)
        if c + 3 < NKC:
            w_start(c + 3)
        else:
            for n in range(2 * (c + 3 - NKC), min(NCH, 2 * (c + 4 - NKC))):
                k_in(n).start()
                v_in(n).start()
        rows = slice(c * KC, (c + 1) * KC)
        a_c = a_buf[:, rows]
        for i in range(8):
            if i < 2:
                w_c = wk_buf[rows, i * HD:(i + 1) * HD]
            elif i < 4:
                w_c = wv_buf[rows, (i - 2) * HD:(i - 1) * HD]
            else:
                w_c = wq_buf[rows, (i - 4) * HD:(i - 3) * HD]
            y = jnp.dot(a_c, w_c, preferred_element_type=jnp.float32)
            if c == 0:
                acc[i] = y
                continue
            y = acc[i] + y
            if c < NKC - 1:
                acc[i] = y
                continue
            lo, hi = y[:, :LANES], y[:, LANES:]
            if 2 <= i < 4:
                h = i - 2
                for rep in range(2):
                    vs[pl.ds((rep * 4 + h) * RP, ROWS), :] = lo
                    vs[pl.ds((rep * 4 + 2 + h) * RP, ROWS), :] = hi
            else:
                cos_t, sin_t = cos_ref[...], sin_ref[...]
                rlo = lo * cos_t - hi * sin_t
                rhi = hi * cos_t + lo * sin_t
                if i < 2:
                    for rep in range(2):
                        ks[pl.ds((rep * 4 + i) * RP, ROWS), :] = rlo
                        ks[pl.ds((rep * 4 + 2 + i) * RP, ROWS), :] = rhi
                else:
                    qs[pl.ds((i - 4) * RP, ROWS), :] = rlo
                    qs[pl.ds((4 + i - 4) * RP, ROWS), :] = rhi

    def before(i):
        k_in(i).wait()
        v_in(i).wait()

    attend_rows(row0, NCH, pos_ref, kbuf, vbuf, qs, ks, vs, o_ref, before, lambda i: None)


def near_kernel(pos_h, qs, ks, vs, kfar, vfar, kc_h, vc_h,
                o_ref, ko_h, vo_h,
                pos_ref, kbuf, vbuf, p_sem, ki_sem, vi_sem, kw_sem, vw_sem, kf_sem, vf_sem):
    yy = lax.axis_index('sp') // 2
    row0 = yy * HALF
    far0 = (1 - yy) * HALF

    def k_in(i):
        return pltpu.make_async_copy(kc_h.at[pl.ds(row0 + i * BCH, BCH)], kbuf.at[pl.ds(i * BCH, BCH)], ki_sem.at[i])

    def v_in(i):
        return pltpu.make_async_copy(vc_h.at[pl.ds(row0 + i * BCH, BCH)], vbuf.at[pl.ds(i * BCH, BCH)], vi_sem.at[i])

    def k_out(i):
        return pltpu.make_async_copy(kbuf.at[pl.ds(i * BCH, BCH)], ko_h.at[pl.ds(row0 + i * BCH, BCH)], kw_sem.at[i])

    def v_out(i):
        return pltpu.make_async_copy(vbuf.at[pl.ds(i * BCH, BCH)], vo_h.at[pl.ds(row0 + i * BCH, BCH)], vw_sem.at[i])

    def kf_out(i):
        return pltpu.make_async_copy(kfar.at[pl.ds(i * BCH, BCH)], ko_h.at[pl.ds(far0 + i * BCH, BCH)], kf_sem.at[i])

    def vf_out(i):
        return pltpu.make_async_copy(vfar.at[pl.ds(i * BCH, BCH)], vo_h.at[pl.ds(far0 + i * BCH, BCH)], vf_sem.at[i])

    p_copy = pltpu.make_async_copy(pos_h, pos_ref, p_sem)
    p_copy.start()
    for i in range(NCH):
        k_in(i).start()
        v_in(i).start()
    p_copy.wait()

    def before(i):
        k_in(i).wait()
        v_in(i).wait()
        kf_out(i).start()
        vf_out(i).start()

    def after(i):
        k_out(i).start()
        v_out(i).start()

    attend_rows(row0, NCH, pos_ref, kbuf, vbuf, qs, ks, vs, o_ref, before, after)
    for i in range(NCH):
        kf_out(i).wait()
        vf_out(i).wait()
        k_out(i).wait()
        v_out(i).wait()


def comm_kernel(o_own, o_got, wo_h, s_all,
                wo_buf, fac, m1, m2, r1, lhs, p_buf, rr, rl, sr, sl,
                w_sem, r1_send, r1_recv,
                right_send, right_recv, left_send, left_recv,
                part_send, part_recv, y_send, y_recv, f_send, f_recv):
    z = lax.axis_index('tp')
    sp = lax.axis_index('sp')
    core = sp % 2
    partner = sp + 1 - 2 * core
    ypeer = (sp + 2) % 4

    def wo_copy(k):
        return pltpu.make_async_copy(wo_h.at[:, pl.ds(pl.multiple_of(k * CW, CW), CW)], wo_buf.at[k], w_sem.at[k])

    for k in range(NC):
        wo_copy(k).start()

    @pl.when(z == 0)
    def _():
        rr[...] = jnp.zeros_like(rr)

    @pl.when(z == 3)
    def _():
        rl[...] = jnp.zeros_like(rl)

    bar = pltpu.get_barrier_semaphore()
    pl.semaphore_signal(bar, inc=1, device_id={'sp': partner}, device_id_type=MESH)
    pl.semaphore_signal(bar, inc=1, device_id={'sp': ypeer}, device_id_type=MESH)

    @pl.when(z > 0)
    def _():
        pl.semaphore_signal(bar, inc=1, device_id={'tp': z - 1}, device_id_type=MESH)

    @pl.when(z < 3)
    def _():
        pl.semaphore_signal(bar, inc=1, device_id={'tp': z + 1}, device_id_type=MESH)

    pl.semaphore_wait(bar, 3 + (z * (3 - z)) // 2)

    def shares(l_a, l_b, slot):
        tot = l_a + l_b
        inv = jnp.where(tot > 0.0, 1.0 / tot, 0.0)
        for w, l in enumerate((l_a, l_b)):
            fac[slot + w] = jnp.concatenate([l * inv, jnp.zeros((LANES - 8, LANES), jnp.float32)], 0).T
        return tot

    mine = pl.multiple_of(core * OWN, OWN)
    theirs = pl.multiple_of((1 - core) * OWN, OWN)
    tot = shares(o_own[pl.ds(HALF, 8, stride=HP), :], o_got[pl.ds(HALF, 8, stride=HP), :], 0)

    def merge_half(r0, dst, stride):
        fa, fb = fac[0, pl.ds(r0, OWN), :], fac[1, pl.ds(r0, OWN), :]
        for j in range(8):
            rows = pl.ds(pl.multiple_of(j * HP + r0, 8), OWN)
            dst[pl.ds(j * stride, OWN), :] = o_own[rows, :] * fa[:, j:j + 1] + o_got[rows, :] * fb[:, j:j + 1]

    merge_half(theirs, m1, MP)
    m1[pl.ds(OWN, 8, stride=MP), :] = tot
    pair = pltpu.make_async_remote_copy(
        src_ref=m1, dst_ref=r1, send_sem=r1_send, recv_sem=r1_recv, device_id={'sp': partner}, device_id_type=MESH)
    pair.start()
    merge_half(mine, m2, OWN)
    pair.wait()
    shares(tot, r1[pl.ds(OWN, 8, stride=MP), :], 2)
    fa, fb = fac[2, pl.ds(mine, OWN), :], fac[3, pl.ds(mine, OWN), :]
    for j in range(8):
        c, hq = j // 4, j % 4
        val = m2[j * OWN:(j + 1) * OWN, :] * fa[:, j:j + 1] + r1[j * MP:j * MP + OWN, :] * fb[:, j:j + 1]
        lhs[:, (hq * 2 + c) * LANES:(hq * 2 + c + 1) * LANES] = val.astype(jnp.bfloat16)

    def right_copy(k):
        return pltpu.make_async_remote_copy(
            src_ref=sr.at[k], dst_ref=rr.at[k], send_sem=right_send.at[k], recv_sem=right_recv.at[k],
            device_id={'tp': z + 1}, device_id_type=MESH)

    def left_copy(k):
        return pltpu.make_async_remote_copy(
            src_ref=sl.at[k], dst_ref=rl.at[k], send_sem=left_send.at[k], recv_sem=left_recv.at[k],
            device_id={'tp': z - 1}, device_id_type=MESH)

    def part_copy(k):
        return pltpu.make_async_remote_copy(
            src_ref=s_all.at[sp, k], dst_ref=s_all.at[sp, k], send_sem=part_send.at[k], recv_sem=part_recv.at[k],
            device_id={'sp': partner}, device_id_type=MESH)

    def y_copy(k):
        return pltpu.make_async_remote_copy(
            src_ref=s_all.at[sp, k], dst_ref=s_all.at[sp, k], send_sem=y_send.at[k], recv_sem=y_recv.at[k],
            device_id={'sp': ypeer}, device_id_type=MESH)

    def fwd_copy(k):
        return pltpu.make_async_remote_copy(
            src_ref=s_all.at[ypeer, k], dst_ref=s_all.at[ypeer, k], send_sem=f_send.at[k], recv_sem=f_recv.at[k],
            device_id={'sp': partner}, device_id_type=MESH)

    hop = 6
    lag_r = hop * z
    lag_l = hop * (3 - z)
    lag_s = hop * (3 - (z * (3 - z)) // 2)

    def tick(i, carry):
        @pl.when(i < NC)
        def _():
            wo_copy(i).wait()
            p_buf[i] = jnp.dot(lhs[...], wo_buf[i], preferred_element_type=jnp.float32)

        kr = i - lag_r

        @pl.when(jnp.logical_and(kr >= 0, kr < NC))
        def _():
            @pl.when(z > 0)
            def _():
                right_copy(kr).wait_recv()

            @pl.when(z < 3)
            def _():
                sr[kr] = p_buf[kr] + rr[kr]
                right_copy(kr).start()

        kl = i - lag_l

        @pl.when(jnp.logical_and(kl >= 0, kl < NC))
        def _():
            @pl.when(z < 3)
            def _():
                left_copy(kl).wait_recv()

            @pl.when(z > 0)
            def _():
                sl[kl] = p_buf[kl] + rl[kl]
                left_copy(kl).start()

        k_s = i - lag_s

        @pl.when(jnp.logical_and(k_s >= 0, k_s < NC))
        def _():
            s_all[sp, k_s] = p_buf[k_s] + rr[k_s] + rl[k_s]
            y_copy(k_s).start()
            part_copy(k_s).start()

        k_y = i - lag_s - hop

        @pl.when(jnp.logical_and(k_y >= 0, k_y < NC))
        def _():
            y_copy(k_y).wait_recv()
            fwd_copy(k_y).start()

        return carry

    lax.fori_loop(0, NC + 4 * hop, tick, 0)

    def drain(k, carry):
        part_copy(k).wait()
        y_copy(k).wait_send()
        fwd_copy(k).wait()

        @pl.when(z < 3)
        def _():
            right_copy(k).wait_send()

        @pl.when(z > 0)
        def _():
            left_copy(k).wait_send()

        return carry

    lax.fori_loop(0, NC, drain, 0)


def finish_kernel(s_all, x_ref, wpost_ref, out_h, out_buf, sem):
    blk = 16

    def out_copy(i):
        rows = pl.ds(i * blk, blk)
        return pltpu.make_async_copy(out_buf.at[rows], out_h.at[rows], sem.at[i])

    for i in range(ROWS // blk):
        g, r = (i * blk) // OWN, (i * blk) % OWN
        parts = [s_all[g, k, r:r + blk, :] for k in range(NC)]
        sq = parts[0] * parts[0]
        for k in range(1, NC):
            sq = sq + parts[k] * parts[k]
        rs = lax.rsqrt(jnp.sum(sq, axis=-1, keepdims=True) * (1.0 / DM) + NORM_EPS)
        for k in range(NC):
            for hf in range(CW // LANES):
                col = k * CW + hf * LANES
                gain = 1.0 + wpost_ref[col // LANES:col // LANES + 1, :]
                val = s_all[g, k, r:r + blk, hf * LANES:(hf + 1) * LANES] * rs * gain
                cs = slice(col, col + LANES)
                out_buf[i * blk:(i + 1) * blk, cs] = (x_ref[i * blk:(i + 1) * blk, cs].astype(jnp.float32) + val).astype(jnp.bfloat16)
        out_copy(i).start()
    for i in range(ROWS // blk):
        out_copy(i).wait()


def solution(mesh):
    cache_spec = P('dp', 'sp', 'tp', None)
    hbm = pl.BlockSpec(memory_space=pltpu.HBM)
    vmem = pl.BlockSpec(memory_space=pltpu.VMEM)

    def in_hbm(arr):
        return pltpu.with_memory_space_constraint(arr, pltpu.HBM)

    def in_vmem(arr):
        return pltpu.with_memory_space_constraint(arr, pltpu.VMEM)

    def to_rows(c):
        b, t, h, d = c.shape
        return c.reshape(b, t, h, 2, LANES).transpose(0, 1, 3, 2, 4).reshape(b, t * 2 * h, LANES)

    def from_rows(r):
        return r.reshape(ROWS, TB, 2, 2, LANES).transpose(0, 1, 3, 2, 4).reshape(ROWS, TB, 2, HD)

    def local_step(x_in, cur_pos, w_pre, w_q, w_k, w_v, w_o, w_post, k_cache, v_cache):
        half = HD // 2
        inv_freq = jnp.asarray((ROPE_BASE ** (-2.0 * np.arange(half) / (2 * half))).astype(np.float32))
        kr, vr = to_rows(k_cache), to_rows(v_cache)
        f32, bf16 = jnp.float32, jnp.bfloat16
        dma = pltpu.SemaphoreType.DMA
        half_shape = (HALF,) + kr.shape[1:]
        o_far, k_far, v_far, qs, ks, vs = pl.pallas_call(
            far_kernel,
            out_shape=(jax.ShapeDtypeStruct((8 * HP, LANES), f32),
                       pltpu.VMEM(half_shape, bf16), pltpu.VMEM(half_shape, bf16),
                       pltpu.VMEM((8 * RP, LANES), f32), pltpu.VMEM((8 * RP, LANES), f32), pltpu.VMEM((8 * RP, LANES), f32)),
            in_specs=[hbm] * 10,
            out_specs=(vmem,) * 6,
            scratch_shapes=[
                pltpu.SMEM((ROWS,), jnp.int32), pltpu.VMEM((1, ROWS), jnp.int32), pltpu.VMEM((1, LANES), f32),
                pltpu.VMEM((DM // LANES, LANES), f32), pltpu.VMEM((ROWS, LANES), f32), pltpu.VMEM((ROWS, LANES), f32),
                pltpu.VMEM((ROWS, DM), bf16), pltpu.VMEM((ROWS, DM), bf16),
                pltpu.VMEM((DM, 1024), bf16), pltpu.VMEM((DM, 512), bf16), pltpu.VMEM((DM, 512), bf16), pltpu.VMEM((8, ROWS, HD), f32),
                dma, dma((4,)), dma((3 * NKC,)), dma((NCH,)), dma((NCH,)),
            ],
            compiler_params=pltpu.CompilerParams(vmem_limit_bytes=40 << 20),
            cost_estimate=pl.CostEstimate(flops=2 * 10 ** 9, bytes_accessed=25 * 10 ** 6, transcendentals=0),
            name='attend_far',
        )(in_hbm(cur_pos), in_hbm(cur_pos.reshape(1, ROWS)), in_hbm(inv_freq.reshape(1, LANES)), in_hbm(x_in),
          in_hbm(w_pre.reshape(DM // LANES, LANES)), in_hbm(w_q), in_hbm(w_k), in_hbm(w_v), in_hbm(kr), in_hbm(vr))
        o_got = lax.ppermute(o_far, 'sp', [(0, 2), (1, 3), (2, 0), (3, 1)])
        o_own, k_new, v_new = pl.pallas_call(
            near_kernel,
            out_shape=(pltpu.VMEM((8 * HP, LANES), f32),
                       jax.ShapeDtypeStruct(kr.shape, bf16), jax.ShapeDtypeStruct(vr.shape, bf16)),
            in_specs=[hbm, vmem, vmem, vmem, vmem, vmem, hbm, hbm],
            out_specs=(vmem, hbm, hbm),
            scratch_shapes=[
                pltpu.SMEM((ROWS,), jnp.int32), pltpu.VMEM(half_shape, bf16), pltpu.VMEM(half_shape, bf16),
                dma, dma((NCH,)), dma((NCH,)), dma((NCH,)), dma((NCH,)), dma((NCH,)), dma((NCH,)),
            ],
            compiler_params=pltpu.CompilerParams(vmem_limit_bytes=28 << 20),
            cost_estimate=pl.CostEstimate(flops=10 ** 10, bytes_accessed=25 * 10 ** 6, transcendentals=0),
            name='attend_near',
        )(in_hbm(cur_pos), in_vmem(qs), in_vmem(ks), in_vmem(vs), in_vmem(k_far), in_vmem(v_far), in_hbm(kr), in_hbm(vr))
        big = pltpu.VMEM((NC, OWN, CW), f32)
        sums = pl.pallas_call(
            comm_kernel,
            out_shape=pltpu.VMEM((4, NC, OWN, CW), f32),
            in_specs=[vmem, vmem, hbm],
            out_specs=vmem,
            scratch_shapes=[
                pltpu.VMEM((NC, 1024, CW), bf16), pltpu.VMEM((4, LANES, LANES), f32), pltpu.VMEM((8 * MP, LANES), f32),
                pltpu.VMEM((8 * OWN, LANES), f32), pltpu.VMEM((8 * MP, LANES), f32), pltpu.VMEM((OWN, 1024), bf16),
                big, big, big, big, big,
                dma((NC,)), dma, dma,
                dma((NC,)), dma((NC,)), dma((NC,)), dma((NC,)),
                dma((NC,)), dma((NC,)), dma((NC,)), dma((NC,)), dma((NC,)), dma((NC,)),
            ],
            compiler_params=pltpu.CompilerParams(vmem_limit_bytes=40 << 20, collective_id=0, has_side_effects=True),
            name='combine',
        )(in_vmem(o_own), o_got, in_hbm(w_o))
        x_out = pl.pallas_call(
            finish_kernel,
            out_shape=jax.ShapeDtypeStruct((ROWS, DM), bf16),
            in_specs=[vmem, vmem, vmem],
            out_specs=hbm,
            scratch_shapes=[pltpu.VMEM((ROWS, DM), bf16), dma((ROWS // 16,))],
            compiler_params=pltpu.CompilerParams(vmem_limit_bytes=16 << 20),
            name='finish',
        )(in_vmem(sums), x_in, w_post.reshape(DM // LANES, LANES))
        return x_out, from_rows(k_new), from_rows(v_new)

    return jax.shard_map(local_step, mesh=mesh,
                         in_specs=(P('dp', None), P('dp'), P(None), P(None, 'tp'), P(None, 'tp'), P(None, 'tp'), P('tp', None), P(None), cache_spec, cache_spec),
                         out_specs=(P('dp', None), cache_spec, cache_spec), check_vma=False)
```

```python
import functools

import jax
import jax.numpy as jnp
import numpy as np
from jax import lax
from jax.experimental import pallas as pl
from jax.experimental.pallas import tpu as pltpu
from jax.sharding import PartitionSpec as P

SOFT_CAP = 50.0
ROPE_BASE = 10000.0
NORM_EPS = 1e-6

ROWS = 128
DM = 3840
HD = 256
TB = 64
RP = 136
LANES = 128
BCH = 16
HALF = ROWS // 2
HP = 72
NCH = HALF // BCH
KC = 768
NKC = DM // KC
SHIFT = 20.0
CW = 256
NC = DM // CW
OWN = 32
MP = 40
MESH = pl.DeviceIdType.MESH


def attend_rows(row0, nchunk, pos_ref, kbuf, vbuf, qs, ks, vs, o_ref, before, after):
    tbase = lax.axis_index('sp') * TB
    lane = lax.broadcasted_iota(jnp.int32, (8, LANES), 1)
    row = lax.broadcasted_iota(jnp.int32, (8, LANES), 0)
    row_c = row // 4
    row_h = (row // 2) % 2
    match = (((lane // 2) % 2) == row_c) & ((lane % 2) == row_h)
    match_f = jnp.where(match, 1.0, 0.0).astype(jnp.float32)
    first = row_c == 0
    t_half = [jnp.where(match, lane // 4 + 32 * hf, 1 << 20) for hf in range(2)]
    quad = lax.broadcasted_iota(jnp.int32, (16, LANES), 0) // 4
    zero = jnp.zeros((8, LANES), jnp.float32)

    def chunk(i, l_acc):
        before(i)
        tls = []
        for u in range(BCH):
            lb = i * BCH + u
            b = row0 + lb
            tl = pos_ref[b] - tbase
            tls.append(tl)
            hit = jnp.logical_and(tl >= 0, tl < TB)
            tc = jnp.clip(tl, 0, TB - 1)
            tile = tc // 4
            tgt = jnp.where(hit, tc - tile * 4, -1)
            sel = quad == tgt
            off = pl.multiple_of(tile * 16, 16)
            kn = ks[pl.ds(b, 8, stride=RP), :]
            vn = vs[pl.ds(b, 8, stride=RP), :]
            kt = kbuf[lb, pl.ds(off, 16), :].astype(jnp.float32)
            vt = vbuf[lb, pl.ds(off, 16), :].astype(jnp.float32)
            kbuf[lb, pl.ds(off, 16), :] = jnp.where(sel, jnp.concatenate([kn, kn], 0), kt).astype(jnp.bfloat16)
            vbuf[lb, pl.ds(off, 16), :] = jnp.where(sel, jnp.concatenate([vn, vn], 0), vt).astype(jnp.bfloat16)
        scores = []
        for u in range(0, BCH, 2):
            lb = i * BCH + u
            q0 = qs[pl.ds(row0 + lb, 8, stride=RP), :]
            q1 = qs[pl.ds(row0 + lb + 1, 8, stride=RP), :]
            lhs = jnp.concatenate([jnp.concatenate([q0, zero], 1), jnp.concatenate([zero, q1], 1)], 0).astype(jnp.bfloat16)
            kk = jnp.concatenate([kbuf[lb], kbuf[lb + 1]], 1)
            scores.append(lax.dot_general(lhs, kk, (((1,), (1,)), ((), ())), preferred_element_type=jnp.float32))
        weights = []
        for u in range(0, BCH, 2):
            pair = []
            for w in range(2):
                part = scores[u // 2][8 * w:8 * w + 8]
                es = []
                for hf in range(2):
                    a = part[:, hf * LANES:(hf + 1) * LANES] * match_f
                    e = pltpu.roll(a, 4, 0)
                    f = jnp.where(first, pltpu.roll(e, LANES - 2, 1), pltpu.roll(e, 2, 1))
                    s = SOFT_CAP * jnp.tanh((a + f) * (HD ** -0.5 / SOFT_CAP))
                    es.append(jnp.where(t_half[hf] <= tls[u + w], jnp.exp(s - SHIFT), 0.0))
                tot = jnp.sum(es[0] + es[1], axis=1, keepdims=True)
                inv = jnp.where(tot > 0.0, 1.0 / tot, 0.0)
                pair.append(jnp.concatenate([es[0] * inv, es[1] * inv], 1))
                l_acc = jnp.where(lane == i * BCH + u + w, tot, l_acc)
            weights.append(jnp.concatenate(pair, 0).astype(jnp.bfloat16))
        for u in range(0, BCH, 2):
            lb = i * BCH + u
            vv = jnp.concatenate([vbuf[lb], vbuf[lb + 1]], 1)
            o = jnp.dot(weights[u // 2], vv, preferred_element_type=jnp.float32)
            o_ref[pl.ds(lb, 8, stride=HP), :] = o[0:8, 0:LANES]
            o_ref[pl.ds(lb + 1, 8, stride=HP), :] = o[8:16, LANES:]
        after(i)
        return l_acc

    l_acc = lax.fori_loop(0, nchunk, chunk, zero)
    o_ref[pl.ds(HALF, 8, stride=HP), :] = l_acc


def far_kernel(pos_h, posv_h, freq_h, x_h, wpre_h, wq_h, wk_h, wv_h, kc_h, vc_h,
               o_ref, kbuf, vbuf, qs, ks, vs,
               pos_ref, posv, freq, wpre_ref, cos_ref, sin_ref, x_buf, a_buf, wq_buf, wk_buf, wv_buf, acc,
               x_sem, s_sem, w_sem, ki_sem, vi_sem):
    row0 = (1 - lax.axis_index('sp') // 2) * HALF

    def w_start(c):
        rows = pl.ds(c * KC, KC)
        for n, (src, dst) in enumerate(((wk_h, wk_buf), (wv_h, wv_buf), (wq_h, wq_buf))):
            pltpu.make_async_copy(src.at[rows, :], dst.at[rows, :], w_sem.at[3 * c + n]).start()

    def w_wait(c):
        rows = pl.ds(c * KC, KC)
        for n, (src, dst) in enumerate(((wk_h, wk_buf), (wv_h, wv_buf), (wq_h, wq_buf))):
            pltpu.make_async_copy(src.at[rows, :], dst.at[rows, :], w_sem.at[3 * c + n]).wait()

    def k_in(i):
        return pltpu.make_async_copy(kc_h.at[pl.ds(row0 + i * BCH, BCH)], kbuf.at[pl.ds(i * BCH, BCH)], ki_sem.at[i])

    def v_in(i):
        return pltpu.make_async_copy(vc_h.at[pl.ds(row0 + i * BCH, BCH)], vbuf.at[pl.ds(i * BCH, BCH)], vi_sem.at[i])

    small = [pltpu.make_async_copy(a, b, s_sem.at[i]) for i, (a, b) in enumerate(
        ((wpre_h, wpre_ref), (posv_h, posv), (freq_h, freq), (pos_h, pos_ref)))]
    for c in small:
        c.start()
    x_copy = pltpu.make_async_copy(x_h, x_buf, x_sem)
    x_copy.start()
    w_start(0)
    for c in small:
        c.wait()
    w_start(1)
    pos_col = jnp.broadcast_to(posv[...].astype(jnp.float32), (ROWS, LANES)).T
    ang = pos_col * freq[...]
    cos_ref[...] = jnp.cos(ang)
    sin_ref[...] = jnp.sin(ang)
    x_copy.wait()
    w_start(2)

    gain = 1.0 + jnp.concatenate([wpre_ref[k:k + 1, :] for k in range(DM // LANES)], 1)

    def norm_rows(i, carry):
        r = pl.multiple_of(i * 16, 16)
        xb = x_buf[pl.ds(r, 16), :].astype(jnp.float32)
        ms = jnp.mean(xb * xb, axis=-1, keepdims=True)
        a_buf[pl.ds(r, 16), :] = (xb * lax.rsqrt(ms + NORM_EPS) * gain).astype(jnp.bfloat16)
        return carry

    lax.fori_loop(0, ROWS // 16, norm_rows, 0)

    for c in range(NKC):
        w_wait(c)
        if c + 3 < NKC:
            w_start(c + 3)
        else:
            for n in range(2 * (c + 3 - NKC), min(NCH, 2 * (c + 4 - NKC))):
                k_in(n).start()
                v_in(n).start()
        rows = slice(c * KC, (c + 1) * KC)
        a_c = a_buf[:, rows]
        for i in range(8):
            if i < 2:
                w_c = wk_buf[rows, i * HD:(i + 1) * HD]
            elif i < 4:
                w_c = wv_buf[rows, (i - 2) * HD:(i - 1) * HD]
            else:
                w_c = wq_buf[rows, (i - 4) * HD:(i - 3) * HD]
            y = jnp.dot(a_c, w_c, preferred_element_type=jnp.float32)
            if c == 0:
                acc[i] = y
                continue
            y = acc[i] + y
            if c < NKC - 1:
                acc[i] = y
                continue
            lo, hi = y[:, :LANES], y[:, LANES:]
            if 2 <= i < 4:
                h = i - 2
                for rep in range(2):
                    vs[pl.ds((rep * 4 + h) * RP, ROWS), :] = lo
                    vs[pl.ds((rep * 4 + 2 + h) * RP, ROWS), :] = hi
            else:
                cos_t, sin_t = cos_ref[...], sin_ref[...]
                rlo = lo * cos_t - hi * sin_t
                rhi = hi * cos_t + lo * sin_t
                if i < 2:
                    for rep in range(2):
                        ks[pl.ds((rep * 4 + i) * RP, ROWS), :] = rlo
                        ks[pl.ds((rep * 4 + 2 + i) * RP, ROWS), :] = rhi
                else:
                    qs[pl.ds((i - 4) * RP, ROWS), :] = rlo
                    qs[pl.ds((4 + i - 4) * RP, ROWS), :] = rhi

    def before(i):
        k_in(i).wait()
        v_in(i).wait()

    attend_rows(row0, NCH, pos_ref, kbuf, vbuf, qs, ks, vs, o_ref, before, lambda i: None)


def near_kernel(pos_h, qs, ks, vs, kfar, vfar, kc_h, vc_h,
                o_ref, ko_h, vo_h,
                pos_ref, kbuf, vbuf, p_sem, ki_sem, vi_sem, kw_sem, vw_sem, kf_sem, vf_sem):
    yy = lax.axis_index('sp') // 2
    row0 = yy * HALF
    far0 = (1 - yy) * HALF

    def k_in(i):
        return pltpu.make_async_copy(kc_h.at[pl.ds(row0 + i * BCH, BCH)], kbuf.at[pl.ds(i * BCH, BCH)], ki_sem.at[i])

    def v_in(i):
        return pltpu.make_async_copy(vc_h.at[pl.ds(row0 + i * BCH, BCH)], vbuf.at[pl.ds(i * BCH, BCH)], vi_sem.at[i])

    def k_out(i):
        return pltpu.make_async_copy(kbuf.at[pl.ds(i * BCH, BCH)], ko_h.at[pl.ds(row0 + i * BCH, BCH)], kw_sem.at[i])

    def v_out(i):
        return pltpu.make_async_copy(vbuf.at[pl.ds(i * BCH, BCH)], vo_h.at[pl.ds(row0 + i * BCH, BCH)], vw_sem.at[i])

    def kf_out(i):
        return pltpu.make_async_copy(kfar.at[pl.ds(i * BCH, BCH)], ko_h.at[pl.ds(far0 + i * BCH, BCH)], kf_sem.at[i])

    def vf_out(i):
        return pltpu.make_async_copy(vfar.at[pl.ds(i * BCH, BCH)], vo_h.at[pl.ds(far0 + i * BCH, BCH)], vf_sem.at[i])

    p_copy = pltpu.make_async_copy(pos_h, pos_ref, p_sem)
    p_copy.start()
    for i in range(NCH):
        k_in(i).start()
        v_in(i).start()
    p_copy.wait()

    def before(i):
        k_in(i).wait()
        v_in(i).wait()
        kf_out(i).start()
        vf_out(i).start()

    def after(i):
        k_out(i).start()
        v_out(i).start()

    attend_rows(row0, NCH, pos_ref, kbuf, vbuf, qs, ks, vs, o_ref, before, after)
    for i in range(NCH):
        kf_out(i).wait()
        vf_out(i).wait()
        k_out(i).wait()
        v_out(i).wait()


def comm_kernel(o_own, o_got, wo_h, s_all,
                wo_buf, fac, m1, m2, r1, lhs, p_buf, rr, rl, sr, sl,
                w_sem, r1_send, r1_recv,
                right_send, right_recv, left_send, left_recv,
                part_send, part_recv, y_send, y_recv, f_send, f_recv):
    z = lax.axis_index('tp')
    sp = lax.axis_index('sp')
    core = sp % 2
    partner = sp + 1 - 2 * core
    ypeer = (sp + 2) % 4

    def wo_copy(k):
        return pltpu.make_async_copy(wo_h.at[:, pl.ds(pl.multiple_of(k * CW, CW), CW)], wo_buf.at[k], w_sem.at[k])

    for k in range(NC):
        wo_copy(k).start()

    @pl.when(z == 0)
    def _():
        rr[...] = jnp.zeros_like(rr)

    @pl.when(z == 3)
    def _():
        rl[...] = jnp.zeros_like(rl)

    bar = pltpu.get_barrier_semaphore()
    pl.semaphore_signal(bar, inc=1, device_id={'sp': partner}, device_id_type=MESH)
    pl.semaphore_signal(bar, inc=1, device_id={'sp': ypeer}, device_id_type=MESH)

    @pl.when(z > 0)
    def _():
        pl.semaphore_signal(bar, inc=1, device_id={'tp': z - 1}, device_id_type=MESH)

    @pl.when(z < 3)
    def _():
        pl.semaphore_signal(bar, inc=1, device_id={'tp': z + 1}, device_id_type=MESH)

    pl.semaphore_wait(bar, 3 + (z * (3 - z)) // 2)

    def shares(l_a, l_b, slot):
        tot = l_a + l_b
        inv = jnp.where(tot > 0.0, 1.0 / tot, 0.0)
        for w, l in enumerate((l_a, l_b)):
            fac[slot + w] = jnp.concatenate([l * inv, jnp.zeros((LANES - 8, LANES), jnp.float32)], 0).T
        return tot

    mine = pl.multiple_of(core * OWN, OWN)
    theirs = pl.multiple_of((1 - core) * OWN, OWN)
    tot = shares(o_own[pl.ds(HALF, 8, stride=HP), :], o_got[pl.ds(HALF, 8, stride=HP), :], 0)

    def merge_half(r0, dst, stride):
        fa, fb = fac[0, pl.ds(r0, OWN), :], fac[1, pl.ds(r0, OWN), :]
        for j in range(8):
            rows = pl.ds(pl.multiple_of(j * HP + r0, 8), OWN)
            dst[pl.ds(j * stride, OWN), :] = o_own[rows, :] * fa[:, j:j + 1] + o_got[rows, :] * fb[:, j:j + 1]

    merge_half(theirs, m1, MP)
    m1[pl.ds(OWN, 8, stride=MP), :] = tot
    pair = pltpu.make_async_remote_copy(
        src_ref=m1, dst_ref=r1, send_sem=r1_send, recv_sem=r1_recv, device_id={'sp': partner}, device_id_type=MESH)
    pair.start()
    merge_half(mine, m2, OWN)
    pair.wait()
    shares(tot, r1[pl.ds(OWN, 8, stride=MP), :], 2)
    fa, fb = fac[2, pl.ds(mine, OWN), :], fac[3, pl.ds(mine, OWN), :]
    for j in range(8):
        c, hq = j // 4, j % 4
        val = m2[j * OWN:(j + 1) * OWN, :] * fa[:, j:j + 1] + r1[j * MP:j * MP + OWN, :] * fb[:, j:j + 1]
        lhs[:, (hq * 2 + c) * LANES:(hq * 2 + c + 1) * LANES] = val.astype(jnp.bfloat16)

    def right_copy(k):
        return pltpu.make_async_remote_copy(
            src_ref=sr.at[k], dst_ref=rr.at[k], send_sem=right_send.at[k], recv_sem=right_recv.at[k],
            device_id={'tp': z + 1}, device_id_type=MESH)

    def left_copy(k):
        return pltpu.make_async_remote_copy(
            src_ref=sl.at[k], dst_ref=rl.at[k], send_sem=left_send.at[k], recv_sem=left_recv.at[k],
            device_id={'tp': z - 1}, device_id_type=MESH)

    def part_copy(k):
        return pltpu.make_async_remote_copy(
            src_ref=s_all.at[sp, k], dst_ref=s_all.at[sp, k], send_sem=part_send.at[k], recv_sem=part_recv.at[k],
            device_id={'sp': partner}, device_id_type=MESH)

    def y_copy(k):
        return pltpu.make_async_remote_copy(
            src_ref=s_all.at[sp, k], dst_ref=s_all.at[sp, k], send_sem=y_send.at[k], recv_sem=y_recv.at[k],
            device_id={'sp': ypeer}, device_id_type=MESH)

    def fwd_copy(k):
        return pltpu.make_async_remote_copy(
            src_ref=s_all.at[ypeer, k], dst_ref=s_all.at[ypeer, k], send_sem=f_send.at[k], recv_sem=f_recv.at[k],
            device_id={'sp': partner}, device_id_type=MESH)

    hop = 9
    late = core * NC
    lag_r = late + hop * z
    lag_l = late + hop * (3 - z)
    lag_s = late + hop * (3 - (z * (3 - z)) // 2)

    def tick(i, carry):
        @pl.when(i < NC)
        def _():
            wo_copy(i).wait()
            p_buf[i] = jnp.dot(lhs[...], wo_buf[i], preferred_element_type=jnp.float32)

        kr = i - lag_r

        @pl.when(jnp.logical_and(kr >= 0, kr < NC))
        def _():
            @pl.when(z > 0)
            def _():
                right_copy(kr).wait_recv()

            @pl.when(z < 3)
            def _():
                sr[kr] = p_buf[kr] + rr[kr]
                right_copy(kr).start()

        kl = i - lag_l

        @pl.when(jnp.logical_and(kl >= 0, kl < NC))
        def _():
            @pl.when(z < 3)
            def _():
                left_copy(kl).wait_recv()

            @pl.when(z > 0)
            def _():
                sl[kl] = p_buf[kl] + rl[kl]
                left_copy(kl).start()

        k_s = i - lag_s

        @pl.when(jnp.logical_and(k_s >= 0, k_s < NC))
        def _():
            s_all[sp, k_s] = p_buf[k_s] + rr[k_s] + rl[k_s]
            y_copy(k_s).start()
            part_copy(k_s).start()

        k_y = i - lag_s - hop

        @pl.when(jnp.logical_and(k_y >= 0, k_y < NC))
        def _():
            y_copy(k_y).wait_recv()
            fwd_copy(k_y).start()

        return carry

    lax.fori_loop(0, 2 * NC + 4 * hop, tick, 0)

    def drain(k, carry):
        part_copy(k).wait()
        y_copy(k).wait_send()
        fwd_copy(k).wait()

        @pl.when(z < 3)
        def _():
            right_copy(k).wait_send()

        @pl.when(z > 0)
        def _():
            left_copy(k).wait_send()

        return carry

    lax.fori_loop(0, NC, drain, 0)


def finish_kernel(s_all, x_ref, wpost_ref, out_h, out_buf, sem):
    blk = 16

    def out_copy(i):
        rows = pl.ds(i * blk, blk)
        return pltpu.make_async_copy(out_buf.at[rows], out_h.at[rows], sem.at[i])

    for i in range(ROWS // blk):
        g, r = (i * blk) // OWN, (i * blk) % OWN
        parts = [s_all[g, k, r:r + blk, :] for k in range(NC)]
        sq = parts[0] * parts[0]
        for k in range(1, NC):
            sq = sq + parts[k] * parts[k]
        rs = lax.rsqrt(jnp.sum(sq, axis=-1, keepdims=True) * (1.0 / DM) + NORM_EPS)
        for k in range(NC):
            for hf in range(CW // LANES):
                col = k * CW + hf * LANES
                gain = 1.0 + wpost_ref[col // LANES:col // LANES + 1, :]
                val = s_all[g, k, r:r + blk, hf * LANES:(hf + 1) * LANES] * rs * gain
                cs = slice(col, col + LANES)
                out_buf[i * blk:(i + 1) * blk, cs] = (x_ref[i * blk:(i + 1) * blk, cs].astype(jnp.float32) + val).astype(jnp.bfloat16)
        out_copy(i).start()
    for i in range(ROWS // blk):
        out_copy(i).wait()


def solution(mesh):
    cache_spec = P('dp', 'sp', 'tp', None)
    hbm = pl.BlockSpec(memory_space=pltpu.HBM)
    vmem = pl.BlockSpec(memory_space=pltpu.VMEM)

    def in_hbm(arr):
        return pltpu.with_memory_space_constraint(arr, pltpu.HBM)

    def in_vmem(arr):
        return pltpu.with_memory_space_constraint(arr, pltpu.VMEM)

    def to_rows(c):
        b, t, h, d = c.shape
        return c.reshape(b, t, h, 2, LANES).transpose(0, 1, 3, 2, 4).reshape(b, t * 2 * h, LANES)

    def from_rows(r):
        return r.reshape(ROWS, TB, 2, 2, LANES).transpose(0, 1, 3, 2, 4).reshape(ROWS, TB, 2, HD)

    def local_step(x_in, cur_pos, w_pre, w_q, w_k, w_v, w_o, w_post, k_cache, v_cache):
        half = HD // 2
        inv_freq = jnp.asarray((ROPE_BASE ** (-2.0 * np.arange(half) / (2 * half))).astype(np.float32))
        kr, vr = to_rows(k_cache), to_rows(v_cache)
        f32, bf16 = jnp.float32, jnp.bfloat16
        dma = pltpu.SemaphoreType.DMA
        half_shape = (HALF,) + kr.shape[1:]
        o_far, k_far, v_far, qs, ks, vs = pl.pallas_call(
            far_kernel,
            out_shape=(jax.ShapeDtypeStruct((8 * HP, LANES), f32),
                       pltpu.VMEM(half_shape, bf16), pltpu.VMEM(half_shape, bf16),
                       pltpu.VMEM((8 * RP, LANES), f32), pltpu.VMEM((8 * RP, LANES), f32), pltpu.VMEM((8 * RP, LANES), f32)),
            in_specs=[hbm] * 10,
            out_specs=(vmem,) * 6,
            scratch_shapes=[
                pltpu.SMEM((ROWS,), jnp.int32), pltpu.VMEM((1, ROWS), jnp.int32), pltpu.VMEM((1, LANES), f32),
                pltpu.VMEM((DM // LANES, LANES), f32), pltpu.VMEM((ROWS, LANES), f32), pltpu.VMEM((ROWS, LANES), f32),
                pltpu.VMEM((ROWS, DM), bf16), pltpu.VMEM((ROWS, DM), bf16),
                pltpu.VMEM((DM, 1024), bf16), pltpu.VMEM((DM, 512), bf16), pltpu.VMEM((DM, 512), bf16), pltpu.VMEM((8, ROWS, HD), f32),
                dma, dma((4,)), dma((3 * NKC,)), dma((NCH,)), dma((NCH,)),
            ],
            compiler_params=pltpu.CompilerParams(vmem_limit_bytes=40 << 20),
            cost_estimate=pl.CostEstimate(flops=2 * 10 ** 9, bytes_accessed=25 * 10 ** 6, transcendentals=0),
            name='attend_far',
        )(in_hbm(cur_pos), in_hbm(cur_pos.reshape(1, ROWS)), in_hbm(inv_freq.reshape(1, LANES)), in_hbm(x_in),
          in_hbm(w_pre.reshape(DM // LANES, LANES)), in_hbm(w_q), in_hbm(w_k), in_hbm(w_v), in_hbm(kr), in_hbm(vr))
        o_got = lax.ppermute(o_far, 'sp', [(0, 2), (1, 3), (2, 0), (3, 1)])
        o_own, k_new, v_new = pl.pallas_call(
            near_kernel,
            out_shape=(pltpu.VMEM((8 * HP, LANES), f32),
                       jax.ShapeDtypeStruct(kr.shape, bf16), jax.ShapeDtypeStruct(vr.shape, bf16)),
            in_specs=[hbm, vmem, vmem, vmem, vmem, vmem, hbm, hbm],
            out_specs=(vmem, hbm, hbm),
            scratch_shapes=[
                pltpu.SMEM((ROWS,), jnp.int32), pltpu.VMEM(half_shape, bf16), pltpu.VMEM(half_shape, bf16),
                dma, dma((NCH,)), dma((NCH,)), dma((NCH,)), dma((NCH,)), dma((NCH,)), dma((NCH,)),
            ],
            compiler_params=pltpu.CompilerParams(vmem_limit_bytes=28 << 20),
            cost_estimate=pl.CostEstimate(flops=10 ** 10, bytes_accessed=25 * 10 ** 6, transcendentals=0),
            name='attend_near',
        )(in_hbm(cur_pos), in_vmem(qs), in_vmem(ks), in_vmem(vs), in_vmem(k_far), in_vmem(v_far), in_hbm(kr), in_hbm(vr))
        big = pltpu.VMEM((NC, OWN, CW), f32)
        sums = pl.pallas_call(
            comm_kernel,
            out_shape=pltpu.VMEM((4, NC, OWN, CW), f32),
            in_specs=[vmem, vmem, hbm],
            out_specs=vmem,
            scratch_shapes=[
                pltpu.VMEM((NC, 1024, CW), bf16), pltpu.VMEM((4, LANES, LANES), f32), pltpu.VMEM((8 * MP, LANES), f32),
                pltpu.VMEM((8 * OWN, LANES), f32), pltpu.VMEM((8 * MP, LANES), f32), pltpu.VMEM((OWN, 1024), bf16),
                big, big, big, big, big,
                dma((NC,)), dma, dma,
                dma((NC,)), dma((NC,)), dma((NC,)), dma((NC,)),
                dma((NC,)), dma((NC,)), dma((NC,)), dma((NC,)), dma((NC,)), dma((NC,)),
            ],
            compiler_params=pltpu.CompilerParams(vmem_limit_bytes=40 << 20, collective_id=0, has_side_effects=True),
            name='combine',
        )(in_vmem(o_own), o_got, in_hbm(w_o))
        x_out = pl.pallas_call(
            finish_kernel,
            out_shape=jax.ShapeDtypeStruct((ROWS, DM), bf16),
            in_specs=[vmem, vmem, vmem],
            out_specs=hbm,
            scratch_shapes=[pltpu.VMEM((ROWS, DM), bf16), dma((ROWS // 16,))],
            compiler_params=pltpu.CompilerParams(vmem_limit_bytes=16 << 20),
            name='finish',
        )(in_vmem(sums), x_in, w_post.reshape(DM // LANES, LANES))
        return x_out, from_rows(k_new), from_rows(v_new)

    return jax.shard_map(local_step, mesh=mesh,
                         in_specs=(P('dp', None), P('dp'), P(None), P(None, 'tp'), P(None, 'tp'), P(None, 'tp'), P('tp', None), P(None), cache_spec, cache_spec),
                         out_specs=(P('dp', None), cache_spec, cache_spec), check_vma=False)
```

```python
import functools

import jax
import jax.numpy as jnp
import numpy as np
from jax import lax
from jax.experimental import pallas as pl
from jax.experimental.pallas import tpu as pltpu
from jax.sharding import PartitionSpec as P

SOFT_CAP = 50.0
ROPE_BASE = 10000.0
NORM_EPS = 1e-6

ROWS = 128
DM = 3840
HD = 256
TB = 64
RP = 136
LANES = 128
BCH = 16
HALF = ROWS // 2
HP = 72
NCH = HALF // BCH
KC = 768
NKC = DM // KC
SHIFT = 20.0
CW = 256
NC = DM // CW
OWN = 32
MP = 40
MESH = pl.DeviceIdType.MESH


def attend_rows(row0, nchunk, pos_ref, kbuf, vbuf, qs, ks, vs, o_ref, before, after):
    tbase = lax.axis_index('sp') * TB
    lane = lax.broadcasted_iota(jnp.int32, (8, LANES), 1)
    row = lax.broadcasted_iota(jnp.int32, (8, LANES), 0)
    row_c = row // 4
    row_h = (row // 2) % 2
    match = (((lane // 2) % 2) == row_c) & ((lane % 2) == row_h)
    match_f = jnp.where(match, 1.0, 0.0).astype(jnp.float32)
    first = row_c == 0
    t_half = [jnp.where(match, lane // 4 + 32 * hf, 1 << 20) for hf in range(2)]
    quad = lax.broadcasted_iota(jnp.int32, (16, LANES), 0) // 4
    zero = jnp.zeros((8, LANES), jnp.float32)

    def chunk(i, l_acc):
        before(i)
        tls = []
        for u in range(BCH):
            lb = i * BCH + u
            b = row0 + lb
            tl = pos_ref[b] - tbase
            tls.append(tl)
            hit = jnp.logical_and(tl >= 0, tl < TB)
            tc = jnp.clip(tl, 0, TB - 1)
            tile = tc // 4
            tgt = jnp.where(hit, tc - tile * 4, -1)
            sel = quad == tgt
            off = pl.multiple_of(tile * 16, 16)
            kn = ks[pl.ds(b, 8, stride=RP), :]
            vn = vs[pl.ds(b, 8, stride=RP), :]
            kt = kbuf[lb, pl.ds(off, 16), :].astype(jnp.float32)
            vt = vbuf[lb, pl.ds(off, 16), :].astype(jnp.float32)
            kbuf[lb, pl.ds(off, 16), :] = jnp.where(sel, jnp.concatenate([kn, kn], 0), kt).astype(jnp.bfloat16)
            vbuf[lb, pl.ds(off, 16), :] = jnp.where(sel, jnp.concatenate([vn, vn], 0), vt).astype(jnp.bfloat16)
        scores = []
        for u in range(0, BCH, 2):
            lb = i * BCH + u
            q0 = qs[pl.ds(row0 + lb, 8, stride=RP), :]
            q1 = qs[pl.ds(row0 + lb + 1, 8, stride=RP), :]
            lhs = jnp.concatenate([jnp.concatenate([q0, zero], 1), jnp.concatenate([zero, q1], 1)], 0).astype(jnp.bfloat16)
            kk = jnp.concatenate([kbuf[lb], kbuf[lb + 1]], 1)
            scores.append(lax.dot_general(lhs, kk, (((1,), (1,)), ((), ())), preferred_element_type=jnp.float32))
        weights = []
        for u in range(0, BCH, 2):
            pair = []
            for w in range(2):
                part = scores[u // 2][8 * w:8 * w + 8]
                es = []
                for hf in range(2):
                    a = part[:, hf * LANES:(hf + 1) * LANES] * match_f
                    e = pltpu.roll(a, 4, 0)
                    f = jnp.where(first, pltpu.roll(e, LANES - 2, 1), pltpu.roll(e, 2, 1))
                    s = SOFT_CAP * jnp.tanh((a + f) * (HD ** -0.5 / SOFT_CAP))
                    es.append(jnp.where(t_half[hf] <= tls[u + w], jnp.exp(s - SHIFT), 0.0))
                tot = jnp.sum(es[0] + es[1], axis=1, keepdims=True)
                inv = jnp.where(tot > 0.0, 1.0 / tot, 0.0)
                pair.append(jnp.concatenate([es[0] * inv, es[1] * inv], 1))
                l_acc = jnp.where(lane == i * BCH + u + w, tot, l_acc)
            weights.append(jnp.concatenate(pair, 0).astype(jnp.bfloat16))
        for u in range(0, BCH, 2):
            lb = i * BCH + u
            vv = jnp.concatenate([vbuf[lb], vbuf[lb + 1]], 1)
            o = jnp.dot(weights[u // 2], vv, preferred_element_type=jnp.float32)
            o_ref[pl.ds(lb, 8, stride=HP), :] = o[0:8, 0:LANES]
            o_ref[pl.ds(lb + 1, 8, stride=HP), :] = o[8:16, LANES:]
        after(i)
        return l_acc

    l_acc = lax.fori_loop(0, nchunk, chunk, zero)
    o_ref[pl.ds(HALF, 8, stride=HP), :] = l_acc


def far_kernel(pos_h, posv_h, freq_h, x_h, wpre_h, wq_h, wk_h, wv_h, kc_h, vc_h,
               o_ref, kbuf, vbuf, qs, ks, vs,
               pos_ref, posv, freq, wpre_ref, cos_ref, sin_ref, x_buf, a_buf, wq_buf, wk_buf, wv_buf, acc,
               x_sem, s_sem, w_sem, ki_sem):
    row0 = (1 - lax.axis_index('sp') // 2) * HALF

    def w_start(c):
        rows = pl.ds(c * KC, KC)
        for n, (src, dst) in enumerate(((wk_h, wk_buf), (wv_h, wv_buf), (wq_h, wq_buf))):
            pltpu.make_async_copy(src.at[rows, :], dst.at[rows, :], w_sem.at[c]).start()

    def w_wait(c):
        rows = pl.ds(c * KC, KC)
        for n, (src, dst) in enumerate(((wk_h, wk_buf), (wv_h, wv_buf), (wq_h, wq_buf))):
            pltpu.make_async_copy(src.at[rows, :], dst.at[rows, :], w_sem.at[c]).wait()

    def k_in(i):
        return pltpu.make_async_copy(kc_h.at[pl.ds(row0 + i * BCH, BCH)], kbuf.at[pl.ds(i * BCH, BCH)], ki_sem.at[i])

    def v_in(i):
        return pltpu.make_async_copy(vc_h.at[pl.ds(row0 + i * BCH, BCH)], vbuf.at[pl.ds(i * BCH, BCH)], ki_sem.at[i])

    small = [pltpu.make_async_copy(a, b, s_sem) for a, b in (
        (wpre_h, wpre_ref), (posv_h, posv), (freq_h, freq), (pos_h, pos_ref))]
    for c in small:
        c.start()
    x_copy = pltpu.make_async_copy(x_h, x_buf, x_sem)
    x_copy.start()
    w_start(0)
    for c in small:
        c.wait()
    w_start(1)
    pos_col = jnp.broadcast_to(posv[...].astype(jnp.float32), (ROWS, LANES)).T
    ang = pos_col * freq[...]
    cos_ref[...] = jnp.cos(ang)
    sin_ref[...] = jnp.sin(ang)
    x_copy.wait()
    w_start(2)

    gain = 1.0 + jnp.concatenate([wpre_ref[k:k + 1, :] for k in range(DM // LANES)], 1)

    def norm_rows(i, carry):
        r = pl.multiple_of(i * 16, 16)
        xb = x_buf[pl.ds(r, 16), :].astype(jnp.float32)
        ms = jnp.mean(xb * xb, axis=-1, keepdims=True)
        a_buf[pl.ds(r, 16), :] = (xb * lax.rsqrt(ms + NORM_EPS) * gain).astype(jnp.bfloat16)
        return carry

    lax.fori_loop(0, ROWS // 16, norm_rows, 0)

    for c in range(NKC):
        w_wait(c)
        if c + 3 < NKC:
            w_start(c + 3)
        else:
            for n in range(2 * (c + 3 - NKC), min(NCH, 2 * (c + 4 - NKC))):
                k_in(n).start()
                v_in(n).start()
        rows = slice(c * KC, (c + 1) * KC)
        a_c = a_buf[:, rows]
        for i in range(8):
            if i < 2:
                w_c = wk_buf[rows, i * HD:(i + 1) * HD]
            elif i < 4:
                w_c = wv_buf[rows, (i - 2) * HD:(i - 1) * HD]
            else:
                w_c = wq_buf[rows, (i - 4) * HD:(i - 3) * HD]
            y = jnp.dot(a_c, w_c, preferred_element_type=jnp.float32)
            if c == 0:
                acc[i] = y
                continue
            y = acc[i] + y
            if c < NKC - 1:
                acc[i] = y
                continue
            lo, hi = y[:, :LANES], y[:, LANES:]
            if 2 <= i < 4:
                h = i - 2
                for rep in range(2):
                    vs[pl.ds((rep * 4 + h) * RP, ROWS), :] = lo
                    vs[pl.ds((rep * 4 + 2 + h) * RP, ROWS), :] = hi
            else:
                cos_t, sin_t = cos_ref[...], sin_ref[...]
                rlo = lo * cos_t - hi * sin_t
                rhi = hi * cos_t + lo * sin_t
                if i < 2:
                    for rep in range(2):
                        ks[pl.ds((rep * 4 + i) * RP, ROWS), :] = rlo
                        ks[pl.ds((rep * 4 + 2 + i) * RP, ROWS), :] = rhi
                else:
                    qs[pl.ds((i - 4) * RP, ROWS), :] = rlo
                    qs[pl.ds((4 + i - 4) * RP, ROWS), :] = rhi

    def before(i):
        k_in(i).wait()
        v_in(i).wait()

    attend_rows(row0, NCH, pos_ref, kbuf, vbuf, qs, ks, vs, o_ref, before, lambda i: None)


def near_kernel(pos_h, qs, ks, vs, kfar, vfar, kc_h, vc_h,
                o_ref, ko_h, vo_h,
                pos_ref, kbuf, vbuf, p_sem, ki_sem, w_sem):
    yy = lax.axis_index('sp') // 2
    row0 = yy * HALF
    far0 = (1 - yy) * HALF

    def k_in(i):
        return pltpu.make_async_copy(kc_h.at[pl.ds(row0 + i * BCH, BCH)], kbuf.at[pl.ds(i * BCH, BCH)], ki_sem.at[i])

    def v_in(i):
        return pltpu.make_async_copy(vc_h.at[pl.ds(row0 + i * BCH, BCH)], vbuf.at[pl.ds(i * BCH, BCH)], ki_sem.at[i])

    def k_out(i):
        return pltpu.make_async_copy(kbuf.at[pl.ds(i * BCH, BCH)], ko_h.at[pl.ds(row0 + i * BCH, BCH)], w_sem)

    def v_out(i):
        return pltpu.make_async_copy(vbuf.at[pl.ds(i * BCH, BCH)], vo_h.at[pl.ds(row0 + i * BCH, BCH)], w_sem)

    def kf_out(i):
        return pltpu.make_async_copy(kfar.at[pl.ds(i * BCH, BCH)], ko_h.at[pl.ds(far0 + i * BCH, BCH)], w_sem)

    def vf_out(i):
        return pltpu.make_async_copy(vfar.at[pl.ds(i * BCH, BCH)], vo_h.at[pl.ds(far0 + i * BCH, BCH)], w_sem)

    p_copy = pltpu.make_async_copy(pos_h, pos_ref, p_sem)
    p_copy.start()
    for i in range(NCH):
        k_in(i).start()
        v_in(i).start()
    p_copy.wait()

    def before(i):
        k_in(i).wait()
        v_in(i).wait()
        kf_out(i).start()
        vf_out(i).start()

    def after(i):
        k_out(i).start()
        v_out(i).start()

    attend_rows(row0, NCH, pos_ref, kbuf, vbuf, qs, ks, vs, o_ref, before, after)
    for i in range(NCH):
        kf_out(i).wait()
        vf_out(i).wait()
        k_out(i).wait()
        v_out(i).wait()


def comm_kernel(o_own, o_got, wo_h, s_all,
                wo_buf, fac, m1, m2, r1, lhs, p_buf, rr, rl, sr, sl,
                w_sem, r1_send, r1_recv,
                right_send, right_recv, left_send, left_recv,
                part_send, part_recv, y_send, y_recv, f_send, f_recv):
    z = lax.axis_index('tp')
    sp = lax.axis_index('sp')
    core = sp % 2
    partner = sp + 1 - 2 * core
    ypeer = (sp + 2) % 4

    def wo_copy(k):
        return pltpu.make_async_copy(wo_h.at[:, pl.ds(pl.multiple_of(k * CW, CW), CW)], wo_buf.at[k], w_sem.at[k])

    for k in range(NC):
        wo_copy(k).start()

    @pl.when(z == 0)
    def _():
        rr[...] = jnp.zeros_like(rr)

    @pl.when(z == 3)
    def _():
        rl[...] = jnp.zeros_like(rl)

    bar = pltpu.get_barrier_semaphore()
    pl.semaphore_signal(bar, inc=1, device_id={'sp': partner}, device_id_type=MESH)
    pl.semaphore_signal(bar, inc=1, device_id={'sp': ypeer}, device_id_type=MESH)

    @pl.when(z > 0)
    def _():
        pl.semaphore_signal(bar, inc=1, device_id={'tp': z - 1}, device_id_type=MESH)

    @pl.when(z < 3)
    def _():
        pl.semaphore_signal(bar, inc=1, device_id={'tp': z + 1}, device_id_type=MESH)

    pl.semaphore_wait(bar, 3 + (z * (3 - z)) // 2)

    def shares(l_a, l_b, slot):
        tot = l_a + l_b
        inv = jnp.where(tot > 0.0, 1.0 / tot, 0.0)
        for w, l in enumerate((l_a, l_b)):
            fac[slot + w] = jnp.concatenate([l * inv, jnp.zeros((LANES - 8, LANES), jnp.float32)], 0).T
        return tot

    mine = pl.multiple_of(core * OWN, OWN)
    theirs = pl.multiple_of((1 - core) * OWN, OWN)
    tot = shares(o_own[pl.ds(HALF, 8, stride=HP), :], o_got[pl.ds(HALF, 8, stride=HP), :], 0)

    def merge_half(r0, dst, stride):
        fa, fb = fac[0, pl.ds(r0, OWN), :], fac[1, pl.ds(r0, OWN), :]
        for j in range(8):
            rows = pl.ds(pl.multiple_of(j * HP + r0, 8), OWN)
            dst[pl.ds(j * stride, OWN), :] = o_own[rows, :] * fa[:, j:j + 1] + o_got[rows, :] * fb[:, j:j + 1]

    merge_half(theirs, m1, MP)
    m1[pl.ds(OWN, 8, stride=MP), :] = tot
    pair = pltpu.make_async_remote_copy(
        src_ref=m1, dst_ref=r1, send_sem=r1_send, recv_sem=r1_recv, device_id={'sp': partner}, device_id_type=MESH)
    pair.start()
    merge_half(mine, m2, OWN)
    pair.wait()
    shares(tot, r1[pl.ds(OWN, 8, stride=MP), :], 2)
    fa, fb = fac[2, pl.ds(mine, OWN), :], fac[3, pl.ds(mine, OWN), :]
    for j in range(8):
        c, hq = j // 4, j % 4
        val = m2[j * OWN:(j + 1) * OWN, :] * fa[:, j:j + 1] + r1[j * MP:j * MP + OWN, :] * fb[:, j:j + 1]
        lhs[:, (hq * 2 + c) * LANES:(hq * 2 + c + 1) * LANES] = val.astype(jnp.bfloat16)

    def right_copy(k):
        return pltpu.make_async_remote_copy(
            src_ref=sr.at[k], dst_ref=rr.at[k], send_sem=right_send, recv_sem=right_recv.at[k],
            device_id={'tp': z + 1}, device_id_type=MESH)

    def left_copy(k):
        return pltpu.make_async_remote_copy(
            src_ref=sl.at[k], dst_ref=rl.at[k], send_sem=left_send, recv_sem=left_recv.at[k],
            device_id={'tp': z - 1}, device_id_type=MESH)

    def part_copy(k):
        return pltpu.make_async_remote_copy(
            src_ref=s_all.at[sp, k], dst_ref=s_all.at[sp, k], send_sem=part_send, recv_sem=part_recv,
            device_id={'sp': partner}, device_id_type=MESH)

    def y_copy(k):
        return pltpu.make_async_remote_copy(
            src_ref=s_all.at[sp, k], dst_ref=s_all.at[sp, k], send_sem=y_send, recv_sem=y_recv.at[k],
            device_id={'sp': ypeer}, device_id_type=MESH)

    def fwd_copy(k):
        return pltpu.make_async_remote_copy(
            src_ref=s_all.at[ypeer, k], dst_ref=s_all.at[ypeer, k], send_sem=f_send, recv_sem=f_recv,
            device_id={'sp': partner}, device_id_type=MESH)

    def whole(ref, sem):
        return pltpu.make_async_copy(ref, ref, sem)

    hop = 6
    lag_r = hop * z
    lag_l = hop * (3 - z)
    lag_s = hop * (3 - (z * (3 - z)) // 2)

    def tick(i, carry):
        @pl.when(i < NC)
        def _():
            wo_copy(i).wait()
            p_buf[i] = jnp.dot(lhs[...], wo_buf[i], preferred_element_type=jnp.float32)

        kr = i - lag_r

        @pl.when(jnp.logical_and(kr >= 0, kr < NC))
        def _():
            @pl.when(z > 0)
            def _():
                right_copy(kr).wait_recv()

            @pl.when(z < 3)
            def _():
                sr[kr] = p_buf[kr] + rr[kr]
                right_copy(kr).start()

        kl = i - lag_l

        @pl.when(jnp.logical_and(kl >= 0, kl < NC))
        def _():
            @pl.when(z < 3)
            def _():
                left_copy(kl).wait_recv()

            @pl.when(z > 0)
            def _():
                sl[kl] = p_buf[kl] + rl[kl]
                left_copy(kl).start()

        k_s = i - lag_s

        @pl.when(jnp.logical_and(k_s >= 0, k_s < NC))
        def _():
            s_all[sp, k_s] = p_buf[k_s] + rr[k_s] + rl[k_s]
            y_copy(k_s).start()
            part_copy(k_s).start()

        k_y = i - lag_s - hop

        @pl.when(jnp.logical_and(k_y >= 0, k_y < NC))
        def _():
            y_copy(k_y).wait_recv()
            fwd_copy(k_y).start()

        return carry

    lax.fori_loop(0, NC + 4 * hop, tick, 0)

    @pl.when(z < 3)
    def _():
        whole(sr, right_send).wait()

    @pl.when(z > 0)
    def _():
        whole(sl, left_send).wait()

    whole(s_all.at[sp], y_send).wait()
    whole(s_all.at[sp], part_send).wait()
    whole(s_all.at[ypeer], f_send).wait()
    whole(s_all.at[partner], part_recv).wait()
    whole(s_all.at[3 - sp], f_recv).wait()


def finish_kernel(s_all, x_ref, wpost_ref, out_h, out_buf, sem):
    blk = 16

    def out_copy(i):
        rows = pl.ds(i * blk, blk)
        return pltpu.make_async_copy(out_buf.at[rows], out_h.at[rows], sem)

    for i in range(ROWS // blk):
        g, r = (i * blk) // OWN, (i * blk) % OWN
        parts = [s_all[g, k, r:r + blk, :] for k in range(NC)]
        sq = parts[0] * parts[0]
        for k in range(1, NC):
            sq = sq + parts[k] * parts[k]
        rs = lax.rsqrt(jnp.sum(sq, axis=-1, keepdims=True) * (1.0 / DM) + NORM_EPS)
        for k in range(NC):
            for hf in range(CW // LANES):
                col = k * CW + hf * LANES
                gain = 1.0 + wpost_ref[col // LANES:col // LANES + 1, :]
                val = s_all[g, k, r:r + blk, hf * LANES:(hf + 1) * LANES] * rs * gain
                cs = slice(col, col + LANES)
                out_buf[i * blk:(i + 1) * blk, cs] = (x_ref[i * blk:(i + 1) * blk, cs].astype(jnp.float32) + val).astype(jnp.bfloat16)
        out_copy(i).start()
    for i in range(ROWS // blk):
        out_copy(i).wait()


def solution(mesh):
    cache_spec = P('dp', 'sp', 'tp', None)
    hbm = pl.BlockSpec(memory_space=pltpu.HBM)
    vmem = pl.BlockSpec(memory_space=pltpu.VMEM)

    def in_hbm(arr):
        return pltpu.with_memory_space_constraint(arr, pltpu.HBM)

    def in_vmem(arr):
        return pltpu.with_memory_space_constraint(arr, pltpu.VMEM)

    def to_rows(c):
        b, t, h, d = c.shape
        return c.reshape(b, t, h, 2, LANES).transpose(0, 1, 3, 2, 4).reshape(b, t * 2 * h, LANES)

    def from_rows(r):
        return r.reshape(ROWS, TB, 2, 2, LANES).transpose(0, 1, 3, 2, 4).reshape(ROWS, TB, 2, HD)

    def local_step(x_in, cur_pos, w_pre, w_q, w_k, w_v, w_o, w_post, k_cache, v_cache):
        half = HD // 2
        inv_freq = jnp.asarray((ROPE_BASE ** (-2.0 * np.arange(half) / (2 * half))).astype(np.float32))
        kr, vr = to_rows(k_cache), to_rows(v_cache)
        f32, bf16 = jnp.float32, jnp.bfloat16
        dma = pltpu.SemaphoreType.DMA
        half_shape = (HALF,) + kr.shape[1:]
        o_far, k_far, v_far, qs, ks, vs = pl.pallas_call(
            far_kernel,
            out_shape=(jax.ShapeDtypeStruct((8 * HP, LANES), f32),
                       pltpu.VMEM(half_shape, bf16), pltpu.VMEM(half_shape, bf16),
                       pltpu.VMEM((8 * RP, LANES), f32), pltpu.VMEM((8 * RP, LANES), f32), pltpu.VMEM((8 * RP, LANES), f32)),
            in_specs=[hbm] * 10,
            out_specs=(vmem,) * 6,
            scratch_shapes=[
                pltpu.SMEM((ROWS,), jnp.int32), pltpu.VMEM((1, ROWS), jnp.int32), pltpu.VMEM((1, LANES), f32),
                pltpu.VMEM((DM // LANES, LANES), f32), pltpu.VMEM((ROWS, LANES), f32), pltpu.VMEM((ROWS, LANES), f32),
                pltpu.VMEM((ROWS, DM), bf16), pltpu.VMEM((ROWS, DM), bf16),
                pltpu.VMEM((DM, 1024), bf16), pltpu.VMEM((DM, 512), bf16), pltpu.VMEM((DM, 512), bf16), pltpu.VMEM((8, ROWS, HD), f32),
                dma, dma, dma((NKC,)), dma((NCH,)),
            ],
            compiler_params=pltpu.CompilerParams(vmem_limit_bytes=40 << 20),
            cost_estimate=pl.CostEstimate(flops=2 * 10 ** 9, bytes_accessed=25 * 10 ** 6, transcendentals=0),
            name='attend_far',
        )(in_hbm(cur_pos), in_hbm(cur_pos.reshape(1, ROWS)), in_hbm(inv_freq.reshape(1, LANES)), in_hbm(x_in),
          in_hbm(w_pre.reshape(DM // LANES, LANES)), in_hbm(w_q), in_hbm(w_k), in_hbm(w_v), in_hbm(kr), in_hbm(vr))
        o_got = lax.ppermute(o_far, 'sp', [(0, 2), (1, 3), (2, 0), (3, 1)])
        o_own, k_new, v_new = pl.pallas_call(
            near_kernel,
            out_shape=(pltpu.VMEM((8 * HP, LANES), f32),
                       jax.ShapeDtypeStruct(kr.shape, bf16), jax.ShapeDtypeStruct(vr.shape, bf16)),
            in_specs=[hbm, vmem, vmem, vmem, vmem, vmem, hbm, hbm],
            out_specs=(vmem, hbm, hbm),
            scratch_shapes=[
                pltpu.SMEM((ROWS,), jnp.int32), pltpu.VMEM(half_shape, bf16), pltpu.VMEM(half_shape, bf16),
                dma, dma((NCH,)), dma,
            ],
            compiler_params=pltpu.CompilerParams(vmem_limit_bytes=28 << 20),
            cost_estimate=pl.CostEstimate(flops=10 ** 10, bytes_accessed=25 * 10 ** 6, transcendentals=0),
            name='attend_near',
        )(in_hbm(cur_pos), in_vmem(qs), in_vmem(ks), in_vmem(vs), in_vmem(k_far), in_vmem(v_far), in_hbm(kr), in_hbm(vr))
        big = pltpu.VMEM((NC, OWN, CW), f32)
        sums = pl.pallas_call(
            comm_kernel,
            out_shape=pltpu.VMEM((4, NC, OWN, CW), f32),
            in_specs=[vmem, vmem, hbm],
            out_specs=vmem,
            scratch_shapes=[
                pltpu.VMEM((NC, 1024, CW), bf16), pltpu.VMEM((4, LANES, LANES), f32), pltpu.VMEM((8 * MP, LANES), f32),
                pltpu.VMEM((8 * OWN, LANES), f32), pltpu.VMEM((8 * MP, LANES), f32), pltpu.VMEM((OWN, 1024), bf16),
                big, big, big, big, big,
                dma((NC,)), dma, dma,
                dma, dma((NC,)), dma, dma((NC,)),
                dma, dma, dma, dma((NC,)), dma, dma,
            ],
            compiler_params=pltpu.CompilerParams(vmem_limit_bytes=40 << 20, collective_id=0, has_side_effects=True),
            name='combine',
        )(in_vmem(o_own), o_got, in_hbm(w_o))
        x_out = pl.pallas_call(
            finish_kernel,
            out_shape=jax.ShapeDtypeStruct((ROWS, DM), bf16),
            in_specs=[vmem, vmem, vmem],
            out_specs=hbm,
            scratch_shapes=[pltpu.VMEM((ROWS, DM), bf16), dma],
            compiler_params=pltpu.CompilerParams(vmem_limit_bytes=16 << 20),
            name='finish',
        )(in_vmem(sums), x_in, w_post.reshape(DM // LANES, LANES))
        return x_out, from_rows(k_new), from_rows(v_new)

    return jax.shard_map(local_step, mesh=mesh,
                         in_specs=(P('dp', None), P('dp'), P(None), P(None, 'tp'), P(None, 'tp'), P(None, 'tp'), P('tp', None), P(None), cache_spec, cache_spec),
                         out_specs=(P('dp', None), cache_spec, cache_spec), check_vma=False)
```

```python
import functools

import jax
import jax.numpy as jnp
import numpy as np
from jax import lax
from jax.experimental import pallas as pl
from jax.experimental.pallas import tpu as pltpu
from jax.sharding import PartitionSpec as P

SOFT_CAP = 50.0
ROPE_BASE = 10000.0
NORM_EPS = 1e-6

ROWS = 128
DM = 3840
HD = 256
TB = 64
RP = 136
LANES = 128
BCH = 16
HALF = ROWS // 2
HP = 72
NCH = HALF // BCH
KC = 768
NKC = DM // KC
SHIFT = 20.0
CW = 384
NC = DM // CW
OWN = 32
MP = 40
MESH = pl.DeviceIdType.MESH


def attend_rows(row0, nchunk, pos_ref, kbuf, vbuf, qs, ks, vs, o_ref, before, after):
    tbase = lax.axis_index('sp') * TB
    lane = lax.broadcasted_iota(jnp.int32, (8, LANES), 1)
    row = lax.broadcasted_iota(jnp.int32, (8, LANES), 0)
    row_c = row // 4
    row_h = (row // 2) % 2
    match = (((lane // 2) % 2) == row_c) & ((lane % 2) == row_h)
    match_f = jnp.where(match, 1.0, 0.0).astype(jnp.float32)
    first = row_c == 0
    t_half = [jnp.where(match, lane // 4 + 32 * hf, 1 << 20) for hf in range(2)]
    quad = lax.broadcasted_iota(jnp.int32, (16, LANES), 0) // 4
    zero = jnp.zeros((8, LANES), jnp.float32)

    def chunk(i, l_acc):
        before(i)
        tls = []
        for u in range(BCH):
            lb = i * BCH + u
            b = row0 + lb
            tl = pos_ref[b] - tbase
            tls.append(tl)
            hit = jnp.logical_and(tl >= 0, tl < TB)
            tc = jnp.clip(tl, 0, TB - 1)
            tile = tc // 4
            tgt = jnp.where(hit, tc - tile * 4, -1)
            sel = quad == tgt
            off = pl.multiple_of(tile * 16, 16)
            kn = ks[pl.ds(b, 8, stride=RP), :]
            vn = vs[pl.ds(b, 8, stride=RP), :]
            kt = kbuf[lb, pl.ds(off, 16), :].astype(jnp.float32)
            vt = vbuf[lb, pl.ds(off, 16), :].astype(jnp.float32)
            kbuf[lb, pl.ds(off, 16), :] = jnp.where(sel, jnp.concatenate([kn, kn], 0), kt).astype(jnp.bfloat16)
            vbuf[lb, pl.ds(off, 16), :] = jnp.where(sel, jnp.concatenate([vn, vn], 0), vt).astype(jnp.bfloat16)
        scores = []
        for u in range(0, BCH, 2):
            lb = i * BCH + u
            q0 = qs[pl.ds(row0 + lb, 8, stride=RP), :]
            q1 = qs[pl.ds(row0 + lb + 1, 8, stride=RP), :]
            lhs = jnp.concatenate([jnp.concatenate([q0, zero], 1), jnp.concatenate([zero, q1], 1)], 0).astype(jnp.bfloat16)
            kk = jnp.concatenate([kbuf[lb], kbuf[lb + 1]], 1)
            scores.append(lax.dot_general(lhs, kk, (((1,), (1,)), ((), ())), preferred_element_type=jnp.float32))
        weights = []
        for u in range(0, BCH, 2):
            pair = []
            for w in range(2):
                part = scores[u // 2][8 * w:8 * w + 8]
                es = []
                for hf in range(2):
                    a = part[:, hf * LANES:(hf + 1) * LANES] * match_f
                    e = pltpu.roll(a, 4, 0)
                    f = jnp.where(first, pltpu.roll(e, LANES - 2, 1), pltpu.roll(e, 2, 1))
                    s = SOFT_CAP * jnp.tanh((a + f) * (HD ** -0.5 / SOFT_CAP))
                    es.append(jnp.where(t_half[hf] <= tls[u + w], jnp.exp(s - SHIFT), 0.0))
                tot = jnp.sum(es[0] + es[1], axis=1, keepdims=True)
                inv = jnp.where(tot > 0.0, 1.0 / tot, 0.0)
                pair.append(jnp.concatenate([es[0] * inv, es[1] * inv], 1))
                l_acc = jnp.where(lane == i * BCH + u + w, tot, l_acc)
            weights.append(jnp.concatenate(pair, 0).astype(jnp.bfloat16))
        for u in range(0, BCH, 2):
            lb = i * BCH + u
            vv = jnp.concatenate([vbuf[lb], vbuf[lb + 1]], 1)
            o = jnp.dot(weights[u // 2], vv, preferred_element_type=jnp.float32)
            o_ref[pl.ds(lb, 8, stride=HP), :] = o[0:8, 0:LANES]
            o_ref[pl.ds(lb + 1, 8, stride=HP), :] = o[8:16, LANES:]
        after(i)
        return l_acc

    l_acc = lax.fori_loop(0, nchunk, chunk, zero)
    o_ref[pl.ds(HALF, 8, stride=HP), :] = l_acc


def far_kernel(pos_h, posv_h, freq_h, x_h, wpre_h, wq_h, wk_h, wv_h, kc_h, vc_h,
               o_ref, kbuf, vbuf, qs, ks, vs,
               pos_ref, posv, freq, wpre_ref, cos_ref, sin_ref, x_buf, a_buf, wq_buf, wk_buf, wv_buf, acc,
               x_sem, s_sem, w_sem, ki_sem):
    row0 = (1 - lax.axis_index('sp') // 2) * HALF

    def w_start(c):
        rows = pl.ds(c * KC, KC)
        for n, (src, dst) in enumerate(((wk_h, wk_buf), (wv_h, wv_buf), (wq_h, wq_buf))):
            pltpu.make_async_copy(src.at[rows, :], dst.at[rows, :], w_sem.at[c]).start()

    def w_wait(c):
        rows = pl.ds(c * KC, KC)
        for n, (src, dst) in enumerate(((wk_h, wk_buf), (wv_h, wv_buf), (wq_h, wq_buf))):
            pltpu.make_async_copy(src.at[rows, :], dst.at[rows, :], w_sem.at[c]).wait()

    def k_in(i):
        return pltpu.make_async_copy(kc_h.at[pl.ds(row0 + i * BCH, BCH)], kbuf.at[pl.ds(i * BCH, BCH)], ki_sem.at[i])

    def v_in(i):
        return pltpu.make_async_copy(vc_h.at[pl.ds(row0 + i * BCH, BCH)], vbuf.at[pl.ds(i * BCH, BCH)], ki_sem.at[i])

    small = [pltpu.make_async_copy(a, b, s_sem) for a, b in (
        (wpre_h, wpre_ref), (posv_h, posv), (freq_h, freq), (pos_h, pos_ref))]
    for c in small:
        c.start()
    x_copy = pltpu.make_async_copy(x_h, x_buf, x_sem)
    x_copy.start()
    w_start(0)
    for c in small:
        c.wait()
    w_start(1)
    pos_col = jnp.broadcast_to(posv[...].astype(jnp.float32), (ROWS, LANES)).T
    ang = pos_col * freq[...]
    cos_ref[...] = jnp.cos(ang)
    sin_ref[...] = jnp.sin(ang)
    x_copy.wait()
    w_start(2)

    gain = 1.0 + jnp.concatenate([wpre_ref[k:k + 1, :] for k in range(DM // LANES)], 1)

    def norm_rows(i, carry):
        r = pl.multiple_of(i * 16, 16)
        xb = x_buf[pl.ds(r, 16), :].astype(jnp.float32)
        ms = jnp.mean(xb * xb, axis=-1, keepdims=True)
        a_buf[pl.ds(r, 16), :] = (xb * lax.rsqrt(ms + NORM_EPS) * gain).astype(jnp.bfloat16)
        return carry

    lax.fori_loop(0, ROWS // 16, norm_rows, 0)

    for c in range(NKC):
        w_wait(c)
        if c + 3 < NKC:
            w_start(c + 3)
        else:
            for n in range(2 * (c + 3 - NKC), min(NCH, 2 * (c + 4 - NKC))):
                k_in(n).start()
                v_in(n).start()
        rows = slice(c * KC, (c + 1) * KC)
        a_c = a_buf[:, rows]
        for i in range(8):
            if i < 2:
                w_c = wk_buf[rows, i * HD:(i + 1) * HD]
            elif i < 4:
                w_c = wv_buf[rows, (i - 2) * HD:(i - 1) * HD]
            else:
                w_c = wq_buf[rows, (i - 4) * HD:(i - 3) * HD]
            y = jnp.dot(a_c, w_c, preferred_element_type=jnp.float32)
            if c == 0:
                acc[i] = y
                continue
            y = acc[i] + y
            if c < NKC - 1:
                acc[i] = y
                continue
            lo, hi = y[:, :LANES], y[:, LANES:]
            if 2 <= i < 4:
                h = i - 2
                for rep in range(2):
                    vs[pl.ds((rep * 4 + h) * RP, ROWS), :] = lo
                    vs[pl.ds((rep * 4 + 2 + h) * RP, ROWS), :] = hi
            else:
                cos_t, sin_t = cos_ref[...], sin_ref[...]
                rlo = lo * cos_t - hi * sin_t
                rhi = hi * cos_t + lo * sin_t
                if i < 2:
                    for rep in range(2):
                        ks[pl.ds((rep * 4 + i) * RP, ROWS), :] = rlo
                        ks[pl.ds((rep * 4 + 2 + i) * RP, ROWS), :] = rhi
                else:
                    qs[pl.ds((i - 4) * RP, ROWS), :] = rlo
                    qs[pl.ds((4 + i - 4) * RP, ROWS), :] = rhi

    def before(i):
        k_in(i).wait()
        v_in(i).wait()

    attend_rows(row0, NCH, pos_ref, kbuf, vbuf, qs, ks, vs, o_ref, before, lambda i: None)


def near_kernel(pos_h, qs, ks, vs, kfar, vfar, kc_h, vc_h,
                o_ref, ko_h, vo_h,
                pos_ref, kbuf, vbuf, p_sem, ki_sem, w_sem):
    yy = lax.axis_index('sp') // 2
    row0 = yy * HALF
    far0 = (1 - yy) * HALF

    def k_in(i):
        return pltpu.make_async_copy(kc_h.at[pl.ds(row0 + i * BCH, BCH)], kbuf.at[pl.ds(i * BCH, BCH)], ki_sem.at[i])

    def v_in(i):
        return pltpu.make_async_copy(vc_h.at[pl.ds(row0 + i * BCH, BCH)], vbuf.at[pl.ds(i * BCH, BCH)], ki_sem.at[i])

    def k_out(i):
        return pltpu.make_async_copy(kbuf.at[pl.ds(i * BCH, BCH)], ko_h.at[pl.ds(row0 + i * BCH, BCH)], w_sem)

    def v_out(i):
        return pltpu.make_async_copy(vbuf.at[pl.ds(i * BCH, BCH)], vo_h.at[pl.ds(row0 + i * BCH, BCH)], w_sem)

    def kf_out(i):
        return pltpu.make_async_copy(kfar.at[pl.ds(i * BCH, BCH)], ko_h.at[pl.ds(far0 + i * BCH, BCH)], w_sem)

    def vf_out(i):
        return pltpu.make_async_copy(vfar.at[pl.ds(i * BCH, BCH)], vo_h.at[pl.ds(far0 + i * BCH, BCH)], w_sem)

    p_copy = pltpu.make_async_copy(pos_h, pos_ref, p_sem)
    p_copy.start()
    for i in range(NCH):
        k_in(i).start()
        v_in(i).start()
    p_copy.wait()

    def before(i):
        k_in(i).wait()
        v_in(i).wait()
        kf_out(i).start()
        vf_out(i).start()

    def after(i):
        k_out(i).start()
        v_out(i).start()

    attend_rows(row0, NCH, pos_ref, kbuf, vbuf, qs, ks, vs, o_ref, before, after)
    for i in range(NCH):
        kf_out(i).wait()
        vf_out(i).wait()
        k_out(i).wait()
        v_out(i).wait()


def comm_kernel(o_own, o_got, wo_h, s_all,
                wo_buf, fac, m1, m2, r1, lhs, p_buf, rr, rl, sr, sl,
                w_sem, r1_send, r1_recv,
                right_send, right_recv, left_send, left_recv,
                part_send, part_recv, y_send, y_recv, f_send, f_recv):
    z = lax.axis_index('tp')
    sp = lax.axis_index('sp')
    core = sp % 2
    partner = sp + 1 - 2 * core
    ypeer = (sp + 2) % 4

    def wo_copy(k):
        return pltpu.make_async_copy(wo_h.at[:, pl.ds(pl.multiple_of(k * CW, CW), CW)], wo_buf.at[k], w_sem.at[k])

    for k in range(NC):
        wo_copy(k).start()

    @pl.when(z == 0)
    def _():
        rr[...] = jnp.zeros_like(rr)

    @pl.when(z == 3)
    def _():
        rl[...] = jnp.zeros_like(rl)

    bar = pltpu.get_barrier_semaphore()
    pl.semaphore_signal(bar, inc=1, device_id={'sp': partner}, device_id_type=MESH)
    pl.semaphore_signal(bar, inc=1, device_id={'sp': ypeer}, device_id_type=MESH)

    @pl.when(z > 0)
    def _():
        pl.semaphore_signal(bar, inc=1, device_id={'tp': z - 1}, device_id_type=MESH)

    @pl.when(z < 3)
    def _():
        pl.semaphore_signal(bar, inc=1, device_id={'tp': z + 1}, device_id_type=MESH)

    pl.semaphore_wait(bar, 3 + (z * (3 - z)) // 2)

    def shares(l_a, l_b, slot):
        tot = l_a + l_b
        inv = jnp.where(tot > 0.0, 1.0 / tot, 0.0)
        for w, l in enumerate((l_a, l_b)):
            fac[slot + w] = jnp.concatenate([l * inv, jnp.zeros((LANES - 8, LANES), jnp.float32)], 0).T
        return tot

    mine = pl.multiple_of(core * OWN, OWN)
    theirs = pl.multiple_of((1 - core) * OWN, OWN)
    tot = shares(o_own[pl.ds(HALF, 8, stride=HP), :], o_got[pl.ds(HALF, 8, stride=HP), :], 0)

    def merge_half(r0, dst, stride):
        fa, fb = fac[0, pl.ds(r0, OWN), :], fac[1, pl.ds(r0, OWN), :]
        for j in range(8):
            rows = pl.ds(pl.multiple_of(j * HP + r0, 8), OWN)
            dst[pl.ds(j * stride, OWN), :] = o_own[rows, :] * fa[:, j:j + 1] + o_got[rows, :] * fb[:, j:j + 1]

    merge_half(theirs, m1, MP)
    m1[pl.ds(OWN, 8, stride=MP), :] = tot
    pair = pltpu.make_async_remote_copy(
        src_ref=m1, dst_ref=r1, send_sem=r1_send, recv_sem=r1_recv, device_id={'sp': partner}, device_id_type=MESH)
    pair.start()
    merge_half(mine, m2, OWN)
    pair.wait()
    shares(tot, r1[pl.ds(OWN, 8, stride=MP), :], 2)
    fa, fb = fac[2, pl.ds(mine, OWN), :], fac[3, pl.ds(mine, OWN), :]
    for j in range(8):
        c, hq = j // 4, j % 4
        val = m2[j * OWN:(j + 1) * OWN, :] * fa[:, j:j + 1] + r1[j * MP:j * MP + OWN, :] * fb[:, j:j + 1]
        lhs[:, (hq * 2 + c) * LANES:(hq * 2 + c + 1) * LANES] = val.astype(jnp.bfloat16)

    def right_copy(k):
        return pltpu.make_async_remote_copy(
            src_ref=sr.at[k], dst_ref=rr.at[k], send_sem=right_send, recv_sem=right_recv.at[k],
            device_id={'tp': z + 1}, device_id_type=MESH)

    def left_copy(k):
        return pltpu.make_async_remote_copy(
            src_ref=sl.at[k], dst_ref=rl.at[k], send_sem=left_send, recv_sem=left_recv.at[k],
            device_id={'tp': z - 1}, device_id_type=MESH)

    def part_copy(k):
        return pltpu.make_async_remote_copy(
            src_ref=s_all.at[sp, k], dst_ref=s_all.at[sp, k], send_sem=part_send, recv_sem=part_recv,
            device_id={'sp': partner}, device_id_type=MESH)

    def y_copy(k):
        return pltpu.make_async_remote_copy(
            src_ref=s_all.at[sp, k], dst_ref=s_all.at[sp, k], send_sem=y_send, recv_sem=y_recv.at[k],
            device_id={'sp': ypeer}, device_id_type=MESH)

    def fwd_copy(k):
        return pltpu.make_async_remote_copy(
            src_ref=s_all.at[ypeer, k], dst_ref=s_all.at[ypeer, k], send_sem=f_send, recv_sem=f_recv,
            device_id={'sp': partner}, device_id_type=MESH)

    def whole(ref, sem):
        return pltpu.make_async_copy(ref, ref, sem)

    hop = 4
    lag_r = hop * z
    lag_l = hop * (3 - z)
    lag_s = hop * (3 - (z * (3 - z)) // 2)

    def tick(i, carry):
        @pl.when(i < NC)
        def _():
            wo_copy(i).wait()
            p_buf[i] = jnp.dot(lhs[...], wo_buf[i], preferred_element_type=jnp.float32)

        kr = i - lag_r

        @pl.when(jnp.logical_and(kr >= 0, kr < NC))
        def _():
            @pl.when(z > 0)
            def _():
                right_copy(kr).wait_recv()

            @pl.when(z < 3)
            def _():
                sr[kr] = p_buf[kr] + rr[kr]
                right_copy(kr).start()

        kl = i - lag_l

        @pl.when(jnp.logical_and(kl >= 0, kl < NC))
        def _():
            @pl.when(z < 3)
            def _():
                left_copy(kl).wait_recv()

            @pl.when(z > 0)
            def _():
                sl[kl] = p_buf[kl] + rl[kl]
                left_copy(kl).start()

        k_s = i - lag_s

        @pl.when(jnp.logical_and(k_s >= 0, k_s < NC))
        def _():
            s_all[sp, k_s] = p_buf[k_s] + rr[k_s] + rl[k_s]
            y_copy(k_s).start()
            part_copy(k_s).start()

        k_y = i - lag_s - hop

        @pl.when(jnp.logical_and(k_y >= 0, k_y < NC))
        def _():
            y_copy(k_y).wait_recv()
            fwd_copy(k_y).start()

        return carry

    lax.fori_loop(0, NC + 4 * hop, tick, 0)

    @pl.when(z < 3)
    def _():
        whole(sr, right_send).wait()

    @pl.when(z > 0)
    def _():
        whole(sl, left_send).wait()

    whole(s_all.at[sp], y_send).wait()
    whole(s_all.at[sp], part_send).wait()
    whole(s_all.at[ypeer], f_send).wait()
    whole(s_all.at[partner], part_recv).wait()
    whole(s_all.at[3 - sp], f_recv).wait()


def finish_kernel(s_all, x_ref, wpost_ref, out_h, out_buf, sem):
    blk = 16

    def out_copy(i):
        rows = pl.ds(i * blk, blk)
        return pltpu.make_async_copy(out_buf.at[rows], out_h.at[rows], sem)

    for i in range(ROWS // blk):
        g, r = (i * blk) // OWN, (i * blk) % OWN
        parts = [s_all[g, k, r:r + blk, :] for k in range(NC)]
        sq = parts[0] * parts[0]
        for k in range(1, NC):
            sq = sq + parts[k] * parts[k]
        rs = lax.rsqrt(jnp.sum(sq, axis=-1, keepdims=True) * (1.0 / DM) + NORM_EPS)
        for k in range(NC):
            for hf in range(CW // LANES):
                col = k * CW + hf * LANES
                gain = 1.0 + wpost_ref[col // LANES:col // LANES + 1, :]
                val = s_all[g, k, r:r + blk, hf * LANES:(hf + 1) * LANES] * rs * gain
                cs = slice(col, col + LANES)
                out_buf[i * blk:(i + 1) * blk, cs] = (x_ref[i * blk:(i + 1) * blk, cs].astype(jnp.float32) + val).astype(jnp.bfloat16)
        out_copy(i).start()
    for i in range(ROWS // blk):
        out_copy(i).wait()


def solution(mesh):
    cache_spec = P('dp', 'sp', 'tp', None)
    hbm = pl.BlockSpec(memory_space=pltpu.HBM)
    vmem = pl.BlockSpec(memory_space=pltpu.VMEM)

    def in_hbm(arr):
        return pltpu.with_memory_space_constraint(arr, pltpu.HBM)

    def in_vmem(arr):
        return pltpu.with_memory_space_constraint(arr, pltpu.VMEM)

    def to_rows(c):
        b, t, h, d = c.shape
        return c.reshape(b, t, h, 2, LANES).transpose(0, 1, 3, 2, 4).reshape(b, t * 2 * h, LANES)

    def from_rows(r):
        return r.reshape(ROWS, TB, 2, 2, LANES).transpose(0, 1, 3, 2, 4).reshape(ROWS, TB, 2, HD)

    def local_step(x_in, cur_pos, w_pre, w_q, w_k, w_v, w_o, w_post, k_cache, v_cache):
        half = HD // 2
        inv_freq = jnp.asarray((ROPE_BASE ** (-2.0 * np.arange(half) / (2 * half))).astype(np.float32))
        kr, vr = to_rows(k_cache), to_rows(v_cache)
        f32, bf16 = jnp.float32, jnp.bfloat16
        dma = pltpu.SemaphoreType.DMA
        half_shape = (HALF,) + kr.shape[1:]
        o_far, k_far, v_far, qs, ks, vs = pl.pallas_call(
            far_kernel,
            out_shape=(jax.ShapeDtypeStruct((8 * HP, LANES), f32),
                       pltpu.VMEM(half_shape, bf16), pltpu.VMEM(half_shape, bf16),
                       pltpu.VMEM((8 * RP, LANES), f32), pltpu.VMEM((8 * RP, LANES), f32), pltpu.VMEM((8 * RP, LANES), f32)),
            in_specs=[hbm] * 10,
            out_specs=(vmem,) * 6,
            scratch_shapes=[
                pltpu.SMEM((ROWS,), jnp.int32), pltpu.VMEM((1, ROWS), jnp.int32), pltpu.VMEM((1, LANES), f32),
                pltpu.VMEM((DM // LANES, LANES), f32), pltpu.VMEM((ROWS, LANES), f32), pltpu.VMEM((ROWS, LANES), f32),
                pltpu.VMEM((ROWS, DM), bf16), pltpu.VMEM((ROWS, DM), bf16),
                pltpu.VMEM((DM, 1024), bf16), pltpu.VMEM((DM, 512), bf16), pltpu.VMEM((DM, 512), bf16), pltpu.VMEM((8, ROWS, HD), f32),
                dma, dma, dma((NKC,)), dma((NCH,)),
            ],
            compiler_params=pltpu.CompilerParams(vmem_limit_bytes=40 << 20),
            cost_estimate=pl.CostEstimate(flops=2 * 10 ** 9, bytes_accessed=25 * 10 ** 6, transcendentals=0),
            name='attend_far',
        )(in_hbm(cur_pos), in_hbm(cur_pos.reshape(1, ROWS)), in_hbm(inv_freq.reshape(1, LANES)), in_hbm(x_in),
          in_hbm(w_pre.reshape(DM // LANES, LANES)), in_hbm(w_q), in_hbm(w_k), in_hbm(w_v), in_hbm(kr), in_hbm(vr))
        o_got = lax.ppermute(o_far, 'sp', [(0, 2), (1, 3), (2, 0), (3, 1)])
        o_own, k_new, v_new = pl.pallas_call(
            near_kernel,
            out_shape=(pltpu.VMEM((8 * HP, LANES), f32),
                       jax.ShapeDtypeStruct(kr.shape, bf16), jax.ShapeDtypeStruct(vr.shape, bf16)),
            in_specs=[hbm, vmem, vmem, vmem, vmem, vmem, hbm, hbm],
            out_specs=(vmem, hbm, hbm),
            scratch_shapes=[
                pltpu.SMEM((ROWS,), jnp.int32), pltpu.VMEM(half_shape, bf16), pltpu.VMEM(half_shape, bf16),
                dma, dma((NCH,)), dma,
            ],
            compiler_params=pltpu.CompilerParams(vmem_limit_bytes=28 << 20),
            cost_estimate=pl.CostEstimate(flops=10 ** 10, bytes_accessed=25 * 10 ** 6, transcendentals=0),
            name='attend_near',
        )(in_hbm(cur_pos), in_vmem(qs), in_vmem(ks), in_vmem(vs), in_vmem(k_far), in_vmem(v_far), in_hbm(kr), in_hbm(vr))
        big = pltpu.VMEM((NC, OWN, CW), f32)
        sums = pl.pallas_call(
            comm_kernel,
            out_shape=pltpu.VMEM((4, NC, OWN, CW), f32),
            in_specs=[vmem, vmem, hbm],
            out_specs=vmem,
            scratch_shapes=[
                pltpu.VMEM((NC, 1024, CW), bf16), pltpu.VMEM((4, LANES, LANES), f32), pltpu.VMEM((8 * MP, LANES), f32),
                pltpu.VMEM((8 * OWN, LANES), f32), pltpu.VMEM((8 * MP, LANES), f32), pltpu.VMEM((OWN, 1024), bf16),
                big, big, big, big, big,
                dma((NC,)), dma, dma,
                dma, dma((NC,)), dma, dma((NC,)),
                dma, dma, dma, dma((NC,)), dma, dma,
            ],
            compiler_params=pltpu.CompilerParams(vmem_limit_bytes=40 << 20, collective_id=0, has_side_effects=True),
            name='combine',
        )(in_vmem(o_own), o_got, in_hbm(w_o))
        x_out = pl.pallas_call(
            finish_kernel,
            out_shape=jax.ShapeDtypeStruct((ROWS, DM), bf16),
            in_specs=[vmem, vmem, vmem],
            out_specs=hbm,
            scratch_shapes=[pltpu.VMEM((ROWS, DM), bf16), dma],
            compiler_params=pltpu.CompilerParams(vmem_limit_bytes=16 << 20),
            name='finish',
        )(in_vmem(sums), x_in, w_post.reshape(DM // LANES, LANES))
        return x_out, from_rows(k_new), from_rows(v_new)

    return jax.shard_map(local_step, mesh=mesh,
                         in_specs=(P('dp', None), P('dp'), P(None), P(None, 'tp'), P(None, 'tp'), P(None, 'tp'), P('tp', None), P(None), cache_spec, cache_spec),
                         out_specs=(P('dp', None), cache_spec, cache_spec), check_vma=False)
```

```python
import functools

import jax
import jax.numpy as jnp
import numpy as np
from jax import lax
from jax.experimental import pallas as pl
from jax.experimental.pallas import tpu as pltpu
from jax.sharding import PartitionSpec as P

SOFT_CAP = 50.0
ROPE_BASE = 10000.0
NORM_EPS = 1e-6

ROWS = 128
DM = 3840
HD = 256
TB = 64
RP = 136
LANES = 128
BCH = 16
HALF = ROWS // 2
HP = 72
NCH = HALF // BCH
KC = 768
NKC = DM // KC
SHIFT = 20.0
CW = 256
NC = DM // CW
WG = 3
OWN = 32
MP = 40
MESH = pl.DeviceIdType.MESH


def attend_rows(row0, nchunk, pos_ref, kbuf, vbuf, qs, ks, vs, o_ref, before, after):
    tbase = lax.axis_index('sp') * TB
    lane = lax.broadcasted_iota(jnp.int32, (8, LANES), 1)
    row = lax.broadcasted_iota(jnp.int32, (8, LANES), 0)
    row_c = row // 4
    row_h = (row // 2) % 2
    match = (((lane // 2) % 2) == row_c) & ((lane % 2) == row_h)
    match_f = jnp.where(match, 1.0, 0.0).astype(jnp.float32)
    first = row_c == 0
    t_half = [jnp.where(match, lane // 4 + 32 * hf, 1 << 20) for hf in range(2)]
    quad = lax.broadcasted_iota(jnp.int32, (16, LANES), 0) // 4
    zero = jnp.zeros((8, LANES), jnp.float32)

    def chunk(i, l_acc):
        before(i)
        tls = []
        for u in range(BCH):
            lb = i * BCH + u
            b = row0 + lb
            tl = pos_ref[b] - tbase
            tls.append(tl)
            hit = jnp.logical_and(tl >= 0, tl < TB)
            tc = jnp.clip(tl, 0, TB - 1)
            tile = tc // 4
            tgt = jnp.where(hit, tc - tile * 4, -1)
            sel = quad == tgt
            off = pl.multiple_of(tile * 16, 16)
            kn = ks[pl.ds(b, 8, stride=RP), :]
            vn = vs[pl.ds(b, 8, stride=RP), :]
            kt = kbuf[lb, pl.ds(off, 16), :].astype(jnp.float32)
            vt = vbuf[lb, pl.ds(off, 16), :].astype(jnp.float32)
            kbuf[lb, pl.ds(off, 16), :] = jnp.where(sel, jnp.concatenate([kn, kn], 0), kt).astype(jnp.bfloat16)
            vbuf[lb, pl.ds(off, 16), :] = jnp.where(sel, jnp.concatenate([vn, vn], 0), vt).astype(jnp.bfloat16)
        scores = []
        for u in range(0, BCH, 2):
            lb = i * BCH + u
            q0 = qs[pl.ds(row0 + lb, 8, stride=RP), :]
            q1 = qs[pl.ds(row0 + lb + 1, 8, stride=RP), :]
            lhs = jnp.concatenate([jnp.concatenate([q0, zero], 1), jnp.concatenate([zero, q1], 1)], 0).astype(jnp.bfloat16)
            kk = jnp.concatenate([kbuf[lb], kbuf[lb + 1]], 1)
            scores.append(lax.dot_general(lhs, kk, (((1,), (1,)), ((), ())), preferred_element_type=jnp.float32))
        weights = []
        for u in range(0, BCH, 2):
            pair = []
            for w in range(2):
                part = scores[u // 2][8 * w:8 * w + 8]
                es = []
                for hf in range(2):
                    a = part[:, hf * LANES:(hf + 1) * LANES] * match_f
                    e = pltpu.roll(a, 4, 0)
                    f = jnp.where(first, pltpu.roll(e, LANES - 2, 1), pltpu.roll(e, 2, 1))
                    s = SOFT_CAP * jnp.tanh((a + f) * (HD ** -0.5 / SOFT_CAP))
                    es.append(jnp.where(t_half[hf] <= tls[u + w], jnp.exp(s - SHIFT), 0.0))
                tot = jnp.sum(es[0] + es[1], axis=1, keepdims=True)
                inv = jnp.where(tot > 0.0, 1.0 / tot, 0.0)
                pair.append(jnp.concatenate([es[0] * inv, es[1] * inv], 1))
                l_acc = jnp.where(lane == i * BCH + u + w, tot, l_acc)
            weights.append(jnp.concatenate(pair, 0).astype(jnp.bfloat16))
        for u in range(0, BCH, 2):
            lb = i * BCH + u
            vv = jnp.concatenate([vbuf[lb], vbuf[lb + 1]], 1)
            o = jnp.dot(weights[u // 2], vv, preferred_element_type=jnp.float32)
            o_ref[pl.ds(lb, 8, stride=HP), :] = o[0:8, 0:LANES]
            o_ref[pl.ds(lb + 1, 8, stride=HP), :] = o[8:16, LANES:]
        after(i)
        return l_acc

    l_acc = lax.fori_loop(0, nchunk, chunk, zero)
    o_ref[pl.ds(HALF, 8, stride=HP), :] = l_acc


def far_kernel(pos_h, posv_h, freq_h, x_h, wpre_h, wq_h, wk_h, wv_h, kc_h, vc_h,
               o_ref, kbuf, vbuf, qs, ks, vs,
               pos_ref, posv, freq, wpre_ref, cos_ref, sin_ref, x_buf, a_buf, wq_buf, wk_buf, wv_buf, acc,
               x_sem, s_sem, w_sem, ki_sem):
    row0 = (1 - lax.axis_index('sp') // 2) * HALF

    def w_start(c):
        rows = pl.ds(c * KC, KC)
        for n, (src, dst) in enumerate(((wk_h, wk_buf), (wv_h, wv_buf), (wq_h, wq_buf))):
            pltpu.make_async_copy(src.at[rows, :], dst.at[rows, :], w_sem.at[c]).start()

    def w_wait(c):
        rows = pl.ds(c * KC, KC)
        for n, (src, dst) in enumerate(((wk_h, wk_buf), (wv_h, wv_buf), (wq_h, wq_buf))):
            pltpu.make_async_copy(src.at[rows, :], dst.at[rows, :], w_sem.at[c]).wait()

    def k_in(i):
        return pltpu.make_async_copy(kc_h.at[pl.ds(row0 + i * BCH, BCH)], kbuf.at[pl.ds(i * BCH, BCH)], ki_sem.at[i])

    def v_in(i):
        return pltpu.make_async_copy(vc_h.at[pl.ds(row0 + i * BCH, BCH)], vbuf.at[pl.ds(i * BCH, BCH)], ki_sem.at[i])

    small = [pltpu.make_async_copy(a, b, s_sem) for a, b in (
        (wpre_h, wpre_ref), (posv_h, posv), (freq_h, freq), (pos_h, pos_ref))]
    for c in small:
        c.start()
    x_copy = pltpu.make_async_copy(x_h, x_buf, x_sem)
    x_copy.start()
    w_start(0)
    for c in small:
        c.wait()
    w_start(1)
    pos_col = jnp.broadcast_to(posv[...].astype(jnp.float32), (ROWS, LANES)).T
    ang = pos_col * freq[...]
    cos_ref[...] = jnp.cos(ang)
    sin_ref[...] = jnp.sin(ang)
    x_copy.wait()
    w_start(2)

    gain = 1.0 + jnp.concatenate([wpre_ref[k:k + 1, :] for k in range(DM // LANES)], 1)

    def norm_rows(i, carry):
        r = pl.multiple_of(i * 16, 16)
        xb = x_buf[pl.ds(r, 16), :].astype(jnp.float32)
        ms = jnp.mean(xb * xb, axis=-1, keepdims=True)
        a_buf[pl.ds(r, 16), :] = (xb * lax.rsqrt(ms + NORM_EPS) * gain).astype(jnp.bfloat16)
        return carry

    lax.fori_loop(0, ROWS // 16, norm_rows, 0)

    for c in range(NKC):
        w_wait(c)
        if c + 3 < NKC:
            w_start(c + 3)
        else:
            for n in range(2 * (c + 3 - NKC), min(NCH, 2 * (c + 4 - NKC))):
                k_in(n).start()
                v_in(n).start()
        rows = slice(c * KC, (c + 1) * KC)
        a_c = a_buf[:, rows]
        for i in range(8):
            if i < 2:
                w_c = wk_buf[rows, i * HD:(i + 1) * HD]
            elif i < 4:
                w_c = wv_buf[rows, (i - 2) * HD:(i - 1) * HD]
            else:
                w_c = wq_buf[rows, (i - 4) * HD:(i - 3) * HD]
            y = jnp.dot(a_c, w_c, preferred_element_type=jnp.float32)
            if c == 0:
                acc[i] = y
                continue
            y = acc[i] + y
            if c < NKC - 1:
                acc[i] = y
                continue
            lo, hi = y[:, :LANES], y[:, LANES:]
            if 2 <= i < 4:
                h = i - 2
                for rep in range(2):
                    vs[pl.ds((rep * 4 + h) * RP, ROWS), :] = lo
                    vs[pl.ds((rep * 4 + 2 + h) * RP, ROWS), :] = hi
            else:
                cos_t, sin_t = cos_ref[...], sin_ref[...]
                rlo = lo * cos_t - hi * sin_t
                rhi = hi * cos_t + lo * sin_t
                if i < 2:
                    for rep in range(2):
                        ks[pl.ds((rep * 4 + i) * RP, ROWS), :] = rlo
                        ks[pl.ds((rep * 4 + 2 + i) * RP, ROWS), :] = rhi
                else:
                    qs[pl.ds((i - 4) * RP, ROWS), :] = rlo
                    qs[pl.ds((4 + i - 4) * RP, ROWS), :] = rhi

    def before(i):
        k_in(i).wait()
        v_in(i).wait()

    attend_rows(row0, NCH, pos_ref, kbuf, vbuf, qs, ks, vs, o_ref, before, lambda i: None)


def near_kernel(pos_h, qs, ks, vs, kfar, vfar, kc_h, vc_h,
                o_ref, ko_h, vo_h,
                pos_ref, kbuf, vbuf, p_sem, ki_sem, w_sem):
    yy = lax.axis_index('sp') // 2
    row0 = yy * HALF
    far0 = (1 - yy) * HALF

    def k_in(i):
        return pltpu.make_async_copy(kc_h.at[pl.ds(row0 + i * BCH, BCH)], kbuf.at[pl.ds(i * BCH, BCH)], ki_sem.at[i])

    def v_in(i):
        return pltpu.make_async_copy(vc_h.at[pl.ds(row0 + i * BCH, BCH)], vbuf.at[pl.ds(i * BCH, BCH)], ki_sem.at[i])

    def k_out(i):
        return pltpu.make_async_copy(kbuf.at[pl.ds(i * BCH, BCH)], ko_h.at[pl.ds(row0 + i * BCH, BCH)], w_sem)

    def v_out(i):
        return pltpu.make_async_copy(vbuf.at[pl.ds(i * BCH, BCH)], vo_h.at[pl.ds(row0 + i * BCH, BCH)], w_sem)

    def kf_out(i):
        return pltpu.make_async_copy(kfar.at[pl.ds(i * BCH, BCH)], ko_h.at[pl.ds(far0 + i * BCH, BCH)], w_sem)

    def vf_out(i):
        return pltpu.make_async_copy(vfar.at[pl.ds(i * BCH, BCH)], vo_h.at[pl.ds(far0 + i * BCH, BCH)], w_sem)

    p_copy = pltpu.make_async_copy(pos_h, pos_ref, p_sem)
    p_copy.start()
    for i in range(NCH):
        k_in(i).start()
        v_in(i).start()
    p_copy.wait()

    def before(i):
        k_in(i).wait()
        v_in(i).wait()
        kf_out(i).start()
        vf_out(i).start()

    def after(i):
        k_out(i).start()
        v_out(i).start()

    attend_rows(row0, NCH, pos_ref, kbuf, vbuf, qs, ks, vs, o_ref, before, after)
    for i in range(NCH):
        kf_out(i).wait()
        vf_out(i).wait()
        k_out(i).wait()
        v_out(i).wait()


def comm_kernel(o_own, o_got, wo_h, s_all,
                wo_buf, fac, m1, m2, r1, lhs, p_buf, rr, rl, sr, sl,
                w_sem, r1_send, r1_recv,
                right_send, right_recv, left_send, left_recv,
                part_send, part_recv, y_send, y_recv, f_send, f_recv):
    z = lax.axis_index('tp')
    sp = lax.axis_index('sp')
    core = sp % 2
    partner = sp + 1 - 2 * core
    ypeer = (sp + 2) % 4

    def wo_copy(k):
        return pltpu.make_async_copy(wo_h.at[:, pl.ds(pl.multiple_of(k * WG * CW, CW), WG * CW)], wo_buf.at[k], w_sem.at[k])

    for k in range(NC // WG):
        wo_copy(k).start()

    @pl.when(z == 0)
    def _():
        rr[...] = jnp.zeros_like(rr)

    @pl.when(z == 3)
    def _():
        rl[...] = jnp.zeros_like(rl)

    bar = pltpu.get_barrier_semaphore()
    pl.semaphore_signal(bar, inc=1, device_id={'sp': partner}, device_id_type=MESH)
    pl.semaphore_signal(bar, inc=1, device_id={'sp': ypeer}, device_id_type=MESH)

    @pl.when(z > 0)
    def _():
        pl.semaphore_signal(bar, inc=1, device_id={'tp': z - 1}, device_id_type=MESH)

    @pl.when(z < 3)
    def _():
        pl.semaphore_signal(bar, inc=1, device_id={'tp': z + 1}, device_id_type=MESH)

    pl.semaphore_wait(bar, 3 + (z * (3 - z)) // 2)

    def shares(l_a, l_b, slot):
        tot = l_a + l_b
        inv = jnp.where(tot > 0.0, 1.0 / tot, 0.0)
        for w, l in enumerate((l_a, l_b)):
            fac[slot + w] = jnp.concatenate([l * inv, jnp.zeros((LANES - 8, LANES), jnp.float32)], 0).T
        return tot

    mine = pl.multiple_of(core * OWN, OWN)
    theirs = pl.multiple_of((1 - core) * OWN, OWN)
    tot = shares(o_own[pl.ds(HALF, 8, stride=HP), :], o_got[pl.ds(HALF, 8, stride=HP), :], 0)

    def merge_half(r0, dst, stride):
        fa, fb = fac[0, pl.ds(r0, OWN), :], fac[1, pl.ds(r0, OWN), :]
        for j in range(8):
            rows = pl.ds(pl.multiple_of(j * HP + r0, 8), OWN)
            dst[pl.ds(j * stride, OWN), :] = o_own[rows, :] * fa[:, j:j + 1] + o_got[rows, :] * fb[:, j:j + 1]

    merge_half(theirs, m1, MP)
    m1[pl.ds(OWN, 8, stride=MP), :] = tot
    pair = pltpu.make_async_remote_copy(
        src_ref=m1, dst_ref=r1, send_sem=r1_send, recv_sem=r1_recv, device_id={'sp': partner}, device_id_type=MESH)
    pair.start()
    merge_half(mine, m2, OWN)
    pair.wait()
    shares(tot, r1[pl.ds(OWN, 8, stride=MP), :], 2)
    fa, fb = fac[2, pl.ds(mine, OWN), :], fac[3, pl.ds(mine, OWN), :]
    for j in range(8):
        c, hq = j // 4, j % 4
        val = m2[j * OWN:(j + 1) * OWN, :] * fa[:, j:j + 1] + r1[j * MP:j * MP + OWN, :] * fb[:, j:j + 1]
        lhs[:, (hq * 2 + c) * LANES:(hq * 2 + c + 1) * LANES] = val.astype(jnp.bfloat16)

    def right_copy(k):
        return pltpu.make_async_remote_copy(
            src_ref=sr.at[k], dst_ref=rr.at[k], send_sem=right_send, recv_sem=right_recv.at[k],
            device_id={'tp': z + 1}, device_id_type=MESH)

    def left_copy(k):
        return pltpu.make_async_remote_copy(
            src_ref=sl.at[k], dst_ref=rl.at[k], send_sem=left_send, recv_sem=left_recv.at[k],
            device_id={'tp': z - 1}, device_id_type=MESH)

    def part_copy(k):
        return pltpu.make_async_remote_copy(
            src_ref=s_all.at[sp, k], dst_ref=s_all.at[sp, k], send_sem=part_send, recv_sem=part_recv,
            device_id={'sp': partner}, device_id_type=MESH)

    def y_copy(k):
        return pltpu.make_async_remote_copy(
            src_ref=s_all.at[sp, k], dst_ref=s_all.at[sp, k], send_sem=y_send, recv_sem=y_recv.at[k],
            device_id={'sp': ypeer}, device_id_type=MESH)

    def fwd_copy(k):
        return pltpu.make_async_remote_copy(
            src_ref=s_all.at[ypeer, k], dst_ref=s_all.at[ypeer, k], send_sem=f_send, recv_sem=f_recv,
            device_id={'sp': partner}, device_id_type=MESH)

    def whole(ref, sem):
        return pltpu.make_async_copy(ref, ref, sem)

    hop = 5
    lag_r = hop * z
    lag_l = hop * (3 - z)
    lag_s = hop * (3 - (z * (3 - z)) // 2)

    def tick(i, carry):
        @pl.when(i < NC)
        def _():
            group, place = i // WG, i % WG

            @pl.when(place == 0)
            def _():
                wo_copy(group).wait()

            w_c = wo_buf[group, :, pl.ds(pl.multiple_of(place * CW, CW), CW)]
            p_buf[i] = jnp.dot(lhs[...], w_c, preferred_element_type=jnp.float32)

        kr = i - lag_r

        @pl.when(jnp.logical_and(kr >= 0, kr < NC))
        def _():
            @pl.when(z > 0)
            def _():
                right_copy(kr).wait_recv()

            @pl.when(z < 3)
            def _():
                sr[kr] = p_buf[kr] + rr[kr]
                right_copy(kr).start()

        kl = i - lag_l

        @pl.when(jnp.logical_and(kl >= 0, kl < NC))
        def _():
            @pl.when(z < 3)
            def _():
                left_copy(kl).wait_recv()

            @pl.when(z > 0)
            def _():
                sl[kl] = p_buf[kl] + rl[kl]
                left_copy(kl).start()

        k_s = i - lag_s

        @pl.when(jnp.logical_and(k_s >= 0, k_s < NC))
        def _():
            s_all[sp, k_s] = p_buf[k_s] + rr[k_s] + rl[k_s]
            y_copy(k_s).start()
            part_copy(k_s).start()

        k_y = i - lag_s - hop

        @pl.when(jnp.logical_and(k_y >= 0, k_y < NC))
        def _():
            y_copy(k_y).wait_recv()
            fwd_copy(k_y).start()

        return carry

    lax.fori_loop(0, NC + 4 * hop, tick, 0)

    @pl.when(z < 3)
    def _():
        whole(sr, right_send).wait()

    @pl.when(z > 0)
    def _():
        whole(sl, left_send).wait()

    whole(s_all.at[sp], y_send).wait()
    whole(s_all.at[sp], part_send).wait()
    whole(s_all.at[ypeer], f_send).wait()
    whole(s_all.at[partner], part_recv).wait()
    whole(s_all.at[3 - sp], f_recv).wait()


def finish_kernel(s_all, x_ref, wpost_ref, out_h, out_buf, sem):
    blk = 16

    def out_copy(i):
        rows = pl.ds(i * blk, blk)
        return pltpu.make_async_copy(out_buf.at[rows], out_h.at[rows], sem)

    for i in range(ROWS // blk):
        g, r = (i * blk) // OWN, (i * blk) % OWN
        parts = [s_all[g, k, r:r + blk, :] for k in range(NC)]
        sq = parts[0] * parts[0]
        for k in range(1, NC):
            sq = sq + parts[k] * parts[k]
        rs = lax.rsqrt(jnp.sum(sq, axis=-1, keepdims=True) * (1.0 / DM) + NORM_EPS)
        for k in range(NC):
            for hf in range(CW // LANES):
                col = k * CW + hf * LANES
                gain = 1.0 + wpost_ref[col // LANES:col // LANES + 1, :]
                val = s_all[g, k, r:r + blk, hf * LANES:(hf + 1) * LANES] * rs * gain
                cs = slice(col, col + LANES)
                out_buf[i * blk:(i + 1) * blk, cs] = (x_ref[i * blk:(i + 1) * blk, cs].astype(jnp.float32) + val).astype(jnp.bfloat16)
        out_copy(i).start()
    for i in range(ROWS // blk):
        out_copy(i).wait()


def solution(mesh):
    cache_spec = P('dp', 'sp', 'tp', None)
    hbm = pl.BlockSpec(memory_space=pltpu.HBM)
    vmem = pl.BlockSpec(memory_space=pltpu.VMEM)

    def in_hbm(arr):
        return pltpu.with_memory_space_constraint(arr, pltpu.HBM)

    def in_vmem(arr):
        return pltpu.with_memory_space_constraint(arr, pltpu.VMEM)

    def to_rows(c):
        b, t, h, d = c.shape
        return c.reshape(b, t, h, 2, LANES).transpose(0, 1, 3, 2, 4).reshape(b, t * 2 * h, LANES)

    def from_rows(r):
        return r.reshape(ROWS, TB, 2, 2, LANES).transpose(0, 1, 3, 2, 4).reshape(ROWS, TB, 2, HD)

    def local_step(x_in, cur_pos, w_pre, w_q, w_k, w_v, w_o, w_post, k_cache, v_cache):
        half = HD // 2
        inv_freq = jnp.asarray((ROPE_BASE ** (-2.0 * np.arange(half) / (2 * half))).astype(np.float32))
        kr, vr = to_rows(k_cache), to_rows(v_cache)
        f32, bf16 = jnp.float32, jnp.bfloat16
        dma = pltpu.SemaphoreType.DMA
        half_shape = (HALF,) + kr.shape[1:]
        o_far, k_far, v_far, qs, ks, vs = pl.pallas_call(
            far_kernel,
            out_shape=(jax.ShapeDtypeStruct((8 * HP, LANES), f32),
                       pltpu.VMEM(half_shape, bf16), pltpu.VMEM(half_shape, bf16),
                       pltpu.VMEM((8 * RP, LANES), f32), pltpu.VMEM((8 * RP, LANES), f32), pltpu.VMEM((8 * RP, LANES), f32)),
            in_specs=[hbm] * 10,
            out_specs=(vmem,) * 6,
            scratch_shapes=[
                pltpu.SMEM((ROWS,), jnp.int32), pltpu.VMEM((1, ROWS), jnp.int32), pltpu.VMEM((1, LANES), f32),
                pltpu.VMEM((DM // LANES, LANES), f32), pltpu.VMEM((ROWS, LANES), f32), pltpu.VMEM((ROWS, LANES), f32),
                pltpu.VMEM((ROWS, DM), bf16), pltpu.VMEM((ROWS, DM), bf16),
                pltpu.VMEM((DM, 1024), bf16), pltpu.VMEM((DM, 512), bf16), pltpu.VMEM((DM, 512), bf16), pltpu.VMEM((8, ROWS, HD), f32),
                dma, dma, dma((NKC,)), dma((NCH,)),
            ],
            compiler_params=pltpu.CompilerParams(vmem_limit_bytes=40 << 20),
            cost_estimate=pl.CostEstimate(flops=2 * 10 ** 9, bytes_accessed=25 * 10 ** 6, transcendentals=0),
            name='attend_far',
        )(in_hbm(cur_pos), in_hbm(cur_pos.reshape(1, ROWS)), in_hbm(inv_freq.reshape(1, LANES)), in_hbm(x_in),
          in_hbm(w_pre.reshape(DM // LANES, LANES)), in_hbm(w_q), in_hbm(w_k), in_hbm(w_v), in_hbm(kr), in_hbm(vr))
        o_got = lax.ppermute(o_far, 'sp', [(0, 2), (1, 3), (2, 0), (3, 1)])
        o_own, k_new, v_new = pl.pallas_call(
            near_kernel,
            out_shape=(pltpu.VMEM((8 * HP, LANES), f32),
                       jax.ShapeDtypeStruct(kr.shape, bf16), jax.ShapeDtypeStruct(vr.shape, bf16)),
            in_specs=[hbm, vmem, vmem, vmem, vmem, vmem, hbm, hbm],
            out_specs=(vmem, hbm, hbm),
            scratch_shapes=[
                pltpu.SMEM((ROWS,), jnp.int32), pltpu.VMEM(half_shape, bf16), pltpu.VMEM(half_shape, bf16),
                dma, dma((NCH,)), dma,
            ],
            compiler_params=pltpu.CompilerParams(vmem_limit_bytes=28 << 20),
            cost_estimate=pl.CostEstimate(flops=10 ** 10, bytes_accessed=25 * 10 ** 6, transcendentals=0),
            name='attend_near',
        )(in_hbm(cur_pos), in_vmem(qs), in_vmem(ks), in_vmem(vs), in_vmem(k_far), in_vmem(v_far), in_hbm(kr), in_hbm(vr))
        big = pltpu.VMEM((NC, OWN, CW), f32)
        sums = pl.pallas_call(
            comm_kernel,
            out_shape=pltpu.VMEM((4, NC, OWN, CW), f32),
            in_specs=[vmem, vmem, hbm],
            out_specs=vmem,
            scratch_shapes=[
                pltpu.VMEM((NC // WG, 1024, WG * CW), bf16), pltpu.VMEM((4, LANES, LANES), f32), pltpu.VMEM((8 * MP, LANES), f32),
                pltpu.VMEM((8 * OWN, LANES), f32), pltpu.VMEM((8 * MP, LANES), f32), pltpu.VMEM((OWN, 1024), bf16),
                big, big, big, big, big,
                dma((NC // WG,)), dma, dma,
                dma, dma((NC,)), dma, dma((NC,)),
                dma, dma, dma, dma((NC,)), dma, dma,
            ],
            compiler_params=pltpu.CompilerParams(vmem_limit_bytes=40 << 20, collective_id=0, has_side_effects=True),
            name='combine',
        )(in_vmem(o_own), o_got, in_hbm(w_o))
        x_out = pl.pallas_call(
            finish_kernel,
            out_shape=jax.ShapeDtypeStruct((ROWS, DM), bf16),
            in_specs=[vmem, vmem, vmem],
            out_specs=hbm,
            scratch_shapes=[pltpu.VMEM((ROWS, DM), bf16), dma],
            compiler_params=pltpu.CompilerParams(vmem_limit_bytes=16 << 20),
            name='finish',
        )(in_vmem(sums), x_in, w_post.reshape(DM // LANES, LANES))
        return x_out, from_rows(k_new), from_rows(v_new)

    return jax.shard_map(local_step, mesh=mesh,
                         in_specs=(P('dp', None), P('dp'), P(None), P(None, 'tp'), P(None, 'tp'), P(None, 'tp'), P('tp', None), P(None), cache_spec, cache_spec),
                         out_specs=(P('dp', None), cache_spec, cache_spec), check_vma=False)
```

```python
import functools

import jax
import jax.numpy as jnp
import numpy as np
from jax import lax
from jax.experimental import pallas as pl
from jax.experimental.pallas import tpu as pltpu
from jax.sharding import PartitionSpec as P

SOFT_CAP = 50.0
ROPE_BASE = 10000.0
NORM_EPS = 1e-6

ROWS = 128
DM = 3840
HD = 256
TB = 64
RP = 136
LANES = 128
BCH = 16
HALF = ROWS // 2
HROWS = 8 * HALF + 8
NCH = HALF // BCH
KC = 768
NKC = DM // KC
SHIFT = 20.0
CW = 256
NC = DM // CW
WG = 3
OWN = 32
MROWS = 8 * OWN + 8
MESH = pl.DeviceIdType.MESH


def attend_rows(row0, nchunk, pos_ref, kbuf, vbuf, qs, ks, vs, o_ref, before, after):
    tbase = lax.axis_index('sp') * TB
    lane = lax.broadcasted_iota(jnp.int32, (8, LANES), 1)
    row = lax.broadcasted_iota(jnp.int32, (8, LANES), 0)
    row_c = row // 4
    row_h = (row // 2) % 2
    match = (((lane // 2) % 2) == row_c) & ((lane % 2) == row_h)
    match_f = jnp.where(match, 1.0, 0.0).astype(jnp.float32)
    first = row_c == 0
    t_half = [jnp.where(match, lane // 4 + 32 * hf, 1 << 20) for hf in range(2)]
    quad = lax.broadcasted_iota(jnp.int32, (16, LANES), 0) // 4
    zero = jnp.zeros((8, LANES), jnp.float32)

    def chunk(i, l_acc):
        before(i)
        tls = []
        for u in range(BCH):
            lb = i * BCH + u
            b = row0 + lb
            tl = pos_ref[b] - tbase
            tls.append(tl)
            hit = jnp.logical_and(tl >= 0, tl < TB)
            tc = jnp.clip(tl, 0, TB - 1)
            tile = tc // 4
            tgt = jnp.where(hit, tc - tile * 4, -1)
            sel = quad == tgt
            off = pl.multiple_of(tile * 16, 16)
            kn = ks[pl.ds(b, 8, stride=RP), :]
            vn = vs[pl.ds(b, 8, stride=RP), :]
            kt = kbuf[lb, pl.ds(off, 16), :].astype(jnp.float32)
            vt = vbuf[lb, pl.ds(off, 16), :].astype(jnp.float32)
            kbuf[lb, pl.ds(off, 16), :] = jnp.where(sel, jnp.concatenate([kn, kn], 0), kt).astype(jnp.bfloat16)
            vbuf[lb, pl.ds(off, 16), :] = jnp.where(sel, jnp.concatenate([vn, vn], 0), vt).astype(jnp.bfloat16)
        scores = []
        for u in range(0, BCH, 2):
            lb = i * BCH + u
            q0 = qs[pl.ds(row0 + lb, 8, stride=RP), :]
            q1 = qs[pl.ds(row0 + lb + 1, 8, stride=RP), :]
            lhs = jnp.concatenate([jnp.concatenate([q0, zero], 1), jnp.concatenate([zero, q1], 1)], 0).astype(jnp.bfloat16)
            kk = jnp.concatenate([kbuf[lb], kbuf[lb + 1]], 1)
            scores.append(lax.dot_general(lhs, kk, (((1,), (1,)), ((), ())), preferred_element_type=jnp.float32))
        weights = []
        for u in range(0, BCH, 2):
            pair = []
            for w in range(2):
                part = scores[u // 2][8 * w:8 * w + 8]
                es = []
                for hf in range(2):
                    a = part[:, hf * LANES:(hf + 1) * LANES] * match_f
                    e = pltpu.roll(a, 4, 0)
                    f = jnp.where(first, pltpu.roll(e, LANES - 2, 1), pltpu.roll(e, 2, 1))
                    s = SOFT_CAP * jnp.tanh((a + f) * (HD ** -0.5 / SOFT_CAP))
                    es.append(jnp.where(t_half[hf] <= tls[u + w], jnp.exp(s - SHIFT), 0.0))
                tot = jnp.sum(es[0] + es[1], axis=1, keepdims=True)
                inv = jnp.where(tot > 0.0, 1.0 / tot, 0.0)
                pair.append(jnp.concatenate([es[0] * inv, es[1] * inv], 1))
                l_acc = jnp.where(lane == i * BCH + u + w, tot, l_acc)
            weights.append(jnp.concatenate(pair, 0).astype(jnp.bfloat16))
        for u in range(0, BCH, 2):
            lb = i * BCH + u
            vv = jnp.concatenate([vbuf[lb], vbuf[lb + 1]], 1)
            o = jnp.dot(weights[u // 2], vv, preferred_element_type=jnp.float32)
            o_ref[pl.ds(lb, 8, stride=HALF), :] = o[0:8, 0:LANES]
            o_ref[pl.ds(lb + 1, 8, stride=HALF), :] = o[8:16, LANES:]
        after(i)
        return l_acc

    l_acc = lax.fori_loop(0, nchunk, chunk, zero)
    o_ref[pl.ds(8 * HALF, 8), :] = l_acc


def far_kernel(pos_h, posv_h, freq_h, x_h, wpre_h, wq_h, wk_h, wv_h, kc_h, vc_h,
               o_ref, kbuf, vbuf, qs, ks, vs,
               pos_ref, posv, freq, wpre_ref, cos_ref, sin_ref, x_buf, a_buf, wq_buf, wk_buf, wv_buf, acc,
               x_sem, s_sem, w_sem, ki_sem):
    row0 = (1 - lax.axis_index('sp') // 2) * HALF

    def w_start(c):
        rows = pl.ds(c * KC, KC)
        for n, (src, dst) in enumerate(((wk_h, wk_buf), (wv_h, wv_buf), (wq_h, wq_buf))):
            pltpu.make_async_copy(src.at[rows, :], dst.at[rows, :], w_sem.at[c]).start()

    def w_wait(c):
        rows = pl.ds(c * KC, KC)
        for n, (src, dst) in enumerate(((wk_h, wk_buf), (wv_h, wv_buf), (wq_h, wq_buf))):
            pltpu.make_async_copy(src.at[rows, :], dst.at[rows, :], w_sem.at[c]).wait()

    def k_in(i):
        return pltpu.make_async_copy(kc_h.at[pl.ds(row0 + i * BCH, BCH)], kbuf.at[pl.ds(i * BCH, BCH)], ki_sem.at[i])

    def v_in(i):
        return pltpu.make_async_copy(vc_h.at[pl.ds(row0 + i * BCH, BCH)], vbuf.at[pl.ds(i * BCH, BCH)], ki_sem.at[i])

    small = [pltpu.make_async_copy(a, b, s_sem) for a, b in (
        (wpre_h, wpre_ref), (posv_h, posv), (freq_h, freq), (pos_h, pos_ref))]
    for c in small:
        c.start()
    x_copy = pltpu.make_async_copy(x_h, x_buf, x_sem)
    x_copy.start()
    w_start(0)
    for c in small:
        c.wait()
    w_start(1)
    pos_col = jnp.broadcast_to(posv[...].astype(jnp.float32), (ROWS, LANES)).T
    ang = pos_col * freq[...]
    cos_ref[...] = jnp.cos(ang)
    sin_ref[...] = jnp.sin(ang)
    x_copy.wait()
    w_start(2)

    gain = 1.0 + jnp.concatenate([wpre_ref[k:k + 1, :] for k in range(DM // LANES)], 1)

    def norm_rows(i, carry):
        r = pl.multiple_of(i * 16, 16)
        xb = x_buf[pl.ds(r, 16), :].astype(jnp.float32)
        ms = jnp.mean(xb * xb, axis=-1, keepdims=True)
        a_buf[pl.ds(r, 16), :] = (xb * lax.rsqrt(ms + NORM_EPS) * gain).astype(jnp.bfloat16)
        return carry

    lax.fori_loop(0, ROWS // 16, norm_rows, 0)

    for c in range(NKC):
        w_wait(c)
        if c + 3 < NKC:
            w_start(c + 3)
        if c >= NKC - 2:
            for n in range(2 * (c + 2 - NKC), 2 * (c + 3 - NKC)):
                k_in(n).start()
                v_in(n).start()
        rows = slice(c * KC, (c + 1) * KC)
        a_c = a_buf[:, rows]
        for i in range(8):
            if i < 2:
                w_c = wk_buf[rows, i * HD:(i + 1) * HD]
            elif i < 4:
                w_c = wv_buf[rows, (i - 2) * HD:(i - 1) * HD]
            else:
                w_c = wq_buf[rows, (i - 4) * HD:(i - 3) * HD]
            y = jnp.dot(a_c, w_c, preferred_element_type=jnp.float32)
            if c == 0:
                acc[i] = y
                continue
            y = acc[i] + y
            if c < NKC - 1:
                acc[i] = y
                continue
            lo, hi = y[:, :LANES], y[:, LANES:]
            if 2 <= i < 4:
                h = i - 2
                for rep in range(2):
                    vs[pl.ds((rep * 4 + h) * RP, ROWS), :] = lo
                    vs[pl.ds((rep * 4 + 2 + h) * RP, ROWS), :] = hi
            else:
                cos_t, sin_t = cos_ref[...], sin_ref[...]
                rlo = lo * cos_t - hi * sin_t
                rhi = hi * cos_t + lo * sin_t
                if i < 2:
                    for rep in range(2):
                        ks[pl.ds((rep * 4 + i) * RP, ROWS), :] = rlo
                        ks[pl.ds((rep * 4 + 2 + i) * RP, ROWS), :] = rhi
                else:
                    qs[pl.ds((i - 4) * RP, ROWS), :] = rlo
                    qs[pl.ds((4 + i - 4) * RP, ROWS), :] = rhi

    def before(i):
        k_in(i).wait()
        v_in(i).wait()

    attend_rows(row0, NCH, pos_ref, kbuf, vbuf, qs, ks, vs, o_ref, before, lambda i: None)


def near_kernel(pos_h, qs, ks, vs, kfar, vfar, kc_h, vc_h,
                o_ref, ko_h, vo_h,
                pos_ref, kbuf, vbuf, p_sem, ki_sem, w_sem):
    yy = lax.axis_index('sp') // 2
    row0 = yy * HALF
    far0 = (1 - yy) * HALF

    def k_in(i):
        return pltpu.make_async_copy(kc_h.at[pl.ds(row0 + i * BCH, BCH)], kbuf.at[pl.ds(i * BCH, BCH)], ki_sem.at[i])

    def v_in(i):
        return pltpu.make_async_copy(vc_h.at[pl.ds(row0 + i * BCH, BCH)], vbuf.at[pl.ds(i * BCH, BCH)], ki_sem.at[i])

    def k_out(i):
        return pltpu.make_async_copy(kbuf.at[pl.ds(i * BCH, BCH)], ko_h.at[pl.ds(row0 + i * BCH, BCH)], w_sem)

    def v_out(i):
        return pltpu.make_async_copy(vbuf.at[pl.ds(i * BCH, BCH)], vo_h.at[pl.ds(row0 + i * BCH, BCH)], w_sem)

    def kf_out(i):
        return pltpu.make_async_copy(kfar.at[pl.ds(i * BCH, BCH)], ko_h.at[pl.ds(far0 + i * BCH, BCH)], w_sem)

    def vf_out(i):
        return pltpu.make_async_copy(vfar.at[pl.ds(i * BCH, BCH)], vo_h.at[pl.ds(far0 + i * BCH, BCH)], w_sem)

    p_copy = pltpu.make_async_copy(pos_h, pos_ref, p_sem)
    p_copy.start()
    for i in range(NCH):
        k_in(i).start()
        v_in(i).start()
    p_copy.wait()

    def before(i):
        k_in(i).wait()
        v_in(i).wait()
        kf_out(i).start()
        vf_out(i).start()

    def after(i):
        k_out(i).start()
        v_out(i).start()

    attend_rows(row0, NCH, pos_ref, kbuf, vbuf, qs, ks, vs, o_ref, before, after)
    for i in range(NCH):
        kf_out(i).wait()
        vf_out(i).wait()
        k_out(i).wait()
        v_out(i).wait()


def comm_kernel(o_own, o_got, wo_h, s_all,
                wo_buf, fac, m1, m2, r1, lhs, p_buf, rr, rl, sr, sl,
                w_sem, r1_send, r1_recv,
                right_send, right_recv, left_send, left_recv,
                part_send, part_recv, y_send, y_recv, f_send, f_recv):
    z = lax.axis_index('tp')
    sp = lax.axis_index('sp')
    core = sp % 2
    partner = sp + 1 - 2 * core
    ypeer = (sp + 2) % 4

    def wo_copy(k):
        return pltpu.make_async_copy(wo_h.at[:, pl.ds(pl.multiple_of(k * WG * CW, CW), WG * CW)], wo_buf.at[k], w_sem.at[k])

    for k in range(NC // WG):
        wo_copy(k).start()

    @pl.when(z == 0)
    def _():
        rr[...] = jnp.zeros_like(rr)

    @pl.when(z == 3)
    def _():
        rl[...] = jnp.zeros_like(rl)

    bar = pltpu.get_barrier_semaphore()
    pl.semaphore_signal(bar, inc=1, device_id={'sp': partner}, device_id_type=MESH)
    pl.semaphore_signal(bar, inc=1, device_id={'sp': ypeer}, device_id_type=MESH)

    @pl.when(z > 0)
    def _():
        pl.semaphore_signal(bar, inc=1, device_id={'tp': z - 1}, device_id_type=MESH)

    @pl.when(z < 3)
    def _():
        pl.semaphore_signal(bar, inc=1, device_id={'tp': z + 1}, device_id_type=MESH)

    pl.semaphore_wait(bar, 3 + (z * (3 - z)) // 2)

    def shares(l_a, l_b, slot):
        tot = l_a + l_b
        inv = jnp.where(tot > 0.0, 1.0 / tot, 0.0)
        for w, l in enumerate((l_a, l_b)):
            fac[slot + w] = jnp.concatenate([l * inv, jnp.zeros((LANES - 8, LANES), jnp.float32)], 0).T
        return tot

    mine = pl.multiple_of(core * OWN, OWN)
    theirs = pl.multiple_of((1 - core) * OWN, OWN)
    tot = shares(o_own[pl.ds(8 * HALF, 8), :], o_got[pl.ds(8 * HALF, 8), :], 0)

    def merge_half(r0, dst):
        fa, fb = fac[0, pl.ds(r0, OWN), :], fac[1, pl.ds(r0, OWN), :]
        for j in range(8):
            rows = pl.ds(pl.multiple_of(j * HALF + r0, 8), OWN)
            dst[pl.ds(j * OWN, OWN), :] = o_own[rows, :] * fa[:, j:j + 1] + o_got[rows, :] * fb[:, j:j + 1]

    merge_half(theirs, m1)
    m1[pl.ds(8 * OWN, 8), :] = tot
    pair = pltpu.make_async_remote_copy(
        src_ref=m1, dst_ref=r1, send_sem=r1_send, recv_sem=r1_recv, device_id={'sp': partner}, device_id_type=MESH)
    pair.start()
    merge_half(mine, m2)
    pair.wait()
    shares(tot, r1[pl.ds(8 * OWN, 8), :], 2)
    fa, fb = fac[2, pl.ds(mine, OWN), :], fac[3, pl.ds(mine, OWN), :]
    for j in range(8):
        c, hq = j // 4, j % 4
        val = m2[j * OWN:(j + 1) * OWN, :] * fa[:, j:j + 1] + r1[j * OWN:(j + 1) * OWN, :] * fb[:, j:j + 1]
        lhs[:, (hq * 2 + c) * LANES:(hq * 2 + c + 1) * LANES] = val.astype(jnp.bfloat16)

    def right_copy(k):
        return pltpu.make_async_remote_copy(
            src_ref=sr.at[k], dst_ref=rr.at[k], send_sem=right_send, recv_sem=right_recv.at[k],
            device_id={'tp': z + 1}, device_id_type=MESH)

    def left_copy(k):
        return pltpu.make_async_remote_copy(
            src_ref=sl.at[k], dst_ref=rl.at[k], send_sem=left_send, recv_sem=left_recv.at[k],
            device_id={'tp': z - 1}, device_id_type=MESH)

    def part_copy(k):
        return pltpu.make_async_remote_copy(
            src_ref=s_all.at[sp, k], dst_ref=s_all.at[sp, k], send_sem=part_send, recv_sem=part_recv,
            device_id={'sp': partner}, device_id_type=MESH)

    def y_copy(k):
        return pltpu.make_async_remote_copy(
            src_ref=s_all.at[sp, k], dst_ref=s_all.at[sp, k], send_sem=y_send, recv_sem=y_recv.at[k],
            device_id={'sp': ypeer}, device_id_type=MESH)

    def fwd_copy(k):
        return pltpu.make_async_remote_copy(
            src_ref=s_all.at[ypeer, k], dst_ref=s_all.at[ypeer, k], send_sem=f_send, recv_sem=f_recv,
            device_id={'sp': partner}, device_id_type=MESH)

    def whole(ref, sem):
        return pltpu.make_async_copy(ref, ref, sem)

    hop = 5
    lag_r = hop * z
    lag_l = hop * (3 - z)
    lag_s = hop * (3 - (z * (3 - z)) // 2)

    def tick(i, carry):
        @pl.when(i < NC)
        def _():
            group, place = i // WG, i % WG

            @pl.when(place == 0)
            def _():
                wo_copy(group).wait()

            w_c = wo_buf[group, :, pl.ds(pl.multiple_of(place * CW, CW), CW)]
            p_buf[i] = jnp.dot(lhs[...], w_c, preferred_element_type=jnp.float32)

        kr = i - lag_r

        @pl.when(jnp.logical_and(kr >= 0, kr < NC))
        def _():
            @pl.when(z > 0)
            def _():
                right_copy(kr).wait_recv()

            @pl.when(z < 3)
            def _():
                sr[kr] = p_buf[kr] + rr[kr]
                right_copy(kr).start()

        kl = i - lag_l

        @pl.when(jnp.logical_and(kl >= 0, kl < NC))
        def _():
            @pl.when(z < 3)
            def _():
                left_copy(kl).wait_recv()

            @pl.when(z > 0)
            def _():
                sl[kl] = p_buf[kl] + rl[kl]
                left_copy(kl).start()

        k_s = i - lag_s

        @pl.when(jnp.logical_and(k_s >= 0, k_s < NC))
        def _():
            s_all[sp, k_s] = p_buf[k_s] + rr[k_s] + rl[k_s]
            y_copy(k_s).start()
            part_copy(k_s).start()

        k_y = i - lag_s - hop

        @pl.when(jnp.logical_and(k_y >= 0, k_y < NC))
        def _():
            y_copy(k_y).wait_recv()
            fwd_copy(k_y).start()

        return carry

    lax.fori_loop(0, NC + 4 * hop, tick, 0)

    @pl.when(z < 3)
    def _():
        whole(sr, right_send).wait()

    @pl.when(z > 0)
    def _():
        whole(sl, left_send).wait()

    whole(s_all.at[sp], y_send).wait()
    whole(s_all.at[sp], part_send).wait()
    whole(s_all.at[ypeer], f_send).wait()
    whole(s_all.at[partner], part_recv).wait()
    whole(s_all.at[3 - sp], f_recv).wait()


def finish_kernel(s_all, x_ref, wpost_ref, out_h, out_buf, sem):
    blk = 16

    def out_copy(i):
        rows = pl.ds(i * blk, blk)
        return pltpu.make_async_copy(out_buf.at[rows], out_h.at[rows], sem)

    for i in range(ROWS // blk):
        g, r = (i * blk) // OWN, (i * blk) % OWN
        parts = [s_all[g, k, r:r + blk, :] for k in range(NC)]
        sq = parts[0] * parts[0]
        for k in range(1, NC):
            sq = sq + parts[k] * parts[k]
        rs = lax.rsqrt(jnp.sum(sq, axis=-1, keepdims=True) * (1.0 / DM) + NORM_EPS)
        for k in range(NC):
            for hf in range(CW // LANES):
                col = k * CW + hf * LANES
                gain = 1.0 + wpost_ref[col // LANES:col // LANES + 1, :]
                val = s_all[g, k, r:r + blk, hf * LANES:(hf + 1) * LANES] * rs * gain
                cs = slice(col, col + LANES)
                out_buf[i * blk:(i + 1) * blk, cs] = (x_ref[i * blk:(i + 1) * blk, cs].astype(jnp.float32) + val).astype(jnp.bfloat16)
        out_copy(i).start()
    for i in range(ROWS // blk):
        out_copy(i).wait()


def solution(mesh):
    cache_spec = P('dp', 'sp', 'tp', None)
    hbm = pl.BlockSpec(memory_space=pltpu.HBM)
    vmem = pl.BlockSpec(memory_space=pltpu.VMEM)

    def in_hbm(arr):
        return pltpu.with_memory_space_constraint(arr, pltpu.HBM)

    def in_vmem(arr):
        return pltpu.with_memory_space_constraint(arr, pltpu.VMEM)

    def to_rows(c):
        b, t, h, d = c.shape
        return c.reshape(b, t, h, 2, LANES).transpose(0, 1, 3, 2, 4).reshape(b, t * 2 * h, LANES)

    def from_rows(r):
        return r.reshape(ROWS, TB, 2, 2, LANES).transpose(0, 1, 3, 2, 4).reshape(ROWS, TB, 2, HD)

    def local_step(x_in, cur_pos, w_pre, w_q, w_k, w_v, w_o, w_post, k_cache, v_cache):
        half = HD // 2
        inv_freq = jnp.asarray((ROPE_BASE ** (-2.0 * np.arange(half) / (2 * half))).astype(np.float32))
        kr, vr = to_rows(k_cache), to_rows(v_cache)
        f32, bf16 = jnp.float32, jnp.bfloat16
        dma = pltpu.SemaphoreType.DMA
        half_shape = (HALF,) + kr.shape[1:]
        o_far, k_far, v_far, qs, ks, vs = pl.pallas_call(
            far_kernel,
            out_shape=(jax.ShapeDtypeStruct((HROWS, LANES), f32),
                       pltpu.VMEM(half_shape, bf16), pltpu.VMEM(half_shape, bf16),
                       pltpu.VMEM((8 * RP, LANES), f32), pltpu.VMEM((8 * RP, LANES), f32), pltpu.VMEM((8 * RP, LANES), f32)),
            in_specs=[hbm] * 10,
            out_specs=(vmem,) * 6,
            scratch_shapes=[
                pltpu.SMEM((ROWS,), jnp.int32), pltpu.VMEM((1, ROWS), jnp.int32), pltpu.VMEM((1, LANES), f32),
                pltpu.VMEM((DM // LANES, LANES), f32), pltpu.VMEM((ROWS, LANES), f32), pltpu.VMEM((ROWS, LANES), f32),
                pltpu.VMEM((ROWS, DM), bf16), pltpu.VMEM((ROWS, DM), bf16),
                pltpu.VMEM((DM, 1024), bf16), pltpu.VMEM((DM, 512), bf16), pltpu.VMEM((DM, 512), bf16), pltpu.VMEM((8, ROWS, HD), f32),
                dma, dma, dma((NKC,)), dma((NCH,)),
            ],
            compiler_params=pltpu.CompilerParams(vmem_limit_bytes=40 << 20),
            cost_estimate=pl.CostEstimate(flops=2 * 10 ** 9, bytes_accessed=25 * 10 ** 6, transcendentals=0),
            name='attend_far',
        )(in_hbm(cur_pos), in_hbm(cur_pos.reshape(1, ROWS)), in_hbm(inv_freq.reshape(1, LANES)), in_hbm(x_in),
          in_hbm(w_pre.reshape(DM // LANES, LANES)), in_hbm(w_q), in_hbm(w_k), in_hbm(w_v), in_hbm(kr), in_hbm(vr))
        o_got = lax.ppermute(o_far, 'sp', [(0, 2), (1, 3), (2, 0), (3, 1)])
        o_own, k_new, v_new = pl.pallas_call(
            near_kernel,
            out_shape=(pltpu.VMEM((HROWS, LANES), f32),
                       jax.ShapeDtypeStruct(kr.shape, bf16), jax.ShapeDtypeStruct(vr.shape, bf16)),
            in_specs=[hbm, vmem, vmem, vmem, vmem, vmem, hbm, hbm],
            out_specs=(vmem, hbm, hbm),
            scratch_shapes=[
                pltpu.SMEM((ROWS,), jnp.int32), pltpu.VMEM(half_shape, bf16), pltpu.VMEM(half_shape, bf16),
                dma, dma((NCH,)), dma,
            ],
            compiler_params=pltpu.CompilerParams(vmem_limit_bytes=28 << 20),
            cost_estimate=pl.CostEstimate(flops=10 ** 10, bytes_accessed=25 * 10 ** 6, transcendentals=0),
            name='attend_near',
        )(in_hbm(cur_pos), in_vmem(qs), in_vmem(ks), in_vmem(vs), in_vmem(k_far), in_vmem(v_far), in_hbm(kr), in_hbm(vr))
        big = pltpu.VMEM((NC, OWN, CW), f32)
        sums = pl.pallas_call(
            comm_kernel,
            out_shape=pltpu.VMEM((4, NC, OWN, CW), f32),
            in_specs=[vmem, vmem, hbm],
            out_specs=vmem,
            scratch_shapes=[
                pltpu.VMEM((NC // WG, 1024, WG * CW), bf16), pltpu.VMEM((4, LANES, LANES), f32), pltpu.VMEM((MROWS, LANES), f32),
                pltpu.VMEM((8 * OWN, LANES), f32), pltpu.VMEM((MROWS, LANES), f32), pltpu.VMEM((OWN, 1024), bf16),
                big, big, big, big, big,
                dma((NC // WG,)), dma, dma,
                dma, dma((NC,)), dma, dma((NC,)),
                dma, dma, dma, dma((NC,)), dma, dma,
            ],
            compiler_params=pltpu.CompilerParams(vmem_limit_bytes=40 << 20, collective_id=0, has_side_effects=True),
            name='combine',
        )(in_vmem(o_own), o_got, in_hbm(w_o))
        x_out = pl.pallas_call(
            finish_kernel,
            out_shape=jax.ShapeDtypeStruct((ROWS, DM), bf16),
            in_specs=[vmem, vmem, vmem],
            out_specs=hbm,
            scratch_shapes=[pltpu.VMEM((ROWS, DM), bf16), dma],
            compiler_params=pltpu.CompilerParams(vmem_limit_bytes=16 << 20),
            name='finish',
        )(in_vmem(sums), x_in, w_post.reshape(DM // LANES, LANES))
        return x_out, from_rows(k_new), from_rows(v_new)

    return jax.shard_map(local_step, mesh=mesh,
                         in_specs=(P('dp', None), P('dp'), P(None), P(None, 'tp'), P(None, 'tp'), P(None, 'tp'), P('tp', None), P(None), cache_spec, cache_spec),
                         out_specs=(P('dp', None), cache_spec, cache_spec), check_vma=False)
```

```python
import functools

import jax
import jax.numpy as jnp
import numpy as np
from jax import lax
from jax.experimental import pallas as pl
from jax.experimental.pallas import tpu as pltpu
from jax.sharding import PartitionSpec as P

SOFT_CAP = 50.0
ROPE_BASE = 10000.0
NORM_EPS = 1e-6

ROWS = 128
DM = 3840
HD = 256
TB = 64
RP = 136
LANES = 128
BCH = 16
HALF = ROWS // 2
HROWS = 8 * HALF + 8
NCH = HALF // BCH
KC = 768
NKC = DM // KC
SHIFT = 20.0
CW = 256
NC = DM // CW
WG = 3
OWN = 32
MROWS = 8 * OWN + 8
MESH = pl.DeviceIdType.MESH


def attend_rows(row0, nchunk, pos_ref, kbuf, vbuf, qs, ks, vs, o_ref, before, after):
    tbase = lax.axis_index('sp') * TB
    lane = lax.broadcasted_iota(jnp.int32, (8, LANES), 1)
    row = lax.broadcasted_iota(jnp.int32, (8, LANES), 0)
    row_c = row // 4
    row_h = (row // 2) % 2
    match = (((lane // 2) % 2) == row_c) & ((lane % 2) == row_h)
    match_f = jnp.where(match, 1.0, 0.0).astype(jnp.float32)
    first = row_c == 0
    t_half = [jnp.where(match, lane // 4 + 32 * hf, 1 << 20) for hf in range(2)]
    quad = lax.broadcasted_iota(jnp.int32, (16, LANES), 0) // 4
    zero = jnp.zeros((8, LANES), jnp.float32)

    def chunk(i, l_acc):
        before(i)
        tls = []
        for u in range(BCH):
            lb = i * BCH + u
            b = row0 + lb
            tl = pos_ref[b] - tbase
            tls.append(tl)
            hit = jnp.logical_and(tl >= 0, tl < TB)
            tc = jnp.clip(tl, 0, TB - 1)
            tile = tc // 4
            tgt = jnp.where(hit, tc - tile * 4, -1)
            sel = quad == tgt
            off = pl.multiple_of(tile * 16, 16)
            kn = ks[pl.ds(b, 8, stride=RP), :]
            vn = vs[pl.ds(b, 8, stride=RP), :]
            kt = kbuf[lb, pl.ds(off, 16), :].astype(jnp.float32)
            vt = vbuf[lb, pl.ds(off, 16), :].astype(jnp.float32)
            kbuf[lb, pl.ds(off, 16), :] = jnp.where(sel, jnp.concatenate([kn, kn], 0), kt).astype(jnp.bfloat16)
            vbuf[lb, pl.ds(off, 16), :] = jnp.where(sel, jnp.concatenate([vn, vn], 0), vt).astype(jnp.bfloat16)
        scores = []
        for u in range(0, BCH, 2):
            lb = i * BCH + u
            q0 = qs[pl.ds(row0 + lb, 8, stride=RP), :]
            q1 = qs[pl.ds(row0 + lb + 1, 8, stride=RP), :]
            lhs = jnp.concatenate([jnp.concatenate([q0, zero], 1), jnp.concatenate([zero, q1], 1)], 0).astype(jnp.bfloat16)
            kk = jnp.concatenate([kbuf[lb], kbuf[lb + 1]], 1)
            scores.append(lax.dot_general(lhs, kk, (((1,), (1,)), ((), ())), preferred_element_type=jnp.float32))
        weights = []
        for u in range(0, BCH, 2):
            pair = []
            for w in range(2):
                part = scores[u // 2][8 * w:8 * w + 8]
                es = []
                for hf in range(2):
                    a = part[:, hf * LANES:(hf + 1) * LANES] * match_f
                    e = pltpu.roll(a, 4, 0)
                    f = jnp.where(first, pltpu.roll(e, LANES - 2, 1), pltpu.roll(e, 2, 1))
                    s = SOFT_CAP * jnp.tanh((a + f) * (HD ** -0.5 / SOFT_CAP))
                    es.append(jnp.where(t_half[hf] <= tls[u + w], jnp.exp(s - SHIFT), 0.0))
                tot = jnp.sum(es[0] + es[1], axis=1, keepdims=True)
                inv = jnp.where(tot > 0.0, 1.0 / tot, 0.0)
                pair.append(jnp.concatenate([es[0] * inv, es[1] * inv], 1))
                l_acc = jnp.where(lane == i * BCH + u + w, tot, l_acc)
            weights.append(jnp.concatenate(pair, 0).astype(jnp.bfloat16))
        for u in range(0, BCH, 2):
            lb = i * BCH + u
            vv = jnp.concatenate([vbuf[lb], vbuf[lb + 1]], 1)
            o = jnp.dot(weights[u // 2], vv, preferred_element_type=jnp.float32)
            o_ref[pl.ds(lb, 8, stride=HALF), :] = o[0:8, 0:LANES]
            o_ref[pl.ds(lb + 1, 8, stride=HALF), :] = o[8:16, LANES:]
        after(i)
        return l_acc

    l_acc = lax.fori_loop(0, nchunk, chunk, zero)
    o_ref[pl.ds(8 * HALF, 8), :] = l_acc


def far_kernel(pos_h, posv_h, freq_h, x_h, wpre_h, wq_h, wk_h, wv_h, kc_h, vc_h,
               o_ref, kbuf, vbuf, qs, ks, vs,
               pos_ref, posv, freq, wpre_ref, cos_ref, sin_ref, x_buf, a_buf, wq_buf, wk_buf, wv_buf, acc,
               x_sem, s_sem, w_sem, ki_sem):
    row0 = (1 - lax.axis_index('sp') // 2) * HALF

    def w_start(c):
        rows = pl.ds(c * KC, KC)
        for n, (src, dst) in enumerate(((wk_h, wk_buf), (wv_h, wv_buf), (wq_h, wq_buf))):
            pltpu.make_async_copy(src.at[rows, :], dst.at[rows, :], w_sem.at[c]).start()

    def w_wait(c):
        rows = pl.ds(c * KC, KC)
        for n, (src, dst) in enumerate(((wk_h, wk_buf), (wv_h, wv_buf), (wq_h, wq_buf))):
            pltpu.make_async_copy(src.at[rows, :], dst.at[rows, :], w_sem.at[c]).wait()

    def k_in(i):
        return pltpu.make_async_copy(kc_h.at[pl.ds(row0 + i * BCH, BCH)], kbuf.at[pl.ds(i * BCH, BCH)], ki_sem.at[i])

    def v_in(i):
        return pltpu.make_async_copy(vc_h.at[pl.ds(row0 + i * BCH, BCH)], vbuf.at[pl.ds(i * BCH, BCH)], ki_sem.at[i])

    small = [pltpu.make_async_copy(a, b, s_sem) for a, b in (
        (wpre_h, wpre_ref), (posv_h, posv), (freq_h, freq), (pos_h, pos_ref))]
    for c in small:
        c.start()
    x_copy = pltpu.make_async_copy(x_h, x_buf, x_sem)
    x_copy.start()
    for c in range(NKC):
        w_start(c)
    for n in range(NCH):
        k_in(n).start()
        v_in(n).start()
    for c in small:
        c.wait()
    pos_col = jnp.broadcast_to(posv[...].astype(jnp.float32), (ROWS, LANES)).T
    ang = pos_col * freq[...]
    cos_ref[...] = jnp.cos(ang)
    sin_ref[...] = jnp.sin(ang)
    x_copy.wait()

    gain = 1.0 + jnp.concatenate([wpre_ref[k:k + 1, :] for k in range(DM // LANES)], 1)

    def norm_rows(i, carry):
        r = pl.multiple_of(i * 16, 16)
        xb = x_buf[pl.ds(r, 16), :].astype(jnp.float32)
        ms = jnp.mean(xb * xb, axis=-1, keepdims=True)
        a_buf[pl.ds(r, 16), :] = (xb * lax.rsqrt(ms + NORM_EPS) * gain).astype(jnp.bfloat16)
        return carry

    lax.fori_loop(0, ROWS // 16, norm_rows, 0)

    for c in range(NKC):
        w_wait(c)
        rows = slice(c * KC, (c + 1) * KC)
        a_c = a_buf[:, rows]
        for i in range(8):
            if i < 2:
                w_c = wk_buf[rows, i * HD:(i + 1) * HD]
            elif i < 4:
                w_c = wv_buf[rows, (i - 2) * HD:(i - 1) * HD]
            else:
                w_c = wq_buf[rows, (i - 4) * HD:(i - 3) * HD]
            y = jnp.dot(a_c, w_c, preferred_element_type=jnp.float32)
            if c == 0:
                acc[i] = y
                continue
            y = acc[i] + y
            if c < NKC - 1:
                acc[i] = y
                continue
            lo, hi = y[:, :LANES], y[:, LANES:]
            if 2 <= i < 4:
                h = i - 2
                for rep in range(2):
                    vs[pl.ds((rep * 4 + h) * RP, ROWS), :] = lo
                    vs[pl.ds((rep * 4 + 2 + h) * RP, ROWS), :] = hi
            else:
                cos_t, sin_t = cos_ref[...], sin_ref[...]
                rlo = lo * cos_t - hi * sin_t
                rhi = hi * cos_t + lo * sin_t
                if i < 2:
                    for rep in range(2):
                        ks[pl.ds((rep * 4 + i) * RP, ROWS), :] = rlo
                        ks[pl.ds((rep * 4 + 2 + i) * RP, ROWS), :] = rhi
                else:
                    qs[pl.ds((i - 4) * RP, ROWS), :] = rlo
                    qs[pl.ds((4 + i - 4) * RP, ROWS), :] = rhi

    def before(i):
        k_in(i).wait()
        v_in(i).wait()

    attend_rows(row0, NCH, pos_ref, kbuf, vbuf, qs, ks, vs, o_ref, before, lambda i: None)


def near_kernel(pos_h, qs, ks, vs, kfar, vfar, kc_h, vc_h,
                o_ref, ko_h, vo_h,
                pos_ref, kbuf, vbuf, p_sem, ki_sem, w_sem):
    yy = lax.axis_index('sp') // 2
    row0 = yy * HALF
    far0 = (1 - yy) * HALF

    def k_in(i):
        return pltpu.make_async_copy(kc_h.at[pl.ds(row0 + i * BCH, BCH)], kbuf.at[pl.ds(i * BCH, BCH)], ki_sem.at[i])

    def v_in(i):
        return pltpu.make_async_copy(vc_h.at[pl.ds(row0 + i * BCH, BCH)], vbuf.at[pl.ds(i * BCH, BCH)], ki_sem.at[i])

    def k_out(i):
        return pltpu.make_async_copy(kbuf.at[pl.ds(i * BCH, BCH)], ko_h.at[pl.ds(row0 + i * BCH, BCH)], w_sem)

    def v_out(i):
        return pltpu.make_async_copy(vbuf.at[pl.ds(i * BCH, BCH)], vo_h.at[pl.ds(row0 + i * BCH, BCH)], w_sem)

    def kf_out(i):
        return pltpu.make_async_copy(kfar.at[pl.ds(i * BCH, BCH)], ko_h.at[pl.ds(far0 + i * BCH, BCH)], w_sem)

    def vf_out(i):
        return pltpu.make_async_copy(vfar.at[pl.ds(i * BCH, BCH)], vo_h.at[pl.ds(far0 + i * BCH, BCH)], w_sem)

    p_copy = pltpu.make_async_copy(pos_h, pos_ref, p_sem)
    p_copy.start()
    for i in range(NCH):
        k_in(i).start()
        v_in(i).start()
    p_copy.wait()

    def before(i):
        k_in(i).wait()
        v_in(i).wait()
        kf_out(i).start()
        vf_out(i).start()

    def after(i):
        k_out(i).start()
        v_out(i).start()

    attend_rows(row0, NCH, pos_ref, kbuf, vbuf, qs, ks, vs, o_ref, before, after)
    for i in range(NCH):
        kf_out(i).wait()
        vf_out(i).wait()
        k_out(i).wait()
        v_out(i).wait()


def comm_kernel(o_own, o_got, wo_h, s_all,
                wo_buf, fac, m1, m2, r1, lhs, p_buf, rr, rl, sr, sl,
                w_sem, r1_send, r1_recv,
                right_send, right_recv, left_send, left_recv,
                part_send, part_recv, y_send, y_recv, f_send, f_recv):
    z = lax.axis_index('tp')
    sp = lax.axis_index('sp')
    core = sp % 2
    partner = sp + 1 - 2 * core
    ypeer = (sp + 2) % 4

    def wo_copy(k):
        return pltpu.make_async_copy(wo_h.at[:, pl.ds(pl.multiple_of(k * WG * CW, CW), WG * CW)], wo_buf.at[k], w_sem.at[k])

    for k in range(NC // WG):
        wo_copy(k).start()

    @pl.when(z == 0)
    def _():
        rr[...] = jnp.zeros_like(rr)

    @pl.when(z == 3)
    def _():
        rl[...] = jnp.zeros_like(rl)

    bar = pltpu.get_barrier_semaphore()
    pl.semaphore_signal(bar, inc=1, device_id={'sp': partner}, device_id_type=MESH)
    pl.semaphore_signal(bar, inc=1, device_id={'sp': ypeer}, device_id_type=MESH)

    @pl.when(z > 0)
    def _():
        pl.semaphore_signal(bar, inc=1, device_id={'tp': z - 1}, device_id_type=MESH)

    @pl.when(z < 3)
    def _():
        pl.semaphore_signal(bar, inc=1, device_id={'tp': z + 1}, device_id_type=MESH)

    pl.semaphore_wait(bar, 3 + (z * (3 - z)) // 2)

    def shares(l_a, l_b, slot):
        tot = l_a + l_b
        inv = jnp.where(tot > 0.0, 1.0 / tot, 0.0)
        for w, l in enumerate((l_a, l_b)):
            fac[slot + w] = jnp.concatenate([l * inv, jnp.zeros((LANES - 8, LANES), jnp.float32)], 0).T
        return tot

    mine = pl.multiple_of(core * OWN, OWN)
    theirs = pl.multiple_of((1 - core) * OWN, OWN)
    tot = shares(o_own[pl.ds(8 * HALF, 8), :], o_got[pl.ds(8 * HALF, 8), :], 0)

    def merge_half(r0, dst):
        fa, fb = fac[0, pl.ds(r0, OWN), :], fac[1, pl.ds(r0, OWN), :]
        for j in range(8):
            rows = pl.ds(pl.multiple_of(j * HALF + r0, 8), OWN)
            dst[pl.ds(j * OWN, OWN), :] = o_own[rows, :] * fa[:, j:j + 1] + o_got[rows, :] * fb[:, j:j + 1]

    merge_half(theirs, m1)
    m1[pl.ds(8 * OWN, 8), :] = tot
    pair = pltpu.make_async_remote_copy(
        src_ref=m1, dst_ref=r1, send_sem=r1_send, recv_sem=r1_recv, device_id={'sp': partner}, device_id_type=MESH)
    pair.start()
    merge_half(mine, m2)
    pair.wait()
    shares(tot, r1[pl.ds(8 * OWN, 8), :], 2)
    fa, fb = fac[2, pl.ds(mine, OWN), :], fac[3, pl.ds(mine, OWN), :]
    for j in range(8):
        c, hq = j // 4, j % 4
        val = m2[j * OWN:(j + 1) * OWN, :] * fa[:, j:j + 1] + r1[j * OWN:(j + 1) * OWN, :] * fb[:, j:j + 1]
        lhs[:, (hq * 2 + c) * LANES:(hq * 2 + c + 1) * LANES] = val.astype(jnp.bfloat16)

    def right_copy(k):
        return pltpu.make_async_remote_copy(
            src_ref=sr.at[k], dst_ref=rr.at[k], send_sem=right_send, recv_sem=right_recv.at[k],
            device_id={'tp': z + 1}, device_id_type=MESH)

    def left_copy(k):
        return pltpu.make_async_remote_copy(
            src_ref=sl.at[k], dst_ref=rl.at[k], send_sem=left_send, recv_sem=left_recv.at[k],
            device_id={'tp': z - 1}, device_id_type=MESH)

    def part_copy(k):
        return pltpu.make_async_remote_copy(
            src_ref=s_all.at[sp, k], dst_ref=s_all.at[sp, k], send_sem=part_send, recv_sem=part_recv,
            device_id={'sp': partner}, device_id_type=MESH)

    def y_copy(k):
        return pltpu.make_async_remote_copy(
            src_ref=s_all.at[sp, k], dst_ref=s_all.at[sp, k], send_sem=y_send, recv_sem=y_recv.at[k],
            device_id={'sp': ypeer}, device_id_type=MESH)

    def fwd_copy(k):
        return pltpu.make_async_remote_copy(
            src_ref=s_all.at[ypeer, k], dst_ref=s_all.at[ypeer, k], send_sem=f_send, recv_sem=f_recv,
            device_id={'sp': partner}, device_id_type=MESH)

    def whole(ref, sem):
        return pltpu.make_async_copy(ref, ref, sem)

    hop = 5
    lag_r = hop * z
    lag_l = hop * (3 - z)
    lag_s = hop * (3 - (z * (3 - z)) // 2)

    def tick(i, carry):
        @pl.when(i < NC)
        def _():
            group, place = i // WG, i % WG

            @pl.when(place == 0)
            def _():
                wo_copy(group).wait()

            w_c = wo_buf[group, :, pl.ds(pl.multiple_of(place * CW, CW), CW)]
            p_buf[i] = jnp.dot(lhs[...], w_c, preferred_element_type=jnp.float32)

        kr = i - lag_r

        @pl.when(jnp.logical_and(kr >= 0, kr < NC))
        def _():
            @pl.when(z > 0)
            def _():
                right_copy(kr).wait_recv()

            @pl.when(z < 3)
            def _():
                sr[kr] = p_buf[kr] + rr[kr]
                right_copy(kr).start()

        kl = i - lag_l

        @pl.when(jnp.logical_and(kl >= 0, kl < NC))
        def _():
            @pl.when(z < 3)
            def _():
                left_copy(kl).wait_recv()

            @pl.when(z > 0)
            def _():
                sl[kl] = p_buf[kl] + rl[kl]
                left_copy(kl).start()

        k_s = i - lag_s

        @pl.when(jnp.logical_and(k_s >= 0, k_s < NC))
        def _():
            s_all[sp, k_s] = p_buf[k_s] + rr[k_s] + rl[k_s]
            y_copy(k_s).start()
            part_copy(k_s).start()

        k_y = i - lag_s - hop

        @pl.when(jnp.logical_and(k_y >= 0, k_y < NC))
        def _():
            y_copy(k_y).wait_recv()
            fwd_copy(k_y).start()

        return carry

    lax.fori_loop(0, NC + 4 * hop, tick, 0)

    @pl.when(z < 3)
    def _():
        whole(sr, right_send).wait()

    @pl.when(z > 0)
    def _():
        whole(sl, left_send).wait()

    whole(s_all.at[sp], y_send).wait()
    whole(s_all.at[sp], part_send).wait()
    whole(s_all.at[ypeer], f_send).wait()
    whole(s_all.at[partner], part_recv).wait()
    whole(s_all.at[3 - sp], f_recv).wait()


def finish_kernel(s_all, x_ref, wpost_ref, out_h, out_buf, sem):
    blk = 16

    def out_copy(i):
        rows = pl.ds(i * blk, blk)
        return pltpu.make_async_copy(out_buf.at[rows], out_h.at[rows], sem)

    for i in range(ROWS // blk):
        g, r = (i * blk) // OWN, (i * blk) % OWN
        parts = [s_all[g, k, r:r + blk, :] for k in range(NC)]
        sq = parts[0] * parts[0]
        for k in range(1, NC):
            sq = sq + parts[k] * parts[k]
        rs = lax.rsqrt(jnp.sum(sq, axis=-1, keepdims=True) * (1.0 / DM) + NORM_EPS)
        for k in range(NC):
            for hf in range(CW // LANES):
                col = k * CW + hf * LANES
                gain = 1.0 + wpost_ref[col // LANES:col // LANES + 1, :]
                val = s_all[g, k, r:r + blk, hf * LANES:(hf + 1) * LANES] * rs * gain
                cs = slice(col, col + LANES)
                out_buf[i * blk:(i + 1) * blk, cs] = (x_ref[i * blk:(i + 1) * blk, cs].astype(jnp.float32) + val).astype(jnp.bfloat16)
        out_copy(i).start()
    for i in range(ROWS // blk):
        out_copy(i).wait()


def solution(mesh):
    cache_spec = P('dp', 'sp', 'tp', None)
    hbm = pl.BlockSpec(memory_space=pltpu.HBM)
    vmem = pl.BlockSpec(memory_space=pltpu.VMEM)

    def in_hbm(arr):
        return pltpu.with_memory_space_constraint(arr, pltpu.HBM)

    def in_vmem(arr):
        return pltpu.with_memory_space_constraint(arr, pltpu.VMEM)

    def to_rows(c):
        b, t, h, d = c.shape
        return c.reshape(b, t, h, 2, LANES).transpose(0, 1, 3, 2, 4).reshape(b, t * 2 * h, LANES)

    def from_rows(r):
        return r.reshape(ROWS, TB, 2, 2, LANES).transpose(0, 1, 3, 2, 4).reshape(ROWS, TB, 2, HD)

    def local_step(x_in, cur_pos, w_pre, w_q, w_k, w_v, w_o, w_post, k_cache, v_cache):
        half = HD // 2
        inv_freq = jnp.asarray((ROPE_BASE ** (-2.0 * np.arange(half) / (2 * half))).astype(np.float32))
        kr, vr = to_rows(k_cache), to_rows(v_cache)
        f32, bf16 = jnp.float32, jnp.bfloat16
        dma = pltpu.SemaphoreType.DMA
        half_shape = (HALF,) + kr.shape[1:]
        o_far, k_far, v_far, qs, ks, vs = pl.pallas_call(
            far_kernel,
            out_shape=(jax.ShapeDtypeStruct((HROWS, LANES), f32),
                       pltpu.VMEM(half_shape, bf16), pltpu.VMEM(half_shape, bf16),
                       pltpu.VMEM((8 * RP, LANES), f32), pltpu.VMEM((8 * RP, LANES), f32), pltpu.VMEM((8 * RP, LANES), f32)),
            in_specs=[hbm] * 10,
            out_specs=(vmem,) * 6,
            scratch_shapes=[
                pltpu.SMEM((ROWS,), jnp.int32), pltpu.VMEM((1, ROWS), jnp.int32), pltpu.VMEM((1, LANES), f32),
                pltpu.VMEM((DM // LANES, LANES), f32), pltpu.VMEM((ROWS, LANES), f32), pltpu.VMEM((ROWS, LANES), f32),
                pltpu.VMEM((ROWS, DM), bf16), pltpu.VMEM((ROWS, DM), bf16),
                pltpu.VMEM((DM, 1024), bf16), pltpu.VMEM((DM, 512), bf16), pltpu.VMEM((DM, 512), bf16), pltpu.VMEM((8, ROWS, HD), f32),
                dma, dma, dma((NKC,)), dma((NCH,)),
            ],
            compiler_params=pltpu.CompilerParams(vmem_limit_bytes=40 << 20),
            cost_estimate=pl.CostEstimate(flops=2 * 10 ** 9, bytes_accessed=25 * 10 ** 6, transcendentals=0),
            name='attend_far',
        )(in_hbm(cur_pos), in_hbm(cur_pos.reshape(1, ROWS)), in_hbm(inv_freq.reshape(1, LANES)), in_hbm(x_in),
          in_hbm(w_pre.reshape(DM // LANES, LANES)), in_hbm(w_q), in_hbm(w_k), in_hbm(w_v), in_hbm(kr), in_hbm(vr))
        o_got = lax.ppermute(o_far, 'sp', [(0, 2), (1, 3), (2, 0), (3, 1)])
        o_own, k_new, v_new = pl.pallas_call(
            near_kernel,
            out_shape=(pltpu.VMEM((HROWS, LANES), f32),
                       jax.ShapeDtypeStruct(kr.shape, bf16), jax.ShapeDtypeStruct(vr.shape, bf16)),
            in_specs=[hbm, vmem, vmem, vmem, vmem, vmem, hbm, hbm],
            out_specs=(vmem, hbm, hbm),
            scratch_shapes=[
                pltpu.SMEM((ROWS,), jnp.int32), pltpu.VMEM(half_shape, bf16), pltpu.VMEM(half_shape, bf16),
                dma, dma((NCH,)), dma,
            ],
            compiler_params=pltpu.CompilerParams(vmem_limit_bytes=28 << 20),
            cost_estimate=pl.CostEstimate(flops=10 ** 10, bytes_accessed=25 * 10 ** 6, transcendentals=0),
            name='attend_near',
        )(in_hbm(cur_pos), in_vmem(qs), in_vmem(ks), in_vmem(vs), in_vmem(k_far), in_vmem(v_far), in_hbm(kr), in_hbm(vr))
        big = pltpu.VMEM((NC, OWN, CW), f32)
        sums = pl.pallas_call(
            comm_kernel,
            out_shape=pltpu.VMEM((4, NC, OWN, CW), f32),
            in_specs=[vmem, vmem, hbm],
            out_specs=vmem,
            scratch_shapes=[
                pltpu.VMEM((NC // WG, 1024, WG * CW), bf16), pltpu.VMEM((4, LANES, LANES), f32), pltpu.VMEM((MROWS, LANES), f32),
                pltpu.VMEM((8 * OWN, LANES), f32), pltpu.VMEM((MROWS, LANES), f32), pltpu.VMEM((OWN, 1024), bf16),
                big, big, big, big, big,
                dma((NC // WG,)), dma, dma,
                dma, dma((NC,)), dma, dma((NC,)),
                dma, dma, dma, dma((NC,)), dma, dma,
            ],
            compiler_params=pltpu.CompilerParams(vmem_limit_bytes=40 << 20, collective_id=0, has_side_effects=True),
            name='combine',
        )(in_vmem(o_own), o_got, in_hbm(w_o))
        x_out = pl.pallas_call(
            finish_kernel,
            out_shape=jax.ShapeDtypeStruct((ROWS, DM), bf16),
            in_specs=[vmem, vmem, vmem],
            out_specs=hbm,
            scratch_shapes=[pltpu.VMEM((ROWS, DM), bf16), dma],
            compiler_params=pltpu.CompilerParams(vmem_limit_bytes=16 << 20),
            name='finish',
        )(in_vmem(sums), x_in, w_post.reshape(DM // LANES, LANES))
        return x_out, from_rows(k_new), from_rows(v_new)

    return jax.shard_map(local_step, mesh=mesh,
                         in_specs=(P('dp', None), P('dp'), P(None), P(None, 'tp'), P(None, 'tp'), P(None, 'tp'), P('tp', None), P(None), cache_spec, cache_spec),
                         out_specs=(P('dp', None), cache_spec, cache_spec), check_vma=False)
```

```python
import functools

import jax
import jax.numpy as jnp
import numpy as np
from jax import lax
from jax.experimental import pallas as pl
from jax.experimental.pallas import tpu as pltpu
from jax.sharding import PartitionSpec as P

SOFT_CAP = 50.0
ROPE_BASE = 10000.0
NORM_EPS = 1e-6

ROWS = 128
DM = 3840
HD = 256
TB = 64
RP = 136
LANES = 128
BCH = 16
HALF = ROWS // 2
HROWS = 8 * HALF + 8
NCH = HALF // BCH
KC = 768
NKC = DM // KC
KP = 256
NKP = DM // KP
WIN = 5
SHIFT = 20.0
CW = 256
NC = DM // CW
WG = 3
OWN = 32
MROWS = 8 * OWN + 8
MESH = pl.DeviceIdType.MESH


def attend_rows(row0, nchunk, pos_ref, kbuf, vbuf, qs, ks, vs, o_ref, before, after):
    tbase = lax.axis_index('sp') * TB
    lane = lax.broadcasted_iota(jnp.int32, (8, LANES), 1)
    row = lax.broadcasted_iota(jnp.int32, (8, LANES), 0)
    row_c = row // 4
    row_h = (row // 2) % 2
    match = (((lane // 2) % 2) == row_c) & ((lane % 2) == row_h)
    match_f = jnp.where(match, 1.0, 0.0).astype(jnp.float32)
    first = row_c == 0
    t_half = [jnp.where(match, lane // 4 + 32 * hf, 1 << 20) for hf in range(2)]
    quad = lax.broadcasted_iota(jnp.int32, (16, LANES), 0) // 4
    zero = jnp.zeros((8, LANES), jnp.float32)

    def chunk(i, l_acc):
        before(i)
        tls = []
        for u in range(BCH):
            lb = i * BCH + u
            b = row0 + lb
            tl = pos_ref[b] - tbase
            tls.append(tl)
            hit = jnp.logical_and(tl >= 0, tl < TB)
            tc = jnp.clip(tl, 0, TB - 1)
            tile = tc // 4
            tgt = jnp.where(hit, tc - tile * 4, -1)
            sel = quad == tgt
            off = pl.multiple_of(tile * 16, 16)
            kn = ks[pl.ds(b, 8, stride=RP), :]
            vn = vs[pl.ds(b, 8, stride=RP), :]
            kt = kbuf[lb, pl.ds(off, 16), :].astype(jnp.float32)
            vt = vbuf[lb, pl.ds(off, 16), :].astype(jnp.float32)
            kbuf[lb, pl.ds(off, 16), :] = jnp.where(sel, jnp.concatenate([kn, kn], 0), kt).astype(jnp.bfloat16)
            vbuf[lb, pl.ds(off, 16), :] = jnp.where(sel, jnp.concatenate([vn, vn], 0), vt).astype(jnp.bfloat16)
        scores = []
        for u in range(0, BCH, 2):
            lb = i * BCH + u
            q0 = qs[pl.ds(row0 + lb, 8, stride=RP), :]
            q1 = qs[pl.ds(row0 + lb + 1, 8, stride=RP), :]
            lhs = jnp.concatenate([jnp.concatenate([q0, zero], 1), jnp.concatenate([zero, q1], 1)], 0).astype(jnp.bfloat16)
            kk = jnp.concatenate([kbuf[lb], kbuf[lb + 1]], 1)
            scores.append(lax.dot_general(lhs, kk, (((1,), (1,)), ((), ())), preferred_element_type=jnp.float32))
        weights = []
        for u in range(0, BCH, 2):
            pair = []
            for w in range(2):
                part = scores[u // 2][8 * w:8 * w + 8]
                es = []
                for hf in range(2):
                    a = part[:, hf * LANES:(hf + 1) * LANES] * match_f
                    e = pltpu.roll(a, 4, 0)
                    f = jnp.where(first, pltpu.roll(e, LANES - 2, 1), pltpu.roll(e, 2, 1))
                    s = SOFT_CAP * jnp.tanh((a + f) * (HD ** -0.5 / SOFT_CAP))
                    es.append(jnp.where(t_half[hf] <= tls[u + w], jnp.exp(s - SHIFT), 0.0))
                tot = jnp.sum(es[0] + es[1], axis=1, keepdims=True)
                inv = jnp.where(tot > 0.0, 1.0 / tot, 0.0)
                pair.append(jnp.concatenate([es[0] * inv, es[1] * inv], 1))
                l_acc = jnp.where(lane == i * BCH + u + w, tot, l_acc)
            weights.append(jnp.concatenate(pair, 0).astype(jnp.bfloat16))
        for u in range(0, BCH, 2):
            lb = i * BCH + u
            vv = jnp.concatenate([vbuf[lb], vbuf[lb + 1]], 1)
            o = jnp.dot(weights[u // 2], vv, preferred_element_type=jnp.float32)
            o_ref[pl.ds(lb, 8, stride=HALF), :] = o[0:8, 0:LANES]
            o_ref[pl.ds(lb + 1, 8, stride=HALF), :] = o[8:16, LANES:]
        after(i)
        return l_acc

    l_acc = lax.fori_loop(0, nchunk, chunk, zero)
    o_ref[pl.ds(8 * HALF, 8), :] = l_acc


def far_kernel(pos_h, posv_h, freq_h, x_h, wpre_h, wq_h, wk_h, wv_h, kc_h, vc_h,
               o_ref, kbuf, vbuf, qs, ks, vs,
               pos_ref, posv, freq, wpre_ref, cos_ref, sin_ref, x_buf, a_buf, wq_buf, wk_buf, wv_buf, acc,
               x_sem, s_sem, w_sem, ki_sem):
    row0 = (1 - lax.axis_index('sp') // 2) * HALF

    def w_start(c):
        rows = pl.ds(c * KP, KP)
        for n, (src, dst) in enumerate(((wk_h, wk_buf), (wv_h, wv_buf), (wq_h, wq_buf))):
            pltpu.make_async_copy(src.at[rows, :], dst.at[rows, :], w_sem.at[c]).start()

    def w_wait(c):
        rows = pl.ds(c * KP, KP)
        for n, (src, dst) in enumerate(((wk_h, wk_buf), (wv_h, wv_buf), (wq_h, wq_buf))):
            pltpu.make_async_copy(src.at[rows, :], dst.at[rows, :], w_sem.at[c]).wait()

    def k_in(i):
        return pltpu.make_async_copy(kc_h.at[pl.ds(row0 + i * BCH, BCH)], kbuf.at[pl.ds(i * BCH, BCH)], ki_sem.at[i])

    def v_in(i):
        return pltpu.make_async_copy(vc_h.at[pl.ds(row0 + i * BCH, BCH)], vbuf.at[pl.ds(i * BCH, BCH)], ki_sem.at[i])

    small = [pltpu.make_async_copy(a, b, s_sem) for a, b in (
        (wpre_h, wpre_ref), (posv_h, posv), (freq_h, freq), (pos_h, pos_ref))]
    for c in small:
        c.start()
    x_copy = pltpu.make_async_copy(x_h, x_buf, x_sem)
    x_copy.start()
    for c in range(3):
        w_start(c)
    for c in small:
        c.wait()
    for c in range(3, WIN):
        w_start(c)
    pos_col = jnp.broadcast_to(posv[...].astype(jnp.float32), (ROWS, LANES)).T
    ang = pos_col * freq[...]
    cos_ref[...] = jnp.cos(ang)
    sin_ref[...] = jnp.sin(ang)
    x_copy.wait()

    gain = 1.0 + jnp.concatenate([wpre_ref[k:k + 1, :] for k in range(DM // LANES)], 1)

    def norm_rows(i, carry):
        r = pl.multiple_of(i * 16, 16)
        xb = x_buf[pl.ds(r, 16), :].astype(jnp.float32)
        ms = jnp.mean(xb * xb, axis=-1, keepdims=True)
        a_buf[pl.ds(r, 16), :] = (xb * lax.rsqrt(ms + NORM_EPS) * gain).astype(jnp.bfloat16)
        return carry

    lax.fori_loop(0, ROWS // 16, norm_rows, 0)

    for c in range(NKC):
        for p in range(c * (KC // KP), (c + 1) * (KC // KP)):
            w_wait(p)
            if p + WIN < NKP:
                w_start(p + WIN)
            elif (p + WIN - NKP) % 2 == 0:
                n = (p + WIN - NKP) // 2
                k_in(n).start()
                v_in(n).start()
        rows = slice(c * KC, (c + 1) * KC)
        a_c = a_buf[:, rows]
        for i in range(8):
            if i < 2:
                w_c = wk_buf[rows, i * HD:(i + 1) * HD]
            elif i < 4:
                w_c = wv_buf[rows, (i - 2) * HD:(i - 1) * HD]
            else:
                w_c = wq_buf[rows, (i - 4) * HD:(i - 3) * HD]
            y = jnp.dot(a_c, w_c, preferred_element_type=jnp.float32)
            if c == 0:
                acc[i] = y
                continue
            y = acc[i] + y
            if c < NKC - 1:
                acc[i] = y
                continue
            lo, hi = y[:, :LANES], y[:, LANES:]
            if 2 <= i < 4:
                h = i - 2
                for rep in range(2):
                    vs[pl.ds((rep * 4 + h) * RP, ROWS), :] = lo
                    vs[pl.ds((rep * 4 + 2 + h) * RP, ROWS), :] = hi
            else:
                cos_t, sin_t = cos_ref[...], sin_ref[...]
                rlo = lo * cos_t - hi * sin_t
                rhi = hi * cos_t + lo * sin_t
                if i < 2:
                    for rep in range(2):
                        ks[pl.ds((rep * 4 + i) * RP, ROWS), :] = rlo
                        ks[pl.ds((rep * 4 + 2 + i) * RP, ROWS), :] = rhi
                else:
                    qs[pl.ds((i - 4) * RP, ROWS), :] = rlo
                    qs[pl.ds((4 + i - 4) * RP, ROWS), :] = rhi

    def before(i):
        k_in(i).wait()
        v_in(i).wait()

        @pl.when(i == 0)
        def _():
            k_in(NCH - 1).start()
            v_in(NCH - 1).start()

    attend_rows(row0, NCH, pos_ref, kbuf, vbuf, qs, ks, vs, o_ref, before, lambda i: None)


def near_kernel(pos_h, qs, ks, vs, kfar, vfar, kc_h, vc_h,
                o_ref, ko_h, vo_h,
                pos_ref, kbuf, vbuf, p_sem, ki_sem, w_sem):
    yy = lax.axis_index('sp') // 2
    row0 = yy * HALF
    far0 = (1 - yy) * HALF

    def k_in(i):
        return pltpu.make_async_copy(kc_h.at[pl.ds(row0 + i * BCH, BCH)], kbuf.at[pl.ds(i * BCH, BCH)], ki_sem.at[i])

    def v_in(i):
        return pltpu.make_async_copy(vc_h.at[pl.ds(row0 + i * BCH, BCH)], vbuf.at[pl.ds(i * BCH, BCH)], ki_sem.at[i])

    def k_out(i):
        return pltpu.make_async_copy(kbuf.at[pl.ds(i * BCH, BCH)], ko_h.at[pl.ds(row0 + i * BCH, BCH)], w_sem)

    def v_out(i):
        return pltpu.make_async_copy(vbuf.at[pl.ds(i * BCH, BCH)], vo_h.at[pl.ds(row0 + i * BCH, BCH)], w_sem)

    def kf_out(i):
        return pltpu.make_async_copy(kfar.at[pl.ds(i * BCH, BCH)], ko_h.at[pl.ds(far0 + i * BCH, BCH)], w_sem)

    def vf_out(i):
        return pltpu.make_async_copy(vfar.at[pl.ds(i * BCH, BCH)], vo_h.at[pl.ds(far0 + i * BCH, BCH)], w_sem)

    p_copy = pltpu.make_async_copy(pos_h, pos_ref, p_sem)
    p_copy.start()
    for i in range(NCH):
        k_in(i).start()
        v_in(i).start()
    p_copy.wait()

    def before(i):
        k_in(i).wait()
        v_in(i).wait()
        kf_out(i).start()
        vf_out(i).start()

    def after(i):
        k_out(i).start()
        v_out(i).start()

    attend_rows(row0, NCH, pos_ref, kbuf, vbuf, qs, ks, vs, o_ref, before, after)
    for i in range(NCH):
        kf_out(i).wait()
        vf_out(i).wait()
        k_out(i).wait()
        v_out(i).wait()


def comm_kernel(o_own, o_got, wo_h, s_all,
                wo_buf, fac, m1, m2, r1, lhs, p_buf, rr, rl, sr, sl,
                w_sem, r1_send, r1_recv,
                right_send, right_recv, left_send, left_recv,
                part_send, part_recv, y_send, y_recv, f_send, f_recv):
    z = lax.axis_index('tp')
    sp = lax.axis_index('sp')
    core = sp % 2
    partner = sp + 1 - 2 * core
    ypeer = (sp + 2) % 4

    def wo_copy(k):
        return pltpu.make_async_copy(wo_h.at[:, pl.ds(pl.multiple_of(k * WG * CW, CW), WG * CW)], wo_buf.at[k], w_sem.at[k])

    for k in range(NC // WG):
        wo_copy(k).start()

    @pl.when(z == 0)
    def _():
        rr[...] = jnp.zeros_like(rr)

    @pl.when(z == 3)
    def _():
        rl[...] = jnp.zeros_like(rl)

    bar = pltpu.get_barrier_semaphore()
    pl.semaphore_signal(bar, inc=1, device_id={'sp': partner}, device_id_type=MESH)
    pl.semaphore_signal(bar, inc=1, device_id={'sp': ypeer}, device_id_type=MESH)

    @pl.when(z > 0)
    def _():
        pl.semaphore_signal(bar, inc=1, device_id={'tp': z - 1}, device_id_type=MESH)

    @pl.when(z < 3)
    def _():
        pl.semaphore_signal(bar, inc=1, device_id={'tp': z + 1}, device_id_type=MESH)

    pl.semaphore_wait(bar, 3 + (z * (3 - z)) // 2)

    def shares(l_a, l_b, slot):
        tot = l_a + l_b
        inv = jnp.where(tot > 0.0, 1.0 / tot, 0.0)
        for w, l in enumerate((l_a, l_b)):
            fac[slot + w] = jnp.concatenate([l * inv, jnp.zeros((LANES - 8, LANES), jnp.float32)], 0).T
        return tot

    mine = pl.multiple_of(core * OWN, OWN)
    theirs = pl.multiple_of((1 - core) * OWN, OWN)
    tot = shares(o_own[pl.ds(8 * HALF, 8), :], o_got[pl.ds(8 * HALF, 8), :], 0)

    def merge_half(r0, dst):
        fa, fb = fac[0, pl.ds(r0, OWN), :], fac[1, pl.ds(r0, OWN), :]
        for j in range(8):
            rows = pl.ds(pl.multiple_of(j * HALF + r0, 8), OWN)
            dst[pl.ds(j * OWN, OWN), :] = o_own[rows, :] * fa[:, j:j + 1] + o_got[rows, :] * fb[:, j:j + 1]

    merge_half(theirs, m1)
    m1[pl.ds(8 * OWN, 8), :] = tot
    pair = pltpu.make_async_remote_copy(
        src_ref=m1, dst_ref=r1, send_sem=r1_send, recv_sem=r1_recv, device_id={'sp': partner}, device_id_type=MESH)
    pair.start()
    merge_half(mine, m2)
    pair.wait()
    shares(tot, r1[pl.ds(8 * OWN, 8), :], 2)
    fa, fb = fac[2, pl.ds(mine, OWN), :], fac[3, pl.ds(mine, OWN), :]
    for j in range(8):
        c, hq = j // 4, j % 4
        val = m2[j * OWN:(j + 1) * OWN, :] * fa[:, j:j + 1] + r1[j * OWN:(j + 1) * OWN, :] * fb[:, j:j + 1]
        lhs[:, (hq * 2 + c) * LANES:(hq * 2 + c + 1) * LANES] = val.astype(jnp.bfloat16)

    def right_copy(k):
        return pltpu.make_async_remote_copy(
            src_ref=sr.at[k], dst_ref=rr.at[k], send_sem=right_send, recv_sem=right_recv.at[k],
            device_id={'tp': z + 1}, device_id_type=MESH)

    def left_copy(k):
        return pltpu.make_async_remote_copy(
            src_ref=sl.at[k], dst_ref=rl.at[k], send_sem=left_send, recv_sem=left_recv.at[k],
            device_id={'tp': z - 1}, device_id_type=MESH)

    def part_copy(k):
        return pltpu.make_async_remote_copy(
            src_ref=s_all.at[sp, k], dst_ref=s_all.at[sp, k], send_sem=part_send, recv_sem=part_recv,
            device_id={'sp': partner}, device_id_type=MESH)

    def y_copy(k):
        return pltpu.make_async_remote_copy(
            src_ref=s_all.at[sp, k], dst_ref=s_all.at[sp, k], send_sem=y_send, recv_sem=y_recv.at[k],
            device_id={'sp': ypeer}, device_id_type=MESH)

    def fwd_copy(k):
        return pltpu.make_async_remote_copy(
            src_ref=s_all.at[ypeer, k], dst_ref=s_all.at[ypeer, k], send_sem=f_send, recv_sem=f_recv,
            device_id={'sp': partner}, device_id_type=MESH)

    def whole(ref, sem):
        return pltpu.make_async_copy(ref, ref, sem)

    hop = 5
    lag_r = hop * z
    lag_l = hop * (3 - z)
    lag_s = hop * (3 - (z * (3 - z)) // 2)

    def tick(i, carry):
        @pl.when(i < NC)
        def _():
            group, place = i // WG, i % WG

            @pl.when(place == 0)
            def _():
                wo_copy(group).wait()

            w_c = wo_buf[group, :, pl.ds(pl.multiple_of(place * CW, CW), CW)]
            p_buf[i] = jnp.dot(lhs[...], w_c, preferred_element_type=jnp.float32)

        kr = i - lag_r

        @pl.when(jnp.logical_and(kr >= 0, kr < NC))
        def _():
            @pl.when(z > 0)
            def _():
                right_copy(kr).wait_recv()

            @pl.when(z < 3)
            def _():
                sr[kr] = p_buf[kr] + rr[kr]
                right_copy(kr).start()

        kl = i - lag_l

        @pl.when(jnp.logical_and(kl >= 0, kl < NC))
        def _():
            @pl.when(z < 3)
            def _():
                left_copy(kl).wait_recv()

            @pl.when(z > 0)
            def _():
                sl[kl] = p_buf[kl] + rl[kl]
                left_copy(kl).start()

        k_s = i - lag_s

        @pl.when(jnp.logical_and(k_s >= 0, k_s < NC))
        def _():
            s_all[sp, k_s] = p_buf[k_s] + rr[k_s] + rl[k_s]
            y_copy(k_s).start()
            part_copy(k_s).start()

        k_y = i - lag_s - hop

        @pl.when(jnp.logical_and(k_y >= 0, k_y < NC))
        def _():
            y_copy(k_y).wait_recv()
            fwd_copy(k_y).start()

        return carry

    lax.fori_loop(0, NC + 4 * hop, tick, 0)

    @pl.when(z < 3)
    def _():
        whole(sr, right_send).wait()

    @pl.when(z > 0)
    def _():
        whole(sl, left_send).wait()

    whole(s_all.at[sp], y_send).wait()
    whole(s_all.at[sp], part_send).wait()
    whole(s_all.at[ypeer], f_send).wait()
    whole(s_all.at[partner], part_recv).wait()
    whole(s_all.at[3 - sp], f_recv).wait()


def finish_kernel(s_all, x_ref, wpost_ref, out_h, out_buf, sem):
    blk = 16

    def out_copy(i):
        rows = pl.ds(i * blk, blk)
        return pltpu.make_async_copy(out_buf.at[rows], out_h.at[rows], sem)

    for i in range(ROWS // blk):
        g, r = (i * blk) // OWN, (i * blk) % OWN
        parts = [s_all[g, k, r:r + blk, :] for k in range(NC)]
        sq = parts[0] * parts[0]
        for k in range(1, NC):
            sq = sq + parts[k] * parts[k]
        rs = lax.rsqrt(jnp.sum(sq, axis=-1, keepdims=True) * (1.0 / DM) + NORM_EPS)
        for k in range(NC):
            for hf in range(CW // LANES):
                col = k * CW + hf * LANES
                gain = 1.0 + wpost_ref[col // LANES:col // LANES + 1, :]
                val = s_all[g, k, r:r + blk, hf * LANES:(hf + 1) * LANES] * rs * gain
                cs = slice(col, col + LANES)
                out_buf[i * blk:(i + 1) * blk, cs] = (x_ref[i * blk:(i + 1) * blk, cs].astype(jnp.float32) + val).astype(jnp.bfloat16)
        out_copy(i).start()
    for i in range(ROWS // blk):
        out_copy(i).wait()


def solution(mesh):
    cache_spec = P('dp', 'sp', 'tp', None)
    hbm = pl.BlockSpec(memory_space=pltpu.HBM)
    vmem = pl.BlockSpec(memory_space=pltpu.VMEM)

    def in_hbm(arr):
        return pltpu.with_memory_space_constraint(arr, pltpu.HBM)

    def in_vmem(arr):
        return pltpu.with_memory_space_constraint(arr, pltpu.VMEM)

    def to_rows(c):
        b, t, h, d = c.shape
        return c.reshape(b, t, h, 2, LANES).transpose(0, 1, 3, 2, 4).reshape(b, t * 2 * h, LANES)

    def from_rows(r):
        return r.reshape(ROWS, TB, 2, 2, LANES).transpose(0, 1, 3, 2, 4).reshape(ROWS, TB, 2, HD)

    def local_step(x_in, cur_pos, w_pre, w_q, w_k, w_v, w_o, w_post, k_cache, v_cache):
        half = HD // 2
        inv_freq = jnp.asarray((ROPE_BASE ** (-2.0 * np.arange(half) / (2 * half))).astype(np.float32))
        kr, vr = to_rows(k_cache), to_rows(v_cache)
        f32, bf16 = jnp.float32, jnp.bfloat16
        dma = pltpu.SemaphoreType.DMA
        half_shape = (HALF,) + kr.shape[1:]
        o_far, k_far, v_far, qs, ks, vs = pl.pallas_call(
            far_kernel,
            out_shape=(jax.ShapeDtypeStruct((HROWS, LANES), f32),
                       pltpu.VMEM(half_shape, bf16), pltpu.VMEM(half_shape, bf16),
                       pltpu.VMEM((8 * RP, LANES), f32), pltpu.VMEM((8 * RP, LANES), f32), pltpu.VMEM((8 * RP, LANES), f32)),
            in_specs=[hbm] * 10,
            out_specs=(vmem,) * 6,
            scratch_shapes=[
                pltpu.SMEM((ROWS,), jnp.int32), pltpu.VMEM((1, ROWS), jnp.int32), pltpu.VMEM((1, LANES), f32),
                pltpu.VMEM((DM // LANES, LANES), f32), pltpu.VMEM((ROWS, LANES), f32), pltpu.VMEM((ROWS, LANES), f32),
                pltpu.VMEM((ROWS, DM), bf16), pltpu.VMEM((ROWS, DM), bf16),
                pltpu.VMEM((DM, 1024), bf16), pltpu.VMEM((DM, 512), bf16), pltpu.VMEM((DM, 512), bf16), pltpu.VMEM((8, ROWS, HD), f32),
                dma, dma, dma((NKP,)), dma((NCH,)),
            ],
            compiler_params=pltpu.CompilerParams(vmem_limit_bytes=40 << 20),
            cost_estimate=pl.CostEstimate(flops=2 * 10 ** 9, bytes_accessed=25 * 10 ** 6, transcendentals=0),
            name='attend_far',
        )(in_hbm(cur_pos), in_hbm(cur_pos.reshape(1, ROWS)), in_hbm(inv_freq.reshape(1, LANES)), in_hbm(x_in),
          in_hbm(w_pre.reshape(DM // LANES, LANES)), in_hbm(w_q), in_hbm(w_k), in_hbm(w_v), in_hbm(kr), in_hbm(vr))
        o_got = lax.ppermute(o_far, 'sp', [(0, 2), (1, 3), (2, 0), (3, 1)])
        o_own, k_new, v_new = pl.pallas_call(
            near_kernel,
            out_shape=(pltpu.VMEM((HROWS, LANES), f32),
                       jax.ShapeDtypeStruct(kr.shape, bf16), jax.ShapeDtypeStruct(vr.shape, bf16)),
            in_specs=[hbm, vmem, vmem, vmem, vmem, vmem, hbm, hbm],
            out_specs=(vmem, hbm, hbm),
            scratch_shapes=[
                pltpu.SMEM((ROWS,), jnp.int32), pltpu.VMEM(half_shape, bf16), pltpu.VMEM(half_shape, bf16),
                dma, dma((NCH,)), dma,
            ],
            compiler_params=pltpu.CompilerParams(vmem_limit_bytes=28 << 20),
            cost_estimate=pl.CostEstimate(flops=10 ** 10, bytes_accessed=25 * 10 ** 6, transcendentals=0),
            name='attend_near',
        )(in_hbm(cur_pos), in_vmem(qs), in_vmem(ks), in_vmem(vs), in_vmem(k_far), in_vmem(v_far), in_hbm(kr), in_hbm(vr))
        big = pltpu.VMEM((NC, OWN, CW), f32)
        sums = pl.pallas_call(
            comm_kernel,
            out_shape=pltpu.VMEM((4, NC, OWN, CW), f32),
            in_specs=[vmem, vmem, hbm],
            out_specs=vmem,
            scratch_shapes=[
                pltpu.VMEM((NC // WG, 1024, WG * CW), bf16), pltpu.VMEM((4, LANES, LANES), f32), pltpu.VMEM((MROWS, LANES), f32),
                pltpu.VMEM((8 * OWN, LANES), f32), pltpu.VMEM((MROWS, LANES), f32), pltpu.VMEM((OWN, 1024), bf16),
                big, big, big, big, big,
                dma((NC // WG,)), dma, dma,
                dma, dma((NC,)), dma, dma((NC,)),
                dma, dma, dma, dma((NC,)), dma, dma,
            ],
            compiler_params=pltpu.CompilerParams(vmem_limit_bytes=40 << 20, collective_id=0, has_side_effects=True),
            name='combine',
        )(in_vmem(o_own), o_got, in_hbm(w_o))
        x_out = pl.pallas_call(
            finish_kernel,
            out_shape=jax.ShapeDtypeStruct((ROWS, DM), bf16),
            in_specs=[vmem, vmem, vmem],
            out_specs=hbm,
            scratch_shapes=[pltpu.VMEM((ROWS, DM), bf16), dma],
            compiler_params=pltpu.CompilerParams(vmem_limit_bytes=16 << 20),
            name='finish',
        )(in_vmem(sums), x_in, w_post.reshape(DM // LANES, LANES))
        return x_out, from_rows(k_new), from_rows(v_new)

    return jax.shard_map(local_step, mesh=mesh,
                         in_specs=(P('dp', None), P('dp'), P(None), P(None, 'tp'), P(None, 'tp'), P(None, 'tp'), P('tp', None), P(None), cache_spec, cache_spec),
                         out_specs=(P('dp', None), cache_spec, cache_spec), check_vma=False)
```

```python
import functools

import jax
import jax.numpy as jnp
import numpy as np
from jax import lax
from jax.experimental import pallas as pl
from jax.experimental.pallas import tpu as pltpu
from jax.sharding import PartitionSpec as P

SOFT_CAP = 50.0
ROPE_BASE = 10000.0
NORM_EPS = 1e-6

ROWS = 128
DM = 3840
HD = 256
TB = 64
RP = 136
LANES = 128
BCH = 16
HALF = ROWS // 2
HROWS = 8 * HALF + 8
NCH = HALF // BCH
KC = 768
NKC = DM // KC
KP = 256
NKP = DM // KP
WIN = 9
SHIFT = 20.0
CW = 256
NC = DM // CW
WG = 3
OWN = 32
MROWS = 8 * OWN + 8
MESH = pl.DeviceIdType.MESH


def attend_rows(row0, nchunk, pos_ref, kbuf, vbuf, qs, ks, vs, o_ref, before, after):
    tbase = lax.axis_index('sp') * TB
    lane = lax.broadcasted_iota(jnp.int32, (8, LANES), 1)
    row = lax.broadcasted_iota(jnp.int32, (8, LANES), 0)
    row_c = row // 4
    row_h = (row // 2) % 2
    match = (((lane // 2) % 2) == row_c) & ((lane % 2) == row_h)
    match_f = jnp.where(match, 1.0, 0.0).astype(jnp.float32)
    first = row_c == 0
    t_half = [jnp.where(match, lane // 4 + 32 * hf, 1 << 20) for hf in range(2)]
    quad = lax.broadcasted_iota(jnp.int32, (16, LANES), 0) // 4
    zero = jnp.zeros((8, LANES), jnp.float32)

    def chunk(i, l_acc):
        before(i)
        tls = []
        for u in range(BCH):
            lb = i * BCH + u
            b = row0 + lb
            tl = pos_ref[b] - tbase
            tls.append(tl)
            hit = jnp.logical_and(tl >= 0, tl < TB)
            tc = jnp.clip(tl, 0, TB - 1)
            tile = tc // 4
            tgt = jnp.where(hit, tc - tile * 4, -1)
            sel = quad == tgt
            off = pl.multiple_of(tile * 16, 16)
            kn = ks[pl.ds(b, 8, stride=RP), :]
            vn = vs[pl.ds(b, 8, stride=RP), :]
            kt = kbuf[lb, pl.ds(off, 16), :].astype(jnp.float32)
            vt = vbuf[lb, pl.ds(off, 16), :].astype(jnp.float32)
            kbuf[lb, pl.ds(off, 16), :] = jnp.where(sel, jnp.concatenate([kn, kn], 0), kt).astype(jnp.bfloat16)
            vbuf[lb, pl.ds(off, 16), :] = jnp.where(sel, jnp.concatenate([vn, vn], 0), vt).astype(jnp.bfloat16)
        scores = []
        for u in range(0, BCH, 2):
            lb = i * BCH + u
            q0 = qs[pl.ds(row0 + lb, 8, stride=RP), :]
            q1 = qs[pl.ds(row0 + lb + 1, 8, stride=RP), :]
            lhs = jnp.concatenate([jnp.concatenate([q0, zero], 1), jnp.concatenate([zero, q1], 1)], 0).astype(jnp.bfloat16)
            kk = jnp.concatenate([kbuf[lb], kbuf[lb + 1]], 1)
            scores.append(lax.dot_general(lhs, kk, (((1,), (1,)), ((), ())), preferred_element_type=jnp.float32))
        weights = []
        for u in range(0, BCH, 2):
            pair = []
            for w in range(2):
                part = scores[u // 2][8 * w:8 * w + 8]
                es = []
                for hf in range(2):
                    a = part[:, hf * LANES:(hf + 1) * LANES] * match_f
                    e = pltpu.roll(a, 4, 0)
                    f = jnp.where(first, pltpu.roll(e, LANES - 2, 1), pltpu.roll(e, 2, 1))
                    s = SOFT_CAP * jnp.tanh((a + f) * (HD ** -0.5 / SOFT_CAP))
                    es.append(jnp.where(t_half[hf] <= tls[u + w], jnp.exp(s - SHIFT), 0.0))
                tot = jnp.sum(es[0] + es[1], axis=1, keepdims=True)
                inv = jnp.where(tot > 0.0, 1.0 / tot, 0.0)
                pair.append(jnp.concatenate([es[0] * inv, es[1] * inv], 1))
                l_acc = jnp.where(lane == i * BCH + u + w, tot, l_acc)
            weights.append(jnp.concatenate(pair, 0).astype(jnp.bfloat16))
        for u in range(0, BCH, 2):
            lb = i * BCH + u
            vv = jnp.concatenate([vbuf[lb], vbuf[lb + 1]], 1)
            o = jnp.dot(weights[u // 2], vv, preferred_element_type=jnp.float32)
            o_ref[pl.ds(lb, 8, stride=HALF), :] = o[0:8, 0:LANES]
            o_ref[pl.ds(lb + 1, 8, stride=HALF), :] = o[8:16, LANES:]
        after(i)
        return l_acc

    l_acc = lax.fori_loop(0, nchunk, chunk, zero)
    o_ref[pl.ds(8 * HALF, 8), :] = l_acc


def far_kernel(pos_h, posv_h, freq_h, x_h, wpre_h, wq_h, wk_h, wv_h, kc_h, vc_h,
               o_ref, kbuf, vbuf, qs, ks, vs,
               pos_ref, posv, freq, wpre_ref, cos_ref, sin_ref, x_buf, a_buf, wq_buf, wk_buf, wv_buf, acc,
               x_sem, s_sem, w_sem, ki_sem):
    row0 = (1 - lax.axis_index('sp') // 2) * HALF

    def w_start(c):
        rows = pl.ds(c * KP, KP)
        for n, (src, dst) in enumerate(((wk_h, wk_buf), (wv_h, wv_buf), (wq_h, wq_buf))):
            pltpu.make_async_copy(src.at[rows, :], dst.at[rows, :], w_sem.at[c]).start()

    def w_wait(c):
        rows = pl.ds(c * KP, KP)
        for n, (src, dst) in enumerate(((wk_h, wk_buf), (wv_h, wv_buf), (wq_h, wq_buf))):
            pltpu.make_async_copy(src.at[rows, :], dst.at[rows, :], w_sem.at[c]).wait()

    def k_in(i):
        return pltpu.make_async_copy(kc_h.at[pl.ds(row0 + i * BCH, BCH)], kbuf.at[pl.ds(i * BCH, BCH)], ki_sem.at[i])

    def v_in(i):
        return pltpu.make_async_copy(vc_h.at[pl.ds(row0 + i * BCH, BCH)], vbuf.at[pl.ds(i * BCH, BCH)], ki_sem.at[i])

    small = [pltpu.make_async_copy(a, b, s_sem) for a, b in (
        (wpre_h, wpre_ref), (posv_h, posv), (freq_h, freq), (pos_h, pos_ref))]
    for c in small:
        c.start()
    x_copy = pltpu.make_async_copy(x_h, x_buf, x_sem)
    x_copy.start()
    for c in range(3):
        w_start(c)
    for c in small:
        c.wait()
    for c in range(3, WIN):
        w_start(c)
    pos_col = jnp.broadcast_to(posv[...].astype(jnp.float32), (ROWS, LANES)).T
    ang = pos_col * freq[...]
    cos_ref[...] = jnp.cos(ang)
    sin_ref[...] = jnp.sin(ang)
    x_copy.wait()

    gain = 1.0 + jnp.concatenate([wpre_ref[k:k + 1, :] for k in range(DM // LANES)], 1)

    def norm_rows(i, carry):
        r = pl.multiple_of(i * 16, 16)
        xb = x_buf[pl.ds(r, 16), :].astype(jnp.float32)
        ms = jnp.mean(xb * xb, axis=-1, keepdims=True)
        a_buf[pl.ds(r, 16), :] = (xb * lax.rsqrt(ms + NORM_EPS) * gain).astype(jnp.bfloat16)
        return carry

    lax.fori_loop(0, ROWS // 16, norm_rows, 0)

    for c in range(NKC):
        for p in range(c * (KC // KP), (c + 1) * (KC // KP)):
            w_wait(p)
            if p + WIN < NKP:
                w_start(p + WIN)
            elif (p + WIN - NKP) % 2 == 0 and (p + WIN - NKP) // 2 < NCH:
                n = (p + WIN - NKP) // 2
                k_in(n).start()
                v_in(n).start()
        rows = slice(c * KC, (c + 1) * KC)
        a_c = a_buf[:, rows]
        for i in range(8):
            if i < 2:
                w_c = wk_buf[rows, i * HD:(i + 1) * HD]
            elif i < 4:
                w_c = wv_buf[rows, (i - 2) * HD:(i - 1) * HD]
            else:
                w_c = wq_buf[rows, (i - 4) * HD:(i - 3) * HD]
            y = jnp.dot(a_c, w_c, preferred_element_type=jnp.float32)
            if c == 0:
                acc[i] = y
                continue
            y = acc[i] + y
            if c < NKC - 1:
                acc[i] = y
                continue
            lo, hi = y[:, :LANES], y[:, LANES:]
            if 2 <= i < 4:
                h = i - 2
                for rep in range(2):
                    vs[pl.ds((rep * 4 + h) * RP, ROWS), :] = lo
                    vs[pl.ds((rep * 4 + 2 + h) * RP, ROWS), :] = hi
            else:
                cos_t, sin_t = cos_ref[...], sin_ref[...]
                rlo = lo * cos_t - hi * sin_t
                rhi = hi * cos_t + lo * sin_t
                if i < 2:
                    for rep in range(2):
                        ks[pl.ds((rep * 4 + i) * RP, ROWS), :] = rlo
                        ks[pl.ds((rep * 4 + 2 + i) * RP, ROWS), :] = rhi
                else:
                    qs[pl.ds((i - 4) * RP, ROWS), :] = rlo
                    qs[pl.ds((4 + i - 4) * RP, ROWS), :] = rhi

    def before(i):
        k_in(i).wait()
        v_in(i).wait()

    attend_rows(row0, NCH, pos_ref, kbuf, vbuf, qs, ks, vs, o_ref, before, lambda i: None)


def near_kernel(pos_h, qs, ks, vs, kfar, vfar, kc_h, vc_h,
                o_ref, ko_h, vo_h,
                pos_ref, kbuf, vbuf, p_sem, ki_sem, w_sem):
    yy = lax.axis_index('sp') // 2
    row0 = yy * HALF
    far0 = (1 - yy) * HALF

    def k_in(i):
        return pltpu.make_async_copy(kc_h.at[pl.ds(row0 + i * BCH, BCH)], kbuf.at[pl.ds(i * BCH, BCH)], ki_sem.at[i])

    def v_in(i):
        return pltpu.make_async_copy(vc_h.at[pl.ds(row0 + i * BCH, BCH)], vbuf.at[pl.ds(i * BCH, BCH)], ki_sem.at[i])

    def k_out(i):
        return pltpu.make_async_copy(kbuf.at[pl.ds(i * BCH, BCH)], ko_h.at[pl.ds(row0 + i * BCH, BCH)], w_sem)

    def v_out(i):
        return pltpu.make_async_copy(vbuf.at[pl.ds(i * BCH, BCH)], vo_h.at[pl.ds(row0 + i * BCH, BCH)], w_sem)

    def kf_out(i):
        return pltpu.make_async_copy(kfar.at[pl.ds(i * BCH, BCH)], ko_h.at[pl.ds(far0 + i * BCH, BCH)], w_sem)

    def vf_out(i):
        return pltpu.make_async_copy(vfar.at[pl.ds(i * BCH, BCH)], vo_h.at[pl.ds(far0 + i * BCH, BCH)], w_sem)

    p_copy = pltpu.make_async_copy(pos_h, pos_ref, p_sem)
    p_copy.start()
    for i in range(NCH):
        k_in(i).start()
        v_in(i).start()
    p_copy.wait()

    def before(i):
        k_in(i).wait()
        v_in(i).wait()
        kf_out(i).start()
        vf_out(i).start()

    def after(i):
        k_out(i).start()
        v_out(i).start()

    attend_rows(row0, NCH, pos_ref, kbuf, vbuf, qs, ks, vs, o_ref, before, after)
    for i in range(NCH):
        kf_out(i).wait()
        vf_out(i).wait()
        k_out(i).wait()
        v_out(i).wait()


def comm_kernel(o_own, o_got, wo_h, s_all,
                wo_buf, fac, m1, m2, r1, lhs, p_buf, rr, rl, sr, sl,
                w_sem, r1_send, r1_recv,
                right_send, right_recv, left_send, left_recv,
                part_send, part_recv, y_send, y_recv, f_send, f_recv):
    z = lax.axis_index('tp')
    sp = lax.axis_index('sp')
    core = sp % 2
    partner = sp + 1 - 2 * core
    ypeer = (sp + 2) % 4

    def wo_copy(k):
        return pltpu.make_async_copy(wo_h.at[:, pl.ds(pl.multiple_of(k * WG * CW, CW), WG * CW)], wo_buf.at[k], w_sem.at[k])

    for k in range(NC // WG):
        wo_copy(k).start()

    @pl.when(z == 0)
    def _():
        rr[...] = jnp.zeros_like(rr)

    @pl.when(z == 3)
    def _():
        rl[...] = jnp.zeros_like(rl)

    bar = pltpu.get_barrier_semaphore()
    pl.semaphore_signal(bar, inc=1, device_id={'sp': partner}, device_id_type=MESH)
    pl.semaphore_signal(bar, inc=1, device_id={'sp': ypeer}, device_id_type=MESH)

    @pl.when(z > 0)
    def _():
        pl.semaphore_signal(bar, inc=1, device_id={'tp': z - 1}, device_id_type=MESH)

    @pl.when(z < 3)
    def _():
        pl.semaphore_signal(bar, inc=1, device_id={'tp': z + 1}, device_id_type=MESH)

    pl.semaphore_wait(bar, 3 + (z * (3 - z)) // 2)

    def shares(l_a, l_b, slot):
        tot = l_a + l_b
        inv = jnp.where(tot > 0.0, 1.0 / tot, 0.0)
        for w, l in enumerate((l_a, l_b)):
            fac[slot + w] = jnp.concatenate([l * inv, jnp.zeros((LANES - 8, LANES), jnp.float32)], 0).T
        return tot

    mine = pl.multiple_of(core * OWN, OWN)
    theirs = pl.multiple_of((1 - core) * OWN, OWN)
    tot = shares(o_own[pl.ds(8 * HALF, 8), :], o_got[pl.ds(8 * HALF, 8), :], 0)

    def merge_half(r0, dst):
        fa, fb = fac[0, pl.ds(r0, OWN), :], fac[1, pl.ds(r0, OWN), :]
        for j in range(8):
            rows = pl.ds(pl.multiple_of(j * HALF + r0, 8), OWN)
            dst[pl.ds(j * OWN, OWN), :] = o_own[rows, :] * fa[:, j:j + 1] + o_got[rows, :] * fb[:, j:j + 1]

    merge_half(theirs, m1)
    m1[pl.ds(8 * OWN, 8), :] = tot
    pair = pltpu.make_async_remote_copy(
        src_ref=m1, dst_ref=r1, send_sem=r1_send, recv_sem=r1_recv, device_id={'sp': partner}, device_id_type=MESH)
    pair.start()
    merge_half(mine, m2)
    pair.wait()
    shares(tot, r1[pl.ds(8 * OWN, 8), :], 2)
    fa, fb = fac[2, pl.ds(mine, OWN), :], fac[3, pl.ds(mine, OWN), :]
    for j in range(8):
        c, hq = j // 4, j % 4
        val = m2[j * OWN:(j + 1) * OWN, :] * fa[:, j:j + 1] + r1[j * OWN:(j + 1) * OWN, :] * fb[:, j:j + 1]
        lhs[:, (hq * 2 + c) * LANES:(hq * 2 + c + 1) * LANES] = val.astype(jnp.bfloat16)

    def right_copy(k):
        return pltpu.make_async_remote_copy(
            src_ref=sr.at[k], dst_ref=rr.at[k], send_sem=right_send, recv_sem=right_recv.at[k],
            device_id={'tp': z + 1}, device_id_type=MESH)

    def left_copy(k):
        return pltpu.make_async_remote_copy(
            src_ref=sl.at[k], dst_ref=rl.at[k], send_sem=left_send, recv_sem=left_recv.at[k],
            device_id={'tp': z - 1}, device_id_type=MESH)

    def part_copy(k):
        return pltpu.make_async_remote_copy(
            src_ref=s_all.at[sp, k], dst_ref=s_all.at[sp, k], send_sem=part_send, recv_sem=part_recv,
            device_id={'sp': partner}, device_id_type=MESH)

    def y_copy(k):
        return pltpu.make_async_remote_copy(
            src_ref=s_all.at[sp, k], dst_ref=s_all.at[sp, k], send_sem=y_send, recv_sem=y_recv.at[k],
            device_id={'sp': ypeer}, device_id_type=MESH)

    def fwd_copy(k):
        return pltpu.make_async_remote_copy(
            src_ref=s_all.at[ypeer, k], dst_ref=s_all.at[ypeer, k], send_sem=f_send, recv_sem=f_recv,
            device_id={'sp': partner}, device_id_type=MESH)

    def whole(ref, sem):
        return pltpu.make_async_copy(ref, ref, sem)

    hop = 5
    lag_r = hop * z
    lag_l = hop * (3 - z)
    lag_s = hop * (3 - (z * (3 - z)) // 2)

    def tick(i, carry):
        @pl.when(i < NC)
        def _():
            group, place = i // WG, i % WG

            @pl.when(place == 0)
            def _():
                wo_copy(group).wait()

            w_c = wo_buf[group, :, pl.ds(pl.multiple_of(place * CW, CW), CW)]
            p_buf[i] = jnp.dot(lhs[...], w_c, preferred_element_type=jnp.float32)

        kr = i - lag_r

        @pl.when(jnp.logical_and(kr >= 0, kr < NC))
        def _():
            @pl.when(z > 0)
            def _():
                right_copy(kr).wait_recv()

            @pl.when(z < 3)
            def _():
                sr[kr] = p_buf[kr] + rr[kr]
                right_copy(kr).start()

        kl = i - lag_l

        @pl.when(jnp.logical_and(kl >= 0, kl < NC))
        def _():
            @pl.when(z < 3)
            def _():
                left_copy(kl).wait_recv()

            @pl.when(z > 0)
            def _():
                sl[kl] = p_buf[kl] + rl[kl]
                left_copy(kl).start()

        k_s = i - lag_s

        @pl.when(jnp.logical_and(k_s >= 0, k_s < NC))
        def _():
            s_all[sp, k_s] = p_buf[k_s] + rr[k_s] + rl[k_s]
            y_copy(k_s).start()
            part_copy(k_s).start()

        k_y = i - lag_s - hop

        @pl.when(jnp.logical_and(k_y >= 0, k_y < NC))
        def _():
            y_copy(k_y).wait_recv()
            fwd_copy(k_y).start()

        return carry

    lax.fori_loop(0, NC + 4 * hop, tick, 0)

    @pl.when(z < 3)
    def _():
        whole(sr, right_send).wait()

    @pl.when(z > 0)
    def _():
        whole(sl, left_send).wait()

    whole(s_all.at[sp], y_send).wait()
    whole(s_all.at[sp], part_send).wait()
    whole(s_all.at[ypeer], f_send).wait()
    whole(s_all.at[partner], part_recv).wait()
    whole(s_all.at[3 - sp], f_recv).wait()


def finish_kernel(s_all, x_ref, wpost_ref, out_h, out_buf, sem):
    blk = 16

    def out_copy(i):
        rows = pl.ds(i * blk, blk)
        return pltpu.make_async_copy(out_buf.at[rows], out_h.at[rows], sem)

    for i in range(ROWS // blk):
        g, r = (i * blk) // OWN, (i * blk) % OWN
        parts = [s_all[g, k, r:r + blk, :] for k in range(NC)]
        sq = parts[0] * parts[0]
        for k in range(1, NC):
            sq = sq + parts[k] * parts[k]
        rs = lax.rsqrt(jnp.sum(sq, axis=-1, keepdims=True) * (1.0 / DM) + NORM_EPS)
        for k in range(NC):
            for hf in range(CW // LANES):
                col = k * CW + hf * LANES
                gain = 1.0 + wpost_ref[col // LANES:col // LANES + 1, :]
                val = s_all[g, k, r:r + blk, hf * LANES:(hf + 1) * LANES] * rs * gain
                cs = slice(col, col + LANES)
                out_buf[i * blk:(i + 1) * blk, cs] = (x_ref[i * blk:(i + 1) * blk, cs].astype(jnp.float32) + val).astype(jnp.bfloat16)
        out_copy(i).start()
    for i in range(ROWS // blk):
        out_copy(i).wait()


def solution(mesh):
    cache_spec = P('dp', 'sp', 'tp', None)
    hbm = pl.BlockSpec(memory_space=pltpu.HBM)
    vmem = pl.BlockSpec(memory_space=pltpu.VMEM)

    def in_hbm(arr):
        return pltpu.with_memory_space_constraint(arr, pltpu.HBM)

    def in_vmem(arr):
        return pltpu.with_memory_space_constraint(arr, pltpu.VMEM)

    def to_rows(c):
        b, t, h, d = c.shape
        return c.reshape(b, t, h, 2, LANES).transpose(0, 1, 3, 2, 4).reshape(b, t * 2 * h, LANES)

    def from_rows(r):
        return r.reshape(ROWS, TB, 2, 2, LANES).transpose(0, 1, 3, 2, 4).reshape(ROWS, TB, 2, HD)

    def local_step(x_in, cur_pos, w_pre, w_q, w_k, w_v, w_o, w_post, k_cache, v_cache):
        half = HD // 2
        inv_freq = jnp.asarray((ROPE_BASE ** (-2.0 * np.arange(half) / (2 * half))).astype(np.float32))
        kr, vr = to_rows(k_cache), to_rows(v_cache)
        f32, bf16 = jnp.float32, jnp.bfloat16
        dma = pltpu.SemaphoreType.DMA
        half_shape = (HALF,) + kr.shape[1:]
        o_far, k_far, v_far, qs, ks, vs = pl.pallas_call(
            far_kernel,
            out_shape=(jax.ShapeDtypeStruct((HROWS, LANES), f32),
                       pltpu.VMEM(half_shape, bf16), pltpu.VMEM(half_shape, bf16),
                       pltpu.VMEM((8 * RP, LANES), f32), pltpu.VMEM((8 * RP, LANES), f32), pltpu.VMEM((8 * RP, LANES), f32)),
            in_specs=[hbm] * 10,
            out_specs=(vmem,) * 6,
            scratch_shapes=[
                pltpu.SMEM((ROWS,), jnp.int32), pltpu.VMEM((1, ROWS), jnp.int32), pltpu.VMEM((1, LANES), f32),
                pltpu.VMEM((DM // LANES, LANES), f32), pltpu.VMEM((ROWS, LANES), f32), pltpu.VMEM((ROWS, LANES), f32),
                pltpu.VMEM((ROWS, DM), bf16), pltpu.VMEM((ROWS, DM), bf16),
                pltpu.VMEM((DM, 1024), bf16), pltpu.VMEM((DM, 512), bf16), pltpu.VMEM((DM, 512), bf16), pltpu.VMEM((8, ROWS, HD), f32),
                dma, dma, dma((NKP,)), dma((NCH,)),
            ],
            compiler_params=pltpu.CompilerParams(vmem_limit_bytes=40 << 20),
            cost_estimate=pl.CostEstimate(flops=2 * 10 ** 9, bytes_accessed=25 * 10 ** 6, transcendentals=0),
            name='attend_far',
        )(in_hbm(cur_pos), in_hbm(cur_pos.reshape(1, ROWS)), in_hbm(inv_freq.reshape(1, LANES)), in_hbm(x_in),
          in_hbm(w_pre.reshape(DM // LANES, LANES)), in_hbm(w_q), in_hbm(w_k), in_hbm(w_v), in_hbm(kr), in_hbm(vr))
        o_got = lax.ppermute(o_far, 'sp', [(0, 2), (1, 3), (2, 0), (3, 1)])
        o_own, k_new, v_new = pl.pallas_call(
            near_kernel,
            out_shape=(pltpu.VMEM((HROWS, LANES), f32),
                       jax.ShapeDtypeStruct(kr.shape, bf16), jax.ShapeDtypeStruct(vr.shape, bf16)),
            in_specs=[hbm, vmem, vmem, vmem, vmem, vmem, hbm, hbm],
            out_specs=(vmem, hbm, hbm),
            scratch_shapes=[
                pltpu.SMEM((ROWS,), jnp.int32), pltpu.VMEM(half_shape, bf16), pltpu.VMEM(half_shape, bf16),
                dma, dma((NCH,)), dma,
            ],
            compiler_params=pltpu.CompilerParams(vmem_limit_bytes=28 << 20),
            cost_estimate=pl.CostEstimate(flops=10 ** 10, bytes_accessed=25 * 10 ** 6, transcendentals=0),
            name='attend_near',
        )(in_hbm(cur_pos), in_vmem(qs), in_vmem(ks), in_vmem(vs), in_vmem(k_far), in_vmem(v_far), in_hbm(kr), in_hbm(vr))
        big = pltpu.VMEM((NC, OWN, CW), f32)
        sums = pl.pallas_call(
            comm_kernel,
            out_shape=pltpu.VMEM((4, NC, OWN, CW), f32),
            in_specs=[vmem, vmem, hbm],
            out_specs=vmem,
            scratch_shapes=[
                pltpu.VMEM((NC // WG, 1024, WG * CW), bf16), pltpu.VMEM((4, LANES, LANES), f32), pltpu.VMEM((MROWS, LANES), f32),
                pltpu.VMEM((8 * OWN, LANES), f32), pltpu.VMEM((MROWS, LANES), f32), pltpu.VMEM((OWN, 1024), bf16),
                big, big, big, big, big,
                dma((NC // WG,)), dma, dma,
                dma, dma((NC,)), dma, dma((NC,)),
                dma, dma, dma, dma((NC,)), dma, dma,
            ],
            compiler_params=pltpu.CompilerParams(vmem_limit_bytes=40 << 20, collective_id=0, has_side_effects=True),
            name='combine',
        )(in_vmem(o_own), o_got, in_hbm(w_o))
        x_out = pl.pallas_call(
            finish_kernel,
            out_shape=jax.ShapeDtypeStruct((ROWS, DM), bf16),
            in_specs=[vmem, vmem, vmem],
            out_specs=hbm,
            scratch_shapes=[pltpu.VMEM((ROWS, DM), bf16), dma],
            compiler_params=pltpu.CompilerParams(vmem_limit_bytes=16 << 20),
            name='finish',
        )(in_vmem(sums), x_in, w_post.reshape(DM // LANES, LANES))
        return x_out, from_rows(k_new), from_rows(v_new)

    return jax.shard_map(local_step, mesh=mesh,
                         in_specs=(P('dp', None), P('dp'), P(None), P(None, 'tp'), P(None, 'tp'), P(None, 'tp'), P('tp', None), P(None), cache_spec, cache_spec),
                         out_specs=(P('dp', None), cache_spec, cache_spec), check_vma=False)
```

```python
import functools

import jax
import jax.numpy as jnp
import numpy as np
from jax import lax
from jax.experimental import pallas as pl
from jax.experimental.pallas import tpu as pltpu
from jax.sharding import PartitionSpec as P

SOFT_CAP = 50.0
ROPE_BASE = 10000.0
NORM_EPS = 1e-6

ROWS = 128
DM = 3840
HD = 256
TB = 64
RP = 136
LANES = 128
BCH = 16
HALF = ROWS // 2
HROWS = 8 * HALF + 8
NCH = HALF // BCH
KC = 768
NKC = DM // KC
SHIFT = 20.0
CW = 256
NC = DM // CW
WG = 3
OWN = 32
MROWS = 8 * OWN + 8
MESH = pl.DeviceIdType.MESH


def attend_rows(row0, nchunk, pos_ref, kbuf, vbuf, qs, ks, vs, o_ref, before, after):
    tbase = lax.axis_index('sp') * TB
    lane = lax.broadcasted_iota(jnp.int32, (8, LANES), 1)
    row = lax.broadcasted_iota(jnp.int32, (8, LANES), 0)
    row_c = row // 4
    row_h = (row // 2) % 2
    match = (((lane // 2) % 2) == row_c) & ((lane % 2) == row_h)
    match_f = jnp.where(match, 1.0, 0.0).astype(jnp.float32)
    first = row_c == 0
    t_half = [jnp.where(match, lane // 4 + 32 * hf, 1 << 20) for hf in range(2)]
    quad = lax.broadcasted_iota(jnp.int32, (16, LANES), 0) // 4
    zero = jnp.zeros((8, LANES), jnp.float32)

    def chunk(i, l_acc):
        before(i)
        tls = []
        for u in range(BCH):
            lb = i * BCH + u
            b = row0 + lb
            tl = pos_ref[b] - tbase
            tls.append(tl)
            hit = jnp.logical_and(tl >= 0, tl < TB)
            tc = jnp.clip(tl, 0, TB - 1)
            tile = tc // 4
            tgt = jnp.where(hit, tc - tile * 4, -1)
            sel = quad == tgt
            off = pl.multiple_of(tile * 16, 16)
            kn = ks[pl.ds(b, 8, stride=RP), :]
            vn = vs[pl.ds(b, 8, stride=RP), :]
            kt = kbuf[lb, pl.ds(off, 16), :].astype(jnp.float32)
            vt = vbuf[lb, pl.ds(off, 16), :].astype(jnp.float32)
            kbuf[lb, pl.ds(off, 16), :] = jnp.where(sel, jnp.concatenate([kn, kn], 0), kt).astype(jnp.bfloat16)
            vbuf[lb, pl.ds(off, 16), :] = jnp.where(sel, jnp.concatenate([vn, vn], 0), vt).astype(jnp.bfloat16)
        scores = []
        for u in range(0, BCH, 2):
            lb = i * BCH + u
            q0 = qs[pl.ds(row0 + lb, 8, stride=RP), :]
            q1 = qs[pl.ds(row0 + lb + 1, 8, stride=RP), :]
            lhs = jnp.concatenate([jnp.concatenate([q0, zero], 1), jnp.concatenate([zero, q1], 1)], 0).astype(jnp.bfloat16)
            kk = jnp.concatenate([kbuf[lb], kbuf[lb + 1]], 1)
            scores.append(lax.dot_general(lhs, kk, (((1,), (1,)), ((), ())), preferred_element_type=jnp.float32))
        weights = []
        for u in range(0, BCH, 2):
            pair = []
            for w in range(2):
                part = scores[u // 2][8 * w:8 * w + 8]
                es = []
                for hf in range(2):
                    a = part[:, hf * LANES:(hf + 1) * LANES] * match_f
                    e = pltpu.roll(a, 4, 0)
                    f = jnp.where(first, pltpu.roll(e, LANES - 2, 1), pltpu.roll(e, 2, 1))
                    s = SOFT_CAP * jnp.tanh((a + f) * (HD ** -0.5 / SOFT_CAP))
                    es.append(jnp.where(t_half[hf] <= tls[u + w], jnp.exp(s - SHIFT), 0.0))
                tot = jnp.sum(es[0] + es[1], axis=1, keepdims=True)
                inv = jnp.where(tot > 0.0, 1.0 / tot, 0.0)
                pair.append(jnp.concatenate([es[0] * inv, es[1] * inv], 1))
                l_acc = jnp.where(lane == i * BCH + u + w, tot, l_acc)
            weights.append(jnp.concatenate(pair, 0).astype(jnp.bfloat16))
        for u in range(0, BCH, 2):
            lb = i * BCH + u
            vv = jnp.concatenate([vbuf[lb], vbuf[lb + 1]], 1)
            o = jnp.dot(weights[u // 2], vv, preferred_element_type=jnp.float32)
            o_ref[pl.ds(lb, 8, stride=HALF), :] = o[0:8, 0:LANES]
            o_ref[pl.ds(lb + 1, 8, stride=HALF), :] = o[8:16, LANES:]
        after(i)
        return l_acc

    l_acc = lax.fori_loop(0, nchunk, chunk, zero)
    o_ref[pl.ds(8 * HALF, 8), :] = l_acc


def far_kernel(pos_h, posv_h, freq_h, x_h, wpre_h, wq_h, wk_h, wv_h, kc_h, vc_h,
               o_ref, kbuf, vbuf, qs, ks, vs,
               pos_ref, posv, freq, wpre_ref, cos_ref, sin_ref, x_buf, a_buf, wq_buf, wk_buf, wv_buf, acc,
               x_sem, s_sem, w_sem, ki_sem):
    row0 = (1 - lax.axis_index('sp') // 2) * HALF

    def w_start(c):
        rows = pl.ds(c * KC, KC)
        for n, (src, dst) in enumerate(((wk_h, wk_buf), (wv_h, wv_buf), (wq_h, wq_buf))):
            pltpu.make_async_copy(src.at[rows, :], dst.at[rows, :], w_sem.at[c]).start()

    def w_wait(c):
        rows = pl.ds(c * KC, KC)
        for n, (src, dst) in enumerate(((wk_h, wk_buf), (wv_h, wv_buf), (wq_h, wq_buf))):
            pltpu.make_async_copy(src.at[rows, :], dst.at[rows, :], w_sem.at[c]).wait()

    def k_in(i):
        return pltpu.make_async_copy(kc_h.at[pl.ds(row0 + i * BCH, BCH)], kbuf.at[pl.ds(i * BCH, BCH)], ki_sem.at[i])

    def v_in(i):
        return pltpu.make_async_copy(vc_h.at[pl.ds(row0 + i * BCH, BCH)], vbuf.at[pl.ds(i * BCH, BCH)], ki_sem.at[i])

    small = [pltpu.make_async_copy(a, b, s_sem) for a, b in (
        (wpre_h, wpre_ref), (posv_h, posv), (freq_h, freq), (pos_h, pos_ref))]
    for c in small:
        c.start()
    x_copy = pltpu.make_async_copy(x_h, x_buf, x_sem)
    x_copy.start()
    w_start(0)
    for c in small:
        c.wait()
    w_start(1)
    pos_col = jnp.broadcast_to(posv[...].astype(jnp.float32), (ROWS, LANES)).T
    ang = pos_col * freq[...]
    cos_ref[...] = jnp.cos(ang)
    sin_ref[...] = jnp.sin(ang)
    x_copy.wait()
    w_start(2)

    gain = 1.0 + jnp.concatenate([wpre_ref[k:k + 1, :] for k in range(DM // LANES)], 1)

    def norm_rows(i, carry):
        r = pl.multiple_of(i * 16, 16)
        xb = x_buf[pl.ds(r, 16), :].astype(jnp.float32)
        ms = jnp.mean(xb * xb, axis=-1, keepdims=True)
        a_buf[pl.ds(r, 16), :] = (xb * lax.rsqrt(ms + NORM_EPS) * gain).astype(jnp.bfloat16)
        return carry

    lax.fori_loop(0, ROWS // 16, norm_rows, 0)

    for c in range(NKC):
        w_wait(c)
        if c + 3 < NKC:
            w_start(c + 3)
        for n in ((), (), (0,), (1,), (2, 3))[c]:
            k_in(n).start()
            v_in(n).start()
        rows = slice(c * KC, (c + 1) * KC)
        a_c = a_buf[:, rows]
        for i in range(8):
            if i < 2:
                w_c = wk_buf[rows, i * HD:(i + 1) * HD]
            elif i < 4:
                w_c = wv_buf[rows, (i - 2) * HD:(i - 1) * HD]
            else:
                w_c = wq_buf[rows, (i - 4) * HD:(i - 3) * HD]
            y = jnp.dot(a_c, w_c, preferred_element_type=jnp.float32)
            if c == 0:
                acc[i] = y
                continue
            y = acc[i] + y
            if c < NKC - 1:
                acc[i] = y
                continue
            lo, hi = y[:, :LANES], y[:, LANES:]
            if 2 <= i < 4:
                h = i - 2
                for rep in range(2):
                    vs[pl.ds((rep * 4 + h) * RP, ROWS), :] = lo
                    vs[pl.ds((rep * 4 + 2 + h) * RP, ROWS), :] = hi
            else:
                cos_t, sin_t = cos_ref[...], sin_ref[...]
                rlo = lo * cos_t - hi * sin_t
                rhi = hi * cos_t + lo * sin_t
                if i < 2:
                    for rep in range(2):
                        ks[pl.ds((rep * 4 + i) * RP, ROWS), :] = rlo
                        ks[pl.ds((rep * 4 + 2 + i) * RP, ROWS), :] = rhi
                else:
                    qs[pl.ds((i - 4) * RP, ROWS), :] = rlo
                    qs[pl.ds((4 + i - 4) * RP, ROWS), :] = rhi

    def before(i):
        k_in(i).wait()
        v_in(i).wait()

    attend_rows(row0, NCH, pos_ref, kbuf, vbuf, qs, ks, vs, o_ref, before, lambda i: None)


def near_kernel(pos_h, qs, ks, vs, kfar, vfar, kc_h, vc_h,
                o_ref, ko_h, vo_h,
                pos_ref, kbuf, vbuf, p_sem, ki_sem, w_sem):
    yy = lax.axis_index('sp') // 2
    row0 = yy * HALF
    far0 = (1 - yy) * HALF

    def k_in(i):
        return pltpu.make_async_copy(kc_h.at[pl.ds(row0 + i * BCH, BCH)], kbuf.at[pl.ds(i * BCH, BCH)], ki_sem.at[i])

    def v_in(i):
        return pltpu.make_async_copy(vc_h.at[pl.ds(row0 + i * BCH, BCH)], vbuf.at[pl.ds(i * BCH, BCH)], ki_sem.at[i])

    def k_out(i):
        return pltpu.make_async_copy(kbuf.at[pl.ds(i * BCH, BCH)], ko_h.at[pl.ds(row0 + i * BCH, BCH)], w_sem)

    def v_out(i):
        return pltpu.make_async_copy(vbuf.at[pl.ds(i * BCH, BCH)], vo_h.at[pl.ds(row0 + i * BCH, BCH)], w_sem)

    def kf_out(i):
        return pltpu.make_async_copy(kfar.at[pl.ds(i * BCH, BCH)], ko_h.at[pl.ds(far0 + i * BCH, BCH)], w_sem)

    def vf_out(i):
        return pltpu.make_async_copy(vfar.at[pl.ds(i * BCH, BCH)], vo_h.at[pl.ds(far0 + i * BCH, BCH)], w_sem)

    p_copy = pltpu.make_async_copy(pos_h, pos_ref, p_sem)
    p_copy.start()
    for i in range(NCH):
        k_in(i).start()
        v_in(i).start()
    p_copy.wait()

    def before(i):
        k_in(i).wait()
        v_in(i).wait()
        kf_out(i).start()
        vf_out(i).start()

    def after(i):
        k_out(i).start()
        v_out(i).start()

    attend_rows(row0, NCH, pos_ref, kbuf, vbuf, qs, ks, vs, o_ref, before, after)
    for i in range(NCH):
        kf_out(i).wait()
        vf_out(i).wait()
        k_out(i).wait()
        v_out(i).wait()


def comm_kernel(o_own, o_got, wo_h, s_all,
                wo_buf, fac, m1, m2, r1, lhs, p_buf, rr, rl, sr, sl,
                w_sem, r1_send, r1_recv,
                right_send, right_recv, left_send, left_recv,
                part_send, part_recv, y_send, y_recv, f_send, f_recv):
    z = lax.axis_index('tp')
    sp = lax.axis_index('sp')
    core = sp % 2
    partner = sp + 1 - 2 * core
    ypeer = (sp + 2) % 4

    def wo_copy(k):
        return pltpu.make_async_copy(wo_h.at[:, pl.ds(pl.multiple_of(k * WG * CW, CW), WG * CW)], wo_buf.at[k], w_sem.at[k])

    for k in range(NC // WG):
        wo_copy(k).start()

    @pl.when(z == 0)
    def _():
        rr[...] = jnp.zeros_like(rr)

    @pl.when(z == 3)
    def _():
        rl[...] = jnp.zeros_like(rl)

    bar = pltpu.get_barrier_semaphore()
    pl.semaphore_signal(bar, inc=1, device_id={'sp': partner}, device_id_type=MESH)
    pl.semaphore_signal(bar, inc=1, device_id={'sp': ypeer}, device_id_type=MESH)

    @pl.when(z > 0)
    def _():
        pl.semaphore_signal(bar, inc=1, device_id={'tp': z - 1}, device_id_type=MESH)

    @pl.when(z < 3)
    def _():
        pl.semaphore_signal(bar, inc=1, device_id={'tp': z + 1}, device_id_type=MESH)

    def shares(l_a, l_b, slot):
        tot = l_a + l_b
        inv = jnp.where(tot > 0.0, 1.0 / tot, 0.0)
        for w, l in enumerate((l_a, l_b)):
            fac[slot + w] = jnp.concatenate([l * inv, jnp.zeros((LANES - 8, LANES), jnp.float32)], 0).T
        return tot

    mine = pl.multiple_of(core * OWN, OWN)
    theirs = pl.multiple_of((1 - core) * OWN, OWN)
    tot = shares(o_own[pl.ds(8 * HALF, 8), :], o_got[pl.ds(8 * HALF, 8), :], 0)

    def merge_half(r0, dst):
        fa, fb = fac[0, pl.ds(r0, OWN), :], fac[1, pl.ds(r0, OWN), :]
        for j in range(8):
            rows = pl.ds(pl.multiple_of(j * HALF + r0, 8), OWN)
            dst[pl.ds(j * OWN, OWN), :] = o_own[rows, :] * fa[:, j:j + 1] + o_got[rows, :] * fb[:, j:j + 1]

    merge_half(theirs, m1)
    m1[pl.ds(8 * OWN, 8), :] = tot
    merge_half(mine, m2)
    pair = pltpu.make_async_remote_copy(
        src_ref=m1, dst_ref=r1, send_sem=r1_send, recv_sem=r1_recv, device_id={'sp': partner}, device_id_type=MESH)
    pl.semaphore_wait(bar, 3 + (z * (3 - z)) // 2)
    pair.start()
    pair.wait()
    shares(tot, r1[pl.ds(8 * OWN, 8), :], 2)
    fa, fb = fac[2, pl.ds(mine, OWN), :], fac[3, pl.ds(mine, OWN), :]
    for j in range(8):
        c, hq = j // 4, j % 4
        val = m2[j * OWN:(j + 1) * OWN, :] * fa[:, j:j + 1] + r1[j * OWN:(j + 1) * OWN, :] * fb[:, j:j + 1]
        lhs[:, (hq * 2 + c) * LANES:(hq * 2 + c + 1) * LANES] = val.astype(jnp.bfloat16)

    def right_copy(k):
        return pltpu.make_async_remote_copy(
            src_ref=sr.at[k], dst_ref=rr.at[k], send_sem=right_send, recv_sem=right_recv.at[k],
            device_id={'tp': z + 1}, device_id_type=MESH)

    def left_copy(k):
        return pltpu.make_async_remote_copy(
            src_ref=sl.at[k], dst_ref=rl.at[k], send_sem=left_send, recv_sem=left_recv.at[k],
            device_id={'tp': z - 1}, device_id_type=MESH)

    def part_copy(k):
        return pltpu.make_async_remote_copy(
            src_ref=s_all.at[sp, k], dst_ref=s_all.at[sp, k], send_sem=part_send, recv_sem=part_recv,
            device_id={'sp': partner}, device_id_type=MESH)

    def y_copy(k):
        return pltpu.make_async_remote_copy(
            src_ref=s_all.at[sp, k], dst_ref=s_all.at[sp, k], send_sem=y_send, recv_sem=y_recv.at[k],
            device_id={'sp': ypeer}, device_id_type=MESH)

    def fwd_copy(k):
        return pltpu.make_async_remote_copy(
            src_ref=s_all.at[ypeer, k], dst_ref=s_all.at[ypeer, k], send_sem=f_send, recv_sem=f_recv,
            device_id={'sp': partner}, device_id_type=MESH)

    def whole(ref, sem):
        return pltpu.make_async_copy(ref, ref, sem)

    hop = 5
    lag_r = hop * z
    lag_l = hop * (3 - z)
    lag_s = hop * (3 - (z * (3 - z)) // 2)

    def tick(i, carry):
        @pl.when(i < NC)
        def _():
            group, place = i // WG, i % WG

            @pl.when(place == 0)
            def _():
                wo_copy(group).wait()

            w_c = wo_buf[group, :, pl.ds(pl.multiple_of(place * CW, CW), CW)]
            p_buf[i] = jnp.dot(lhs[...], w_c, preferred_element_type=jnp.float32)

        kr = i - lag_r

        @pl.when(jnp.logical_and(kr >= 0, kr < NC))
        def _():
            @pl.when(z > 0)
            def _():
                right_copy(kr).wait_recv()

            @pl.when(z < 3)
            def _():
                sr[kr] = p_buf[kr] + rr[kr]
                right_copy(kr).start()

        kl = i - lag_l

        @pl.when(jnp.logical_and(kl >= 0, kl < NC))
        def _():
            @pl.when(z < 3)
            def _():
                left_copy(kl).wait_recv()

            @pl.when(z > 0)
            def _():
                sl[kl] = p_buf[kl] + rl[kl]
                left_copy(kl).start()

        k_s = i - lag_s

        @pl.when(jnp.logical_and(k_s >= 0, k_s < NC))
        def _():
            s_all[sp, k_s] = p_buf[k_s] + rr[k_s] + rl[k_s]
            y_copy(k_s).start()
            part_copy(k_s).start()

        k_y = i - lag_s - hop

        @pl.when(jnp.logical_and(k_y >= 0, k_y < NC))
        def _():
            y_copy(k_y).wait_recv()
            fwd_copy(k_y).start()

        return carry

    lax.fori_loop(0, NC + 4 * hop, tick, 0)

    @pl.when(z < 3)
    def _():
        whole(sr, right_send).wait()

    @pl.when(z > 0)
    def _():
        whole(sl, left_send).wait()

    whole(s_all.at[sp], y_send).wait()
    whole(s_all.at[sp], part_send).wait()
    whole(s_all.at[ypeer], f_send).wait()
    whole(s_all.at[partner], part_recv).wait()
    whole(s_all.at[3 - sp], f_recv).wait()


def finish_kernel(s_all, x_ref, wpost_ref, out_h, out_buf, sem):
    blk = 16

    def out_copy(i):
        rows = pl.ds(i * blk, blk)
        return pltpu.make_async_copy(out_buf.at[rows], out_h.at[rows], sem)

    for i in range(ROWS // blk):
        g, r = (i * blk) // OWN, (i * blk) % OWN
        parts = [s_all[g, k, r:r + blk, :] for k in range(NC)]
        sq = parts[0] * parts[0]
        for k in range(1, NC):
            sq = sq + parts[k] * parts[k]
        rs = lax.rsqrt(jnp.sum(sq, axis=-1, keepdims=True) * (1.0 / DM) + NORM_EPS)
        for k in range(NC):
            for hf in range(CW // LANES):
                col = k * CW + hf * LANES
                gain = 1.0 + wpost_ref[col // LANES:col // LANES + 1, :]
                val = s_all[g, k, r:r + blk, hf * LANES:(hf + 1) * LANES] * rs * gain
                cs = slice(col, col + LANES)
                out_buf[i * blk:(i + 1) * blk, cs] = (x_ref[i * blk:(i + 1) * blk, cs].astype(jnp.float32) + val).astype(jnp.bfloat16)
        out_copy(i).start()
    for i in range(ROWS // blk):
        out_copy(i).wait()


def solution(mesh):
    cache_spec = P('dp', 'sp', 'tp', None)
    hbm = pl.BlockSpec(memory_space=pltpu.HBM)
    vmem = pl.BlockSpec(memory_space=pltpu.VMEM)

    def in_hbm(arr):
        return pltpu.with_memory_space_constraint(arr, pltpu.HBM)

    def in_vmem(arr):
        return pltpu.with_memory_space_constraint(arr, pltpu.VMEM)

    def to_rows(c):
        b, t, h, d = c.shape
        return c.reshape(b, t, h, 2, LANES).transpose(0, 1, 3, 2, 4).reshape(b, t * 2 * h, LANES)

    def from_rows(r):
        return r.reshape(ROWS, TB, 2, 2, LANES).transpose(0, 1, 3, 2, 4).reshape(ROWS, TB, 2, HD)

    def local_step(x_in, cur_pos, w_pre, w_q, w_k, w_v, w_o, w_post, k_cache, v_cache):
        half = HD // 2
        inv_freq = jnp.asarray((ROPE_BASE ** (-2.0 * np.arange(half) / (2 * half))).astype(np.float32))
        kr, vr = to_rows(k_cache), to_rows(v_cache)
        f32, bf16 = jnp.float32, jnp.bfloat16
        dma = pltpu.SemaphoreType.DMA
        half_shape = (HALF,) + kr.shape[1:]
        o_far, k_far, v_far, qs, ks, vs = pl.pallas_call(
            far_kernel,
            out_shape=(jax.ShapeDtypeStruct((HROWS, LANES), f32),
                       pltpu.VMEM(half_shape, bf16), pltpu.VMEM(half_shape, bf16),
                       pltpu.VMEM((8 * RP, LANES), f32), pltpu.VMEM((8 * RP, LANES), f32), pltpu.VMEM((8 * RP, LANES), f32)),
            in_specs=[hbm] * 10,
            out_specs=(vmem,) * 6,
            scratch_shapes=[
                pltpu.SMEM((ROWS,), jnp.int32), pltpu.VMEM((1, ROWS), jnp.int32), pltpu.VMEM((1, LANES), f32),
                pltpu.VMEM((DM // LANES, LANES), f32), pltpu.VMEM((ROWS, LANES), f32), pltpu.VMEM((ROWS, LANES), f32),
                pltpu.VMEM((ROWS, DM), bf16), pltpu.VMEM((ROWS, DM), bf16),
                pltpu.VMEM((DM, 1024), bf16), pltpu.VMEM((DM, 512), bf16), pltpu.VMEM((DM, 512), bf16), pltpu.VMEM((8, ROWS, HD), f32),
                dma, dma, dma((NKC,)), dma((NCH,)),
            ],
            compiler_params=pltpu.CompilerParams(vmem_limit_bytes=40 << 20),
            cost_estimate=pl.CostEstimate(flops=2 * 10 ** 9, bytes_accessed=25 * 10 ** 6, transcendentals=0),
            name='attend_far',
        )(in_hbm(cur_pos), in_hbm(cur_pos.reshape(1, ROWS)), in_hbm(inv_freq.reshape(1, LANES)), in_hbm(x_in),
          in_hbm(w_pre.reshape(DM // LANES, LANES)), in_hbm(w_q), in_hbm(w_k), in_hbm(w_v), in_hbm(kr), in_hbm(vr))
        o_got = lax.ppermute(o_far, 'sp', [(0, 2), (1, 3), (2, 0), (3, 1)])
        o_own, k_new, v_new = pl.pallas_call(
            near_kernel,
            out_shape=(pltpu.VMEM((HROWS, LANES), f32),
                       jax.ShapeDtypeStruct(kr.shape, bf16), jax.ShapeDtypeStruct(vr.shape, bf16)),
            in_specs=[hbm, vmem, vmem, vmem, vmem, vmem, hbm, hbm],
            out_specs=(vmem, hbm, hbm),
            scratch_shapes=[
                pltpu.SMEM((ROWS,), jnp.int32), pltpu.VMEM(half_shape, bf16), pltpu.VMEM(half_shape, bf16),
                dma, dma((NCH,)), dma,
            ],
            compiler_params=pltpu.CompilerParams(vmem_limit_bytes=28 << 20),
            cost_estimate=pl.CostEstimate(flops=10 ** 10, bytes_accessed=25 * 10 ** 6, transcendentals=0),
            name='attend_near',
        )(in_hbm(cur_pos), in_vmem(qs), in_vmem(ks), in_vmem(vs), in_vmem(k_far), in_vmem(v_far), in_hbm(kr), in_hbm(vr))
        big = pltpu.VMEM((NC, OWN, CW), f32)
        sums = pl.pallas_call(
            comm_kernel,
            out_shape=pltpu.VMEM((4, NC, OWN, CW), f32),
            in_specs=[vmem, vmem, hbm],
            out_specs=vmem,
            scratch_shapes=[
                pltpu.VMEM((NC // WG, 1024, WG * CW), bf16), pltpu.VMEM((4, LANES, LANES), f32), pltpu.VMEM((MROWS, LANES), f32),
                pltpu.VMEM((8 * OWN, LANES), f32), pltpu.VMEM((MROWS, LANES), f32), pltpu.VMEM((OWN, 1024), bf16),
                big, big, big, big, big,
                dma((NC // WG,)), dma, dma,
                dma, dma((NC,)), dma, dma((NC,)),
                dma, dma, dma, dma((NC,)), dma, dma,
            ],
            compiler_params=pltpu.CompilerParams(vmem_limit_bytes=40 << 20, collective_id=0, has_side_effects=True),
            name='combine',
        )(in_vmem(o_own), o_got, in_hbm(w_o))
        x_out = pl.pallas_call(
            finish_kernel,
            out_shape=jax.ShapeDtypeStruct((ROWS, DM), bf16),
            in_specs=[vmem, vmem, vmem],
            out_specs=hbm,
            scratch_shapes=[pltpu.VMEM((ROWS, DM), bf16), dma],
            compiler_params=pltpu.CompilerParams(vmem_limit_bytes=16 << 20),
            name='finish',
        )(in_vmem(sums), x_in, w_post.reshape(DM // LANES, LANES))
        return x_out, from_rows(k_new), from_rows(v_new)

    return jax.shard_map(local_step, mesh=mesh,
                         in_specs=(P('dp', None), P('dp'), P(None), P(None, 'tp'), P(None, 'tp'), P(None, 'tp'), P('tp', None), P(None), cache_spec, cache_spec),
                         out_specs=(P('dp', None), cache_spec, cache_spec), check_vma=False)
```

```python
import functools

import jax
import jax.numpy as jnp
import numpy as np
from jax import lax
from jax.experimental import pallas as pl
from jax.experimental.pallas import tpu as pltpu
from jax.sharding import PartitionSpec as P

SOFT_CAP = 50.0
ROPE_BASE = 10000.0
NORM_EPS = 1e-6

ROWS = 128
DM = 3840
HD = 256
TB = 64
RP = 136
LANES = 128
BCH = 16
HALF = ROWS // 2
HROWS = 8 * HALF + 8
NCH = HALF // BCH
KC = 768
NKC = DM // KC
SHIFT = 20.0
CW = 256
NC = DM // CW
WG = 3
OWN = 32
MROWS = 8 * OWN + 8
MESH = pl.DeviceIdType.MESH


def attend_rows(row0, nchunk, pos_ref, kbuf, vbuf, qs, ks, vs, o_ref, before, after):
    tbase = lax.axis_index('sp') * TB
    lane = lax.broadcasted_iota(jnp.int32, (8, LANES), 1)
    row = lax.broadcasted_iota(jnp.int32, (8, LANES), 0)
    row_c = row // 4
    row_h = (row // 2) % 2
    match = (((lane // 2) % 2) == row_c) & ((lane % 2) == row_h)
    match_f = jnp.where(match, 1.0, 0.0).astype(jnp.float32)
    first = row_c == 0
    t_half = [jnp.where(match, lane // 4 + 32 * hf, 1 << 20) for hf in range(2)]
    quad = lax.broadcasted_iota(jnp.int32, (16, LANES), 0) // 4
    zero = jnp.zeros((8, LANES), jnp.float32)

    def chunk(i, l_acc):
        before(i)
        tls = []
        for u in range(BCH):
            lb = i * BCH + u
            b = row0 + lb
            tl = pos_ref[b] - tbase
            tls.append(tl)
            hit = jnp.logical_and(tl >= 0, tl < TB)
            tc = jnp.clip(tl, 0, TB - 1)
            tile = tc // 4
            tgt = jnp.where(hit, tc - tile * 4, -1)
            sel = quad == tgt
            off = pl.multiple_of(tile * 16, 16)
            kn = ks[pl.ds(b, 8, stride=RP), :]
            vn = vs[pl.ds(b, 8, stride=RP), :]
            kt = kbuf[lb, pl.ds(off, 16), :].astype(jnp.float32)
            vt = vbuf[lb, pl.ds(off, 16), :].astype(jnp.float32)
            kbuf[lb, pl.ds(off, 16), :] = jnp.where(sel, jnp.concatenate([kn, kn], 0), kt).astype(jnp.bfloat16)
            vbuf[lb, pl.ds(off, 16), :] = jnp.where(sel, jnp.concatenate([vn, vn], 0), vt).astype(jnp.bfloat16)
        scores = []
        for u in range(0, BCH, 2):
            lb = i * BCH + u
            q0 = qs[pl.ds(row0 + lb, 8, stride=RP), :]
            q1 = qs[pl.ds(row0 + lb + 1, 8, stride=RP), :]
            lhs = jnp.concatenate([jnp.concatenate([q0, zero], 1), jnp.concatenate([zero, q1], 1)], 0).astype(jnp.bfloat16)
            kk = jnp.concatenate([kbuf[lb], kbuf[lb + 1]], 1)
            scores.append(lax.dot_general(lhs, kk, (((1,), (1,)), ((), ())), preferred_element_type=jnp.float32))
        weights = []
        for u in range(0, BCH, 2):
            pair = []
            for w in range(2):
                part = scores[u // 2][8 * w:8 * w + 8]
                es = []
                for hf in range(2):
                    a = part[:, hf * LANES:(hf + 1) * LANES] * match_f
                    e = pltpu.roll(a, 4, 0)
                    f = jnp.where(first, pltpu.roll(e, LANES - 2, 1), pltpu.roll(e, 2, 1))
                    s = SOFT_CAP * jnp.tanh((a + f) * (HD ** -0.5 / SOFT_CAP))
                    es.append(jnp.where(t_half[hf] <= tls[u + w], jnp.exp(s - SHIFT), 0.0))
                tot = jnp.sum(es[0] + es[1], axis=1, keepdims=True)
                inv = jnp.where(tot > 0.0, 1.0 / tot, 0.0)
                pair.append(jnp.concatenate([es[0] * inv, es[1] * inv], 1))
                l_acc = jnp.where(lane == i * BCH + u + w, tot, l_acc)
            weights.append(jnp.concatenate(pair, 0).astype(jnp.bfloat16))
        for u in range(0, BCH, 2):
            lb = i * BCH + u
            vv = jnp.concatenate([vbuf[lb], vbuf[lb + 1]], 1)
            o = jnp.dot(weights[u // 2], vv, preferred_element_type=jnp.float32)
            o_ref[pl.ds(lb, 8, stride=HALF), :] = o[0:8, 0:LANES]
            o_ref[pl.ds(lb + 1, 8, stride=HALF), :] = o[8:16, LANES:]
        after(i)
        return l_acc

    l_acc = lax.fori_loop(0, nchunk, chunk, zero)
    o_ref[pl.ds(8 * HALF, 8), :] = l_acc


def far_kernel(pos_h, posv_h, freq_h, x_h, wpre_h, wq_h, wk_h, wv_h, kc_h, vc_h,
               o_ref, kbuf, vbuf, qs, ks, vs,
               pos_ref, posv, freq, wpre_ref, cos_ref, sin_ref, x_buf, a_buf, wq_buf, wk_buf, wv_buf, acc,
               x_sem, s_sem, w_sem, ki_sem):
    row0 = (1 - lax.axis_index('sp') // 2) * HALF

    def w_start(c):
        rows = pl.ds(c * KC, KC)
        for n, (src, dst) in enumerate(((wk_h, wk_buf), (wv_h, wv_buf), (wq_h, wq_buf))):
            pltpu.make_async_copy(src.at[rows, :], dst.at[rows, :], w_sem.at[c]).start()

    def w_wait(c):
        rows = pl.ds(c * KC, KC)
        for n, (src, dst) in enumerate(((wk_h, wk_buf), (wv_h, wv_buf), (wq_h, wq_buf))):
            pltpu.make_async_copy(src.at[rows, :], dst.at[rows, :], w_sem.at[c]).wait()

    def k_in(i):
        return pltpu.make_async_copy(kc_h.at[pl.ds(row0 + i * BCH, BCH)], kbuf.at[pl.ds(i * BCH, BCH)], ki_sem.at[i])

    def v_in(i):
        return pltpu.make_async_copy(vc_h.at[pl.ds(row0 + i * BCH, BCH)], vbuf.at[pl.ds(i * BCH, BCH)], ki_sem.at[i])

    small = [pltpu.make_async_copy(a, b, s_sem) for a, b in (
        (wpre_h, wpre_ref), (posv_h, posv), (freq_h, freq), (pos_h, pos_ref))]
    for c in small:
        c.start()
    x_copy = pltpu.make_async_copy(x_h, x_buf, x_sem)
    x_copy.start()
    w_start(0)
    for c in small:
        c.wait()
    w_start(1)
    pos_col = jnp.broadcast_to(posv[...].astype(jnp.float32), (ROWS, LANES)).T
    ang = pos_col * freq[...]
    cos_ref[...] = jnp.cos(ang)
    sin_ref[...] = jnp.sin(ang)
    x_copy.wait()
    w_start(2)

    gain = 1.0 + jnp.concatenate([wpre_ref[k:k + 1, :] for k in range(DM // LANES)], 1)

    def norm_rows(i, carry):
        r = pl.multiple_of(i * 16, 16)
        xb = x_buf[pl.ds(r, 16), :].astype(jnp.float32)
        ms = jnp.mean(xb * xb, axis=-1, keepdims=True)
        a_buf[pl.ds(r, 16), :] = (xb * lax.rsqrt(ms + NORM_EPS) * gain).astype(jnp.bfloat16)
        return carry

    lax.fori_loop(0, ROWS // 16, norm_rows, 0)

    for c in range(NKC):
        w_wait(c)
        if c + 3 < NKC:
            w_start(c + 3)
        for n in ((), (), (0,), (1,), (2, 3))[c]:
            k_in(n).start()
            v_in(n).start()
        rows = slice(c * KC, (c + 1) * KC)
        a_c = a_buf[:, rows]
        for i in range(8):
            if i < 2:
                w_c = wk_buf[rows, i * HD:(i + 1) * HD]
            elif i < 4:
                w_c = wv_buf[rows, (i - 2) * HD:(i - 1) * HD]
            else:
                w_c = wq_buf[rows, (i - 4) * HD:(i - 3) * HD]
            y = jnp.dot(a_c, w_c, preferred_element_type=jnp.float32)
            if c == 0:
                acc[i] = y
                continue
            y = acc[i] + y
            if c < NKC - 1:
                acc[i] = y
                continue
            lo, hi = y[:, :LANES], y[:, LANES:]
            if 2 <= i < 4:
                h = i - 2
                for rep in range(2):
                    vs[pl.ds((rep * 4 + h) * RP, ROWS), :] = lo
                    vs[pl.ds((rep * 4 + 2 + h) * RP, ROWS), :] = hi
            else:
                cos_t, sin_t = cos_ref[...], sin_ref[...]
                rlo = lo * cos_t - hi * sin_t
                rhi = hi * cos_t + lo * sin_t
                if i < 2:
                    for rep in range(2):
                        ks[pl.ds((rep * 4 + i) * RP, ROWS), :] = rlo
                        ks[pl.ds((rep * 4 + 2 + i) * RP, ROWS), :] = rhi
                else:
                    qs[pl.ds((i - 4) * RP, ROWS), :] = rlo
                    qs[pl.ds((4 + i - 4) * RP, ROWS), :] = rhi

    def before(i):
        k_in(i).wait()
        v_in(i).wait()

    attend_rows(row0, NCH, pos_ref, kbuf, vbuf, qs, ks, vs, o_ref, before, lambda i: None)


def near_kernel(pos_h, qs, ks, vs, kfar, vfar, kc_h, vc_h,
                o_ref, ko_h, vo_h,
                pos_ref, kbuf, vbuf, p_sem, ki_sem, w_sem):
    yy = lax.axis_index('sp') // 2
    row0 = yy * HALF
    far0 = (1 - yy) * HALF

    def k_in(i):
        return pltpu.make_async_copy(kc_h.at[pl.ds(row0 + i * BCH, BCH)], kbuf.at[pl.ds(i * BCH, BCH)], ki_sem.at[i])

    def v_in(i):
        return pltpu.make_async_copy(vc_h.at[pl.ds(row0 + i * BCH, BCH)], vbuf.at[pl.ds(i * BCH, BCH)], ki_sem.at[i])

    def k_out(i):
        return pltpu.make_async_copy(kbuf.at[pl.ds(i * BCH, BCH)], ko_h.at[pl.ds(row0 + i * BCH, BCH)], w_sem)

    def v_out(i):
        return pltpu.make_async_copy(vbuf.at[pl.ds(i * BCH, BCH)], vo_h.at[pl.ds(row0 + i * BCH, BCH)], w_sem)

    def kf_out(i):
        return pltpu.make_async_copy(kfar.at[pl.ds(i * BCH, BCH)], ko_h.at[pl.ds(far0 + i * BCH, BCH)], w_sem)

    def vf_out(i):
        return pltpu.make_async_copy(vfar.at[pl.ds(i * BCH, BCH)], vo_h.at[pl.ds(far0 + i * BCH, BCH)], w_sem)

    p_copy = pltpu.make_async_copy(pos_h, pos_ref, p_sem)
    p_copy.start()
    for i in range(NCH):
        k_in(i).start()
        v_in(i).start()
    p_copy.wait()

    def before(i):
        k_in(i).wait()
        v_in(i).wait()
        kf_out(i).start()
        vf_out(i).start()

    def after(i):
        k_out(i).start()
        v_out(i).start()

    attend_rows(row0, NCH, pos_ref, kbuf, vbuf, qs, ks, vs, o_ref, before, after)
    for i in range(NCH):
        kf_out(i).wait()
        vf_out(i).wait()
        k_out(i).wait()
        v_out(i).wait()


def comm_kernel(o_own, o_got, wo_h, s_all,
                wo_buf, fac, m1, m2, r1, lhs, p_buf, rr, rl, sr, sl,
                w_sem, r1_send, r1_recv,
                right_send, right_recv, left_send, left_recv,
                part_send, part_recv, y_send, y_recv, f_send, f_recv):
    z = lax.axis_index('tp')
    sp = lax.axis_index('sp')
    core = sp % 2
    partner = sp + 1 - 2 * core
    ypeer = (sp + 2) % 4

    def wo_copy(k):
        return pltpu.make_async_copy(wo_h.at[:, pl.ds(pl.multiple_of(k * WG * CW, CW), WG * CW)], wo_buf.at[k], w_sem.at[k])

    for k in range(NC // WG):
        wo_copy(k).start()

    @pl.when(z == 0)
    def _():
        rr[...] = jnp.zeros_like(rr)

    @pl.when(z == 3)
    def _():
        rl[...] = jnp.zeros_like(rl)

    bar = pltpu.get_barrier_semaphore()
    pl.semaphore_signal(bar, inc=1, device_id={'sp': partner}, device_id_type=MESH)
    pl.semaphore_signal(bar, inc=1, device_id={'sp': ypeer}, device_id_type=MESH)

    @pl.when(z > 0)
    def _():
        pl.semaphore_signal(bar, inc=1, device_id={'tp': z - 1}, device_id_type=MESH)

    @pl.when(z < 3)
    def _():
        pl.semaphore_signal(bar, inc=1, device_id={'tp': z + 1}, device_id_type=MESH)

    def shares(l_a, l_b, slot):
        tot = l_a + l_b
        inv = jnp.where(tot > 0.0, 1.0 / tot, 0.0)
        for w, l in enumerate((l_a, l_b)):
            fac[slot + w] = jnp.concatenate([l * inv, jnp.zeros((LANES - 8, LANES), jnp.float32)], 0).T
        return tot

    mine = pl.multiple_of(core * OWN, OWN)
    theirs = pl.multiple_of((1 - core) * OWN, OWN)
    tot = shares(o_own[pl.ds(8 * HALF, 8), :], o_got[pl.ds(8 * HALF, 8), :], 0)

    def merge_half(r0, dst):
        fa, fb = fac[0, pl.ds(r0, OWN), :], fac[1, pl.ds(r0, OWN), :]
        for j in range(8):
            rows = pl.ds(pl.multiple_of(j * HALF + r0, 8), OWN)
            dst[pl.ds(j * OWN, OWN), :] = o_own[rows, :] * fa[:, j:j + 1] + o_got[rows, :] * fb[:, j:j + 1]

    merge_half(theirs, m1)
    m1[pl.ds(8 * OWN, 8), :] = tot
    merge_half(mine, m2)
    pair = pltpu.make_async_remote_copy(
        src_ref=m1, dst_ref=r1, send_sem=r1_send, recv_sem=r1_recv, device_id={'sp': partner}, device_id_type=MESH)
    pl.semaphore_wait(bar, 3 + (z * (3 - z)) // 2)
    pair.start()
    pair.wait()
    shares(tot, r1[pl.ds(8 * OWN, 8), :], 2)
    fa, fb = fac[2, pl.ds(mine, OWN), :], fac[3, pl.ds(mine, OWN), :]
    for j in range(8):
        c, hq = j // 4, j % 4
        val = m2[j * OWN:(j + 1) * OWN, :] * fa[:, j:j + 1] + r1[j * OWN:(j + 1) * OWN, :] * fb[:, j:j + 1]
        lhs[:, (hq * 2 + c) * LANES:(hq * 2 + c + 1) * LANES] = val.astype(jnp.bfloat16)

    def right_copy(k):
        return pltpu.make_async_remote_copy(
            src_ref=sr.at[k], dst_ref=rr.at[k], send_sem=right_send, recv_sem=right_recv.at[k],
            device_id={'tp': z + 1}, device_id_type=MESH)

    def left_copy(k):
        return pltpu.make_async_remote_copy(
            src_ref=sl.at[k], dst_ref=rl.at[k], send_sem=left_send, recv_sem=left_recv.at[k],
            device_id={'tp': z - 1}, device_id_type=MESH)

    def part_copy(k):
        return pltpu.make_async_remote_copy(
            src_ref=s_all.at[sp, k], dst_ref=s_all.at[sp, k], send_sem=part_send, recv_sem=part_recv,
            device_id={'sp': partner}, device_id_type=MESH)

    def y_copy(k):
        return pltpu.make_async_remote_copy(
            src_ref=s_all.at[sp, k], dst_ref=s_all.at[sp, k], send_sem=y_send, recv_sem=y_recv.at[k],
            device_id={'sp': ypeer}, device_id_type=MESH)

    def fwd_copy(k):
        return pltpu.make_async_remote_copy(
            src_ref=s_all.at[ypeer, k], dst_ref=s_all.at[ypeer, k], send_sem=f_send, recv_sem=f_recv,
            device_id={'sp': partner}, device_id_type=MESH)

    def whole(ref, sem):
        return pltpu.make_async_copy(ref, ref, sem)

    hop = 5
    lag_r = hop * z
    lag_l = hop * (3 - z)
    lag_s = hop * (3 - (z * (3 - z)) // 2)

    def tick(i, carry):
        @pl.when(i < NC)
        def _():
            group, place = i // WG, i % WG

            @pl.when(place == 0)
            def _():
                wo_copy(group).wait()

            w_c = wo_buf[group, :, pl.ds(pl.multiple_of(place * CW, CW), CW)]
            p_buf[i] = jnp.dot(lhs[...], w_c, preferred_element_type=jnp.float32)

        kr, kl = i - lag_r, i - lag_l
        r_live = jnp.logical_and(kr >= 0, kr < NC)
        l_live = jnp.logical_and(kl >= 0, kl < NC)

        def step_right():
            @pl.when(z > 0)
            def _():
                right_copy(kr).wait_recv()

            @pl.when(z < 3)
            def _():
                sr[kr] = p_buf[kr] + rr[kr]
                right_copy(kr).start()

        def step_left():
            @pl.when(z < 3)
            def _():
                left_copy(kl).wait_recv()

            @pl.when(z > 0)
            def _():
                sl[kl] = p_buf[kl] + rl[kl]
                left_copy(kl).start()

        pl.when(jnp.logical_and(l_live, z < 2))(step_left)
        pl.when(r_live)(step_right)
        pl.when(jnp.logical_and(l_live, z >= 2))(step_left)

        k_s = i - lag_s

        @pl.when(jnp.logical_and(k_s >= 0, k_s < NC))
        def _():
            s_all[sp, k_s] = p_buf[k_s] + rr[k_s] + rl[k_s]
            y_copy(k_s).start()
            part_copy(k_s).start()

        k_y = i - lag_s - hop

        @pl.when(jnp.logical_and(k_y >= 0, k_y < NC))
        def _():
            y_copy(k_y).wait_recv()
            fwd_copy(k_y).start()

        return carry

    lax.fori_loop(0, NC + 4 * hop, tick, 0)

    @pl.when(z < 3)
    def _():
        whole(sr, right_send).wait()

    @pl.when(z > 0)
    def _():
        whole(sl, left_send).wait()

    whole(s_all.at[sp], y_send).wait()
    whole(s_all.at[sp], part_send).wait()
    whole(s_all.at[ypeer], f_send).wait()
    whole(s_all.at[partner], part_recv).wait()
    whole(s_all.at[3 - sp], f_recv).wait()


def finish_kernel(s_all, x_ref, wpost_ref, out_h, out_buf, sem):
    blk = 16

    def out_copy(i):
        rows = pl.ds(i * blk, blk)
        return pltpu.make_async_copy(out_buf.at[rows], out_h.at[rows], sem)

    for i in range(ROWS // blk):
        g, r = (i * blk) // OWN, (i * blk) % OWN
        parts = [s_all[g, k, r:r + blk, :] for k in range(NC)]
        sq = parts[0] * parts[0]
        for k in range(1, NC):
            sq = sq + parts[k] * parts[k]
        rs = lax.rsqrt(jnp.sum(sq, axis=-1, keepdims=True) * (1.0 / DM) + NORM_EPS)
        for k in range(NC):
            for hf in range(CW // LANES):
                col = k * CW + hf * LANES
                gain = 1.0 + wpost_ref[col // LANES:col // LANES + 1, :]
                val = s_all[g, k, r:r + blk, hf * LANES:(hf + 1) * LANES] * rs * gain
                cs = slice(col, col + LANES)
                out_buf[i * blk:(i + 1) * blk, cs] = (x_ref[i * blk:(i + 1) * blk, cs].astype(jnp.float32) + val).astype(jnp.bfloat16)
        out_copy(i).start()
    for i in range(ROWS // blk):
        out_copy(i).wait()


def solution(mesh):
    cache_spec = P('dp', 'sp', 'tp', None)
    hbm = pl.BlockSpec(memory_space=pltpu.HBM)
    vmem = pl.BlockSpec(memory_space=pltpu.VMEM)

    def in_hbm(arr):
        return pltpu.with_memory_space_constraint(arr, pltpu.HBM)

    def in_vmem(arr):
        return pltpu.with_memory_space_constraint(arr, pltpu.VMEM)

    def to_rows(c):
        b, t, h, d = c.shape
        return c.reshape(b, t, h, 2, LANES).transpose(0, 1, 3, 2, 4).reshape(b, t * 2 * h, LANES)

    def from_rows(r):
        return r.reshape(ROWS, TB, 2, 2, LANES).transpose(0, 1, 3, 2, 4).reshape(ROWS, TB, 2, HD)

    def local_step(x_in, cur_pos, w_pre, w_q, w_k, w_v, w_o, w_post, k_cache, v_cache):
        half = HD // 2
        inv_freq = jnp.asarray((ROPE_BASE ** (-2.0 * np.arange(half) / (2 * half))).astype(np.float32))
        kr, vr = to_rows(k_cache), to_rows(v_cache)
        f32, bf16 = jnp.float32, jnp.bfloat16
        dma = pltpu.SemaphoreType.DMA
        half_shape = (HALF,) + kr.shape[1:]
        o_far, k_far, v_far, qs, ks, vs = pl.pallas_call(
            far_kernel,
            out_shape=(jax.ShapeDtypeStruct((HROWS, LANES), f32),
                       pltpu.VMEM(half_shape, bf16), pltpu.VMEM(half_shape, bf16),
                       pltpu.VMEM((8 * RP, LANES), f32), pltpu.VMEM((8 * RP, LANES), f32), pltpu.VMEM((8 * RP, LANES), f32)),
            in_specs=[hbm] * 10,
            out_specs=(vmem,) * 6,
            scratch_shapes=[
                pltpu.SMEM((ROWS,), jnp.int32), pltpu.VMEM((1, ROWS), jnp.int32), pltpu.VMEM((1, LANES), f32),
                pltpu.VMEM((DM // LANES, LANES), f32), pltpu.VMEM((ROWS, LANES), f32), pltpu.VMEM((ROWS, LANES), f32),
                pltpu.VMEM((ROWS, DM), bf16), pltpu.VMEM((ROWS, DM), bf16),
                pltpu.VMEM((DM, 1024), bf16), pltpu.VMEM((DM, 512), bf16), pltpu.VMEM((DM, 512), bf16), pltpu.VMEM((8, ROWS, HD), f32),
                dma, dma, dma((NKC,)), dma((NCH,)),
            ],
            compiler_params=pltpu.CompilerParams(vmem_limit_bytes=40 << 20),
            cost_estimate=pl.CostEstimate(flops=2 * 10 ** 9, bytes_accessed=25 * 10 ** 6, transcendentals=0),
            name='attend_far',
        )(in_hbm(cur_pos), in_hbm(cur_pos.reshape(1, ROWS)), in_hbm(inv_freq.reshape(1, LANES)), in_hbm(x_in),
          in_hbm(w_pre.reshape(DM // LANES, LANES)), in_hbm(w_q), in_hbm(w_k), in_hbm(w_v), in_hbm(kr), in_hbm(vr))
        o_got = lax.ppermute(o_far, 'sp', [(0, 2), (1, 3), (2, 0), (3, 1)])
        o_own, k_new, v_new = pl.pallas_call(
            near_kernel,
            out_shape=(pltpu.VMEM((HROWS, LANES), f32),
                       jax.ShapeDtypeStruct(kr.shape, bf16), jax.ShapeDtypeStruct(vr.shape, bf16)),
            in_specs=[hbm, vmem, vmem, vmem, vmem, vmem, hbm, hbm],
            out_specs=(vmem, hbm, hbm),
            scratch_shapes=[
                pltpu.SMEM((ROWS,), jnp.int32), pltpu.VMEM(half_shape, bf16), pltpu.VMEM(half_shape, bf16),
                dma, dma((NCH,)), dma,
            ],
            compiler_params=pltpu.CompilerParams(vmem_limit_bytes=28 << 20),
            cost_estimate=pl.CostEstimate(flops=10 ** 10, bytes_accessed=25 * 10 ** 6, transcendentals=0),
            name='attend_near',
        )(in_hbm(cur_pos), in_vmem(qs), in_vmem(ks), in_vmem(vs), in_vmem(k_far), in_vmem(v_far), in_hbm(kr), in_hbm(vr))
        big = pltpu.VMEM((NC, OWN, CW), f32)
        sums = pl.pallas_call(
            comm_kernel,
            out_shape=pltpu.VMEM((4, NC, OWN, CW), f32),
            in_specs=[vmem, vmem, hbm],
            out_specs=vmem,
            scratch_shapes=[
                pltpu.VMEM((NC // WG, 1024, WG * CW), bf16), pltpu.VMEM((4, LANES, LANES), f32), pltpu.VMEM((MROWS, LANES), f32),
                pltpu.VMEM((8 * OWN, LANES), f32), pltpu.VMEM((MROWS, LANES), f32), pltpu.VMEM((OWN, 1024), bf16),
                big, big, big, big, big,
                dma((NC // WG,)), dma, dma,
                dma, dma((NC,)), dma, dma((NC,)),
                dma, dma, dma, dma((NC,)), dma, dma,
            ],
            compiler_params=pltpu.CompilerParams(vmem_limit_bytes=40 << 20, collective_id=0, has_side_effects=True),
            name='combine',
        )(in_vmem(o_own), o_got, in_hbm(w_o))
        x_out = pl.pallas_call(
            finish_kernel,
            out_shape=jax.ShapeDtypeStruct((ROWS, DM), bf16),
            in_specs=[vmem, vmem, vmem],
            out_specs=hbm,
            scratch_shapes=[pltpu.VMEM((ROWS, DM), bf16), dma],
            compiler_params=pltpu.CompilerParams(vmem_limit_bytes=16 << 20),
            name='finish',
        )(in_vmem(sums), x_in, w_post.reshape(DM // LANES, LANES))
        return x_out, from_rows(k_new), from_rows(v_new)

    return jax.shard_map(local_step, mesh=mesh,
                         in_specs=(P('dp', None), P('dp'), P(None), P(None, 'tp'), P(None, 'tp'), P(None, 'tp'), P('tp', None), P(None), cache_spec, cache_spec),
                         out_specs=(P('dp', None), cache_spec, cache_spec), check_vma=False)
```

```python
import functools

import jax
import jax.numpy as jnp
import numpy as np
from jax import lax
from jax.experimental import pallas as pl
from jax.experimental.pallas import tpu as pltpu
from jax.sharding import PartitionSpec as P

SOFT_CAP = 50.0
ROPE_BASE = 10000.0
NORM_EPS = 1e-6

ROWS = 128
DM = 3840
HD = 256
TB = 64
RP = 136
LANES = 128
BCH = 16
HALF = ROWS // 2
HROWS = 8 * HALF + 8
NCH = HALF // BCH
KC = 768
NKC = DM // KC
SHIFT = 20.0
CW = 256
NC = DM // CW
WG = 3
OWN = 32
MROWS = 8 * OWN + 8
MESH = pl.DeviceIdType.MESH


def attend_rows(row0, bch, pos_ref, kbuf, vbuf, qs, ks, vs, o_ref, before, after):
    tbase = lax.axis_index('sp') * TB
    lane = lax.broadcasted_iota(jnp.int32, (8, LANES), 1)
    row = lax.broadcasted_iota(jnp.int32, (8, LANES), 0)
    row_c = row // 4
    row_h = (row // 2) % 2
    match = (((lane // 2) % 2) == row_c) & ((lane % 2) == row_h)
    match_f = jnp.where(match, 1.0, 0.0).astype(jnp.float32)
    first = row_c == 0
    t_half = [jnp.where(match, lane // 4 + 32 * hf, 1 << 20) for hf in range(2)]
    quad = lax.broadcasted_iota(jnp.int32, (16, LANES), 0) // 4
    zero = jnp.zeros((8, LANES), jnp.float32)

    def chunk(i, l_acc):
        before(i)
        tls = []
        for u in range(bch):
            lb = i * bch + u
            b = row0 + lb
            tl = pos_ref[b] - tbase
            tls.append(tl)
            hit = jnp.logical_and(tl >= 0, tl < TB)
            tc = jnp.clip(tl, 0, TB - 1)
            tile = tc // 4
            tgt = jnp.where(hit, tc - tile * 4, -1)
            sel = quad == tgt
            off = pl.multiple_of(tile * 16, 16)
            kn = ks[pl.ds(b, 8, stride=RP), :]
            vn = vs[pl.ds(b, 8, stride=RP), :]
            kt = kbuf[lb, pl.ds(off, 16), :].astype(jnp.float32)
            vt = vbuf[lb, pl.ds(off, 16), :].astype(jnp.float32)
            kbuf[lb, pl.ds(off, 16), :] = jnp.where(sel, jnp.concatenate([kn, kn], 0), kt).astype(jnp.bfloat16)
            vbuf[lb, pl.ds(off, 16), :] = jnp.where(sel, jnp.concatenate([vn, vn], 0), vt).astype(jnp.bfloat16)
        scores = []
        for u in range(0, bch, 2):
            lb = i * bch + u
            q0 = qs[pl.ds(row0 + lb, 8, stride=RP), :]
            q1 = qs[pl.ds(row0 + lb + 1, 8, stride=RP), :]
            lhs = jnp.concatenate([jnp.concatenate([q0, zero], 1), jnp.concatenate([zero, q1], 1)], 0).astype(jnp.bfloat16)
            kk = jnp.concatenate([kbuf[lb], kbuf[lb + 1]], 1)
            scores.append(lax.dot_general(lhs, kk, (((1,), (1,)), ((), ())), preferred_element_type=jnp.float32))
        weights = []
        for u in range(0, bch, 2):
            pair = []
            for w in range(2):
                part = scores[u // 2][8 * w:8 * w + 8]
                es = []
                for hf in range(2):
                    a = part[:, hf * LANES:(hf + 1) * LANES] * match_f
                    e = pltpu.roll(a, 4, 0)
                    f = jnp.where(first, pltpu.roll(e, LANES - 2, 1), pltpu.roll(e, 2, 1))
                    s = SOFT_CAP * jnp.tanh((a + f) * (HD ** -0.5 / SOFT_CAP))
                    es.append(jnp.where(t_half[hf] <= tls[u + w], jnp.exp(s - SHIFT), 0.0))
                tot = jnp.sum(es[0] + es[1], axis=1, keepdims=True)
                inv = jnp.where(tot > 0.0, 1.0 / tot, 0.0)
                pair.append(jnp.concatenate([es[0] * inv, es[1] * inv], 1))
                l_acc = jnp.where(lane == i * bch + u + w, tot, l_acc)
            weights.append(jnp.concatenate(pair, 0).astype(jnp.bfloat16))
        for u in range(0, bch, 2):
            lb = i * bch + u
            vv = jnp.concatenate([vbuf[lb], vbuf[lb + 1]], 1)
            o = jnp.dot(weights[u // 2], vv, preferred_element_type=jnp.float32)
            o_ref[pl.ds(lb, 8, stride=HALF), :] = o[0:8, 0:LANES]
            o_ref[pl.ds(lb + 1, 8, stride=HALF), :] = o[8:16, LANES:]
        after(i)
        return l_acc

    l_acc = lax.fori_loop(0, HALF // bch, chunk, zero)
    o_ref[pl.ds(8 * HALF, 8), :] = l_acc


def far_kernel(pos_h, posv_h, freq_h, x_h, wpre_h, wq_h, wk_h, wv_h, kc_h, vc_h,
               o_ref, kbuf, vbuf, qs, ks, vs,
               pos_ref, posv, freq, wpre_ref, cos_ref, sin_ref, x_buf, a_buf, wq_buf, wk_buf, wv_buf, acc,
               x_sem, s_sem, w_sem, ki_sem):
    row0 = (1 - lax.axis_index('sp') // 2) * HALF

    def w_start(c):
        rows = pl.ds(c * KC, KC)
        for n, (src, dst) in enumerate(((wk_h, wk_buf), (wv_h, wv_buf), (wq_h, wq_buf))):
            pltpu.make_async_copy(src.at[rows, :], dst.at[rows, :], w_sem.at[c]).start()

    def w_wait(c):
        rows = pl.ds(c * KC, KC)
        for n, (src, dst) in enumerate(((wk_h, wk_buf), (wv_h, wv_buf), (wq_h, wq_buf))):
            pltpu.make_async_copy(src.at[rows, :], dst.at[rows, :], w_sem.at[c]).wait()

    def k_in(i):
        return pltpu.make_async_copy(kc_h.at[pl.ds(row0 + i * BCH, BCH)], kbuf.at[pl.ds(i * BCH, BCH)], ki_sem.at[i])

    def v_in(i):
        return pltpu.make_async_copy(vc_h.at[pl.ds(row0 + i * BCH, BCH)], vbuf.at[pl.ds(i * BCH, BCH)], ki_sem.at[i])

    small = [pltpu.make_async_copy(a, b, s_sem) for a, b in (
        (wpre_h, wpre_ref), (posv_h, posv), (freq_h, freq), (pos_h, pos_ref))]
    for c in small:
        c.start()
    x_copy = pltpu.make_async_copy(x_h, x_buf, x_sem)
    x_copy.start()
    w_start(0)
    for c in small:
        c.wait()
    w_start(1)
    pos_col = jnp.broadcast_to(posv[...].astype(jnp.float32), (ROWS, LANES)).T
    ang = pos_col * freq[...]
    cos_ref[...] = jnp.cos(ang)
    sin_ref[...] = jnp.sin(ang)
    x_copy.wait()
    w_start(2)

    gain = 1.0 + jnp.concatenate([wpre_ref[k:k + 1, :] for k in range(DM // LANES)], 1)

    def norm_rows(i, carry):
        r = pl.multiple_of(i * 16, 16)
        xb = x_buf[pl.ds(r, 16), :].astype(jnp.float32)
        ms = jnp.mean(xb * xb, axis=-1, keepdims=True)
        a_buf[pl.ds(r, 16), :] = (xb * lax.rsqrt(ms + NORM_EPS) * gain).astype(jnp.bfloat16)
        return carry

    lax.fori_loop(0, ROWS // 16, norm_rows, 0)

    for c in range(NKC):
        w_wait(c)
        if c + 3 < NKC:
            w_start(c + 3)
        for n in ((), (), (0,), (1,), (2, 3))[c]:
            k_in(n).start()
            v_in(n).start()
        rows = slice(c * KC, (c + 1) * KC)
        a_c = a_buf[:, rows]
        for i in range(8):
            if i < 2:
                w_c = wk_buf[rows, i * HD:(i + 1) * HD]
            elif i < 4:
                w_c = wv_buf[rows, (i - 2) * HD:(i - 1) * HD]
            else:
                w_c = wq_buf[rows, (i - 4) * HD:(i - 3) * HD]
            y = jnp.dot(a_c, w_c, preferred_element_type=jnp.float32)
            if c == 0:
                acc[i] = y
                continue
            y = acc[i] + y
            if c < NKC - 1:
                acc[i] = y
                continue
            lo, hi = y[:, :LANES], y[:, LANES:]
            if 2 <= i < 4:
                h = i - 2
                for rep in range(2):
                    vs[pl.ds((rep * 4 + h) * RP, ROWS), :] = lo
                    vs[pl.ds((rep * 4 + 2 + h) * RP, ROWS), :] = hi
            else:
                cos_t, sin_t = cos_ref[...], sin_ref[...]
                rlo = lo * cos_t - hi * sin_t
                rhi = hi * cos_t + lo * sin_t
                if i < 2:
                    for rep in range(2):
                        ks[pl.ds((rep * 4 + i) * RP, ROWS), :] = rlo
                        ks[pl.ds((rep * 4 + 2 + i) * RP, ROWS), :] = rhi
                else:
                    qs[pl.ds((i - 4) * RP, ROWS), :] = rlo
                    qs[pl.ds((4 + i - 4) * RP, ROWS), :] = rhi

    def before(i):
        for n in range(2):
            k_in(2 * i + n).wait()
            v_in(2 * i + n).wait()

    attend_rows(row0, 2 * BCH, pos_ref, kbuf, vbuf, qs, ks, vs, o_ref, before, lambda i: None)


def near_kernel(pos_h, qs, ks, vs, kfar, vfar, kc_h, vc_h,
                o_ref, ko_h, vo_h,
                pos_ref, kbuf, vbuf, p_sem, ki_sem, w_sem):
    yy = lax.axis_index('sp') // 2
    row0 = yy * HALF
    far0 = (1 - yy) * HALF

    def k_in(i):
        return pltpu.make_async_copy(kc_h.at[pl.ds(row0 + i * BCH, BCH)], kbuf.at[pl.ds(i * BCH, BCH)], ki_sem.at[i])

    def v_in(i):
        return pltpu.make_async_copy(vc_h.at[pl.ds(row0 + i * BCH, BCH)], vbuf.at[pl.ds(i * BCH, BCH)], ki_sem.at[i])

    def k_out(i):
        return pltpu.make_async_copy(kbuf.at[pl.ds(i * BCH, BCH)], ko_h.at[pl.ds(row0 + i * BCH, BCH)], w_sem)

    def v_out(i):
        return pltpu.make_async_copy(vbuf.at[pl.ds(i * BCH, BCH)], vo_h.at[pl.ds(row0 + i * BCH, BCH)], w_sem)

    def kf_out(i):
        return pltpu.make_async_copy(kfar.at[pl.ds(i * BCH, BCH)], ko_h.at[pl.ds(far0 + i * BCH, BCH)], w_sem)

    def vf_out(i):
        return pltpu.make_async_copy(vfar.at[pl.ds(i * BCH, BCH)], vo_h.at[pl.ds(far0 + i * BCH, BCH)], w_sem)

    p_copy = pltpu.make_async_copy(pos_h, pos_ref, p_sem)
    p_copy.start()
    for i in range(NCH):
        k_in(i).start()
        v_in(i).start()
    p_copy.wait()

    def before(i):
        k_in(i).wait()
        v_in(i).wait()
        kf_out(i).start()
        vf_out(i).start()

    def after(i):
        k_out(i).start()
        v_out(i).start()

    attend_rows(row0, BCH, pos_ref, kbuf, vbuf, qs, ks, vs, o_ref, before, after)
    for i in range(NCH):
        kf_out(i).wait()
        vf_out(i).wait()
        k_out(i).wait()
        v_out(i).wait()


def comm_kernel(o_own, o_got, wo_h, s_all,
                wo_buf, fac, m1, m2, r1, lhs, p_buf, rr, rl, sr, sl,
                w_sem, r1_send, r1_recv,
                right_send, right_recv, left_send, left_recv,
                part_send, part_recv, y_send, y_recv, f_send, f_recv):
    z = lax.axis_index('tp')
    sp = lax.axis_index('sp')
    core = sp % 2
    partner = sp + 1 - 2 * core
    ypeer = (sp + 2) % 4

    def wo_copy(k):
        return pltpu.make_async_copy(wo_h.at[:, pl.ds(pl.multiple_of(k * WG * CW, CW), WG * CW)], wo_buf.at[k], w_sem.at[k])

    for k in range(NC // WG):
        wo_copy(k).start()

    @pl.when(z == 0)
    def _():
        rr[...] = jnp.zeros_like(rr)

    @pl.when(z == 3)
    def _():
        rl[...] = jnp.zeros_like(rl)

    bar = pltpu.get_barrier_semaphore()
    pl.semaphore_signal(bar, inc=1, device_id={'sp': partner}, device_id_type=MESH)
    pl.semaphore_signal(bar, inc=1, device_id={'sp': ypeer}, device_id_type=MESH)

    @pl.when(z > 0)
    def _():
        pl.semaphore_signal(bar, inc=1, device_id={'tp': z - 1}, device_id_type=MESH)

    @pl.when(z < 3)
    def _():
        pl.semaphore_signal(bar, inc=1, device_id={'tp': z + 1}, device_id_type=MESH)

    def shares(l_a, l_b, slot):
        tot = l_a + l_b
        inv = jnp.where(tot > 0.0, 1.0 / tot, 0.0)
        for w, l in enumerate((l_a, l_b)):
            fac[slot + w] = jnp.concatenate([l * inv, jnp.zeros((LANES - 8, LANES), jnp.float32)], 0).T
        return tot

    mine = pl.multiple_of(core * OWN, OWN)
    theirs = pl.multiple_of((1 - core) * OWN, OWN)
    tot = shares(o_own[pl.ds(8 * HALF, 8), :], o_got[pl.ds(8 * HALF, 8), :], 0)

    def merge_half(r0, dst):
        fa, fb = fac[0, pl.ds(r0, OWN), :], fac[1, pl.ds(r0, OWN), :]
        for j in range(8):
            rows = pl.ds(pl.multiple_of(j * HALF + r0, 8), OWN)
            dst[pl.ds(j * OWN, OWN), :] = o_own[rows, :] * fa[:, j:j + 1] + o_got[rows, :] * fb[:, j:j + 1]

    merge_half(theirs, m1)
    m1[pl.ds(8 * OWN, 8), :] = tot
    merge_half(mine, m2)
    pair = pltpu.make_async_remote_copy(
        src_ref=m1, dst_ref=r1, send_sem=r1_send, recv_sem=r1_recv, device_id={'sp': partner}, device_id_type=MESH)
    pl.semaphore_wait(bar, 3 + (z * (3 - z)) // 2)
    pair.start()
    pair.wait()
    shares(tot, r1[pl.ds(8 * OWN, 8), :], 2)
    fa, fb = fac[2, pl.ds(mine, OWN), :], fac[3, pl.ds(mine, OWN), :]
    for j in range(8):
        c, hq = j // 4, j % 4
        val = m2[j * OWN:(j + 1) * OWN, :] * fa[:, j:j + 1] + r1[j * OWN:(j + 1) * OWN, :] * fb[:, j:j + 1]
        lhs[:, (hq * 2 + c) * LANES:(hq * 2 + c + 1) * LANES] = val.astype(jnp.bfloat16)

    def right_copy(k):
        return pltpu.make_async_remote_copy(
            src_ref=sr.at[k], dst_ref=rr.at[k], send_sem=right_send, recv_sem=right_recv.at[k],
            device_id={'tp': z + 1}, device_id_type=MESH)

    def left_copy(k):
        return pltpu.make_async_remote_copy(
            src_ref=sl.at[k], dst_ref=rl.at[k], send_sem=left_send, recv_sem=left_recv.at[k],
            device_id={'tp': z - 1}, device_id_type=MESH)

    def part_copy(k):
        return pltpu.make_async_remote_copy(
            src_ref=s_all.at[sp, k], dst_ref=s_all.at[sp, k], send_sem=part_send, recv_sem=part_recv,
            device_id={'sp': partner}, device_id_type=MESH)

    def y_copy(k):
        return pltpu.make_async_remote_copy(
            src_ref=s_all.at[sp, k], dst_ref=s_all.at[sp, k], send_sem=y_send, recv_sem=y_recv.at[k],
            device_id={'sp': ypeer}, device_id_type=MESH)

    def fwd_copy(k):
        return pltpu.make_async_remote_copy(
            src_ref=s_all.at[ypeer, k], dst_ref=s_all.at[ypeer, k], send_sem=f_send, recv_sem=f_recv,
            device_id={'sp': partner}, device_id_type=MESH)

    def whole(ref, sem):
        return pltpu.make_async_copy(ref, ref, sem)

    hop = 5
    lag_r = hop * z
    lag_l = hop * (3 - z)
    lag_s = hop * (3 - (z * (3 - z)) // 2)

    def tick(i, carry):
        @pl.when(i < NC)
        def _():
            group, place = i // WG, i % WG

            @pl.when(place == 0)
            def _():
                wo_copy(group).wait()

            w_c = wo_buf[group, :, pl.ds(pl.multiple_of(place * CW, CW), CW)]
            p_buf[i] = jnp.dot(lhs[...], w_c, preferred_element_type=jnp.float32)

        kr, kl = i - lag_r, i - lag_l
        r_live = jnp.logical_and(kr >= 0, kr < NC)
        l_live = jnp.logical_and(kl >= 0, kl < NC)

        def step_right():
            @pl.when(z > 0)
            def _():
                right_copy(kr).wait_recv()

            @pl.when(z < 3)
            def _():
                sr[kr] = p_buf[kr] + rr[kr]
                right_copy(kr).start()

        def step_left():
            @pl.when(z < 3)
            def _():
                left_copy(kl).wait_recv()

            @pl.when(z > 0)
            def _():
                sl[kl] = p_buf[kl] + rl[kl]
                left_copy(kl).start()

        pl.when(jnp.logical_and(l_live, z < 2))(step_left)
        pl.when(r_live)(step_right)
        pl.when(jnp.logical_and(l_live, z >= 2))(step_left)

        k_s = i - lag_s

        @pl.when(jnp.logical_and(k_s >= 0, k_s < NC))
        def _():
            s_all[sp, k_s] = p_buf[k_s] + rr[k_s] + rl[k_s]
            y_copy(k_s).start()
            part_copy(k_s).start()

        k_y = i - lag_s - hop

        @pl.when(jnp.logical_and(k_y >= 0, k_y < NC))
        def _():
            y_copy(k_y).wait_recv()
            fwd_copy(k_y).start()

        return carry

    lax.fori_loop(0, NC + 4 * hop, tick, 0)

    @pl.when(z < 3)
    def _():
        whole(sr, right_send).wait()

    @pl.when(z > 0)
    def _():
        whole(sl, left_send).wait()

    whole(s_all.at[sp], y_send).wait()
    whole(s_all.at[sp], part_send).wait()
    whole(s_all.at[ypeer], f_send).wait()
    whole(s_all.at[partner], part_recv).wait()
    whole(s_all.at[3 - sp], f_recv).wait()


def finish_kernel(s_all, x_ref, wpost_ref, out_h, out_buf, sem):
    blk = 16

    def out_copy(i):
        rows = pl.ds(i * blk, blk)
        return pltpu.make_async_copy(out_buf.at[rows], out_h.at[rows], sem)

    for i in range(ROWS // blk):
        g, r = (i * blk) // OWN, (i * blk) % OWN
        parts = [s_all[g, k, r:r + blk, :] for k in range(NC)]
        sq = parts[0] * parts[0]
        for k in range(1, NC):
            sq = sq + parts[k] * parts[k]
        rs = lax.rsqrt(jnp.sum(sq, axis=-1, keepdims=True) * (1.0 / DM) + NORM_EPS)
        for k in range(NC):
            for hf in range(CW // LANES):
                col = k * CW + hf * LANES
                gain = 1.0 + wpost_ref[col // LANES:col // LANES + 1, :]
                val = s_all[g, k, r:r + blk, hf * LANES:(hf + 1) * LANES] * rs * gain
                cs = slice(col, col + LANES)
                out_buf[i * blk:(i + 1) * blk, cs] = (x_ref[i * blk:(i + 1) * blk, cs].astype(jnp.float32) + val).astype(jnp.bfloat16)
        out_copy(i).start()
    for i in range(ROWS // blk):
        out_copy(i).wait()


def solution(mesh):
    cache_spec = P('dp', 'sp', 'tp', None)
    hbm = pl.BlockSpec(memory_space=pltpu.HBM)
    vmem = pl.BlockSpec(memory_space=pltpu.VMEM)

    def in_hbm(arr):
        return pltpu.with_memory_space_constraint(arr, pltpu.HBM)

    def in_vmem(arr):
        return pltpu.with_memory_space_constraint(arr, pltpu.VMEM)

    def to_rows(c):
        b, t, h, d = c.shape
        return c.reshape(b, t, h, 2, LANES).transpose(0, 1, 3, 2, 4).reshape(b, t * 2 * h, LANES)

    def from_rows(r):
        return r.reshape(ROWS, TB, 2, 2, LANES).transpose(0, 1, 3, 2, 4).reshape(ROWS, TB, 2, HD)

    def local_step(x_in, cur_pos, w_pre, w_q, w_k, w_v, w_o, w_post, k_cache, v_cache):
        half = HD // 2
        inv_freq = jnp.asarray((ROPE_BASE ** (-2.0 * np.arange(half) / (2 * half))).astype(np.float32))
        kr, vr = to_rows(k_cache), to_rows(v_cache)
        f32, bf16 = jnp.float32, jnp.bfloat16
        dma = pltpu.SemaphoreType.DMA
        half_shape = (HALF,) + kr.shape[1:]
        o_far, k_far, v_far, qs, ks, vs = pl.pallas_call(
            far_kernel,
            out_shape=(jax.ShapeDtypeStruct((HROWS, LANES), f32),
                       pltpu.VMEM(half_shape, bf16), pltpu.VMEM(half_shape, bf16),
                       pltpu.VMEM((8 * RP, LANES), f32), pltpu.VMEM((8 * RP, LANES), f32), pltpu.VMEM((8 * RP, LANES), f32)),
            in_specs=[hbm] * 10,
            out_specs=(vmem,) * 6,
            scratch_shapes=[
                pltpu.SMEM((ROWS,), jnp.int32), pltpu.VMEM((1, ROWS), jnp.int32), pltpu.VMEM((1, LANES), f32),
                pltpu.VMEM((DM // LANES, LANES), f32), pltpu.VMEM((ROWS, LANES), f32), pltpu.VMEM((ROWS, LANES), f32),
                pltpu.VMEM((ROWS, DM), bf16), pltpu.VMEM((ROWS, DM), bf16),
                pltpu.VMEM((DM, 1024), bf16), pltpu.VMEM((DM, 512), bf16), pltpu.VMEM((DM, 512), bf16), pltpu.VMEM((8, ROWS, HD), f32),
                dma, dma, dma((NKC,)), dma((NCH,)),
            ],
            compiler_params=pltpu.CompilerParams(vmem_limit_bytes=40 << 20),
            cost_estimate=pl.CostEstimate(flops=2 * 10 ** 9, bytes_accessed=25 * 10 ** 6, transcendentals=0),
            name='attend_far',
        )(in_hbm(cur_pos), in_hbm(cur_pos.reshape(1, ROWS)), in_hbm(inv_freq.reshape(1, LANES)), in_hbm(x_in),
          in_hbm(w_pre.reshape(DM // LANES, LANES)), in_hbm(w_q), in_hbm(w_k), in_hbm(w_v), in_hbm(kr), in_hbm(vr))
        o_got = lax.ppermute(o_far, 'sp', [(0, 2), (1, 3), (2, 0), (3, 1)])
        o_own, k_new, v_new = pl.pallas_call(
            near_kernel,
            out_shape=(pltpu.VMEM((HROWS, LANES), f32),
                       jax.ShapeDtypeStruct(kr.shape, bf16), jax.ShapeDtypeStruct(vr.shape, bf16)),
            in_specs=[hbm, vmem, vmem, vmem, vmem, vmem, hbm, hbm],
            out_specs=(vmem, hbm, hbm),
            scratch_shapes=[
                pltpu.SMEM((ROWS,), jnp.int32), pltpu.VMEM(half_shape, bf16), pltpu.VMEM(half_shape, bf16),
                dma, dma((NCH,)), dma,
            ],
            compiler_params=pltpu.CompilerParams(vmem_limit_bytes=28 << 20),
            cost_estimate=pl.CostEstimate(flops=10 ** 10, bytes_accessed=25 * 10 ** 6, transcendentals=0),
            name='attend_near',
        )(in_hbm(cur_pos), in_vmem(qs), in_vmem(ks), in_vmem(vs), in_vmem(k_far), in_vmem(v_far), in_hbm(kr), in_hbm(vr))
        big = pltpu.VMEM((NC, OWN, CW), f32)
        sums = pl.pallas_call(
            comm_kernel,
            out_shape=pltpu.VMEM((4, NC, OWN, CW), f32),
            in_specs=[vmem, vmem, hbm],
            out_specs=vmem,
            scratch_shapes=[
                pltpu.VMEM((NC // WG, 1024, WG * CW), bf16), pltpu.VMEM((4, LANES, LANES), f32), pltpu.VMEM((MROWS, LANES), f32),
                pltpu.VMEM((8 * OWN, LANES), f32), pltpu.VMEM((MROWS, LANES), f32), pltpu.VMEM((OWN, 1024), bf16),
                big, big, big, big, big,
                dma((NC // WG,)), dma, dma,
                dma, dma((NC,)), dma, dma((NC,)),
                dma, dma, dma, dma((NC,)), dma, dma,
            ],
            compiler_params=pltpu.CompilerParams(vmem_limit_bytes=40 << 20, collective_id=0, has_side_effects=True),
            name='combine',
        )(in_vmem(o_own), o_got, in_hbm(w_o))
        x_out = pl.pallas_call(
            finish_kernel,
            out_shape=jax.ShapeDtypeStruct((ROWS, DM), bf16),
            in_specs=[vmem, vmem, vmem],
            out_specs=hbm,
            scratch_shapes=[pltpu.VMEM((ROWS, DM), bf16), dma],
            compiler_params=pltpu.CompilerParams(vmem_limit_bytes=16 << 20),
            name='finish',
        )(in_vmem(sums), x_in, w_post.reshape(DM // LANES, LANES))
        return x_out, from_rows(k_new), from_rows(v_new)

    return jax.shard_map(local_step, mesh=mesh,
                         in_specs=(P('dp', None), P('dp'), P(None), P(None, 'tp'), P(None, 'tp'), P(None, 'tp'), P('tp', None), P(None), cache_spec, cache_spec),
                         out_specs=(P('dp', None), cache_spec, cache_spec), check_vma=False)
```

```python
import functools

import jax
import jax.numpy as jnp
import numpy as np
from jax import lax
from jax.experimental import pallas as pl
from jax.experimental.pallas import tpu as pltpu
from jax.sharding import PartitionSpec as P

SOFT_CAP = 50.0
ROPE_BASE = 10000.0
NORM_EPS = 1e-6

ROWS = 128
DM = 3840
HD = 256
TB = 64
RP = 136
LANES = 128
BCH = 16
HALF = ROWS // 2
HROWS = 8 * HALF + 8
NCH = HALF // BCH
KC = 768
NKC = DM // KC
SHIFT = 20.0
CW = 256
NC = DM // CW
WG = 3
OWN = 32
MROWS = 8 * OWN + 8
MESH = pl.DeviceIdType.MESH


def attend_rows(row0, bch, pos_ref, kbuf, vbuf, qs, ks, vs, o_ref, before, after):
    tbase = lax.axis_index('sp') * TB
    lane = lax.broadcasted_iota(jnp.int32, (8, LANES), 1)
    row = lax.broadcasted_iota(jnp.int32, (8, LANES), 0)
    row_c = row // 4
    row_h = (row // 2) % 2
    match = (((lane // 2) % 2) == row_c) & ((lane % 2) == row_h)
    match_f = jnp.where(match, 1.0, 0.0).astype(jnp.float32)
    first = row_c == 0
    t_half = [jnp.where(match, lane // 4 + 32 * hf, 1 << 20) for hf in range(2)]
    quad = lax.broadcasted_iota(jnp.int32, (16, LANES), 0) // 4
    zero = jnp.zeros((8, LANES), jnp.float32)

    def chunk(i, l_acc):
        before(i)
        tls = []
        for u in range(bch):
            lb = i * bch + u
            b = row0 + lb
            tl = pos_ref[b] - tbase
            tls.append(tl)
            hit = jnp.logical_and(tl >= 0, tl < TB)
            tc = jnp.clip(tl, 0, TB - 1)
            tile = tc // 4
            tgt = jnp.where(hit, tc - tile * 4, -1)
            sel = quad == tgt
            off = pl.multiple_of(tile * 16, 16)
            kn = ks[pl.ds(b, 8, stride=RP), :]
            vn = vs[pl.ds(b, 8, stride=RP), :]
            kt = kbuf[lb, pl.ds(off, 16), :].astype(jnp.float32)
            vt = vbuf[lb, pl.ds(off, 16), :].astype(jnp.float32)
            kbuf[lb, pl.ds(off, 16), :] = jnp.where(sel, jnp.concatenate([kn, kn], 0), kt).astype(jnp.bfloat16)
            vbuf[lb, pl.ds(off, 16), :] = jnp.where(sel, jnp.concatenate([vn, vn], 0), vt).astype(jnp.bfloat16)
        scores = []
        for u in range(0, bch, 2):
            lb = i * bch + u
            q0 = qs[pl.ds(row0 + lb, 8, stride=RP), :]
            q1 = qs[pl.ds(row0 + lb + 1, 8, stride=RP), :]
            lhs = jnp.concatenate([jnp.concatenate([q0, zero], 1), jnp.concatenate([zero, q1], 1)], 0).astype(jnp.bfloat16)
            kk = jnp.concatenate([kbuf[lb], kbuf[lb + 1]], 1)
            scores.append(lax.dot_general(lhs, kk, (((1,), (1,)), ((), ())), preferred_element_type=jnp.float32))
        weights = []
        for u in range(0, bch, 2):
            pair = []
            for w in range(2):
                part = scores[u // 2][8 * w:8 * w + 8]
                es = []
                for hf in range(2):
                    a = part[:, hf * LANES:(hf + 1) * LANES] * match_f
                    e = pltpu.roll(a, 4, 0)
                    f = jnp.where(first, pltpu.roll(e, LANES - 2, 1), pltpu.roll(e, 2, 1))
                    s = SOFT_CAP * jnp.tanh((a + f) * (HD ** -0.5 / SOFT_CAP))
                    es.append(jnp.where(t_half[hf] <= tls[u + w], jnp.exp(s - SHIFT), 0.0))
                tot = jnp.sum(es[0] + es[1], axis=1, keepdims=True)
                inv = jnp.where(tot > 0.0, 1.0 / tot, 0.0)
                pair.append(jnp.concatenate([es[0] * inv, es[1] * inv], 1))
                l_acc = jnp.where(lane == i * bch + u + w, tot, l_acc)
            weights.append(jnp.concatenate(pair, 0).astype(jnp.bfloat16))
        for u in range(0, bch, 2):
            lb = i * bch + u
            vv = jnp.concatenate([vbuf[lb], vbuf[lb + 1]], 1)
            o = jnp.dot(weights[u // 2], vv, preferred_element_type=jnp.float32)
            o_ref[pl.ds(lb, 8, stride=HALF), :] = o[0:8, 0:LANES]
            o_ref[pl.ds(lb + 1, 8, stride=HALF), :] = o[8:16, LANES:]
        after(i)
        return l_acc

    l_acc = lax.fori_loop(0, HALF // bch, chunk, zero)
    o_ref[pl.ds(8 * HALF, 8), :] = l_acc


def far_kernel(pos_h, posv_h, freq_h, x_h, wpre_h, wq_h, wk_h, wv_h, kc_h, vc_h,
               o_ref, kbuf, vbuf, qs, ks, vs,
               pos_ref, posv, freq, wpre_ref, cos_ref, sin_ref, x_buf, a_buf, wq_buf, wk_buf, wv_buf, acc,
               x_sem, s_sem, w_sem, ki_sem):
    row0 = (1 - lax.axis_index('sp') // 2) * HALF

    def w_start(c):
        rows = pl.ds(c * KC, KC)
        for n, (src, dst) in enumerate(((wk_h, wk_buf), (wv_h, wv_buf), (wq_h, wq_buf))):
            pltpu.make_async_copy(src.at[rows, :], dst.at[rows, :], w_sem.at[c]).start()

    def w_wait(c):
        rows = pl.ds(c * KC, KC)
        for n, (src, dst) in enumerate(((wk_h, wk_buf), (wv_h, wv_buf), (wq_h, wq_buf))):
            pltpu.make_async_copy(src.at[rows, :], dst.at[rows, :], w_sem.at[c]).wait()

    def k_in(i):
        return pltpu.make_async_copy(kc_h.at[pl.ds(row0 + i * BCH, BCH)], kbuf.at[pl.ds(i * BCH, BCH)], ki_sem.at[i])

    def v_in(i):
        return pltpu.make_async_copy(vc_h.at[pl.ds(row0 + i * BCH, BCH)], vbuf.at[pl.ds(i * BCH, BCH)], ki_sem.at[i])

    small = [pltpu.make_async_copy(a, b, s_sem) for a, b in (
        (wpre_h, wpre_ref), (posv_h, posv), (freq_h, freq), (pos_h, pos_ref))]
    for c in small:
        c.start()
    x_copy = pltpu.make_async_copy(x_h, x_buf, x_sem)
    x_copy.start()
    w_start(0)
    for c in small:
        c.wait()
    w_start(1)
    pos_col = jnp.broadcast_to(posv[...].astype(jnp.float32), (ROWS, LANES)).T
    ang = pos_col * freq[...]
    cos_ref[...] = jnp.cos(ang)
    sin_ref[...] = jnp.sin(ang)
    x_copy.wait()
    w_start(2)

    gain = 1.0 + jnp.concatenate([wpre_ref[k:k + 1, :] for k in range(DM // LANES)], 1)

    def norm_rows(i, carry):
        r = pl.multiple_of(i * 16, 16)
        xb = x_buf[pl.ds(r, 16), :].astype(jnp.float32)
        ms = jnp.mean(xb * xb, axis=-1, keepdims=True)
        a_buf[pl.ds(r, 16), :] = (xb * lax.rsqrt(ms + NORM_EPS) * gain).astype(jnp.bfloat16)
        return carry

    lax.fori_loop(0, ROWS // 16, norm_rows, 0)

    for c in range(NKC):
        w_wait(c)
        if c + 3 < NKC:
            w_start(c + 3)
        for n in ((), (), (0,), (1,), (2, 3))[c]:
            k_in(n).start()
            v_in(n).start()
        rows = slice(c * KC, (c + 1) * KC)
        a_c = a_buf[:, rows]
        for i in range(8):
            if i < 2:
                w_c = wk_buf[rows, i * HD:(i + 1) * HD]
            elif i < 4:
                w_c = wv_buf[rows, (i - 2) * HD:(i - 1) * HD]
            else:
                w_c = wq_buf[rows, (i - 4) * HD:(i - 3) * HD]
            y = jnp.dot(a_c, w_c, preferred_element_type=jnp.float32)
            if c == 0:
                acc[i] = y
                continue
            y = acc[i] + y
            if c < NKC - 1:
                acc[i] = y
                continue
            lo, hi = y[:, :LANES], y[:, LANES:]
            if 2 <= i < 4:
                h = i - 2
                for rep in range(2):
                    vs[pl.ds((rep * 4 + h) * RP, ROWS), :] = lo
                    vs[pl.ds((rep * 4 + 2 + h) * RP, ROWS), :] = hi
            else:
                cos_t, sin_t = cos_ref[...], sin_ref[...]
                rlo = lo * cos_t - hi * sin_t
                rhi = hi * cos_t + lo * sin_t
                if i < 2:
                    for rep in range(2):
                        ks[pl.ds((rep * 4 + i) * RP, ROWS), :] = rlo
                        ks[pl.ds((rep * 4 + 2 + i) * RP, ROWS), :] = rhi
                else:
                    qs[pl.ds((i - 4) * RP, ROWS), :] = rlo
                    qs[pl.ds((4 + i - 4) * RP, ROWS), :] = rhi

    def before(i):
        for n in range(2):
            k_in(2 * i + n).wait()
            v_in(2 * i + n).wait()

    attend_rows(row0, 2 * BCH, pos_ref, kbuf, vbuf, qs, ks, vs, o_ref, before, lambda i: None)


def near_kernel(pos_h, qs, ks, vs, kfar, vfar, kc_h, vc_h,
                o_ref, ko_h, vo_h,
                pos_ref, kbuf, vbuf, p_sem, ki_sem, w_sem):
    yy = lax.axis_index('sp') // 2
    row0 = yy * HALF
    far0 = (1 - yy) * HALF

    def k_in(i):
        return pltpu.make_async_copy(kc_h.at[pl.ds(row0 + i * BCH, BCH)], kbuf.at[pl.ds(i * BCH, BCH)], ki_sem.at[i])

    def v_in(i):
        return pltpu.make_async_copy(vc_h.at[pl.ds(row0 + i * BCH, BCH)], vbuf.at[pl.ds(i * BCH, BCH)], ki_sem.at[i])

    def k_out(i):
        return pltpu.make_async_copy(kbuf.at[pl.ds(i * BCH, BCH)], ko_h.at[pl.ds(row0 + i * BCH, BCH)], w_sem)

    def v_out(i):
        return pltpu.make_async_copy(vbuf.at[pl.ds(i * BCH, BCH)], vo_h.at[pl.ds(row0 + i * BCH, BCH)], w_sem)

    def kf_out(i):
        return pltpu.make_async_copy(kfar.at[pl.ds(i * BCH, BCH)], ko_h.at[pl.ds(far0 + i * BCH, BCH)], w_sem)

    def vf_out(i):
        return pltpu.make_async_copy(vfar.at[pl.ds(i * BCH, BCH)], vo_h.at[pl.ds(far0 + i * BCH, BCH)], w_sem)

    p_copy = pltpu.make_async_copy(pos_h, pos_ref, p_sem)
    p_copy.start()
    for i in range(NCH):
        k_in(i).start()
        v_in(i).start()
    p_copy.wait()

    def before(i):
        k_in(i).wait()
        v_in(i).wait()
        kf_out(i).start()
        vf_out(i).start()

    def after(i):
        k_out(i).start()
        v_out(i).start()

    attend_rows(row0, BCH, pos_ref, kbuf, vbuf, qs, ks, vs, o_ref, before, after)
    for i in range(NCH):
        kf_out(i).wait()
        vf_out(i).wait()
        k_out(i).wait()
        v_out(i).wait()


def comm_kernel(o_own, o_got, wo_h, s_all,
                wo_buf, fac, m1, m2, r1, lhs, p_buf, rr, rl, sr, sl,
                w_sem, r1_send, r1_recv,
                right_send, right_recv, left_send, left_recv,
                part_send, part_recv, y_send, y_recv, f_send, f_recv, a_send):
    z = lax.axis_index('tp')
    sp = lax.axis_index('sp')
    core = sp % 2
    partner = sp + 1 - 2 * core
    ypeer = (sp + 2) % 4
    middle = (z * (3 - z)) // 2
    across = z + 1 - 2 * (z % 2)

    def wo_copy(k):
        return pltpu.make_async_copy(wo_h.at[:, pl.ds(pl.multiple_of(k * WG * CW, CW), WG * CW)], wo_buf.at[k], w_sem.at[k])

    for k in range(NC // WG):
        wo_copy(k).start()

    @pl.when(z == 0)
    def _():
        rr[...] = jnp.zeros_like(rr)

    @pl.when(z == 3)
    def _():
        rl[...] = jnp.zeros_like(rl)

    bar = pltpu.get_barrier_semaphore()
    pl.semaphore_signal(bar, inc=1, device_id={'sp': partner}, device_id_type=MESH)
    pl.semaphore_signal(bar, inc=1, device_id={'sp': ypeer}, device_id_type=MESH)
    pl.semaphore_signal(bar, inc=1, device_id={'sp': ypeer, 'tp': across}, device_id_type=MESH)

    @pl.when(z > 0)
    def _():
        pl.semaphore_signal(bar, inc=1, device_id={'tp': z - 1}, device_id_type=MESH)

    @pl.when(z < 3)
    def _():
        pl.semaphore_signal(bar, inc=1, device_id={'tp': z + 1}, device_id_type=MESH)

    def shares(l_a, l_b, slot):
        tot = l_a + l_b
        inv = jnp.where(tot > 0.0, 1.0 / tot, 0.0)
        for w, l in enumerate((l_a, l_b)):
            fac[slot + w] = jnp.concatenate([l * inv, jnp.zeros((LANES - 8, LANES), jnp.float32)], 0).T
        return tot

    mine = pl.multiple_of(core * OWN, OWN)
    theirs = pl.multiple_of((1 - core) * OWN, OWN)
    tot = shares(o_own[pl.ds(8 * HALF, 8), :], o_got[pl.ds(8 * HALF, 8), :], 0)

    def merge_half(r0, dst):
        fa, fb = fac[0, pl.ds(r0, OWN), :], fac[1, pl.ds(r0, OWN), :]
        for j in range(8):
            rows = pl.ds(pl.multiple_of(j * HALF + r0, 8), OWN)
            dst[pl.ds(j * OWN, OWN), :] = o_own[rows, :] * fa[:, j:j + 1] + o_got[rows, :] * fb[:, j:j + 1]

    merge_half(theirs, m1)
    m1[pl.ds(8 * OWN, 8), :] = tot
    merge_half(mine, m2)
    pair = pltpu.make_async_remote_copy(
        src_ref=m1, dst_ref=r1, send_sem=r1_send, recv_sem=r1_recv, device_id={'sp': partner}, device_id_type=MESH)
    pl.semaphore_wait(bar, 4 + middle)
    pair.start()
    pair.wait()
    shares(tot, r1[pl.ds(8 * OWN, 8), :], 2)
    fa, fb = fac[2, pl.ds(mine, OWN), :], fac[3, pl.ds(mine, OWN), :]
    for j in range(8):
        c, hq = j // 4, j % 4
        val = m2[j * OWN:(j + 1) * OWN, :] * fa[:, j:j + 1] + r1[j * OWN:(j + 1) * OWN, :] * fb[:, j:j + 1]
        lhs[:, (hq * 2 + c) * LANES:(hq * 2 + c + 1) * LANES] = val.astype(jnp.bfloat16)

    def right_copy(k):
        return pltpu.make_async_remote_copy(
            src_ref=sr.at[k], dst_ref=rr.at[k], send_sem=right_send, recv_sem=right_recv.at[k],
            device_id={'tp': z + 1}, device_id_type=MESH)

    def left_copy(k):
        return pltpu.make_async_remote_copy(
            src_ref=sl.at[k], dst_ref=rl.at[k], send_sem=left_send, recv_sem=left_recv.at[k],
            device_id={'tp': z - 1}, device_id_type=MESH)

    def part_copy(k):
        return pltpu.make_async_remote_copy(
            src_ref=s_all.at[sp, k], dst_ref=s_all.at[sp, k], send_sem=part_send, recv_sem=part_recv,
            device_id={'sp': partner}, device_id_type=MESH)

    def y_copy(k):
        return pltpu.make_async_remote_copy(
            src_ref=s_all.at[sp, k], dst_ref=s_all.at[sp, k], send_sem=y_send, recv_sem=y_recv.at[k],
            device_id={'sp': ypeer}, device_id_type=MESH)

    def across_copy():
        last = NC - 1
        return pltpu.make_async_remote_copy(
            src_ref=s_all.at[sp, last], dst_ref=s_all.at[sp, last], send_sem=a_send, recv_sem=y_recv.at[last],
            device_id={'sp': ypeer, 'tp': across}, device_id_type=MESH)

    def fwd_copy(k):
        return pltpu.make_async_remote_copy(
            src_ref=s_all.at[ypeer, k], dst_ref=s_all.at[ypeer, k], send_sem=f_send, recv_sem=f_recv,
            device_id={'sp': partner}, device_id_type=MESH)

    def whole(ref, sem):
        return pltpu.make_async_copy(ref, ref, sem)

    hop = 5
    lag_r = hop * z
    lag_l = hop * (3 - z)
    lag_s = hop * (3 - (z * (3 - z)) // 2)

    def tick(i, carry):
        @pl.when(i < NC)
        def _():
            group, place = i // WG, i % WG

            @pl.when(place == 0)
            def _():
                wo_copy(group).wait()

            w_c = wo_buf[group, :, pl.ds(pl.multiple_of(place * CW, CW), CW)]
            p_buf[i] = jnp.dot(lhs[...], w_c, preferred_element_type=jnp.float32)

        kr, kl = i - lag_r, i - lag_l
        r_live = jnp.logical_and(kr >= 0, kr < NC)
        l_live = jnp.logical_and(kl >= 0, kl < NC)

        def step_right():
            @pl.when(z > 0)
            def _():
                right_copy(kr).wait_recv()

            @pl.when(z < 3)
            def _():
                sr[kr] = p_buf[kr] + rr[kr]
                right_copy(kr).start()

        def step_left():
            @pl.when(z < 3)
            def _():
                left_copy(kl).wait_recv()

            @pl.when(z > 0)
            def _():
                sl[kl] = p_buf[kl] + rl[kl]
                left_copy(kl).start()

        pl.when(jnp.logical_and(l_live, z < 2))(step_left)
        pl.when(r_live)(step_right)
        pl.when(jnp.logical_and(l_live, z >= 2))(step_left)

        k_s = i - lag_s

        @pl.when(jnp.logical_and(k_s >= 0, k_s < NC))
        def _():
            s_all[sp, k_s] = p_buf[k_s] + rr[k_s] + rl[k_s]

            @pl.when(jnp.logical_or(k_s < NC - 1, middle == 1))
            def _():
                y_copy(k_s).start()

            @pl.when(jnp.logical_and(k_s == NC - 1, middle == 1))
            def _():
                across_copy().start()

            part_copy(k_s).start()

        k_y = i - lag_s - hop

        @pl.when(jnp.logical_and(k_y >= 0, k_y < NC))
        def _():
            y_copy(k_y).wait_recv()
            fwd_copy(k_y).start()

        return carry

    lax.fori_loop(0, NC + 4 * hop, tick, 0)

    @pl.when(z < 3)
    def _():
        whole(sr, right_send).wait()

    @pl.when(z > 0)
    def _():
        whole(sl, left_send).wait()

    @pl.when(middle == 1)
    def _():
        whole(s_all.at[sp], y_send).wait()
        whole(s_all.at[sp, NC - 1], a_send).wait()

    @pl.when(middle == 0)
    def _():
        whole(s_all.at[sp, pl.ds(0, NC - 1)], y_send).wait()

    whole(s_all.at[sp], part_send).wait()
    whole(s_all.at[ypeer], f_send).wait()
    whole(s_all.at[partner], part_recv).wait()
    whole(s_all.at[3 - sp], f_recv).wait()


def finish_kernel(s_all, x_ref, wpost_ref, out_h, out_buf, sem):
    blk = 16

    def out_copy(i):
        rows = pl.ds(i * blk, blk)
        return pltpu.make_async_copy(out_buf.at[rows], out_h.at[rows], sem)

    for i in range(ROWS // blk):
        g, r = (i * blk) // OWN, (i * blk) % OWN
        parts = [s_all[g, k, r:r + blk, :] for k in range(NC)]
        sq = parts[0] * parts[0]
        for k in range(1, NC):
            sq = sq + parts[k] * parts[k]
        rs = lax.rsqrt(jnp.sum(sq, axis=-1, keepdims=True) * (1.0 / DM) + NORM_EPS)
        for k in range(NC):
            for hf in range(CW // LANES):
                col = k * CW + hf * LANES
                gain = 1.0 + wpost_ref[col // LANES:col // LANES + 1, :]
                val = s_all[g, k, r:r + blk, hf * LANES:(hf + 1) * LANES] * rs * gain
                cs = slice(col, col + LANES)
                out_buf[i * blk:(i + 1) * blk, cs] = (x_ref[i * blk:(i + 1) * blk, cs].astype(jnp.float32) + val).astype(jnp.bfloat16)
        out_copy(i).start()
    for i in range(ROWS // blk):
        out_copy(i).wait()


def solution(mesh):
    cache_spec = P('dp', 'sp', 'tp', None)
    hbm = pl.BlockSpec(memory_space=pltpu.HBM)
    vmem = pl.BlockSpec(memory_space=pltpu.VMEM)

    def in_hbm(arr):
        return pltpu.with_memory_space_constraint(arr, pltpu.HBM)

    def in_vmem(arr):
        return pltpu.with_memory_space_constraint(arr, pltpu.VMEM)

    def to_rows(c):
        b, t, h, d = c.shape
        return c.reshape(b, t, h, 2, LANES).transpose(0, 1, 3, 2, 4).reshape(b, t * 2 * h, LANES)

    def from_rows(r):
        return r.reshape(ROWS, TB, 2, 2, LANES).transpose(0, 1, 3, 2, 4).reshape(ROWS, TB, 2, HD)

    def local_step(x_in, cur_pos, w_pre, w_q, w_k, w_v, w_o, w_post, k_cache, v_cache):
        half = HD // 2
        inv_freq = jnp.asarray((ROPE_BASE ** (-2.0 * np.arange(half) / (2 * half))).astype(np.float32))
        kr, vr = to_rows(k_cache), to_rows(v_cache)
        f32, bf16 = jnp.float32, jnp.bfloat16
        dma = pltpu.SemaphoreType.DMA
        half_shape = (HALF,) + kr.shape[1:]
        o_far, k_far, v_far, qs, ks, vs = pl.pallas_call(
            far_kernel,
            out_shape=(jax.ShapeDtypeStruct((HROWS, LANES), f32),
                       pltpu.VMEM(half_shape, bf16), pltpu.VMEM(half_shape, bf16),
                       pltpu.VMEM((8 * RP, LANES), f32), pltpu.VMEM((8 * RP, LANES), f32), pltpu.VMEM((8 * RP, LANES), f32)),
            in_specs=[hbm] * 10,
            out_specs=(vmem,) * 6,
            scratch_shapes=[
                pltpu.SMEM((ROWS,), jnp.int32), pltpu.VMEM((1, ROWS), jnp.int32), pltpu.VMEM((1, LANES), f32),
                pltpu.VMEM((DM // LANES, LANES), f32), pltpu.VMEM((ROWS, LANES), f32), pltpu.VMEM((ROWS, LANES), f32),
                pltpu.VMEM((ROWS, DM), bf16), pltpu.VMEM((ROWS, DM), bf16),
                pltpu.VMEM((DM, 1024), bf16), pltpu.VMEM((DM, 512), bf16), pltpu.VMEM((DM, 512), bf16), pltpu.VMEM((8, ROWS, HD), f32),
                dma, dma, dma((NKC,)), dma((NCH,)),
            ],
            compiler_params=pltpu.CompilerParams(vmem_limit_bytes=40 << 20),
            cost_estimate=pl.CostEstimate(flops=2 * 10 ** 9, bytes_accessed=25 * 10 ** 6, transcendentals=0),
            name='attend_far',
        )(in_hbm(cur_pos), in_hbm(cur_pos.reshape(1, ROWS)), in_hbm(inv_freq.reshape(1, LANES)), in_hbm(x_in),
          in_hbm(w_pre.reshape(DM // LANES, LANES)), in_hbm(w_q), in_hbm(w_k), in_hbm(w_v), in_hbm(kr), in_hbm(vr))
        o_got = lax.ppermute(o_far, 'sp', [(0, 2), (1, 3), (2, 0), (3, 1)])
        o_own, k_new, v_new = pl.pallas_call(
            near_kernel,
            out_shape=(pltpu.VMEM((HROWS, LANES), f32),
                       jax.ShapeDtypeStruct(kr.shape, bf16), jax.ShapeDtypeStruct(vr.shape, bf16)),
            in_specs=[hbm, vmem, vmem, vmem, vmem, vmem, hbm, hbm],
            out_specs=(vmem, hbm, hbm),
            scratch_shapes=[
                pltpu.SMEM((ROWS,), jnp.int32), pltpu.VMEM(half_shape, bf16), pltpu.VMEM(half_shape, bf16),
                dma, dma((NCH,)), dma,
            ],
            compiler_params=pltpu.CompilerParams(vmem_limit_bytes=28 << 20),
            cost_estimate=pl.CostEstimate(flops=10 ** 10, bytes_accessed=25 * 10 ** 6, transcendentals=0),
            name='attend_near',
        )(in_hbm(cur_pos), in_vmem(qs), in_vmem(ks), in_vmem(vs), in_vmem(k_far), in_vmem(v_far), in_hbm(kr), in_hbm(vr))
        big = pltpu.VMEM((NC, OWN, CW), f32)
        sums = pl.pallas_call(
            comm_kernel,
            out_shape=pltpu.VMEM((4, NC, OWN, CW), f32),
            in_specs=[vmem, vmem, hbm],
            out_specs=vmem,
            scratch_shapes=[
                pltpu.VMEM((NC // WG, 1024, WG * CW), bf16), pltpu.VMEM((4, LANES, LANES), f32), pltpu.VMEM((MROWS, LANES), f32),
                pltpu.VMEM((8 * OWN, LANES), f32), pltpu.VMEM((MROWS, LANES), f32), pltpu.VMEM((OWN, 1024), bf16),
                big, big, big, big, big,
                dma((NC // WG,)), dma, dma,
                dma, dma((NC,)), dma, dma((NC,)),
                dma, dma, dma, dma((NC,)), dma, dma, dma,
            ],
            compiler_params=pltpu.CompilerParams(vmem_limit_bytes=40 << 20, collective_id=0, has_side_effects=True),
            name='combine',
        )(in_vmem(o_own), o_got, in_hbm(w_o))
        x_out = pl.pallas_call(
            finish_kernel,
            out_shape=jax.ShapeDtypeStruct((ROWS, DM), bf16),
            in_specs=[vmem, vmem, vmem],
            out_specs=hbm,
            scratch_shapes=[pltpu.VMEM((ROWS, DM), bf16), dma],
            compiler_params=pltpu.CompilerParams(vmem_limit_bytes=16 << 20),
            name='finish',
        )(in_vmem(sums), x_in, w_post.reshape(DM // LANES, LANES))
        return x_out, from_rows(k_new), from_rows(v_new)

    return jax.shard_map(local_step, mesh=mesh,
                         in_specs=(P('dp', None), P('dp'), P(None), P(None, 'tp'), P(None, 'tp'), P(None, 'tp'), P('tp', None), P(None), cache_spec, cache_spec),
                         out_specs=(P('dp', None), cache_spec, cache_spec), check_vma=False)
```

```python
import functools

import jax
import jax.numpy as jnp
import numpy as np
from jax import lax
from jax.experimental import pallas as pl
from jax.experimental.pallas import tpu as pltpu
from jax.sharding import PartitionSpec as P

SOFT_CAP = 50.0
ROPE_BASE = 10000.0
NORM_EPS = 1e-6

ROWS = 128
DM = 3840
HD = 256
TB = 64
RP = 136
LANES = 128
BCH = 16
HALF = ROWS // 2
HROWS = 8 * HALF + 8
NCH = HALF // BCH
KC = 768
NKC = DM // KC
SHIFT = 20.0
CW = 256
NC = DM // CW
WG = 3
LASTS = 3
OWN = 32
MROWS = 8 * OWN + 8
MESH = pl.DeviceIdType.MESH


def attend_rows(row0, bch, pos_ref, kbuf, vbuf, qs, ks, vs, o_ref, before, after):
    tbase = lax.axis_index('sp') * TB
    lane = lax.broadcasted_iota(jnp.int32, (8, LANES), 1)
    row = lax.broadcasted_iota(jnp.int32, (8, LANES), 0)
    row_c = row // 4
    row_h = (row // 2) % 2
    match = (((lane // 2) % 2) == row_c) & ((lane % 2) == row_h)
    match_f = jnp.where(match, 1.0, 0.0).astype(jnp.float32)
    first = row_c == 0
    t_half = [jnp.where(match, lane // 4 + 32 * hf, 1 << 20) for hf in range(2)]
    quad = lax.broadcasted_iota(jnp.int32, (16, LANES), 0) // 4
    zero = jnp.zeros((8, LANES), jnp.float32)

    def chunk(i, l_acc):
        before(i)
        tls = []
        for u in range(bch):
            lb = i * bch + u
            b = row0 + lb
            tl = pos_ref[b] - tbase
            tls.append(tl)
            hit = jnp.logical_and(tl >= 0, tl < TB)
            tc = jnp.clip(tl, 0, TB - 1)
            tile = tc // 4
            tgt = jnp.where(hit, tc - tile * 4, -1)
            sel = quad == tgt
            off = pl.multiple_of(tile * 16, 16)
            kn = ks[pl.ds(b, 8, stride=RP), :]
            vn = vs[pl.ds(b, 8, stride=RP), :]
            kt = kbuf[lb, pl.ds(off, 16), :].astype(jnp.float32)
            vt = vbuf[lb, pl.ds(off, 16), :].astype(jnp.float32)
            kbuf[lb, pl.ds(off, 16), :] = jnp.where(sel, jnp.concatenate([kn, kn], 0), kt).astype(jnp.bfloat16)
            vbuf[lb, pl.ds(off, 16), :] = jnp.where(sel, jnp.concatenate([vn, vn], 0), vt).astype(jnp.bfloat16)
        scores = []
        for u in range(0, bch, 2):
            lb = i * bch + u
            q0 = qs[pl.ds(row0 + lb, 8, stride=RP), :]
            q1 = qs[pl.ds(row0 + lb + 1, 8, stride=RP), :]
            lhs = jnp.concatenate([jnp.concatenate([q0, zero], 1), jnp.concatenate([zero, q1], 1)], 0).astype(jnp.bfloat16)
            kk = jnp.concatenate([kbuf[lb], kbuf[lb + 1]], 1)
            scores.append(lax.dot_general(lhs, kk, (((1,), (1,)), ((), ())), preferred_element_type=jnp.float32))
        weights = []
        for u in range(0, bch, 2):
            pair = []
            for w in range(2):
                part = scores[u // 2][8 * w:8 * w + 8]
                es = []
                for hf in range(2):
                    a = part[:, hf * LANES:(hf + 1) * LANES] * match_f
                    e = pltpu.roll(a, 4, 0)
                    f = jnp.where(first, pltpu.roll(e, LANES - 2, 1), pltpu.roll(e, 2, 1))
                    s = SOFT_CAP * jnp.tanh((a + f) * (HD ** -0.5 / SOFT_CAP))
                    es.append(jnp.where(t_half[hf] <= tls[u + w], jnp.exp(s - SHIFT), 0.0))
                tot = jnp.sum(es[0] + es[1], axis=1, keepdims=True)
                inv = jnp.where(tot > 0.0, 1.0 / tot, 0.0)
                pair.append(jnp.concatenate([es[0] * inv, es[1] * inv], 1))
                l_acc = jnp.where(lane == i * bch + u + w, tot, l_acc)
            weights.append(jnp.concatenate(pair, 0).astype(jnp.bfloat16))
        for u in range(0, bch, 2):
            lb = i * bch + u
            vv = jnp.concatenate([vbuf[lb], vbuf[lb + 1]], 1)
            o = jnp.dot(weights[u // 2], vv, preferred_element_type=jnp.float32)
            o_ref[pl.ds(lb, 8, stride=HALF), :] = o[0:8, 0:LANES]
            o_ref[pl.ds(lb + 1, 8, stride=HALF), :] = o[8:16, LANES:]
        after(i)
        return l_acc

    l_acc = lax.fori_loop(0, HALF // bch, chunk, zero)
    o_ref[pl.ds(8 * HALF, 8), :] = l_acc


def far_kernel(pos_h, posv_h, freq_h, x_h, wpre_h, wq_h, wk_h, wv_h, kc_h, vc_h,
               o_ref, kbuf, vbuf, qs, ks, vs,
               pos_ref, posv, freq, wpre_ref, cos_ref, sin_ref, x_buf, a_buf, wq_buf, wk_buf, wv_buf, acc,
               x_sem, s_sem, w_sem, ki_sem):
    row0 = (1 - lax.axis_index('sp') // 2) * HALF

    def w_start(c):
        rows = pl.ds(c * KC, KC)
        for n, (src, dst) in enumerate(((wk_h, wk_buf), (wv_h, wv_buf), (wq_h, wq_buf))):
            pltpu.make_async_copy(src.at[rows, :], dst.at[rows, :], w_sem.at[c]).start()

    def w_wait(c):
        rows = pl.ds(c * KC, KC)
        for n, (src, dst) in enumerate(((wk_h, wk_buf), (wv_h, wv_buf), (wq_h, wq_buf))):
            pltpu.make_async_copy(src.at[rows, :], dst.at[rows, :], w_sem.at[c]).wait()

    def k_in(i):
        return pltpu.make_async_copy(kc_h.at[pl.ds(row0 + i * BCH, BCH)], kbuf.at[pl.ds(i * BCH, BCH)], ki_sem.at[i])

    def v_in(i):
        return pltpu.make_async_copy(vc_h.at[pl.ds(row0 + i * BCH, BCH)], vbuf.at[pl.ds(i * BCH, BCH)], ki_sem.at[i])

    small = [pltpu.make_async_copy(a, b, s_sem) for a, b in (
        (wpre_h, wpre_ref), (posv_h, posv), (freq_h, freq), (pos_h, pos_ref))]
    for c in small:
        c.start()
    x_copy = pltpu.make_async_copy(x_h, x_buf, x_sem)
    x_copy.start()
    w_start(0)
    for c in small:
        c.wait()
    w_start(1)
    pos_col = jnp.broadcast_to(posv[...].astype(jnp.float32), (ROWS, LANES)).T
    ang = pos_col * freq[...]
    cos_ref[...] = jnp.cos(ang)
    sin_ref[...] = jnp.sin(ang)
    x_copy.wait()
    w_start(2)

    gain = 1.0 + jnp.concatenate([wpre_ref[k:k + 1, :] for k in range(DM // LANES)], 1)

    def norm_rows(i, carry):
        r = pl.multiple_of(i * 16, 16)
        xb = x_buf[pl.ds(r, 16), :].astype(jnp.float32)
        ms = jnp.mean(xb * xb, axis=-1, keepdims=True)
        a_buf[pl.ds(r, 16), :] = (xb * lax.rsqrt(ms + NORM_EPS) * gain).astype(jnp.bfloat16)
        return carry

    lax.fori_loop(0, ROWS // 16, norm_rows, 0)

    for c in range(NKC):
        w_wait(c)
        if c + 3 < NKC:
            w_start(c + 3)
        for n in ((), (), (0,), (1,), (2, 3))[c]:
            k_in(n).start()
            v_in(n).start()
        rows = slice(c * KC, (c + 1) * KC)
        a_c = a_buf[:, rows]
        for i in range(8):
            if i < 2:
                w_c = wk_buf[rows, i * HD:(i + 1) * HD]
            elif i < 4:
                w_c = wv_buf[rows, (i - 2) * HD:(i - 1) * HD]
            else:
                w_c = wq_buf[rows, (i - 4) * HD:(i - 3) * HD]
            y = jnp.dot(a_c, w_c, preferred_element_type=jnp.float32)
            if c == 0:
                acc[i] = y
                continue
            y = acc[i] + y
            if c < NKC - 1:
                acc[i] = y
                continue
            lo, hi = y[:, :LANES], y[:, LANES:]
            if 2 <= i < 4:
                h = i - 2
                for rep in range(2):
                    vs[pl.ds((rep * 4 + h) * RP, ROWS), :] = lo
                    vs[pl.ds((rep * 4 + 2 + h) * RP, ROWS), :] = hi
            else:
                cos_t, sin_t = cos_ref[...], sin_ref[...]
                rlo = lo * cos_t - hi * sin_t
                rhi = hi * cos_t + lo * sin_t
                if i < 2:
                    for rep in range(2):
                        ks[pl.ds((rep * 4 + i) * RP, ROWS), :] = rlo
                        ks[pl.ds((rep * 4 + 2 + i) * RP, ROWS), :] = rhi
                else:
                    qs[pl.ds((i - 4) * RP, ROWS), :] = rlo
                    qs[pl.ds((4 + i - 4) * RP, ROWS), :] = rhi

    def before(i):
        for n in range(2):
            k_in(2 * i + n).wait()
            v_in(2 * i + n).wait()

    attend_rows(row0, 2 * BCH, pos_ref, kbuf, vbuf, qs, ks, vs, o_ref, before, lambda i: None)


def near_kernel(pos_h, qs, ks, vs, kfar, vfar, kc_h, vc_h,
                o_ref, ko_h, vo_h,
                pos_ref, kbuf, vbuf, p_sem, ki_sem, w_sem):
    yy = lax.axis_index('sp') // 2
    row0 = yy * HALF
    far0 = (1 - yy) * HALF

    def k_in(i):
        return pltpu.make_async_copy(kc_h.at[pl.ds(row0 + i * BCH, BCH)], kbuf.at[pl.ds(i * BCH, BCH)], ki_sem.at[i])

    def v_in(i):
        return pltpu.make_async_copy(vc_h.at[pl.ds(row0 + i * BCH, BCH)], vbuf.at[pl.ds(i * BCH, BCH)], ki_sem.at[i])

    def k_out(i):
        return pltpu.make_async_copy(kbuf.at[pl.ds(i * BCH, BCH)], ko_h.at[pl.ds(row0 + i * BCH, BCH)], w_sem)

    def v_out(i):
        return pltpu.make_async_copy(vbuf.at[pl.ds(i * BCH, BCH)], vo_h.at[pl.ds(row0 + i * BCH, BCH)], w_sem)

    def kf_out(i):
        return pltpu.make_async_copy(kfar.at[pl.ds(i * BCH, BCH)], ko_h.at[pl.ds(far0 + i * BCH, BCH)], w_sem)

    def vf_out(i):
        return pltpu.make_async_copy(vfar.at[pl.ds(i * BCH, BCH)], vo_h.at[pl.ds(far0 + i * BCH, BCH)], w_sem)

    p_copy = pltpu.make_async_copy(pos_h, pos_ref, p_sem)
    p_copy.start()
    for i in range(NCH):
        k_in(i).start()
        v_in(i).start()
    p_copy.wait()

    def before(i):
        k_in(i).wait()
        v_in(i).wait()
        kf_out(i).start()
        vf_out(i).start()

    def after(i):
        k_out(i).start()
        v_out(i).start()

    attend_rows(row0, BCH, pos_ref, kbuf, vbuf, qs, ks, vs, o_ref, before, after)
    for i in range(NCH):
        kf_out(i).wait()
        vf_out(i).wait()
        k_out(i).wait()
        v_out(i).wait()


def comm_kernel(o_own, o_got, wo_h, s_all,
                wo_buf, fac, m1, m2, r1, lhs, p_buf, rr, rl, sr, sl,
                w_sem, r1_send, r1_recv,
                right_send, right_recv, left_send, left_recv,
                part_send, part_recv, y_send, y_recv, f_send, f_recv, a_send):
    z = lax.axis_index('tp')
    sp = lax.axis_index('sp')
    core = sp % 2
    partner = sp + 1 - 2 * core
    ypeer = (sp + 2) % 4
    middle = (z * (3 - z)) // 2
    across = z + 1 - 2 * (z % 2)

    def wo_copy(k):
        return pltpu.make_async_copy(wo_h.at[:, pl.ds(pl.multiple_of(k * WG * CW, CW), WG * CW)], wo_buf.at[k], w_sem.at[k])

    for k in range(NC // WG):
        wo_copy(k).start()

    @pl.when(z == 0)
    def _():
        rr[...] = jnp.zeros_like(rr)

    @pl.when(z == 3)
    def _():
        rl[...] = jnp.zeros_like(rl)

    bar = pltpu.get_barrier_semaphore()
    pl.semaphore_signal(bar, inc=1, device_id={'sp': partner}, device_id_type=MESH)
    pl.semaphore_signal(bar, inc=1, device_id={'sp': ypeer}, device_id_type=MESH)
    pl.semaphore_signal(bar, inc=1, device_id={'sp': ypeer, 'tp': across}, device_id_type=MESH)

    @pl.when(z > 0)
    def _():
        pl.semaphore_signal(bar, inc=1, device_id={'tp': z - 1}, device_id_type=MESH)

    @pl.when(z < 3)
    def _():
        pl.semaphore_signal(bar, inc=1, device_id={'tp': z + 1}, device_id_type=MESH)

    def shares(l_a, l_b, slot):
        tot = l_a + l_b
        inv = jnp.where(tot > 0.0, 1.0 / tot, 0.0)
        for w, l in enumerate((l_a, l_b)):
            fac[slot + w] = jnp.concatenate([l * inv, jnp.zeros((LANES - 8, LANES), jnp.float32)], 0).T
        return tot

    mine = pl.multiple_of(core * OWN, OWN)
    theirs = pl.multiple_of((1 - core) * OWN, OWN)
    tot = shares(o_own[pl.ds(8 * HALF, 8), :], o_got[pl.ds(8 * HALF, 8), :], 0)

    def merge_half(r0, dst):
        fa, fb = fac[0, pl.ds(r0, OWN), :], fac[1, pl.ds(r0, OWN), :]
        for j in range(8):
            rows = pl.ds(pl.multiple_of(j * HALF + r0, 8), OWN)
            dst[pl.ds(j * OWN, OWN), :] = o_own[rows, :] * fa[:, j:j + 1] + o_got[rows, :] * fb[:, j:j + 1]

    merge_half(theirs, m1)
    m1[pl.ds(8 * OWN, 8), :] = tot
    merge_half(mine, m2)
    pair = pltpu.make_async_remote_copy(
        src_ref=m1, dst_ref=r1, send_sem=r1_send, recv_sem=r1_recv, device_id={'sp': partner}, device_id_type=MESH)
    pl.semaphore_wait(bar, 4 + middle)
    pair.start()
    pair.wait()
    shares(tot, r1[pl.ds(8 * OWN, 8), :], 2)
    fa, fb = fac[2, pl.ds(mine, OWN), :], fac[3, pl.ds(mine, OWN), :]
    for j in range(8):
        c, hq = j // 4, j % 4
        val = m2[j * OWN:(j + 1) * OWN, :] * fa[:, j:j + 1] + r1[j * OWN:(j + 1) * OWN, :] * fb[:, j:j + 1]
        lhs[:, (hq * 2 + c) * LANES:(hq * 2 + c + 1) * LANES] = val.astype(jnp.bfloat16)

    def right_copy(k):
        return pltpu.make_async_remote_copy(
            src_ref=sr.at[k], dst_ref=rr.at[k], send_sem=right_send, recv_sem=right_recv.at[k],
            device_id={'tp': z + 1}, device_id_type=MESH)

    def left_copy(k):
        return pltpu.make_async_remote_copy(
            src_ref=sl.at[k], dst_ref=rl.at[k], send_sem=left_send, recv_sem=left_recv.at[k],
            device_id={'tp': z - 1}, device_id_type=MESH)

    def part_copy(k):
        return pltpu.make_async_remote_copy(
            src_ref=s_all.at[sp, k], dst_ref=s_all.at[sp, k], send_sem=part_send, recv_sem=part_recv,
            device_id={'sp': partner}, device_id_type=MESH)

    def y_copy(k):
        return pltpu.make_async_remote_copy(
            src_ref=s_all.at[sp, k], dst_ref=s_all.at[sp, k], send_sem=y_send, recv_sem=y_recv.at[k],
            device_id={'sp': ypeer}, device_id_type=MESH)

    def across_copy(k):
        return pltpu.make_async_remote_copy(
            src_ref=s_all.at[sp, k], dst_ref=s_all.at[sp, k], send_sem=a_send, recv_sem=y_recv.at[k],
            device_id={'sp': ypeer, 'tp': across}, device_id_type=MESH)

    def fwd_copy(k):
        return pltpu.make_async_remote_copy(
            src_ref=s_all.at[ypeer, k], dst_ref=s_all.at[ypeer, k], send_sem=f_send, recv_sem=f_recv,
            device_id={'sp': partner}, device_id_type=MESH)

    def whole(ref, sem):
        return pltpu.make_async_copy(ref, ref, sem)

    hop = 5
    lag_r = hop * z
    lag_l = hop * (3 - z)
    lag_s = hop * (3 - (z * (3 - z)) // 2)

    def tick(i, carry):
        @pl.when(i < NC)
        def _():
            group, place = i // WG, i % WG

            @pl.when(place == 0)
            def _():
                wo_copy(group).wait()

            w_c = wo_buf[group, :, pl.ds(pl.multiple_of(place * CW, CW), CW)]
            p_buf[i] = jnp.dot(lhs[...], w_c, preferred_element_type=jnp.float32)

        kr, kl = i - lag_r, i - lag_l
        r_live = jnp.logical_and(kr >= 0, kr < NC)
        l_live = jnp.logical_and(kl >= 0, kl < NC)

        def step_right():
            @pl.when(z > 0)
            def _():
                right_copy(kr).wait_recv()

            @pl.when(z < 3)
            def _():
                sr[kr] = p_buf[kr] + rr[kr]
                right_copy(kr).start()

        def step_left():
            @pl.when(z < 3)
            def _():
                left_copy(kl).wait_recv()

            @pl.when(z > 0)
            def _():
                sl[kl] = p_buf[kl] + rl[kl]
                left_copy(kl).start()

        pl.when(jnp.logical_and(l_live, z < 2))(step_left)
        pl.when(r_live)(step_right)
        pl.when(jnp.logical_and(l_live, z >= 2))(step_left)

        k_s = i - lag_s

        @pl.when(jnp.logical_and(k_s >= 0, k_s < NC))
        def _():
            s_all[sp, k_s] = p_buf[k_s] + rr[k_s] + rl[k_s]

            @pl.when(jnp.logical_or(k_s < NC - LASTS, middle == 1))
            def _():
                y_copy(k_s).start()

            @pl.when(jnp.logical_and(k_s >= NC - LASTS, middle == 1))
            def _():
                across_copy(k_s).start()

            part_copy(k_s).start()

        k_y = i - lag_s - hop

        @pl.when(jnp.logical_and(k_y >= 0, k_y < NC))
        def _():
            y_copy(k_y).wait_recv()
            fwd_copy(k_y).start()

        return carry

    lax.fori_loop(0, NC + 4 * hop, tick, 0)

    @pl.when(z < 3)
    def _():
        whole(sr, right_send).wait()

    @pl.when(z > 0)
    def _():
        whole(sl, left_send).wait()

    @pl.when(middle == 1)
    def _():
        whole(s_all.at[sp], y_send).wait()
        whole(s_all.at[sp, pl.ds(NC - LASTS, LASTS)], a_send).wait()

    @pl.when(middle == 0)
    def _():
        whole(s_all.at[sp, pl.ds(0, NC - LASTS)], y_send).wait()

    whole(s_all.at[sp], part_send).wait()
    whole(s_all.at[ypeer], f_send).wait()
    whole(s_all.at[partner], part_recv).wait()
    whole(s_all.at[3 - sp], f_recv).wait()


def finish_kernel(s_all, x_ref, wpost_ref, out_h, out_buf, sem):
    blk = 16

    def out_copy(i):
        rows = pl.ds(i * blk, blk)
        return pltpu.make_async_copy(out_buf.at[rows], out_h.at[rows], sem)

    for i in range(ROWS // blk):
        g, r = (i * blk) // OWN, (i * blk) % OWN
        parts = [s_all[g, k, r:r + blk, :] for k in range(NC)]
        sq = parts[0] * parts[0]
        for k in range(1, NC):
            sq = sq + parts[k] * parts[k]
        rs = lax.rsqrt(jnp.sum(sq, axis=-1, keepdims=True) * (1.0 / DM) + NORM_EPS)
        for k in range(NC):
            for hf in range(CW // LANES):
                col = k * CW + hf * LANES
                gain = 1.0 + wpost_ref[col // LANES:col // LANES + 1, :]
                val = s_all[g, k, r:r + blk, hf * LANES:(hf + 1) * LANES] * rs * gain
                cs = slice(col, col + LANES)
                out_buf[i * blk:(i + 1) * blk, cs] = (x_ref[i * blk:(i + 1) * blk, cs].astype(jnp.float32) + val).astype(jnp.bfloat16)
        out_copy(i).start()
    for i in range(ROWS // blk):
        out_copy(i).wait()


def solution(mesh):
    cache_spec = P('dp', 'sp', 'tp', None)
    hbm = pl.BlockSpec(memory_space=pltpu.HBM)
    vmem = pl.BlockSpec(memory_space=pltpu.VMEM)

    def in_hbm(arr):
        return pltpu.with_memory_space_constraint(arr, pltpu.HBM)

    def in_vmem(arr):
        return pltpu.with_memory_space_constraint(arr, pltpu.VMEM)

    def to_rows(c):
        b, t, h, d = c.shape
        return c.reshape(b, t, h, 2, LANES).transpose(0, 1, 3, 2, 4).reshape(b, t * 2 * h, LANES)

    def from_rows(r):
        return r.reshape(ROWS, TB, 2, 2, LANES).transpose(0, 1, 3, 2, 4).reshape(ROWS, TB, 2, HD)

    def local_step(x_in, cur_pos, w_pre, w_q, w_k, w_v, w_o, w_post, k_cache, v_cache):
        half = HD // 2
        inv_freq = jnp.asarray((ROPE_BASE ** (-2.0 * np.arange(half) / (2 * half))).astype(np.float32))
        kr, vr = to_rows(k_cache), to_rows(v_cache)
        f32, bf16 = jnp.float32, jnp.bfloat16
        dma = pltpu.SemaphoreType.DMA
        half_shape = (HALF,) + kr.shape[1:]
        o_far, k_far, v_far, qs, ks, vs = pl.pallas_call(
            far_kernel,
            out_shape=(jax.ShapeDtypeStruct((HROWS, LANES), f32),
                       pltpu.VMEM(half_shape, bf16), pltpu.VMEM(half_shape, bf16),
                       pltpu.VMEM((8 * RP, LANES), f32), pltpu.VMEM((8 * RP, LANES), f32), pltpu.VMEM((8 * RP, LANES), f32)),
            in_specs=[hbm] * 10,
            out_specs=(vmem,) * 6,
            scratch_shapes=[
                pltpu.SMEM((ROWS,), jnp.int32), pltpu.VMEM((1, ROWS), jnp.int32), pltpu.VMEM((1, LANES), f32),
                pltpu.VMEM((DM // LANES, LANES), f32), pltpu.VMEM((ROWS, LANES), f32), pltpu.VMEM((ROWS, LANES), f32),
                pltpu.VMEM((ROWS, DM), bf16), pltpu.VMEM((ROWS, DM), bf16),
                pltpu.VMEM((DM, 1024), bf16), pltpu.VMEM((DM, 512), bf16), pltpu.VMEM((DM, 512), bf16), pltpu.VMEM((8, ROWS, HD), f32),
                dma, dma, dma((NKC,)), dma((NCH,)),
            ],
            compiler_params=pltpu.CompilerParams(vmem_limit_bytes=40 << 20),
            cost_estimate=pl.CostEstimate(flops=2 * 10 ** 9, bytes_accessed=25 * 10 ** 6, transcendentals=0),
            name='attend_far',
        )(in_hbm(cur_pos), in_hbm(cur_pos.reshape(1, ROWS)), in_hbm(inv_freq.reshape(1, LANES)), in_hbm(x_in),
          in_hbm(w_pre.reshape(DM // LANES, LANES)), in_hbm(w_q), in_hbm(w_k), in_hbm(w_v), in_hbm(kr), in_hbm(vr))
        o_got = lax.ppermute(o_far, 'sp', [(0, 2), (1, 3), (2, 0), (3, 1)])
        o_own, k_new, v_new = pl.pallas_call(
            near_kernel,
            out_shape=(pltpu.VMEM((HROWS, LANES), f32),
                       jax.ShapeDtypeStruct(kr.shape, bf16), jax.ShapeDtypeStruct(vr.shape, bf16)),
            in_specs=[hbm, vmem, vmem, vmem, vmem, vmem, hbm, hbm],
            out_specs=(vmem, hbm, hbm),
            scratch_shapes=[
                pltpu.SMEM((ROWS,), jnp.int32), pltpu.VMEM(half_shape, bf16), pltpu.VMEM(half_shape, bf16),
                dma, dma((NCH,)), dma,
            ],
            compiler_params=pltpu.CompilerParams(vmem_limit_bytes=28 << 20),
            cost_estimate=pl.CostEstimate(flops=10 ** 10, bytes_accessed=25 * 10 ** 6, transcendentals=0),
            name='attend_near',
        )(in_hbm(cur_pos), in_vmem(qs), in_vmem(ks), in_vmem(vs), in_vmem(k_far), in_vmem(v_far), in_hbm(kr), in_hbm(vr))
        big = pltpu.VMEM((NC, OWN, CW), f32)
        sums = pl.pallas_call(
            comm_kernel,
            out_shape=pltpu.VMEM((4, NC, OWN, CW), f32),
            in_specs=[vmem, vmem, hbm],
            out_specs=vmem,
            scratch_shapes=[
                pltpu.VMEM((NC // WG, 1024, WG * CW), bf16), pltpu.VMEM((4, LANES, LANES), f32), pltpu.VMEM((MROWS, LANES), f32),
                pltpu.VMEM((8 * OWN, LANES), f32), pltpu.VMEM((MROWS, LANES), f32), pltpu.VMEM((OWN, 1024), bf16),
                big, big, big, big, big,
                dma((NC // WG,)), dma, dma,
                dma, dma((NC,)), dma, dma((NC,)),
                dma, dma, dma, dma((NC,)), dma, dma, dma,
            ],
            compiler_params=pltpu.CompilerParams(vmem_limit_bytes=40 << 20, collective_id=0, has_side_effects=True),
            name='combine',
        )(in_vmem(o_own), o_got, in_hbm(w_o))
        x_out = pl.pallas_call(
            finish_kernel,
            out_shape=jax.ShapeDtypeStruct((ROWS, DM), bf16),
            in_specs=[vmem, vmem, vmem],
            out_specs=hbm,
            scratch_shapes=[pltpu.VMEM((ROWS, DM), bf16), dma],
            compiler_params=pltpu.CompilerParams(vmem_limit_bytes=16 << 20),
            name='finish',
        )(in_vmem(sums), x_in, w_post.reshape(DM // LANES, LANES))
        return x_out, from_rows(k_new), from_rows(v_new)

    return jax.shard_map(local_step, mesh=mesh,
                         in_specs=(P('dp', None), P('dp'), P(None), P(None, 'tp'), P(None, 'tp'), P(None, 'tp'), P('tp', None), P(None), cache_spec, cache_spec),
                         out_specs=(P('dp', None), cache_spec, cache_spec), check_vma=False)
```

```python
import functools

import jax
import jax.numpy as jnp
import numpy as np
from jax import lax
from jax.experimental import pallas as pl
from jax.experimental.pallas import tpu as pltpu
from jax.sharding import PartitionSpec as P

SOFT_CAP = 50.0
ROPE_BASE = 10000.0
NORM_EPS = 1e-6

ROWS = 128
DM = 3840
HD = 256
TB = 64
RP = 136
LANES = 128
BCH = 16
HALF = ROWS // 2
HROWS = 8 * HALF + 8
NCH = HALF // BCH
KC = 768
NKC = DM // KC
SHIFT = 20.0
CW = 256
NC = DM // CW
WG = 3
LASTS = 6
OWN = 32
MROWS = 8 * OWN + 8
MESH = pl.DeviceIdType.MESH


def attend_rows(row0, bch, pos_ref, kbuf, vbuf, qs, ks, vs, o_ref, before, after):
    tbase = lax.axis_index('sp') * TB
    lane = lax.broadcasted_iota(jnp.int32, (8, LANES), 1)
    row = lax.broadcasted_iota(jnp.int32, (8, LANES), 0)
    row_c = row // 4
    row_h = (row // 2) % 2
    match = (((lane // 2) % 2) == row_c) & ((lane % 2) == row_h)
    match_f = jnp.where(match, 1.0, 0.0).astype(jnp.float32)
    first = row_c == 0
    t_half = [jnp.where(match, lane // 4 + 32 * hf, 1 << 20) for hf in range(2)]
    quad = lax.broadcasted_iota(jnp.int32, (16, LANES), 0) // 4
    zero = jnp.zeros((8, LANES), jnp.float32)

    def chunk(i, l_acc):
        before(i)
        tls = []
        for u in range(bch):
            lb = i * bch + u
            b = row0 + lb
            tl = pos_ref[b] - tbase
            tls.append(tl)
            hit = jnp.logical_and(tl >= 0, tl < TB)
            tc = jnp.clip(tl, 0, TB - 1)
            tile = tc // 4
            tgt = jnp.where(hit, tc - tile * 4, -1)
            sel = quad == tgt
            off = pl.multiple_of(tile * 16, 16)
            kn = ks[pl.ds(b, 8, stride=RP), :]
            vn = vs[pl.ds(b, 8, stride=RP), :]
            kt = kbuf[lb, pl.ds(off, 16), :].astype(jnp.float32)
            vt = vbuf[lb, pl.ds(off, 16), :].astype(jnp.float32)
            kbuf[lb, pl.ds(off, 16), :] = jnp.where(sel, jnp.concatenate([kn, kn], 0), kt).astype(jnp.bfloat16)
            vbuf[lb, pl.ds(off, 16), :] = jnp.where(sel, jnp.concatenate([vn, vn], 0), vt).astype(jnp.bfloat16)
        scores = []
        for u in range(0, bch, 2):
            lb = i * bch + u
            q0 = qs[pl.ds(row0 + lb, 8, stride=RP), :]
            q1 = qs[pl.ds(row0 + lb + 1, 8, stride=RP), :]
            lhs = jnp.concatenate([jnp.concatenate([q0, zero], 1), jnp.concatenate([zero, q1], 1)], 0).astype(jnp.bfloat16)
            kk = jnp.concatenate([kbuf[lb], kbuf[lb + 1]], 1)
            scores.append(lax.dot_general(lhs, kk, (((1,), (1,)), ((), ())), preferred_element_type=jnp.float32))
        weights = []
        for u in range(0, bch, 2):
            pair = []
            for w in range(2):
                part = scores[u // 2][8 * w:8 * w + 8]
                es = []
                for hf in range(2):
                    a = part[:, hf * LANES:(hf + 1) * LANES] * match_f
                    e = pltpu.roll(a, 4, 0)
                    f = jnp.where(first, pltpu.roll(e, LANES - 2, 1), pltpu.roll(e, 2, 1))
                    s = SOFT_CAP * jnp.tanh((a + f) * (HD ** -0.5 / SOFT_CAP))
                    es.append(jnp.where(t_half[hf] <= tls[u + w], jnp.exp(s - SHIFT), 0.0))
                tot = jnp.sum(es[0] + es[1], axis=1, keepdims=True)
                inv = jnp.where(tot > 0.0, 1.0 / tot, 0.0)
                pair.append(jnp.concatenate([es[0] * inv, es[1] * inv], 1))
                l_acc = jnp.where(lane == i * bch + u + w, tot, l_acc)
            weights.append(jnp.concatenate(pair, 0).astype(jnp.bfloat16))
        for u in range(0, bch, 2):
            lb = i * bch + u
            vv = jnp.concatenate([vbuf[lb], vbuf[lb + 1]], 1)
            o = jnp.dot(weights[u // 2], vv, preferred_element_type=jnp.float32)
            o_ref[pl.ds(lb, 8, stride=HALF), :] = o[0:8, 0:LANES]
            o_ref[pl.ds(lb + 1, 8, stride=HALF), :] = o[8:16, LANES:]
        after(i)
        return l_acc

    l_acc = lax.fori_loop(0, HALF // bch, chunk, zero)
    o_ref[pl.ds(8 * HALF, 8), :] = l_acc


def far_kernel(pos_h, posv_h, freq_h, x_h, wpre_h, wq_h, wk_h, wv_h, kc_h, vc_h,
               o_ref, kbuf, vbuf, qs, ks, vs,
               pos_ref, posv, freq, wpre_ref, cos_ref, sin_ref, x_buf, a_buf, wq_buf, wk_buf, wv_buf, acc,
               x_sem, s_sem, w_sem, ki_sem):
    row0 = (1 - lax.axis_index('sp') // 2) * HALF

    def w_start(c):
        rows = pl.ds(c * KC, KC)
        for n, (src, dst) in enumerate(((wk_h, wk_buf), (wv_h, wv_buf), (wq_h, wq_buf))):
            pltpu.make_async_copy(src.at[rows, :], dst.at[rows, :], w_sem.at[c]).start()

    def w_wait(c):
        rows = pl.ds(c * KC, KC)
        for n, (src, dst) in enumerate(((wk_h, wk_buf), (wv_h, wv_buf), (wq_h, wq_buf))):
            pltpu.make_async_copy(src.at[rows, :], dst.at[rows, :], w_sem.at[c]).wait()

    def k_in(i):
        return pltpu.make_async_copy(kc_h.at[pl.ds(row0 + i * BCH, BCH)], kbuf.at[pl.ds(i * BCH, BCH)], ki_sem.at[i])

    def v_in(i):
        return pltpu.make_async_copy(vc_h.at[pl.ds(row0 + i * BCH, BCH)], vbuf.at[pl.ds(i * BCH, BCH)], ki_sem.at[i])

    small = [pltpu.make_async_copy(a, b, s_sem) for a, b in (
        (wpre_h, wpre_ref), (posv_h, posv), (freq_h, freq), (pos_h, pos_ref))]
    for c in small:
        c.start()
    x_copy = pltpu.make_async_copy(x_h, x_buf, x_sem)
    x_copy.start()
    w_start(0)
    for c in small:
        c.wait()
    w_start(1)
    pos_col = jnp.broadcast_to(posv[...].astype(jnp.float32), (ROWS, LANES)).T
    ang = pos_col * freq[...]
    cos_ref[...] = jnp.cos(ang)
    sin_ref[...] = jnp.sin(ang)
    x_copy.wait()
    w_start(2)

    gain = 1.0 + jnp.concatenate([wpre_ref[k:k + 1, :] for k in range(DM // LANES)], 1)

    def norm_rows(i, carry):
        r = pl.multiple_of(i * 16, 16)
        xb = x_buf[pl.ds(r, 16), :].astype(jnp.float32)
        ms = jnp.mean(xb * xb, axis=-1, keepdims=True)
        a_buf[pl.ds(r, 16), :] = (xb * lax.rsqrt(ms + NORM_EPS) * gain).astype(jnp.bfloat16)
        return carry

    lax.fori_loop(0, ROWS // 16, norm_rows, 0)

    for c in range(NKC):
        w_wait(c)
        if c + 3 < NKC:
            w_start(c + 3)
        for n in ((), (), (0,), (1,), (2, 3))[c]:
            k_in(n).start()
            v_in(n).start()
        rows = slice(c * KC, (c + 1) * KC)
        a_c = a_buf[:, rows]
        for i in range(8):
            if i < 2:
                w_c = wk_buf[rows, i * HD:(i + 1) * HD]
            elif i < 4:
                w_c = wv_buf[rows, (i - 2) * HD:(i - 1) * HD]
            else:
                w_c = wq_buf[rows, (i - 4) * HD:(i - 3) * HD]
            y = jnp.dot(a_c, w_c, preferred_element_type=jnp.float32)
            if c == 0:
                acc[i] = y
                continue
            y = acc[i] + y
            if c < NKC - 1:
                acc[i] = y
                continue
            lo, hi = y[:, :LANES], y[:, LANES:]
            if 2 <= i < 4:
                h = i - 2
                for rep in range(2):
                    vs[pl.ds((rep * 4 + h) * RP, ROWS), :] = lo
                    vs[pl.ds((rep * 4 + 2 + h) * RP, ROWS), :] = hi
            else:
                cos_t, sin_t = cos_ref[...], sin_ref[...]
                rlo = lo * cos_t - hi * sin_t
                rhi = hi * cos_t + lo * sin_t
                if i < 2:
                    for rep in range(2):
                        ks[pl.ds((rep * 4 + i) * RP, ROWS), :] = rlo
                        ks[pl.ds((rep * 4 + 2 + i) * RP, ROWS), :] = rhi
                else:
                    qs[pl.ds((i - 4) * RP, ROWS), :] = rlo
                    qs[pl.ds((4 + i - 4) * RP, ROWS), :] = rhi

    def before(i):
        for n in range(2):
            k_in(2 * i + n).wait()
            v_in(2 * i + n).wait()

    attend_rows(row0, 2 * BCH, pos_ref, kbuf, vbuf, qs, ks, vs, o_ref, before, lambda i: None)


def near_kernel(pos_h, qs, ks, vs, kfar, vfar, kc_h, vc_h,
                o_ref, ko_h, vo_h,
                pos_ref, kbuf, vbuf, p_sem, ki_sem, w_sem):
    yy = lax.axis_index('sp') // 2
    row0 = yy * HALF
    far0 = (1 - yy) * HALF

    def k_in(i):
        return pltpu.make_async_copy(kc_h.at[pl.ds(row0 + i * BCH, BCH)], kbuf.at[pl.ds(i * BCH, BCH)], ki_sem.at[i])

    def v_in(i):
        return pltpu.make_async_copy(vc_h.at[pl.ds(row0 + i * BCH, BCH)], vbuf.at[pl.ds(i * BCH, BCH)], ki_sem.at[i])

    def k_out(i):
        return pltpu.make_async_copy(kbuf.at[pl.ds(i * BCH, BCH)], ko_h.at[pl.ds(row0 + i * BCH, BCH)], w_sem)

    def v_out(i):
        return pltpu.make_async_copy(vbuf.at[pl.ds(i * BCH, BCH)], vo_h.at[pl.ds(row0 + i * BCH, BCH)], w_sem)

    def kf_out(i):
        return pltpu.make_async_copy(kfar.at[pl.ds(i * BCH, BCH)], ko_h.at[pl.ds(far0 + i * BCH, BCH)], w_sem)

    def vf_out(i):
        return pltpu.make_async_copy(vfar.at[pl.ds(i * BCH, BCH)], vo_h.at[pl.ds(far0 + i * BCH, BCH)], w_sem)

    p_copy = pltpu.make_async_copy(pos_h, pos_ref, p_sem)
    p_copy.start()
    for i in range(NCH):
        k_in(i).start()
        v_in(i).start()
    p_copy.wait()

    def before(i):
        k_in(i).wait()
        v_in(i).wait()
        kf_out(i).start()
        vf_out(i).start()

    def after(i):
        k_out(i).start()
        v_out(i).start()

    attend_rows(row0, BCH, pos_ref, kbuf, vbuf, qs, ks, vs, o_ref, before, after)
    for i in range(NCH):
        kf_out(i).wait()
        vf_out(i).wait()
        k_out(i).wait()
        v_out(i).wait()


def comm_kernel(o_own, o_got, wo_h, s_all,
                wo_buf, fac, m1, m2, r1, lhs, p_buf, rr, rl, sr, sl,
                w_sem, r1_send, r1_recv,
                right_send, right_recv, left_send, left_recv,
                part_send, part_recv, y_send, y_recv, f_send, f_recv, a_send):
    z = lax.axis_index('tp')
    sp = lax.axis_index('sp')
    core = sp % 2
    partner = sp + 1 - 2 * core
    ypeer = (sp + 2) % 4
    middle = (z * (3 - z)) // 2
    across = z + 1 - 2 * (z % 2)

    def wo_copy(k):
        return pltpu.make_async_copy(wo_h.at[:, pl.ds(pl.multiple_of(k * WG * CW, CW), WG * CW)], wo_buf.at[k], w_sem.at[k])

    for k in range(NC // WG):
        wo_copy(k).start()

    @pl.when(z == 0)
    def _():
        rr[...] = jnp.zeros_like(rr)

    @pl.when(z == 3)
    def _():
        rl[...] = jnp.zeros_like(rl)

    bar = pltpu.get_barrier_semaphore()
    pl.semaphore_signal(bar, inc=1, device_id={'sp': partner}, device_id_type=MESH)
    pl.semaphore_signal(bar, inc=1, device_id={'sp': ypeer}, device_id_type=MESH)
    pl.semaphore_signal(bar, inc=1, device_id={'sp': ypeer, 'tp': across}, device_id_type=MESH)

    @pl.when(z > 0)
    def _():
        pl.semaphore_signal(bar, inc=1, device_id={'tp': z - 1}, device_id_type=MESH)

    @pl.when(z < 3)
    def _():
        pl.semaphore_signal(bar, inc=1, device_id={'tp': z + 1}, device_id_type=MESH)

    def shares(l_a, l_b, slot):
        tot = l_a + l_b
        inv = jnp.where(tot > 0.0, 1.0 / tot, 0.0)
        for w, l in enumerate((l_a, l_b)):
            fac[slot + w] = jnp.concatenate([l * inv, jnp.zeros((LANES - 8, LANES), jnp.float32)], 0).T
        return tot

    mine = pl.multiple_of(core * OWN, OWN)
    theirs = pl.multiple_of((1 - core) * OWN, OWN)
    tot = shares(o_own[pl.ds(8 * HALF, 8), :], o_got[pl.ds(8 * HALF, 8), :], 0)

    def merge_half(r0, dst):
        fa, fb = fac[0, pl.ds(r0, OWN), :], fac[1, pl.ds(r0, OWN), :]
        for j in range(8):
            rows = pl.ds(pl.multiple_of(j * HALF + r0, 8), OWN)
            dst[pl.ds(j * OWN, OWN), :] = o_own[rows, :] * fa[:, j:j + 1] + o_got[rows, :] * fb[:, j:j + 1]

    merge_half(theirs, m1)
    m1[pl.ds(8 * OWN, 8), :] = tot
    merge_half(mine, m2)
    pair = pltpu.make_async_remote_copy(
        src_ref=m1, dst_ref=r1, send_sem=r1_send, recv_sem=r1_recv, device_id={'sp': partner}, device_id_type=MESH)
    pl.semaphore_wait(bar, 4 + middle)
    pair.start()
    pair.wait()
    shares(tot, r1[pl.ds(8 * OWN, 8), :], 2)
    fa, fb = fac[2, pl.ds(mine, OWN), :], fac[3, pl.ds(mine, OWN), :]
    for j in range(8):
        c, hq = j // 4, j % 4
        val = m2[j * OWN:(j + 1) * OWN, :] * fa[:, j:j + 1] + r1[j * OWN:(j + 1) * OWN, :] * fb[:, j:j + 1]
        lhs[:, (hq * 2 + c) * LANES:(hq * 2 + c + 1) * LANES] = val.astype(jnp.bfloat16)

    def right_copy(k):
        return pltpu.make_async_remote_copy(
            src_ref=sr.at[k], dst_ref=rr.at[k], send_sem=right_send, recv_sem=right_recv.at[k],
            device_id={'tp': z + 1}, device_id_type=MESH)

    def left_copy(k):
        return pltpu.make_async_remote_copy(
            src_ref=sl.at[k], dst_ref=rl.at[k], send_sem=left_send, recv_sem=left_recv.at[k],
            device_id={'tp': z - 1}, device_id_type=MESH)

    def part_copy(k):
        return pltpu.make_async_remote_copy(
            src_ref=s_all.at[sp, k], dst_ref=s_all.at[sp, k], send_sem=part_send, recv_sem=part_recv,
            device_id={'sp': partner}, device_id_type=MESH)

    def y_copy(k):
        return pltpu.make_async_remote_copy(
            src_ref=s_all.at[sp, k], dst_ref=s_all.at[sp, k], send_sem=y_send, recv_sem=y_recv.at[k],
            device_id={'sp': ypeer}, device_id_type=MESH)

    def across_copy(k):
        return pltpu.make_async_remote_copy(
            src_ref=s_all.at[sp, k], dst_ref=s_all.at[sp, k], send_sem=a_send, recv_sem=y_recv.at[k],
            device_id={'sp': ypeer, 'tp': across}, device_id_type=MESH)

    def fwd_copy(k):
        return pltpu.make_async_remote_copy(
            src_ref=s_all.at[ypeer, k], dst_ref=s_all.at[ypeer, k], send_sem=f_send, recv_sem=f_recv,
            device_id={'sp': partner}, device_id_type=MESH)

    def whole(ref, sem):
        return pltpu.make_async_copy(ref, ref, sem)

    hop = 5
    lag_r = hop * z
    lag_l = hop * (3 - z)
    lag_s = hop * (3 - (z * (3 - z)) // 2)

    def tick(i, carry):
        @pl.when(i < NC)
        def _():
            group, place = i // WG, i % WG

            @pl.when(place == 0)
            def _():
                wo_copy(group).wait()

            w_c = wo_buf[group, :, pl.ds(pl.multiple_of(place * CW, CW), CW)]
            p_buf[i] = jnp.dot(lhs[...], w_c, preferred_element_type=jnp.float32)

        kr, kl = i - lag_r, i - lag_l
        r_live = jnp.logical_and(kr >= 0, kr < NC)
        l_live = jnp.logical_and(kl >= 0, kl < NC)

        def step_right():
            @pl.when(z > 0)
            def _():
                right_copy(kr).wait_recv()

            @pl.when(z < 3)
            def _():
                sr[kr] = p_buf[kr] + rr[kr]
                right_copy(kr).start()

        def step_left():
            @pl.when(z < 3)
            def _():
                left_copy(kl).wait_recv()

            @pl.when(z > 0)
            def _():
                sl[kl] = p_buf[kl] + rl[kl]
                left_copy(kl).start()

        pl.when(jnp.logical_and(l_live, z < 2))(step_left)
        pl.when(r_live)(step_right)
        pl.when(jnp.logical_and(l_live, z >= 2))(step_left)

        k_s = i - lag_s

        @pl.when(jnp.logical_and(k_s >= 0, k_s < NC))
        def _():
            s_all[sp, k_s] = p_buf[k_s] + rr[k_s] + rl[k_s]

            @pl.when(jnp.logical_or(k_s < NC - LASTS, middle == 1))
            def _():
                y_copy(k_s).start()

            @pl.when(jnp.logical_and(k_s >= NC - LASTS, middle == 1))
            def _():
                across_copy(k_s).start()

            part_copy(k_s).start()

        k_y = i - lag_s - hop

        @pl.when(jnp.logical_and(k_y >= 0, k_y < NC))
        def _():
            y_copy(k_y).wait_recv()
            fwd_copy(k_y).start()

        return carry

    lax.fori_loop(0, NC + 4 * hop, tick, 0)

    @pl.when(z < 3)
    def _():
        whole(sr, right_send).wait()

    @pl.when(z > 0)
    def _():
        whole(sl, left_send).wait()

    @pl.when(middle == 1)
    def _():
        whole(s_all.at[sp], y_send).wait()
        whole(s_all.at[sp, pl.ds(NC - LASTS, LASTS)], a_send).wait()

    @pl.when(middle == 0)
    def _():
        whole(s_all.at[sp, pl.ds(0, NC - LASTS)], y_send).wait()

    whole(s_all.at[sp], part_send).wait()
    whole(s_all.at[ypeer], f_send).wait()
    whole(s_all.at[partner], part_recv).wait()
    whole(s_all.at[3 - sp], f_recv).wait()


def finish_kernel(s_all, x_ref, wpost_ref, out_h, out_buf, sem):
    blk = 16

    def out_copy(i):
        rows = pl.ds(i * blk, blk)
        return pltpu.make_async_copy(out_buf.at[rows], out_h.at[rows], sem)

    for i in range(ROWS // blk):
        g, r = (i * blk) // OWN, (i * blk) % OWN
        parts = [s_all[g, k, r:r + blk, :] for k in range(NC)]
        sq = parts[0] * parts[0]
        for k in range(1, NC):
            sq = sq + parts[k] * parts[k]
        rs = lax.rsqrt(jnp.sum(sq, axis=-1, keepdims=True) * (1.0 / DM) + NORM_EPS)
        for k in range(NC):
            for hf in range(CW // LANES):
                col = k * CW + hf * LANES
                gain = 1.0 + wpost_ref[col // LANES:col // LANES + 1, :]
                val = s_all[g, k, r:r + blk, hf * LANES:(hf + 1) * LANES] * rs * gain
                cs = slice(col, col + LANES)
                out_buf[i * blk:(i + 1) * blk, cs] = (x_ref[i * blk:(i + 1) * blk, cs].astype(jnp.float32) + val).astype(jnp.bfloat16)
        out_copy(i).start()
    for i in range(ROWS // blk):
        out_copy(i).wait()


def solution(mesh):
    cache_spec = P('dp', 'sp', 'tp', None)
    hbm = pl.BlockSpec(memory_space=pltpu.HBM)
    vmem = pl.BlockSpec(memory_space=pltpu.VMEM)

    def in_hbm(arr):
        return pltpu.with_memory_space_constraint(arr, pltpu.HBM)

    def in_vmem(arr):
        return pltpu.with_memory_space_constraint(arr, pltpu.VMEM)

    def to_rows(c):
        b, t, h, d = c.shape
        return c.reshape(b, t, h, 2, LANES).transpose(0, 1, 3, 2, 4).reshape(b, t * 2 * h, LANES)

    def from_rows(r):
        return r.reshape(ROWS, TB, 2, 2, LANES).transpose(0, 1, 3, 2, 4).reshape(ROWS, TB, 2, HD)

    def local_step(x_in, cur_pos, w_pre, w_q, w_k, w_v, w_o, w_post, k_cache, v_cache):
        half = HD // 2
        inv_freq = jnp.asarray((ROPE_BASE ** (-2.0 * np.arange(half) / (2 * half))).astype(np.float32))
        kr, vr = to_rows(k_cache), to_rows(v_cache)
        f32, bf16 = jnp.float32, jnp.bfloat16
        dma = pltpu.SemaphoreType.DMA
        half_shape = (HALF,) + kr.shape[1:]
        o_far, k_far, v_far, qs, ks, vs = pl.pallas_call(
            far_kernel,
            out_shape=(jax.ShapeDtypeStruct((HROWS, LANES), f32),
                       pltpu.VMEM(half_shape, bf16), pltpu.VMEM(half_shape, bf16),
                       pltpu.VMEM((8 * RP, LANES), f32), pltpu.VMEM((8 * RP, LANES), f32), pltpu.VMEM((8 * RP, LANES), f32)),
            in_specs=[hbm] * 10,
            out_specs=(vmem,) * 6,
            scratch_shapes=[
                pltpu.SMEM((ROWS,), jnp.int32), pltpu.VMEM((1, ROWS), jnp.int32), pltpu.VMEM((1, LANES), f32),
                pltpu.VMEM((DM // LANES, LANES), f32), pltpu.VMEM((ROWS, LANES), f32), pltpu.VMEM((ROWS, LANES), f32),
                pltpu.VMEM((ROWS, DM), bf16), pltpu.VMEM((ROWS, DM), bf16),
                pltpu.VMEM((DM, 1024), bf16), pltpu.VMEM((DM, 512), bf16), pltpu.VMEM((DM, 512), bf16), pltpu.VMEM((8, ROWS, HD), f32),
                dma, dma, dma((NKC,)), dma((NCH,)),
            ],
            compiler_params=pltpu.CompilerParams(vmem_limit_bytes=40 << 20),
            cost_estimate=pl.CostEstimate(flops=2 * 10 ** 9, bytes_accessed=25 * 10 ** 6, transcendentals=0),
            name='attend_far',
        )(in_hbm(cur_pos), in_hbm(cur_pos.reshape(1, ROWS)), in_hbm(inv_freq.reshape(1, LANES)), in_hbm(x_in),
          in_hbm(w_pre.reshape(DM // LANES, LANES)), in_hbm(w_q), in_hbm(w_k), in_hbm(w_v), in_hbm(kr), in_hbm(vr))
        o_got = lax.ppermute(o_far, 'sp', [(0, 2), (1, 3), (2, 0), (3, 1)])
        o_own, k_new, v_new = pl.pallas_call(
            near_kernel,
            out_shape=(pltpu.VMEM((HROWS, LANES), f32),
                       jax.ShapeDtypeStruct(kr.shape, bf16), jax.ShapeDtypeStruct(vr.shape, bf16)),
            in_specs=[hbm, vmem, vmem, vmem, vmem, vmem, hbm, hbm],
            out_specs=(vmem, hbm, hbm),
            scratch_shapes=[
                pltpu.SMEM((ROWS,), jnp.int32), pltpu.VMEM(half_shape, bf16), pltpu.VMEM(half_shape, bf16),
                dma, dma((NCH,)), dma,
            ],
            compiler_params=pltpu.CompilerParams(vmem_limit_bytes=28 << 20),
            cost_estimate=pl.CostEstimate(flops=10 ** 10, bytes_accessed=25 * 10 ** 6, transcendentals=0),
            name='attend_near',
        )(in_hbm(cur_pos), in_vmem(qs), in_vmem(ks), in_vmem(vs), in_vmem(k_far), in_vmem(v_far), in_hbm(kr), in_hbm(vr))
        big = pltpu.VMEM((NC, OWN, CW), f32)
        sums = pl.pallas_call(
            comm_kernel,
            out_shape=pltpu.VMEM((4, NC, OWN, CW), f32),
            in_specs=[vmem, vmem, hbm],
            out_specs=vmem,
            scratch_shapes=[
                pltpu.VMEM((NC // WG, 1024, WG * CW), bf16), pltpu.VMEM((4, LANES, LANES), f32), pltpu.VMEM((MROWS, LANES), f32),
                pltpu.VMEM((8 * OWN, LANES), f32), pltpu.VMEM((MROWS, LANES), f32), pltpu.VMEM((OWN, 1024), bf16),
                big, big, big, big, big,
                dma((NC // WG,)), dma, dma,
                dma, dma((NC,)), dma, dma((NC,)),
                dma, dma, dma, dma((NC,)), dma, dma, dma,
            ],
            compiler_params=pltpu.CompilerParams(vmem_limit_bytes=40 << 20, collective_id=0, has_side_effects=True),
            name='combine',
        )(in_vmem(o_own), o_got, in_hbm(w_o))
        x_out = pl.pallas_call(
            finish_kernel,
            out_shape=jax.ShapeDtypeStruct((ROWS, DM), bf16),
            in_specs=[vmem, vmem, vmem],
            out_specs=hbm,
            scratch_shapes=[pltpu.VMEM((ROWS, DM), bf16), dma],
            compiler_params=pltpu.CompilerParams(vmem_limit_bytes=16 << 20),
            name='finish',
        )(in_vmem(sums), x_in, w_post.reshape(DM // LANES, LANES))
        return x_out, from_rows(k_new), from_rows(v_new)

    return jax.shard_map(local_step, mesh=mesh,
                         in_specs=(P('dp', None), P('dp'), P(None), P(None, 'tp'), P(None, 'tp'), P(None, 'tp'), P('tp', None), P(None), cache_spec, cache_spec),
                         out_specs=(P('dp', None), cache_spec, cache_spec), check_vma=False)
```

```python
import functools

import jax
import jax.numpy as jnp
import numpy as np
from jax import lax
from jax.experimental import pallas as pl
from jax.experimental.pallas import tpu as pltpu
from jax.sharding import PartitionSpec as P

SOFT_CAP = 50.0
ROPE_BASE = 10000.0
NORM_EPS = 1e-6

ROWS = 128
DM = 3840
HD = 256
TB = 64
RP = 136
LANES = 128
BCH = 16
HALF = ROWS // 2
HROWS = 8 * HALF + 8
NCH = HALF // BCH
KC = 768
NKC = DM // KC
SHIFT = 20.0
CW = 256
NC = DM // CW
WG = 3
LASTS = 2
OWN = 32
MROWS = 8 * OWN + 8
MESH = pl.DeviceIdType.MESH


def attend_rows(row0, bch, pos_ref, kbuf, vbuf, qs, ks, vs, o_ref, before, after):
    tbase = lax.axis_index('sp') * TB
    lane = lax.broadcasted_iota(jnp.int32, (8, LANES), 1)
    row = lax.broadcasted_iota(jnp.int32, (8, LANES), 0)
    row_c = row // 4
    row_h = (row // 2) % 2
    match = (((lane // 2) % 2) == row_c) & ((lane % 2) == row_h)
    match_f = jnp.where(match, 1.0, 0.0).astype(jnp.float32)
    first = row_c == 0
    t_half = [jnp.where(match, lane // 4 + 32 * hf, 1 << 20) for hf in range(2)]
    quad = lax.broadcasted_iota(jnp.int32, (16, LANES), 0) // 4
    zero = jnp.zeros((8, LANES), jnp.float32)

    def chunk(i, l_acc):
        before(i)
        tls = []
        for u in range(bch):
            lb = i * bch + u
            b = row0 + lb
            tl = pos_ref[b] - tbase
            tls.append(tl)
            hit = jnp.logical_and(tl >= 0, tl < TB)
            tc = jnp.clip(tl, 0, TB - 1)
            tile = tc // 4
            tgt = jnp.where(hit, tc - tile * 4, -1)
            sel = quad == tgt
            off = pl.multiple_of(tile * 16, 16)
            kn = ks[pl.ds(b, 8, stride=RP), :]
            vn = vs[pl.ds(b, 8, stride=RP), :]
            kt = kbuf[lb, pl.ds(off, 16), :].astype(jnp.float32)
            vt = vbuf[lb, pl.ds(off, 16), :].astype(jnp.float32)
            kbuf[lb, pl.ds(off, 16), :] = jnp.where(sel, jnp.concatenate([kn, kn], 0), kt).astype(jnp.bfloat16)
            vbuf[lb, pl.ds(off, 16), :] = jnp.where(sel, jnp.concatenate([vn, vn], 0), vt).astype(jnp.bfloat16)
        scores = []
        for u in range(0, bch, 2):
            lb = i * bch + u
            q0 = qs[pl.ds(row0 + lb, 8, stride=RP), :]
            q1 = qs[pl.ds(row0 + lb + 1, 8, stride=RP), :]
            lhs = jnp.concatenate([jnp.concatenate([q0, zero], 1), jnp.concatenate([zero, q1], 1)], 0).astype(jnp.bfloat16)
            kk = jnp.concatenate([kbuf[lb], kbuf[lb + 1]], 1)
            scores.append(lax.dot_general(lhs, kk, (((1,), (1,)), ((), ())), preferred_element_type=jnp.float32))
        weights = []
        for u in range(0, bch, 2):
            pair = []
            for w in range(2):
                part = scores[u // 2][8 * w:8 * w + 8]
                es = []
                for hf in range(2):
                    a = part[:, hf * LANES:(hf + 1) * LANES] * match_f
                    e = pltpu.roll(a, 4, 0)
                    f = jnp.where(first, pltpu.roll(e, LANES - 2, 1), pltpu.roll(e, 2, 1))
                    s = SOFT_CAP * jnp.tanh((a + f) * (HD ** -0.5 / SOFT_CAP))
                    es.append(jnp.where(t_half[hf] <= tls[u + w], jnp.exp(s - SHIFT), 0.0))
                tot = jnp.sum(es[0] + es[1], axis=1, keepdims=True)
                inv = jnp.where(tot > 0.0, 1.0 / tot, 0.0)
                pair.append(jnp.concatenate([es[0] * inv, es[1] * inv], 1))
                l_acc = jnp.where(lane == i * bch + u + w, tot, l_acc)
            weights.append(jnp.concatenate(pair, 0).astype(jnp.bfloat16))
        for u in range(0, bch, 2):
            lb = i * bch + u
            vv = jnp.concatenate([vbuf[lb], vbuf[lb + 1]], 1)
            o = jnp.dot(weights[u // 2], vv, preferred_element_type=jnp.float32)
            o_ref[pl.ds(lb, 8, stride=HALF), :] = o[0:8, 0:LANES]
            o_ref[pl.ds(lb + 1, 8, stride=HALF), :] = o[8:16, LANES:]
        after(i)
        return l_acc

    l_acc = lax.fori_loop(0, HALF // bch, chunk, zero)
    o_ref[pl.ds(8 * HALF, 8), :] = l_acc


def far_kernel(pos_h, posv_h, freq_h, x_h, wpre_h, wq_h, wk_h, wv_h, kc_h, vc_h,
               o_ref, kbuf, vbuf, qs, ks, vs,
               pos_ref, posv, freq, wpre_ref, cos_ref, sin_ref, x_buf, a_buf, wq_buf, wk_buf, wv_buf, acc,
               x_sem, s_sem, w_sem, ki_sem):
    row0 = (1 - lax.axis_index('sp') // 2) * HALF

    def w_start(c):
        rows = pl.ds(c * KC, KC)
        for n, (src, dst) in enumerate(((wk_h, wk_buf), (wv_h, wv_buf), (wq_h, wq_buf))):
            pltpu.make_async_copy(src.at[rows, :], dst.at[rows, :], w_sem.at[c]).start()

    def w_wait(c):
        rows = pl.ds(c * KC, KC)
        for n, (src, dst) in enumerate(((wk_h, wk_buf), (wv_h, wv_buf), (wq_h, wq_buf))):
            pltpu.make_async_copy(src.at[rows, :], dst.at[rows, :], w_sem.at[c]).wait()

    def k_in(i):
        return pltpu.make_async_copy(kc_h.at[pl.ds(row0 + i * BCH, BCH)], kbuf.at[pl.ds(i * BCH, BCH)], ki_sem.at[i])

    def v_in(i):
        return pltpu.make_async_copy(vc_h.at[pl.ds(row0 + i * BCH, BCH)], vbuf.at[pl.ds(i * BCH, BCH)], ki_sem.at[i])

    small = [pltpu.make_async_copy(a, b, s_sem) for a, b in (
        (wpre_h, wpre_ref), (posv_h, posv), (freq_h, freq), (pos_h, pos_ref))]
    for c in small:
        c.start()
    x_copy = pltpu.make_async_copy(x_h, x_buf, x_sem)
    x_copy.start()
    w_start(0)
    for c in small:
        c.wait()
    w_start(1)
    pos_col = jnp.broadcast_to(posv[...].astype(jnp.float32), (ROWS, LANES)).T
    ang = pos_col * freq[...]
    cos_ref[...] = jnp.cos(ang)
    sin_ref[...] = jnp.sin(ang)
    x_copy.wait()
    w_start(2)

    gain = 1.0 + jnp.concatenate([wpre_ref[k:k + 1, :] for k in range(DM // LANES)], 1)

    def norm_rows(i, carry):
        r = pl.multiple_of(i * 16, 16)
        xb = x_buf[pl.ds(r, 16), :].astype(jnp.float32)
        ms = jnp.mean(xb * xb, axis=-1, keepdims=True)
        a_buf[pl.ds(r, 16), :] = (xb * lax.rsqrt(ms + NORM_EPS) * gain).astype(jnp.bfloat16)
        return carry

    lax.fori_loop(0, ROWS // 16, norm_rows, 0)

    for c in range(NKC):
        w_wait(c)
        if c + 3 < NKC:
            w_start(c + 3)
        for n in ((), (), (0,), (1,), (2, 3))[c]:
            k_in(n).start()
            v_in(n).start()
        rows = slice(c * KC, (c + 1) * KC)
        a_c = a_buf[:, rows]
        for i in range(8):
            if i < 2:
                w_c = wk_buf[rows, i * HD:(i + 1) * HD]
            elif i < 4:
                w_c = wv_buf[rows, (i - 2) * HD:(i - 1) * HD]
            else:
                w_c = wq_buf[rows, (i - 4) * HD:(i - 3) * HD]
            y = jnp.dot(a_c, w_c, preferred_element_type=jnp.float32)
            if c == 0:
                acc[i] = y
                continue
            y = acc[i] + y
            if c < NKC - 1:
                acc[i] = y
                continue
            lo, hi = y[:, :LANES], y[:, LANES:]
            if 2 <= i < 4:
                h = i - 2
                for rep in range(2):
                    vs[pl.ds((rep * 4 + h) * RP, ROWS), :] = lo
                    vs[pl.ds((rep * 4 + 2 + h) * RP, ROWS), :] = hi
            else:
                cos_t, sin_t = cos_ref[...], sin_ref[...]
                rlo = lo * cos_t - hi * sin_t
                rhi = hi * cos_t + lo * sin_t
                if i < 2:
                    for rep in range(2):
                        ks[pl.ds((rep * 4 + i) * RP, ROWS), :] = rlo
                        ks[pl.ds((rep * 4 + 2 + i) * RP, ROWS), :] = rhi
                else:
                    qs[pl.ds((i - 4) * RP, ROWS), :] = rlo
                    qs[pl.ds((4 + i - 4) * RP, ROWS), :] = rhi

    def before(i):
        for n in range(2):
            k_in(2 * i + n).wait()
            v_in(2 * i + n).wait()

    attend_rows(row0, 2 * BCH, pos_ref, kbuf, vbuf, qs, ks, vs, o_ref, before, lambda i: None)


def near_kernel(pos_h, qs, ks, vs, kfar, vfar, kc_h, vc_h,
                o_ref, ko_h, vo_h,
                pos_ref, kbuf, vbuf, p_sem, ki_sem, w_sem):
    yy = lax.axis_index('sp') // 2
    row0 = yy * HALF
    far0 = (1 - yy) * HALF

    def k_in(i):
        return pltpu.make_async_copy(kc_h.at[pl.ds(row0 + i * BCH, BCH)], kbuf.at[pl.ds(i * BCH, BCH)], ki_sem.at[i])

    def v_in(i):
        return pltpu.make_async_copy(vc_h.at[pl.ds(row0 + i * BCH, BCH)], vbuf.at[pl.ds(i * BCH, BCH)], ki_sem.at[i])

    def k_out(i):
        return pltpu.make_async_copy(kbuf.at[pl.ds(i * BCH, BCH)], ko_h.at[pl.ds(row0 + i * BCH, BCH)], w_sem)

    def v_out(i):
        return pltpu.make_async_copy(vbuf.at[pl.ds(i * BCH, BCH)], vo_h.at[pl.ds(row0 + i * BCH, BCH)], w_sem)

    def kf_out(i):
        return pltpu.make_async_copy(kfar.at[pl.ds(i * BCH, BCH)], ko_h.at[pl.ds(far0 + i * BCH, BCH)], w_sem)

    def vf_out(i):
        return pltpu.make_async_copy(vfar.at[pl.ds(i * BCH, BCH)], vo_h.at[pl.ds(far0 + i * BCH, BCH)], w_sem)

    p_copy = pltpu.make_async_copy(pos_h, pos_ref, p_sem)
    p_copy.start()
    for i in range(NCH):
        k_in(i).start()
        v_in(i).start()
    p_copy.wait()

    def before(i):
        k_in(i).wait()
        v_in(i).wait()
        kf_out(i).start()
        vf_out(i).start()

    def after(i):
        k_out(i).start()
        v_out(i).start()

    attend_rows(row0, BCH, pos_ref, kbuf, vbuf, qs, ks, vs, o_ref, before, after)
    for i in range(NCH):
        kf_out(i).wait()
        vf_out(i).wait()
        k_out(i).wait()
        v_out(i).wait()


def comm_kernel(o_own, o_got, wo_h, s_all,
                wo_buf, fac, m1, m2, r1, lhs, p_buf, rr, rl, sr, sl,
                w_sem, r1_send, r1_recv,
                right_send, right_recv, left_send, left_recv,
                part_send, part_recv, y_send, y_recv, f_send, f_recv, a_send):
    z = lax.axis_index('tp')
    sp = lax.axis_index('sp')
    core = sp % 2
    partner = sp + 1 - 2 * core
    ypeer = (sp + 2) % 4
    middle = (z * (3 - z)) // 2
    across = z + 1 - 2 * (z % 2)

    def wo_copy(k):
        return pltpu.make_async_copy(wo_h.at[:, pl.ds(pl.multiple_of(k * WG * CW, CW), WG * CW)], wo_buf.at[k], w_sem.at[k])

    for k in range(NC // WG):
        wo_copy(k).start()

    @pl.when(z == 0)
    def _():
        rr[...] = jnp.zeros_like(rr)

    @pl.when(z == 3)
    def _():
        rl[...] = jnp.zeros_like(rl)

    bar = pltpu.get_barrier_semaphore()
    pl.semaphore_signal(bar, inc=1, device_id={'sp': partner}, device_id_type=MESH)
    pl.semaphore_signal(bar, inc=1, device_id={'sp': ypeer}, device_id_type=MESH)
    pl.semaphore_signal(bar, inc=1, device_id={'sp': ypeer, 'tp': across}, device_id_type=MESH)

    @pl.when(z > 0)
    def _():
        pl.semaphore_signal(bar, inc=1, device_id={'tp': z - 1}, device_id_type=MESH)

    @pl.when(z < 3)
    def _():
        pl.semaphore_signal(bar, inc=1, device_id={'tp': z + 1}, device_id_type=MESH)

    def shares(l_a, l_b, slot):
        tot = l_a + l_b
        inv = jnp.where(tot > 0.0, 1.0 / tot, 0.0)
        for w, l in enumerate((l_a, l_b)):
            fac[slot + w] = jnp.concatenate([l * inv, jnp.zeros((LANES - 8, LANES), jnp.float32)], 0).T
        return tot

    mine = pl.multiple_of(core * OWN, OWN)
    theirs = pl.multiple_of((1 - core) * OWN, OWN)
    tot = shares(o_own[pl.ds(8 * HALF, 8), :], o_got[pl.ds(8 * HALF, 8), :], 0)

    def merge_half(r0, dst):
        fa, fb = fac[0, pl.ds(r0, OWN), :], fac[1, pl.ds(r0, OWN), :]
        for j in range(8):
            rows = pl.ds(pl.multiple_of(j * HALF + r0, 8), OWN)
            dst[pl.ds(j * OWN, OWN), :] = o_own[rows, :] * fa[:, j:j + 1] + o_got[rows, :] * fb[:, j:j + 1]

    merge_half(theirs, m1)
    m1[pl.ds(8 * OWN, 8), :] = tot
    merge_half(mine, m2)
    pair = pltpu.make_async_remote_copy(
        src_ref=m1, dst_ref=r1, send_sem=r1_send, recv_sem=r1_recv, device_id={'sp': partner}, device_id_type=MESH)
    pl.semaphore_wait(bar, 4 + middle)
    pair.start()
    pair.wait()
    shares(tot, r1[pl.ds(8 * OWN, 8), :], 2)
    fa, fb = fac[2, pl.ds(mine, OWN), :], fac[3, pl.ds(mine, OWN), :]
    for j in range(8):
        c, hq = j // 4, j % 4
        val = m2[j * OWN:(j + 1) * OWN, :] * fa[:, j:j + 1] + r1[j * OWN:(j + 1) * OWN, :] * fb[:, j:j + 1]
        lhs[:, (hq * 2 + c) * LANES:(hq * 2 + c + 1) * LANES] = val.astype(jnp.bfloat16)

    def right_copy(k):
        return pltpu.make_async_remote_copy(
            src_ref=sr.at[k], dst_ref=rr.at[k], send_sem=right_send, recv_sem=right_recv.at[k],
            device_id={'tp': z + 1}, device_id_type=MESH)

    def left_copy(k):
        return pltpu.make_async_remote_copy(
            src_ref=sl.at[k], dst_ref=rl.at[k], send_sem=left_send, recv_sem=left_recv.at[k],
            device_id={'tp': z - 1}, device_id_type=MESH)

    def part_copy(k):
        return pltpu.make_async_remote_copy(
            src_ref=s_all.at[sp, k], dst_ref=s_all.at[sp, k], send_sem=part_send, recv_sem=part_recv,
            device_id={'sp': partner}, device_id_type=MESH)

    def y_copy(k):
        return pltpu.make_async_remote_copy(
            src_ref=s_all.at[sp, k], dst_ref=s_all.at[sp, k], send_sem=y_send, recv_sem=y_recv.at[k],
            device_id={'sp': ypeer}, device_id_type=MESH)

    def across_copy(k):
        return pltpu.make_async_remote_copy(
            src_ref=s_all.at[sp, k], dst_ref=s_all.at[sp, k], send_sem=a_send, recv_sem=y_recv.at[k],
            device_id={'sp': ypeer, 'tp': across}, device_id_type=MESH)

    def fwd_copy(k):
        return pltpu.make_async_remote_copy(
            src_ref=s_all.at[ypeer, k], dst_ref=s_all.at[ypeer, k], send_sem=f_send, recv_sem=f_recv,
            device_id={'sp': partner}, device_id_type=MESH)

    def whole(ref, sem):
        return pltpu.make_async_copy(ref, ref, sem)

    hop = 5
    lag_r = hop * z
    lag_l = hop * (3 - z)
    lag_s = hop * (3 - (z * (3 - z)) // 2)

    def tick(i, carry):
        @pl.when(i < NC)
        def _():
            group, place = i // WG, i % WG

            @pl.when(place == 0)
            def _():
                wo_copy(group).wait()

            w_c = wo_buf[group, :, pl.ds(pl.multiple_of(place * CW, CW), CW)]
            p_buf[i] = jnp.dot(lhs[...], w_c, preferred_element_type=jnp.float32)

        kr, kl = i - lag_r, i - lag_l
        r_live = jnp.logical_and(kr >= 0, kr < NC)
        l_live = jnp.logical_and(kl >= 0, kl < NC)

        def step_right():
            @pl.when(z > 0)
            def _():
                right_copy(kr).wait_recv()

            @pl.when(z < 3)
            def _():
                sr[kr] = p_buf[kr] + rr[kr]
                right_copy(kr).start()

        def step_left():
            @pl.when(z < 3)
            def _():
                left_copy(kl).wait_recv()

            @pl.when(z > 0)
            def _():
                sl[kl] = p_buf[kl] + rl[kl]
                left_copy(kl).start()

        pl.when(jnp.logical_and(l_live, z < 2))(step_left)
        pl.when(r_live)(step_right)
        pl.when(jnp.logical_and(l_live, z >= 2))(step_left)

        k_s = i - lag_s

        @pl.when(jnp.logical_and(k_s >= 0, k_s < NC))
        def _():
            s_all[sp, k_s] = p_buf[k_s] + rr[k_s] + rl[k_s]

            @pl.when(jnp.logical_or(k_s < NC - LASTS, middle == 1))
            def _():
                y_copy(k_s).start()

            @pl.when(jnp.logical_and(k_s >= NC - LASTS, middle == 1))
            def _():
                across_copy(k_s).start()

            part_copy(k_s).start()

        k_y = i - lag_s - hop

        @pl.when(jnp.logical_and(k_y >= 0, k_y < NC))
        def _():
            y_copy(k_y).wait_recv()
            fwd_copy(k_y).start()

        return carry

    lax.fori_loop(0, NC + 4 * hop, tick, 0)

    @pl.when(z < 3)
    def _():
        whole(sr, right_send).wait()

    @pl.when(z > 0)
    def _():
        whole(sl, left_send).wait()

    @pl.when(middle == 1)
    def _():
        whole(s_all.at[sp], y_send).wait()
        whole(s_all.at[sp, pl.ds(NC - LASTS, LASTS)], a_send).wait()

    @pl.when(middle == 0)
    def _():
        whole(s_all.at[sp, pl.ds(0, NC - LASTS)], y_send).wait()

    whole(s_all.at[sp], part_send).wait()
    whole(s_all.at[ypeer], f_send).wait()
    whole(s_all.at[partner], part_recv).wait()
    whole(s_all.at[3 - sp], f_recv).wait()


def finish_kernel(s_all, x_ref, wpost_ref, out_h, out_buf, sem):
    blk = 16

    def out_copy(i):
        rows = pl.ds(i * blk, blk)
        return pltpu.make_async_copy(out_buf.at[rows], out_h.at[rows], sem)

    for i in range(ROWS // blk):
        g, r = (i * blk) // OWN, (i * blk) % OWN
        parts = [s_all[g, k, r:r + blk, :] for k in range(NC)]
        sq = parts[0] * parts[0]
        for k in range(1, NC):
            sq = sq + parts[k] * parts[k]
        rs = lax.rsqrt(jnp.sum(sq, axis=-1, keepdims=True) * (1.0 / DM) + NORM_EPS)
        for k in range(NC):
            for hf in range(CW // LANES):
                col = k * CW + hf * LANES
                gain = 1.0 + wpost_ref[col // LANES:col // LANES + 1, :]
                val = s_all[g, k, r:r + blk, hf * LANES:(hf + 1) * LANES] * rs * gain
                cs = slice(col, col + LANES)
                out_buf[i * blk:(i + 1) * blk, cs] = (x_ref[i * blk:(i + 1) * blk, cs].astype(jnp.float32) + val).astype(jnp.bfloat16)
        out_copy(i).start()
    for i in range(ROWS // blk):
        out_copy(i).wait()


def solution(mesh):
    cache_spec = P('dp', 'sp', 'tp', None)
    hbm = pl.BlockSpec(memory_space=pltpu.HBM)
    vmem = pl.BlockSpec(memory_space=pltpu.VMEM)

    def in_hbm(arr):
        return pltpu.with_memory_space_constraint(arr, pltpu.HBM)

    def in_vmem(arr):
        return pltpu.with_memory_space_constraint(arr, pltpu.VMEM)

    def to_rows(c):
        b, t, h, d = c.shape
        return c.reshape(b, t, h, 2, LANES).transpose(0, 1, 3, 2, 4).reshape(b, t * 2 * h, LANES)

    def from_rows(r):
        return r.reshape(ROWS, TB, 2, 2, LANES).transpose(0, 1, 3, 2, 4).reshape(ROWS, TB, 2, HD)

    def local_step(x_in, cur_pos, w_pre, w_q, w_k, w_v, w_o, w_post, k_cache, v_cache):
        half = HD // 2
        inv_freq = jnp.asarray((ROPE_BASE ** (-2.0 * np.arange(half) / (2 * half))).astype(np.float32))
        kr, vr = to_rows(k_cache), to_rows(v_cache)
        f32, bf16 = jnp.float32, jnp.bfloat16
        dma = pltpu.SemaphoreType.DMA
        half_shape = (HALF,) + kr.shape[1:]
        o_far, k_far, v_far, qs, ks, vs = pl.pallas_call(
            far_kernel,
            out_shape=(jax.ShapeDtypeStruct((HROWS, LANES), f32),
                       pltpu.VMEM(half_shape, bf16), pltpu.VMEM(half_shape, bf16),
                       pltpu.VMEM((8 * RP, LANES), f32), pltpu.VMEM((8 * RP, LANES), f32), pltpu.VMEM((8 * RP, LANES), f32)),
            in_specs=[hbm] * 10,
            out_specs=(vmem,) * 6,
            scratch_shapes=[
                pltpu.SMEM((ROWS,), jnp.int32), pltpu.VMEM((1, ROWS), jnp.int32), pltpu.VMEM((1, LANES), f32),
                pltpu.VMEM((DM // LANES, LANES), f32), pltpu.VMEM((ROWS, LANES), f32), pltpu.VMEM((ROWS, LANES), f32),
                pltpu.VMEM((ROWS, DM), bf16), pltpu.VMEM((ROWS, DM), bf16),
                pltpu.VMEM((DM, 1024), bf16), pltpu.VMEM((DM, 512), bf16), pltpu.VMEM((DM, 512), bf16), pltpu.VMEM((8, ROWS, HD), f32),
                dma, dma, dma((NKC,)), dma((NCH,)),
            ],
            compiler_params=pltpu.CompilerParams(vmem_limit_bytes=40 << 20),
            cost_estimate=pl.CostEstimate(flops=2 * 10 ** 9, bytes_accessed=25 * 10 ** 6, transcendentals=0),
            name='attend_far',
        )(in_hbm(cur_pos), in_hbm(cur_pos.reshape(1, ROWS)), in_hbm(inv_freq.reshape(1, LANES)), in_hbm(x_in),
          in_hbm(w_pre.reshape(DM // LANES, LANES)), in_hbm(w_q), in_hbm(w_k), in_hbm(w_v), in_hbm(kr), in_hbm(vr))
        o_got = lax.ppermute(o_far, 'sp', [(0, 2), (1, 3), (2, 0), (3, 1)])
        o_own, k_new, v_new = pl.pallas_call(
            near_kernel,
            out_shape=(pltpu.VMEM((HROWS, LANES), f32),
                       jax.ShapeDtypeStruct(kr.shape, bf16), jax.ShapeDtypeStruct(vr.shape, bf16)),
            in_specs=[hbm, vmem, vmem, vmem, vmem, vmem, hbm, hbm],
            out_specs=(vmem, hbm, hbm),
            scratch_shapes=[
                pltpu.SMEM((ROWS,), jnp.int32), pltpu.VMEM(half_shape, bf16), pltpu.VMEM(half_shape, bf16),
                dma, dma((NCH,)), dma,
            ],
            compiler_params=pltpu.CompilerParams(vmem_limit_bytes=28 << 20),
            cost_estimate=pl.CostEstimate(flops=10 ** 10, bytes_accessed=25 * 10 ** 6, transcendentals=0),
            name='attend_near',
        )(in_hbm(cur_pos), in_vmem(qs), in_vmem(ks), in_vmem(vs), in_vmem(k_far), in_vmem(v_far), in_hbm(kr), in_hbm(vr))
        big = pltpu.VMEM((NC, OWN, CW), f32)
        sums = pl.pallas_call(
            comm_kernel,
            out_shape=pltpu.VMEM((4, NC, OWN, CW), f32),
            in_specs=[vmem, vmem, hbm],
            out_specs=vmem,
            scratch_shapes=[
                pltpu.VMEM((NC // WG, 1024, WG * CW), bf16), pltpu.VMEM((4, LANES, LANES), f32), pltpu.VMEM((MROWS, LANES), f32),
                pltpu.VMEM((8 * OWN, LANES), f32), pltpu.VMEM((MROWS, LANES), f32), pltpu.VMEM((OWN, 1024), bf16),
                big, big, big, big, big,
                dma((NC // WG,)), dma, dma,
                dma, dma((NC,)), dma, dma((NC,)),
                dma, dma, dma, dma((NC,)), dma, dma, dma,
            ],
            compiler_params=pltpu.CompilerParams(vmem_limit_bytes=40 << 20, collective_id=0, has_side_effects=True),
            name='combine',
        )(in_vmem(o_own), o_got, in_hbm(w_o))
        x_out = pl.pallas_call(
            finish_kernel,
            out_shape=jax.ShapeDtypeStruct((ROWS, DM), bf16),
            in_specs=[vmem, vmem, vmem],
            out_specs=hbm,
            scratch_shapes=[pltpu.VMEM((ROWS, DM), bf16), dma],
            compiler_params=pltpu.CompilerParams(vmem_limit_bytes=16 << 20),
            name='finish',
        )(in_vmem(sums), x_in, w_post.reshape(DM // LANES, LANES))
        return x_out, from_rows(k_new), from_rows(v_new)

    return jax.shard_map(local_step, mesh=mesh,
                         in_specs=(P('dp', None), P('dp'), P(None), P(None, 'tp'), P(None, 'tp'), P(None, 'tp'), P('tp', None), P(None), cache_spec, cache_spec),
                         out_specs=(P('dp', None), cache_spec, cache_spec), check_vma=False)
```
